32 devices in a mesh: fsdp: 16 (over z, y, x), sp: 2 (over core).
Axes of the slice: x: 2, y: 2, z: 4, core: 2. Of those that a mesh axis runs over, the one named last changes fastest.
Arguments:
- tokens: bfloat16 [4096, 1536], P(('fsdp', 'sp')), may hold values from -6 to 6
- text: bfloat16 [8192, 1536], P(('fsdp', 'sp')), may hold values from -6 to 6
- clip_frames: int32 [16], P('fsdp'), may hold values from 1 to 4, as said below
- timestep: int32 [16, 4], P('fsdp'), may hold values from 0 to 999
- mod_weight: bfloat16 [1, 256, 9216], P(None, 'fsdp'), may hold values from -0.375 to 0.375
- mod_bias: bfloat16 [1, 9216], P(None, 'fsdp'), may hold values from -3 to 3
- qk_gains: bfloat16 [1, 4, 1536], P(None, None, 'fsdp'), may hold values from 0.099609375 to 1.8984375
- self_in: bfloat16 [1, 1536, 4608], P(None, 'fsdp'), may hold values from -0.15625 to 0.15625
- self_out: bfloat16 [1, 1536, 1536], P(None, 'fsdp'), may hold values from -1.25 to 1.25
- cross_q: bfloat16 [1, 1536, 1536], P(None, 'fsdp'), may hold values from -0.15625 to 0.15625
- cross_kv: bfloat16 [1, 1536, 3072], P(None, 'fsdp'), may hold values from -0.15625 to 0.15625
- cross_out: bfloat16 [1, 1536, 1536], P(None, 'fsdp'), may hold values from -1.25 to 1.25
- mlp_in: bfloat16 [1, 1536, 8960], P(None, 'fsdp'), may hold values from -0.15625 to 0.15625
- mlp_out: bfloat16 [1, 8960, 1536], P(None, 'fsdp'), may hold values from -0.0625 to 0.0625
- cotangent: bfloat16 [4096, 1536], P(('fsdp', 'sp')), may hold values from -6 to 6
Outputs:
- output: bfloat16 [4096, 1536], P(('fsdp', 'sp'))
- tokens_grad: float32 [4096, 1536], P(('fsdp', 'sp'))
- mod_weight_grad: float32 [1, 256, 9216], P(None, 'fsdp')
- mod_bias_grad: float32 [1, 9216], P(None, 'fsdp')
- qk_gains_grad: float32 [1, 4, 1536], P(None, None, 'fsdp')
- self_in_grad: float32 [1, 1536, 4608], P(None, 'fsdp')
- self_out_grad: float32 [1, 1536, 1536], P(None, 'fsdp')
- cross_q_grad: float32 [1, 1536, 1536], P(None, 'fsdp')
- cross_kv_grad: float32 [1, 1536, 3072], P(None, 'fsdp')
- cross_out_grad: float32 [1, 1536, 1536], P(None, 'fsdp')
- mlp_in_grad: float32 [1, 1536, 8960], P(None, 'fsdp')
- mlp_out_grad: float32 [1, 8960, 1536], P(None, 'fsdp')
The draws below stay inside these ranges and needn't reach their ends.
Inputs may be any that keep to these rules, and one draw needn't show every extreme that they name: `clip_frames`: some clip has all 4 frames live in every draw.
All inputs are finite; a program needn't handle non-finite values.
Results may differ from the reference program's by a relative error of at most 0.019.
Values may be sent and summed in bfloat16 or wider, within the bound.
A program may use at most 448 MiB of HBM per device.

```python
import math
import jax
import jax.numpy as jnp
from jax import lax

D = 1536
HEADS = 12
HD = 128
FF = 8960
TXT = 512
FREQ = 256
LAYERS = 1
WP = 8
FRAME_TOK = 64
GROUP_FRAMES = 4
GROUPS = 16
TOKENS = 4096
TEXT_ROWS = 8192


def draw_clip_frames(key, part):
    counts = jax.random.randint(jax.random.fold_in(key, 11), (GROUPS,), 1, GROUP_FRAMES + 1)
    longest = jax.random.randint(jax.random.fold_in(key, 12), (), 0, GROUPS)
    return counts.at[longest].set(GROUP_FRAMES).astype(jnp.int32)


def place_ends(entries, stream_key, smallest, top_value):
    index_at = [jax.random.randint(jax.random.fold_in(stream_key, axis), (), 0, length) for axis, length in enumerate(entries.shape)]
    widest = entries.shape.index(max(entries.shape))
    beside = index_at[:widest] + [(index_at[widest] + 1) % entries.shape[widest]] + index_at[widest + 1:]
    return entries.at[tuple(index_at)].set(smallest).at[tuple(beside)].set(top_value)


def shard_levels(rng, shape, cuts, least, high):
    level = 1.0
    for position, parts in cuts:
        draws = jax.random.uniform(jax.random.fold_in(jax.random.fold_in(rng, 6), position), (parts,), jnp.float32, least / len(cuts), high / len(cuts))
        level = level * jnp.repeat(jnp.exp(draws), shape[position] // parts).reshape((-1,) + (1,) * (len(shape) - 1 - position))
    return level


def gaussian(rng, dims, spread, bound, cuts=(), kind=jnp.bfloat16):
    level = shard_levels(rng, dims, cuts, -0.22, 0.18) if cuts else 1.0
    values = jax.random.normal(rng, dims, jnp.float32) * spread * level
    return jnp.minimum(jnp.maximum(values, -bound), bound).astype(kind)


def setup_inputs(seed: int = 0) -> dict:
    key_list = jax.random.split(jax.random.key(seed), 16)
    tokens = gaussian(key_list[0], (TOKENS, D), 1.0, 6.0, ((0, 32),))
    text = gaussian(key_list[1], (TEXT_ROWS, D), 1.0, 6.0, ((0, 32),))
    clip_frames = draw_clip_frames(jax.random.fold_in(key_list[15], 71), 0)
    timestep = place_ends(jax.random.randint(key_list[3], (GROUPS, GROUP_FRAMES), 0, 1000), jax.random.fold_in(key_list[3], 1), 0, 999).astype(jnp.int32)
    mod_weight = gaussian(key_list[4], (LAYERS, FREQ, 6 * D), FREQ ** -0.5, 0.375, ((1, 16),))
    mod_bias = gaussian(key_list[5], (LAYERS, 6 * D), 0.5, 3.0, ((1, 16),))
    qk_gains = jnp.clip(1.0 + 0.18 * jax.random.normal(key_list[6], (LAYERS, 4, D), jnp.float32), 0.099609375, 1.8984375).astype(jnp.bfloat16)
    self_in = gaussian(key_list[7], (LAYERS, D, 3 * D), D ** -0.5, 0.15625, ((1, 16),))
    self_out = gaussian(key_list[8], (LAYERS, D, D), (D // 64) ** -0.5, 1.25, ((1, 16),))
    cross_q = gaussian(key_list[9], (LAYERS, D, D), D ** -0.5, 0.15625, ((1, 16),))
    cross_kv = gaussian(key_list[10], (LAYERS, D, 2 * D), D ** -0.5, 0.15625, ((1, 16),))
    cross_out = gaussian(key_list[11], (LAYERS, D, D), (D // 64) ** -0.5, 1.25, ((1, 16),))
    mlp_in = gaussian(key_list[12], (LAYERS, D, FF), D ** -0.5, 0.15625, ((1, 16),))
    mlp_out = gaussian(key_list[13], (LAYERS, FF, D), FF ** -0.5, 0.0625, ((1, 16),))
    cotangent = gaussian(key_list[14], (TOKENS, D), 1.0, 6.0, ((0, 32),))
    return {"tokens": tokens, "text": text, "clip_frames": clip_frames, "timestep": timestep, "mod_weight": mod_weight, "mod_bias": mod_bias, "qk_gains": qk_gains, "self_in": self_in, "self_out": self_out, "cross_q": cross_q, "cross_kv": cross_kv, "cross_out": cross_out, "mlp_in": mlp_in, "mlp_out": mlp_out, "cotangent": cotangent}


@jax.custom_vjp
def low(v):
    return lax.optimization_barrier(v.astype(jnp.bfloat16)).astype(jnp.float32)

@jax.custom_vjp
def low_back(v):
    return v

def low_keep(v):
    return (low(v), None)

def low_pass(kept, grad):
    return (grad,)

def back_keep(v):
    return (v, None)

def back_low(kept, grad):
    return (low(grad),)
low.defvjp(low_keep, low_pass)
low_back.defvjp(back_keep, back_low)
EPSILON = 1e-06
PRECISE = lax.Precision.HIGHEST
NEGATIVE = -1e+30

def matmul(left, right):
    return jnp.dot(left, right, precision=PRECISE, preferred_element_type=jnp.float32)

def layer_norm(values):
    centred = values - lax.optimization_barrier(jnp.mean(values, axis=-1, keepdims=True))
    return centred * lax.rsqrt(lax.optimization_barrier(jnp.mean(centred * centred, axis=-1, keepdims=True)) + EPSILON)

def rms_norm(values, gain):
    return values * lax.rsqrt(lax.optimization_barrier(jnp.mean(values * values, axis=-1, keepdims=True)) + EPSILON) * gain

def sinus_features(steps):
    half_dim = FREQ // 2
    rates = jnp.exp(jnp.arange(half_dim).astype(jnp.float32) * (-math.log(10000.0) / half_dim))
    angles = steps.astype(jnp.float32)[:, None] * rates[None, :]
    return jnp.concatenate([jnp.cos(angles), jnp.sin(angles)], axis=1)

def rotary_tables(frame_pos, token_spot):
    half_dim = HD // 2
    side_pairs = HD // 6
    lead_pairs = half_dim - 2 * side_pairs
    pair_index = jnp.arange(half_dim)
    log_base = -math.log(10000.0)
    lead_part = pair_index < lead_pairs
    side_part = jnp.logical_and(pair_index >= lead_pairs, pair_index < lead_pairs + side_pairs)
    last_part = pair_index >= lead_pairs + side_pairs
    frame_rate = jnp.where(lead_part, jnp.exp(log_base * pair_index.astype(jnp.float32) / lead_pairs), 0.0)
    row_rate = jnp.where(side_part, jnp.exp(log_base * (pair_index - lead_pairs).astype(jnp.float32) / side_pairs), 0.0)
    column_rate = jnp.where(last_part, jnp.exp(log_base * (pair_index - lead_pairs - side_pairs).astype(jnp.float32) / side_pairs), 0.0)
    patch_row = (token_spot // WP).astype(jnp.float32)
    patch_column = (token_spot % WP).astype(jnp.float32)
    angles = frame_pos.astype(jnp.float32)[:, None] * frame_rate[None, :] + patch_row[:, None] * row_rate[None, :] + patch_column[:, None] * column_rate[None, :]
    return (jnp.cos(angles), jnp.sin(angles))

def rotate(values, cosine, sine):
    row_count = values.shape[0]
    shaped = values.reshape(row_count, -1, HD)
    half_dim = HD // 2
    first_half = shaped[:, :, :half_dim]
    second_half = shaped[:, :, half_dim:]
    cos_rows = cosine[:, None, :]
    sin_rows = sine[:, None, :]
    turned = jnp.concatenate([first_half * cos_rows - second_half * sin_rows, second_half * cos_rows + first_half * sin_rows], axis=2)
    return turned.reshape(row_count, -1)

def modulated(residual, shift, scale):
    frames = shift.shape[0]
    normed = layer_norm(residual).reshape(frames, -1, residual.shape[1])
    return (normed * (1.0 + scale[:, None, :]) + shift[:, None, :]).reshape(residual.shape)

def gated_add(residual, branch, gate):
    frames = gate.shape[0]
    return residual + (branch.reshape(frames, -1, branch.shape[1]) * gate[:, None, :]).reshape(branch.shape)

def attend(query, key_rows, value_rows, key_live):
    score_scale = 1.0 / math.sqrt(HD)

    def one_group(pieces):
        query_block, key_block, value_block, live_keys = pieces
        query_heads = query_block.reshape(query_block.shape[0], HEADS, HD)
        key_heads = key_block.reshape(key_block.shape[0], HEADS, HD)
        value_heads = value_block.reshape(value_block.shape[0], HEADS, HD)
        raw_scores = jnp.einsum('qhd,khd->hqk', query_heads, key_heads, precision=PRECISE) * score_scale
        raw_scores = low_back(raw_scores)
        allowed = (live_keys > 0)[None, None, :]
        scores = jnp.where(allowed, raw_scores, NEGATIVE)
        row_max = lax.optimization_barrier(jnp.max(scores, axis=2, keepdims=True))
        log_total = row_max + jnp.log(lax.optimization_barrier(jnp.sum(jnp.exp(scores - row_max), axis=2, keepdims=True)))
        attn_weights = low(jnp.exp(scores - log_total))
        mixed_heads = jnp.einsum('hqk,khd->qhd', attn_weights, value_heads, precision=PRECISE)
        return mixed_heads.reshape(query_block.shape[0], HEADS * HD)
    return lax.map(jax.checkpoint(one_group), (query, key_rows, value_rows, key_live))

def run_layers(residual, params, text_float, sinus, cosine, sine, seq_live, text_live):
    mod_matrix, mod_offset, gain_table, self_proj, self_back, cross_qproj, cross_kvproj, cross_back, up_matrix, down_matrix = params
    groups = seq_live.shape[0]
    for block_no in range(LAYERS):
        modulation = low_back(matmul(sinus, mod_matrix[block_no])) + mod_offset[block_no][None, :]
        shift_one, scale_one, gate_one, shift_two, scale_two, gate_two = jnp.split(modulation, 6, axis=1)
        attn_input = low(modulated(residual, shift_one, scale_one))
        joined = low_back(matmul(attn_input, self_proj[block_no]))
        query_rows = low_back(low(rotate(rms_norm(joined[:, :D], gain_table[block_no, 0]), cosine, sine)))
        key_rows = low_back(low(rotate(rms_norm(joined[:, D:2 * D], gain_table[block_no, 1]), cosine, sine)))
        value_rows = low_back(low(joined[:, 2 * D:]))
        self_mixed = attend(query_rows.reshape(groups, -1, D), key_rows.reshape(groups, -1, D), value_rows.reshape(groups, -1, D), seq_live).reshape(-1, D)
        self_mixed = low_back(low(self_mixed))
        residual = gated_add(residual, low_back(matmul(self_mixed, self_back[block_no])), gate_one)
        cross_input = low(layer_norm(residual))
        cross_query = low_back(low(rms_norm(low_back(matmul(cross_input, cross_qproj[block_no])), gain_table[block_no, 2])))
        cross_keyval = low_back(matmul(text_float, cross_kvproj[block_no]))
        cross_keys = low_back(low(rms_norm(cross_keyval[:, :D], gain_table[block_no, 3])))
        cross_values = low_back(low(cross_keyval[:, D:]))
        cross_mixed = attend(cross_query.reshape(groups, -1, D), cross_keys.reshape(groups, -1, D), cross_values.reshape(groups, -1, D), text_live).reshape(-1, D)
        cross_mixed = low_back(low(cross_mixed))
        residual = residual + low_back(matmul(cross_mixed, cross_back[block_no]))
        mlp_input = low(modulated(residual, shift_two, scale_two))
        up_proj = low_back(matmul(mlp_input, up_matrix[block_no]))
        activated = low(jax.nn.gelu(up_proj, approximate=True))
        residual = gated_add(residual, low_back(matmul(activated, down_matrix[block_no])), gate_two)
    return residual

def reference(tokens, text, clip_frames, timestep, mod_weight, mod_bias, qk_gains, self_in, self_out, cross_q, cross_kv, cross_out, mlp_in, mlp_out, cotangent):
    groups = timestep.shape[0]
    frames = timestep.shape[1]
    frame_index = jnp.arange(frames, dtype=jnp.int32)
    frame_pos = jnp.tile(frame_index, groups)
    token_frame = jnp.repeat(frame_pos, FRAME_TOK)
    token_spot = jnp.tile(jnp.arange(FRAME_TOK, dtype=jnp.int32), groups * frames)
    cosine, sine = rotary_tables(token_frame, token_spot)
    sinus = low(sinus_features(timestep.reshape(-1)))
    frame_live = (frame_index[None, :] < clip_frames[:, None]).astype(jnp.int32)
    seq_live = jnp.repeat(frame_live, FRAME_TOK, axis=1)
    text_live = jnp.ones((groups, TXT), jnp.int32)
    params = (mod_weight.astype(jnp.float32), mod_bias.astype(jnp.float32), qk_gains.astype(jnp.float32), self_in.astype(jnp.float32), self_out.astype(jnp.float32), cross_q.astype(jnp.float32), cross_kv.astype(jnp.float32), cross_out.astype(jnp.float32), mlp_in.astype(jnp.float32), mlp_out.astype(jnp.float32))
    text_float = text.astype(jnp.float32)

    def forward(residual, weights):
        return run_layers(residual, weights, text_float, sinus, cosine, sine, seq_live, text_live)
    result, backward = jax.vjp(forward, tokens.astype(jnp.float32), params)
    input_grad, weight_grads = backward(cotangent.astype(jnp.float32))
    return (result.astype(jnp.bfloat16), input_grad, weight_grads[0], weight_grads[1], weight_grads[2], weight_grads[3], weight_grads[4], weight_grads[5], weight_grads[6], weight_grads[7], weight_grads[8], weight_grads[9])
```

```python
import math

import jax
import jax.numpy as jnp
from jax import lax
from jax.experimental import pallas as pl
from jax.experimental.pallas import tpu as pltpu
from jax.sharding import Mesh
from jax.sharding import PartitionSpec as P

D = 1536
HD = 128
TXT = 512
FREQ = 256
WP = 8
FRAME_TOK = 64
PLANE = 4

EPSILON = 1e-06
NEGATIVE = -1e30

FS = ("za", "yb", "xc")
PL = ("yb", "xc")
ALL = ("za", "yb", "xc", "sp")
SCALE = 1.0 / math.sqrt(HD)
BF = jnp.bfloat16
F32 = jnp.float32


def product(left, right):
    return jnp.dot(left, right, preferred_element_type=F32)


def product_tn(left, right):
    return lax.dot_general(left, right, (((0,), (0,)), ((), ())), preferred_element_type=F32)


def product_nt(left, right):
    return lax.dot_general(left, right, (((1,), (1,)), ((), ())), preferred_element_type=F32)


def layer_norm(values):
    centred = values - jnp.mean(values, axis=-1, keepdims=True)
    return centred * lax.rsqrt(jnp.mean(centred * centred, axis=-1, keepdims=True) + EPSILON)


def sinus_features(steps):
    half_dim = FREQ // 2
    rates = jnp.exp(jnp.arange(half_dim).astype(F32) * (-math.log(10000.0) / half_dim))
    angles = steps.astype(F32)[:, None] * rates[None, :]
    return jnp.concatenate([jnp.cos(angles), jnp.sin(angles)], axis=1)


def rotary_tables(frame_pos, token_spot):
    half_dim = HD // 2
    side_pairs = HD // 6
    lead_pairs = half_dim - 2 * side_pairs
    pair_index = jnp.arange(half_dim)
    log_base = -math.log(10000.0)
    lead_part = pair_index < lead_pairs
    side_part = jnp.logical_and(pair_index >= lead_pairs, pair_index < lead_pairs + side_pairs)
    last_part = pair_index >= lead_pairs + side_pairs
    frame_rate = jnp.where(
        lead_part, jnp.exp(log_base * pair_index.astype(F32) / lead_pairs), 0.0
    )
    row_rate = jnp.where(
        side_part, jnp.exp(log_base * (pair_index - lead_pairs).astype(F32) / side_pairs), 0.0
    )
    column_rate = jnp.where(
        last_part,
        jnp.exp(log_base * (pair_index - lead_pairs - side_pairs).astype(F32) / side_pairs),
        0.0,
    )
    patch_row = (token_spot // WP).astype(F32)
    patch_column = (token_spot % WP).astype(F32)
    angles = (
        frame_pos.astype(F32)[:, None] * frame_rate[None, :]
        + patch_row[:, None] * row_rate[None, :]
        + patch_column[:, None] * column_rate[None, :]
    )
    return (jnp.cos(angles), jnp.sin(angles))


def rotate(values, cosine, sine):
    row_count = values.shape[0]
    shaped = values.reshape(row_count, -1, HD)
    half_dim = HD // 2
    first_half = shaped[:, :, :half_dim]
    second_half = shaped[:, :, half_dim:]
    cos_rows = cosine[:, None, :]
    sin_rows = sine[:, None, :]
    turned = jnp.concatenate(
        [
            first_half * cos_rows - second_half * sin_rows,
            second_half * cos_rows + first_half * sin_rows,
        ],
        axis=2,
    )
    return turned.reshape(row_count, -1)


def modulated(residual, shift, scale):
    frames = shift.shape[0]
    normed = layer_norm(residual).reshape(frames, -1, residual.shape[1])
    return (normed * (1.0 + scale[:, None, :]) + shift[:, None, :]).reshape(residual.shape)


def frame_scaled(rows, gate):
    frames = gate.shape[0]
    return (rows.reshape(frames, -1, rows.shape[1]) * gate[:, None, :]).reshape(rows.shape)


def frame_sum(values, frames):
    return jnp.sum(values.reshape(frames, -1, values.shape[1]), axis=1)


def attend_forward_kernel(live_ref, q_ref, k_ref, v_ref, out_ref, lse_ref):
    rows, keys = q_ref.shape[0], k_ref.shape[0]
    spot = lax.broadcasted_iota(jnp.int32, (rows, keys), 1)
    allowed = spot < live_ref[0]
    for head in range(q_ref.shape[1] // HD):
        part = slice(head * HD, (head + 1) * HD)
        scores = jnp.where(allowed, product_nt(q_ref[:, part], k_ref[:, part]) * SCALE, NEGATIVE)
        row_max = jnp.max(scores, axis=1, keepdims=True)
        log_total = row_max + jnp.log(jnp.sum(jnp.exp(scores - row_max), axis=1, keepdims=True))
        weights = jnp.exp(scores - log_total).astype(BF)
        out_ref[:, part] = product(weights, v_ref[:, part]).astype(BF)
        lse_ref[:, part] = jnp.broadcast_to(log_total, (rows, HD))


def attend_backward_kernel(
    live_ref, q_ref, k_ref, v_ref, lse_ref, do_ref, dq_ref, dk_ref, dv_ref
):
    rows, keys = q_ref.shape[0], k_ref.shape[0]
    spot = lax.broadcasted_iota(jnp.int32, (rows, keys), 1)
    allowed = spot < live_ref[0]
    for head in range(q_ref.shape[1] // HD):
        part = slice(head * HD, (head + 1) * HD)
        query, key, value, grad = q_ref[:, part], k_ref[:, part], v_ref[:, part], do_ref[:, part]
        scores = jnp.where(allowed, product_nt(query, key) * SCALE, NEGATIVE)
        weights = jnp.exp(scores - lse_ref[:, head * HD : head * HD + 1])
        grad_weights = product_nt(grad, value)
        delta = jnp.sum(weights * grad_weights, axis=1, keepdims=True)
        grad_scores = (weights * (grad_weights - delta)).astype(BF)
        dq_ref[:, part] = (product(grad_scores, key) * SCALE).astype(BF)
        dk_ref[:, part] = (product_tn(grad_scores, query) * SCALE).astype(BF)
        dv_ref[:, part] = product_tn(weights.astype(BF), grad).astype(BF)


VM = pl.BlockSpec(memory_space=pltpu.VMEM)
SM = pl.BlockSpec(memory_space=pltpu.SMEM)


def attend_forward(live, query, key, value):
    rows, width = query.shape
    keys = key.shape[0]
    heads = width // HD
    return pl.pallas_call(
        attend_forward_kernel,
        out_shape=(
            jax.ShapeDtypeStruct((rows, width), BF),
            jax.ShapeDtypeStruct((rows, width), F32),
        ),
        in_specs=[SM, VM, VM, VM],
        out_specs=(VM, VM),
        cost_estimate=pl.CostEstimate(
            flops=4 * rows * keys * width,
            bytes_accessed=8 * rows * width + 4 * keys * width,
            transcendentals=2 * rows * keys * heads,
        ),
    )(live, query, key, value)


def attend_backward(live, query, key, value, lse, grad):
    rows, width = query.shape
    keys = key.shape[0]
    heads = width // HD
    return pl.pallas_call(
        attend_backward_kernel,
        out_shape=(
            jax.ShapeDtypeStruct((rows, width), BF),
            jax.ShapeDtypeStruct((keys, width), BF),
            jax.ShapeDtypeStruct((keys, width), BF),
        ),
        in_specs=[SM, VM, VM, VM, VM, VM],
        out_specs=(VM, VM, VM),
        cost_estimate=pl.CostEstimate(
            flops=10 * rows * keys * width,
            bytes_accessed=10 * rows * width + 8 * keys * width,
            transcendentals=rows * keys * heads,
        ),
    )(live, query, key, value, lse, grad)


def gather(value, axes, axis=0):
    return lax.all_gather(value, axes, axis=axis, tiled=True)


def scatter(value, axes, axis=0):
    return lax.psum_scatter(value, axes, scatter_dimension=axis, tiled=True)


def swap(value, split_axis, concat_axis):
    return lax.all_to_all(value, "sp", split_axis=split_axis, concat_axis=concat_axis, tiled=True)


def rms_scale(total):
    return lax.rsqrt(total / D + EPSILON)


def square_sum(values):
    return jnp.sum(values * values, axis=1)


def rms_back(values, inverse, gain, grad):
    scaled = grad * gain
    return scaled, jnp.sum(scaled * values, axis=1)


def rms_finish(values, inverse, scaled, total):
    column = inverse[:, None]
    return scaled * column - values * (column * column * column) * (total / D)[:, None]


def body(
    tokens,
    text,
    clip_frames,
    timestep,
    mod_weight,
    mod_bias,
    qk_gains,
    self_in,
    self_out,
    cross_q,
    cross_kv,
    cross_out,
    mlp_in,
    mlp_out,
    cotangent,
):
    half = D // 2
    row_count = tokens.shape[0]
    frame_count = row_count // FRAME_TOK
    group_frames = timestep.shape[1]
    shards = D // self_in.shape[1]
    outer = shards // PLANE
    core = lax.axis_index("sp")
    chip = lax.axis_index(FS)
    own_frame = core * frame_count

    small = jnp.concatenate(
        [mod_bias[0].astype(F32), qk_gains[0].reshape(-1).astype(F32), timestep[0].astype(F32)]
    )
    small_all = gather(small[None], FS)
    bias_len, gain_len = mod_bias.shape[1], qk_gains.shape[2]
    bias_all = small_all[:, :bias_len].reshape(-1)
    gain_all = (
        small_all[:, bias_len : bias_len + 4 * gain_len]
        .reshape(shards, 4, gain_len)
        .transpose(1, 0, 2)
        .reshape(4, 2, half)
    )
    gain_own = lax.dynamic_index_in_dim(gain_all, core, 1, keepdims=False)
    steps_all = small_all[:, bias_len + 4 * gain_len :].reshape(-1)

    def own_half(weight, parts):
        shaped = weight[0].reshape(weight.shape[1], parts, 2, -1)
        return lax.dynamic_index_in_dim(shaped, core, 2, keepdims=False).reshape(
            weight.shape[1], -1
        )

    mod_matrix = gather(own_half(mod_weight, 1), FS)
    self_proj = gather(own_half(self_in, 3), FS)
    self_back = swap(gather(own_half(self_out, 1), FS), 0, 1)
    cross_kvproj = gather(own_half(cross_kv, 2), FS)
    cross_qproj = gather(own_half(cross_q, 1), FS)
    cross_back = swap(gather(own_half(cross_out, 1), FS), 0, 1)

    hid = mlp_out.shape[1] // 2
    in_rows = mlp_in.shape[1]
    up_part = lax.dynamic_index_in_dim(
        mlp_in[0].reshape(in_rows, outer, PLANE, 2, hid), core, 3, keepdims=False
    )
    up_part = up_part.transpose(2, 0, 1, 3).reshape(PLANE * in_rows, outer * hid)
    up_part = lax.all_to_all(up_part, PL, split_axis=0, concat_axis=0, tiled=True)
    up_matrix = gather(up_part, "za")
    down_part = lax.dynamic_slice_in_dim(mlp_out[0], core * hid, hid, 0)
    down_matrix = gather(down_part, "za")

    live_keys = clip_frames * FRAME_TOK
    all_keys = jnp.full((1,), TXT, jnp.int32)
    own_steps = lax.dynamic_slice_in_dim(timestep[0], own_frame, frame_count)
    clip_pos = jnp.arange(group_frames, dtype=jnp.int32)
    cosine, sine = rotary_tables(
        jnp.repeat(clip_pos, FRAME_TOK),
        jnp.tile(jnp.arange(FRAME_TOK, dtype=jnp.int32), group_frames),
    )
    sinus = sinus_features(timestep[0]).astype(BF)

    mod_half = product(sinus, mod_matrix)
    mod_half = mod_half + lax.dynamic_slice_in_dim(bias_all, core * 3 * D, 3 * D)[None]
    modulation = swap(mod_half, 0, 1)
    shift_one, scale_one, gate_one, shift_two, scale_two, gate_two = jnp.split(
        modulation, 6, axis=1
    )

    text_all = gather(text, "sp")

    residual = tokens.astype(F32)
    attn_float, back_attn_input = jax.vjp(modulated, residual, shift_one, scale_one)
    attn_input = gather(attn_float.astype(BF), "sp")
    joined = product(attn_input, self_proj)
    raw_q, raw_k, raw_v = joined[:, :half], joined[:, half : 2 * half], joined[:, 2 * half :]
    totals = lax.psum(jnp.stack([square_sum(raw_q), square_sum(raw_k)]), "sp")
    inv_q, inv_k = rms_scale(totals[0]), rms_scale(totals[1])
    query = rotate(raw_q * inv_q[:, None] * gain_own[0], cosine, sine).astype(BF)
    key = rotate(raw_k * inv_k[:, None] * gain_own[1], cosine, sine).astype(BF)
    value = raw_v.astype(BF)
    self_mixed, self_lse = attend_forward(live_keys, query, key, value)
    self_branch = scatter(product(self_mixed, self_back), "sp")
    residual = residual + frame_scaled(self_branch, gate_one)

    text_raw = product(text_all, cross_kvproj)
    raw_ck, raw_cv = text_raw[:, :half], text_raw[:, half:]
    inv_ck = rms_scale(lax.psum(square_sum(raw_ck)[None], "sp")[0])
    cross_key = (raw_ck * inv_ck[:, None] * gain_own[3]).astype(BF)
    cross_value = raw_cv.astype(BF)

    cross_float, back_cross_norm = jax.vjp(layer_norm, residual)
    cross_input = gather(cross_float.astype(BF), "sp")
    cross_raw = product(cross_input, cross_qproj)
    inv_cq = rms_scale(lax.psum(square_sum(cross_raw)[None], "sp")[0])
    cross_query = (cross_raw * inv_cq[:, None] * gain_own[2]).astype(BF)
    cross_mixed, cross_lse = attend_forward(all_keys, cross_query, cross_key, cross_value)
    residual = residual + scatter(product(cross_mixed, cross_back), "sp")

    mlp_float, back_mlp_input = jax.vjp(modulated, residual, shift_two, scale_two)
    mlp_input = gather(gather(mlp_float.astype(BF), PL), "sp")
    up_proj = product(mlp_input, up_matrix)
    activated_float, back_gelu = jax.vjp(
        lambda inner: jax.nn.gelu(inner, approximate=True), up_proj
    )
    activated = activated_float.astype(BF)

    def plane_sum(partial):
        half_sum = scatter(partial, "sp")
        return scatter(half_sum.astype(BF), PL).astype(F32)

    mlp_branch = plane_sum(product(activated, down_matrix))
    output = (residual + frame_scaled(mlp_branch, gate_two)).astype(BF)

    grad_rows = cotangent.astype(F32)
    grad_branch = frame_scaled(grad_rows, gate_two).astype(BF)
    grad_gate_two = frame_sum(grad_rows * mlp_branch, frame_count)
    grad_branch_all = gather(gather(grad_branch, PL), "sp")
    grad_down = product_tn(activated, grad_branch_all).astype(BF)
    down_owned = scatter(grad_down, "za")
    grad_up_low = back_gelu(product_nt(grad_branch_all, down_matrix))[0].astype(BF)
    grad_up = product_tn(mlp_input, grad_up_low).astype(BF)
    up_owned = scatter(grad_up, "za")
    grad_mlp_input = plane_sum(product_nt(grad_up_low, up_matrix))
    grad_from_mlp, grad_shift_two, grad_scale_two = back_mlp_input(grad_mlp_input)
    grad_rows = grad_rows + grad_from_mlp

    grad_low = gather(grad_rows.astype(BF), "sp")
    grad_cross_back = swap(product_tn(cross_mixed, grad_low).astype(BF), 1, 0)
    cross_back_owned = scatter(grad_cross_back, FS)
    grad_cross_mixed = product_nt(grad_low, cross_back).astype(BF)
    grad_cq, grad_ck, grad_cv = attend_backward(
        all_keys, cross_query, cross_key, cross_value, cross_lse, grad_cross_mixed
    )
    grad_cq, grad_ck = grad_cq.astype(F32), grad_ck.astype(F32)
    grad_gain_two = jnp.sum(grad_cq * cross_raw * inv_cq[:, None], axis=0)
    grad_gain_three = jnp.sum(grad_ck * raw_ck * inv_ck[:, None], axis=0)
    scaled_cq, dots_cq = rms_back(cross_raw, inv_cq, gain_own[2], grad_cq)
    scaled_ck, dots_ck = rms_back(raw_ck, inv_ck, gain_own[3], grad_ck)
    dots_cq = lax.psum(dots_cq[None], "sp")[0]
    dots_ck = lax.psum(dots_ck[None], "sp")[0]
    grad_cross_low = rms_finish(cross_raw, inv_cq, scaled_cq, dots_cq).astype(BF)
    grad_text_low = jnp.concatenate(
        [rms_finish(raw_ck, inv_ck, scaled_ck, dots_ck).astype(BF), grad_cv], axis=1
    )
    cross_q_owned = scatter(product_tn(cross_input, grad_cross_low).astype(BF), FS)
    cross_kv_owned = scatter(product_tn(text_all, grad_text_low).astype(BF), FS)
    grad_cross_input = scatter(product_nt(grad_cross_low, cross_qproj), "sp")
    grad_rows = grad_rows + back_cross_norm(grad_cross_input)[0]

    grad_gate_one = frame_sum(grad_rows * self_branch, frame_count)
    grad_self_low = gather(frame_scaled(grad_rows, gate_one).astype(BF), "sp")
    grad_self_back = swap(product_tn(self_mixed, grad_self_low).astype(BF), 1, 0)
    self_back_owned = scatter(grad_self_back, FS)
    grad_self_mixed = product_nt(grad_self_low, self_back).astype(BF)
    grad_q, grad_k, grad_v = attend_backward(
        live_keys, query, key, value, self_lse, grad_self_mixed
    )
    grad_q = rotate(grad_q.astype(F32), cosine, -sine)
    grad_k = rotate(grad_k.astype(F32), cosine, -sine)
    grad_gain_zero = jnp.sum(grad_q * raw_q * inv_q[:, None], axis=0)
    grad_gain_one = jnp.sum(grad_k * raw_k * inv_k[:, None], axis=0)
    scaled_q, dots_q = rms_back(raw_q, inv_q, gain_own[0], grad_q)
    scaled_k, dots_k = rms_back(raw_k, inv_k, gain_own[1], grad_k)
    dots = lax.psum(jnp.stack([dots_q, dots_k]), "sp")
    grad_joined_low = jnp.concatenate(
        [
            rms_finish(raw_q, inv_q, scaled_q, dots[0]).astype(BF),
            rms_finish(raw_k, inv_k, scaled_k, dots[1]).astype(BF),
            grad_v,
        ],
        axis=1,
    )
    self_in_owned = scatter(product_tn(attn_input, grad_joined_low).astype(BF), FS)
    grad_attn_input = scatter(product_nt(grad_joined_low, self_proj), "sp")
    grad_from_attn, grad_shift_one, grad_scale_one = back_attn_input(grad_attn_input)
    grad_rows = grad_rows + grad_from_attn

    grad_modulation = jnp.concatenate(
        [grad_shift_one, grad_scale_one, grad_gate_one, grad_shift_two, grad_scale_two, grad_gate_two],
        axis=1,
    )
    grad_mod_half = swap(grad_modulation, 1, 0)
    grad_mod_all = gather(grad_mod_half.astype(BF), FS)
    sinus_all = sinus_features(steps_all).astype(BF)
    own_features = mod_weight.shape[1]
    sinus_own = lax.dynamic_slice_in_dim(sinus_all, chip * own_features, own_features, 1)
    mod_weight_grad = gather(product_tn(sinus_own, grad_mod_all), "sp", 1)

    grad_gains = jnp.stack([grad_gain_zero, grad_gain_one, grad_gain_two, grad_gain_three])
    both = jnp.arange(2)[None, :, None] == core
    grad_gains = jnp.where(both, grad_gains[:, None, :], 0.0).reshape(4, shards, gain_len)
    grad_small = jnp.concatenate(
        [
            jnp.sum(grad_modulation, axis=0).reshape(shards, bias_len),
            grad_gains.transpose(1, 0, 2).reshape(shards, 4 * gain_len),
        ],
        axis=1,
    )
    small_owned = lax.psum(scatter(grad_small, FS), "sp")[0]

    def join(owned, parts):
        rows = owned.shape[0]
        pair = gather(owned.reshape(1, rows, parts, -1), "sp").astype(F32)
        return pair.transpose(1, 2, 0, 3).reshape(1, rows, -1)

    up_rows = lax.all_to_all(up_owned, PL, split_axis=0, concat_axis=0, tiled=True)
    up_pair = gather(up_rows.reshape(1, PLANE, in_rows, outer, hid), "sp").astype(F32)
    mlp_in_grad = up_pair.transpose(2, 3, 1, 0, 4).reshape(1, in_rows, -1)
    return (
        output,
        grad_rows,
        mod_weight_grad[None],
        small_owned[None, :bias_len],
        small_owned[bias_len:].reshape(1, 4, gain_len),
        join(self_in_owned, 3),
        join(self_back_owned, 1),
        join(cross_q_owned, 1),
        join(cross_kv_owned, 2),
        join(cross_back_owned, 1),
        mlp_in_grad,
        gather(down_owned, "sp").astype(F32)[None],
    )


def solution(mesh):
    chips, cores = mesh.shape["fsdp"], mesh.shape["sp"]
    grid = mesh.devices.reshape(chips // PLANE, 2, PLANE // 2, cores)
    inner = Mesh(grid, ALL)
    rows, second = P(ALL, None), P(None, FS, None)
    in_specs = (
        rows,
        rows,
        P(FS),
        P(FS, None),
        second,
        P(None, FS),
        P(None, None, FS),
        *([second] * 7),
        rows,
    )
    out_specs = (rows, rows, second, P(None, FS), P(None, None, FS), *([second] * 7))
    return jax.shard_map(body, mesh=inner, in_specs=in_specs, out_specs=out_specs, check_vma=False)
```

```python
import functools
import math

import jax
import jax.numpy as jnp
from jax import lax
from jax.experimental import pallas as pl
from jax.experimental.pallas import tpu as pltpu
from jax.sharding import Mesh
from jax.sharding import PartitionSpec as P

D = 1536
HD = 128
TXT = 512
FREQ = 256
WP = 8
FRAME_TOK = 64
PLANE = 4

EPSILON = 1e-06
NEGATIVE = -1e30

FS = ("za", "yb", "xc")
PL = ("yb", "xc")
ALL = ("za", "yb", "xc", "sp")
SCALE = 1.0 / math.sqrt(HD)
MESH = pl.DeviceIdType.MESH
BF = jnp.bfloat16
F32 = jnp.float32


def product(left, right):
    return jnp.dot(left, right, preferred_element_type=F32)


def product_tn(left, right):
    return lax.dot_general(left, right, (((0,), (0,)), ((), ())), preferred_element_type=F32)


def product_nt(left, right):
    return lax.dot_general(left, right, (((1,), (1,)), ((), ())), preferred_element_type=F32)


def layer_norm(values):
    centred = values - jnp.mean(values, axis=-1, keepdims=True)
    return centred * lax.rsqrt(jnp.mean(centred * centred, axis=-1, keepdims=True) + EPSILON)


def sinus_features(steps):
    half_dim = FREQ // 2
    rates = jnp.exp(jnp.arange(half_dim).astype(F32) * (-math.log(10000.0) / half_dim))
    angles = steps.astype(F32)[:, None] * rates[None, :]
    return jnp.concatenate([jnp.cos(angles), jnp.sin(angles)], axis=1)


def rotary_tables(frame_pos, token_spot):
    half_dim = HD // 2
    side_pairs = HD // 6
    lead_pairs = half_dim - 2 * side_pairs
    pair_index = jnp.arange(half_dim)
    log_base = -math.log(10000.0)
    lead_part = pair_index < lead_pairs
    side_part = jnp.logical_and(pair_index >= lead_pairs, pair_index < lead_pairs + side_pairs)
    last_part = pair_index >= lead_pairs + side_pairs
    frame_rate = jnp.where(
        lead_part, jnp.exp(log_base * pair_index.astype(F32) / lead_pairs), 0.0
    )
    row_rate = jnp.where(
        side_part, jnp.exp(log_base * (pair_index - lead_pairs).astype(F32) / side_pairs), 0.0
    )
    column_rate = jnp.where(
        last_part,
        jnp.exp(log_base * (pair_index - lead_pairs - side_pairs).astype(F32) / side_pairs),
        0.0,
    )
    patch_row = (token_spot // WP).astype(F32)
    patch_column = (token_spot % WP).astype(F32)
    angles = (
        frame_pos.astype(F32)[:, None] * frame_rate[None, :]
        + patch_row[:, None] * row_rate[None, :]
        + patch_column[:, None] * column_rate[None, :]
    )
    return (jnp.cos(angles), jnp.sin(angles))


def rotate(values, cosine, sine):
    row_count = values.shape[0]
    shaped = values.reshape(row_count, -1, HD)
    half_dim = HD // 2
    first_half = shaped[:, :, :half_dim]
    second_half = shaped[:, :, half_dim:]
    cos_rows = cosine[:, None, :]
    sin_rows = sine[:, None, :]
    turned = jnp.concatenate(
        [
            first_half * cos_rows - second_half * sin_rows,
            second_half * cos_rows + first_half * sin_rows,
        ],
        axis=2,
    )
    return turned.reshape(row_count, -1)


def modulated(residual, shift, scale):
    frames = shift.shape[0]
    normed = layer_norm(residual).reshape(frames, -1, residual.shape[1])
    return (normed * (1.0 + scale[:, None, :]) + shift[:, None, :]).reshape(residual.shape)


def frame_scaled(rows, gate):
    frames = gate.shape[0]
    return (rows.reshape(frames, -1, rows.shape[1]) * gate[:, None, :]).reshape(rows.shape)


def frame_sum(values, frames):
    return jnp.sum(values.reshape(frames, -1, values.shape[1]), axis=1)


def attend_forward_kernel(live_ref, q_ref, k_ref, v_ref, out_ref, lse_ref):
    rows, keys = q_ref.shape[0], k_ref.shape[0]
    spot = lax.broadcasted_iota(jnp.int32, (rows, keys), 1)
    allowed = spot < live_ref[0]
    for head in range(q_ref.shape[1] // HD):
        part = slice(head * HD, (head + 1) * HD)
        scores = jnp.where(allowed, product_nt(q_ref[:, part], k_ref[:, part]) * SCALE, NEGATIVE)
        row_max = jnp.max(scores, axis=1, keepdims=True)
        log_total = row_max + jnp.log(jnp.sum(jnp.exp(scores - row_max), axis=1, keepdims=True))
        weights = jnp.exp(scores - log_total).astype(BF)
        out_ref[:, part] = product(weights, v_ref[:, part]).astype(BF)
        lse_ref[:, part] = jnp.broadcast_to(log_total, (rows, HD))


def attend_backward_kernel(
    live_ref, q_ref, k_ref, v_ref, lse_ref, do_ref, dq_ref, dk_ref, dv_ref
):
    rows, keys = q_ref.shape[0], k_ref.shape[0]
    spot = lax.broadcasted_iota(jnp.int32, (rows, keys), 1)
    allowed = spot < live_ref[0]
    for head in range(q_ref.shape[1] // HD):
        part = slice(head * HD, (head + 1) * HD)
        query, key, value, grad = q_ref[:, part], k_ref[:, part], v_ref[:, part], do_ref[:, part]
        scores = jnp.where(allowed, product_nt(query, key) * SCALE, NEGATIVE)
        weights = jnp.exp(scores - lse_ref[:, head * HD : head * HD + 1])
        grad_weights = product_nt(grad, value)
        delta = jnp.sum(weights * grad_weights, axis=1, keepdims=True)
        grad_scores = (weights * (grad_weights - delta)).astype(BF)
        dq_ref[:, part] = (product(grad_scores, key) * SCALE).astype(BF)
        dk_ref[:, part] = (product_tn(grad_scores, query) * SCALE).astype(BF)
        dv_ref[:, part] = product_tn(weights.astype(BF), grad).astype(BF)


VM = pl.BlockSpec(memory_space=pltpu.VMEM)
SM = pl.BlockSpec(memory_space=pltpu.SMEM)
ANY = pl.BlockSpec(memory_space=pl.ANY)


def attend_forward(live, query, key, value):
    rows, width = query.shape
    keys = key.shape[0]
    heads = width // HD
    return pl.pallas_call(
        attend_forward_kernel,
        out_shape=(
            jax.ShapeDtypeStruct((rows, width), BF),
            jax.ShapeDtypeStruct((rows, width), F32),
        ),
        in_specs=[SM, VM, VM, VM],
        out_specs=(VM, VM),
        cost_estimate=pl.CostEstimate(
            flops=4 * rows * keys * width,
            bytes_accessed=8 * rows * width + 4 * keys * width,
            transcendentals=2 * rows * keys * heads,
        ),
    )(live, query, key, value)


def attend_backward(live, query, key, value, lse, grad):
    rows, width = query.shape
    keys = key.shape[0]
    heads = width // HD
    return pl.pallas_call(
        attend_backward_kernel,
        out_shape=(
            jax.ShapeDtypeStruct((rows, width), BF),
            jax.ShapeDtypeStruct((keys, width), BF),
            jax.ShapeDtypeStruct((keys, width), BF),
        ),
        in_specs=[SM, VM, VM, VM, VM, VM],
        out_specs=(VM, VM, VM),
        cost_estimate=pl.CostEstimate(
            flops=10 * rows * keys * width,
            bytes_accessed=10 * rows * width + 8 * keys * width,
            transcendentals=rows * keys * heads,
        ),
    )(live, query, key, value, lse, grad)


def row_add(target, left, right, rows):
    step = 16 if rows % 16 == 0 else rows

    def chunk(index, carry):
        at = pl.ds(pl.multiple_of(index * step, step), step)
        total = left[at, :].astype(F32) + right[at, :].astype(F32)
        target[at, :] = total.astype(target.dtype)
        return carry

    lax.fori_loop(0, rows // step, chunk, 0)


class Flights:
    def __init__(self):
        self.sent = []

    def send(self, source, target, send_sem, recv_sem, device, when=None):
        copy = pltpu.make_async_remote_copy(
            src_ref=source,
            dst_ref=target,
            send_sem=send_sem,
            recv_sem=recv_sem,
            device_id=device,
            device_id_type=MESH,
        )
        if when is None:
            copy.start()
        else:
            pl.when(when)(copy.start)
        self.sent.append((when, copy))

    def local(self, source, target, sem):
        copy = pltpu.make_async_copy(source, target, sem)
        copy.start()
        return copy

    def drain(self):
        for when, copy in self.sent:
            if when is None:
                copy.wait_send()
            else:
                pl.when(when)(copy.wait_send)


def landed(target, sem, device):
    pltpu.make_async_remote_copy(
        src_ref=target,
        dst_ref=target,
        send_sem=sem,
        recv_sem=sem,
        device_id=device,
        device_id_type=MESH,
    ).wait_recv()


def greet(devices, optional=()):
    barrier = pltpu.get_barrier_semaphore()
    for device in devices:
        pl.semaphore_signal(barrier, inc=1, device_id=device, device_id_type=MESH)
    for when, device in optional:

        @pl.when(when)
        def _(device=device):
            pl.semaphore_signal(barrier, inc=1, device_id=device, device_id_type=MESH)

    count = len(devices)
    for when, _ in optional:
        count = count + when.astype(jnp.int32)
    pl.semaphore_wait(barrier, count)


def gather_kernel(outer, full, halves, *refs):
    count = full + 2
    ins, refs = refs[:count], refs[count:]
    outs, refs = refs[:count], refs[count:]
    fins, refs = refs[: len(halves)], refs[len(halves) :]
    local_sem, zs, zr, s1, r1, s2, r2, a_s, a_r, f_s, f_r, f_l = refs
    z, y, x = (lax.axis_index(name) for name in FS)
    core = lax.axis_index("sp")
    here = 2 * y + x
    up, down = full, full + 1
    fly = Flights()
    x_peer, y_peer = {"xc": 1 - x}, {"yb": 1 - y}
    diagonal = {"yb": 1 - y, "xc": 1 - x}
    above, below = {"za": z + 1}, {"za": z - 1}
    core_peer = {"sp": 1 - core}
    has_above, has_below = z + 1 < outer, z >= 1
    greet((x_peer, y_peer, diagonal, core_peer), ((has_above, above), (has_below, below)))

    locals_ = [fly.local(ins[i], outs[i].at[z, y, x], local_sem.at[i]) for i in range(full)]
    local_up = fly.local(ins[up].at[here], outs[up].at[z, here], local_sem.at[up])
    local_down = fly.local(ins[down], outs[down].at[z], local_sem.at[down])

    def shard(i, slot):
        return outs[i].at[slot, y, x] if i < full else outs[i].at[slot]

    def z_send(i, way, hop, source=None):
        if hop > outer - 2:
            return
        slot = z - hop if way == 0 else z + hop
        when = jnp.logical_and(has_above, slot >= 0) if way == 0 else jnp.logical_and(has_below, slot < outer)
        fly.send(
            shard(i, slot) if source is None else source,
            shard(i, slot),
            zs.at[i, way, hop],
            zr.at[i, way, hop],
            above if way == 0 else below,
            when,
        )

    def z_slot(way, hop):
        slot = z - 1 - hop if way == 0 else z + 1 + hop
        return slot, (slot >= 0 if way == 0 else slot < outer)

    def z_wait(i, way, hop):
        slot, when = z_slot(way, hop)

        @pl.when(when)
        def _():
            landed(shard(i, slot), zr.at[i, way, hop], below if way == 0 else above)

    def turns(i, slot):
        turn = (slot + i) % 2
        first = ((y + turn) % 2, (x + 1 - turn) % 2)
        second = ((y + 1 - turn) % 2, (x + turn) % 2)
        return first, second

    def xy_own(i, slot, when=None, source=None):
        first, second = turns(i, slot)
        mine = outs[i].at[slot, y, x]
        source = mine if source is None else source
        fly.send(source, mine, s1.at[i, slot], r1.at[i, slot], {"yb": first[0], "xc": first[1]}, when)
        fly.send(source, mine, s2.at[i, slot, 0], r2.at[i, slot, 0], {"yb": second[0], "xc": second[1]}, when)

    def xy_pass(i, slot, when=None):
        first, second = turns(i, slot)
        theirs = outs[i].at[slot, first[0], first[1]]

        def wait():
            landed(theirs, r1.at[i, slot], {"yb": first[0], "xc": first[1]})

        if when is None:
            wait()
        else:
            pl.when(when)(wait)
        fly.send(theirs, theirs, s2.at[i, slot, 1], r2.at[i, slot, 1], {"yb": second[0], "xc": second[1]}, when)

    def xy_end(i, slot):
        _, second = turns(i, slot)
        device = {"yb": second[0], "xc": second[1]}
        landed(outs[i].at[slot, second[0], second[1]], r2.at[i, slot, 0], device)
        landed(outs[i].at[slot, 1 - y, 1 - x], r2.at[i, slot, 1], device)

    for i in range(full):
        for way in range(2):
            z_send(i, way, 0, ins[i])
        xy_own(i, z, None, ins[i])
    for hop in range(outer - 1):
        for i in range(full):
            for way in range(2):
                slot, when = z_slot(way, hop)
                z_wait(i, way, hop)
                z_send(i, way, hop + 1)
                xy_own(i, slot, when)
        if hop == 0:
            for turn, device in enumerate((x_peer, y_peer, diagonal)):
                ty = y if turn == 0 else 1 - y
                tx = x if turn == 1 else 1 - x
                fly.send(
                    ins[up].at[2 * ty + tx],
                    outs[up].at[z, here],
                    a_s.at[turn],
                    a_r.at[turn],
                    device,
                )
    for way in range(2):
        z_send(down, way, 0, ins[down])
    local_up.wait()
    for turn, device in enumerate((x_peer, y_peer, diagonal)):
        ty = y if turn == 0 else 1 - y
        tx = x if turn == 1 else 1 - x
        landed(outs[up].at[z, 2 * ty + tx], a_r.at[turn], device)
    for way in range(2):
        z_send(up, way, 0)
    for i in range(full):
        xy_pass(i, z)
    for hop in range(outer - 1):
        for i in range(full):
            for way in range(2):
                slot, when = z_slot(way, hop)
                xy_pass(i, slot, when)
        for i in (down, up):
            for way in range(2):
                z_wait(i, way, hop)
                z_send(i, way, hop + 1)
    for i in range(full):
        for slot in range(outer):
            xy_end(i, slot)
    for copy in locals_:
        copy.wait()
    local_down.wait()

    part = outer // 2
    for j, i in enumerate(halves):
        width = ins[i].shape[-1]
        columns = pl.ds(pl.multiple_of(core * width, width), width)
        theirs = pl.ds((1 - core) * part, part)
        ours = pl.ds(core * part, part)
        fly.send(outs[i].at[theirs], fins[j].at[:, :, :, :, columns], f_s.at[j], f_r.at[j], core_peer)
        fly.local(outs[i].at[ours], fins[j].at[:, :, :, :, columns], f_l.at[j])
    for j, i in enumerate(halves):
        width = ins[i].shape[-1]
        columns = pl.ds(pl.multiple_of(core * width, width), width)
        others = pl.ds(pl.multiple_of((1 - core) * width, width), width)
        ours = pl.ds(core * part, part)
        pltpu.make_async_copy(outs[i].at[ours], fins[j].at[:, :, :, :, columns], f_l.at[j]).wait()
        landed(fins[j].at[:, :, :, :, others], f_r.at[j], core_peer)
    fly.drain()


def gather_weights(outer, full, halves, up, down):
    count = len(full) + 2
    arrays = [*full, up, down]
    shapes = [jax.ShapeDtypeStruct((outer, 2, 2, *a.shape), a.dtype) for a in full]
    shapes.append(jax.ShapeDtypeStruct((outer, *up.shape), up.dtype))
    shapes.append(jax.ShapeDtypeStruct((outer, *down.shape), down.dtype))
    for i in halves:
        r, n = full[i].shape
        shapes.append(jax.ShapeDtypeStruct((outer // 2, 2, 2, r, 2 * n), full[i].dtype))
    dma = pltpu.SemaphoreType.DMA
    hops = outer - 1
    nf, nh = len(full), len(halves)
    results = pl.pallas_call(
        functools.partial(gather_kernel, outer, nf, halves),
        out_shape=shapes,
        in_specs=[VM] * count,
        out_specs=[ANY] * len(shapes),
        scratch_shapes=[
            dma((count,)),
            dma((count, 2, hops)),
            dma((count, 2, hops)),
            dma((nf, outer)),
            dma((nf, outer)),
            dma((nf, outer, 2)),
            dma((nf, outer, 2)),
            dma((3,)),
            dma((3,)),
            dma((nh,)),
            dma((nh,)),
            dma((nh,)),
        ],
        compiler_params=pltpu.CompilerParams(collective_id=0, has_side_effects=True),
        name="gather_weights",
    )(*arrays)
    gathered = [v.reshape(-1, v.shape[-1]) for v in results[: nf + 2]]
    for j, i in enumerate(halves):
        gathered[i] = results[nf + 2 + j].reshape(-1, results[nf + 2 + j].shape[-1])
    return gathered, results[: nf + 2]


def plane_gather_kernel(own_ref, out_ref, local_sem, send, recv):
    y, x, core = lax.axis_index("yb"), lax.axis_index("xc"), lax.axis_index("sp")
    x_peer, y_peer, core_peer = {"xc": 1 - x}, {"yb": 1 - y}, {"sp": 1 - core}
    fly = Flights()
    greet((x_peer, y_peer, core_peer))
    size = own_ref.shape[0] // 2
    top, low = pl.ds(0, size), pl.ds(size, size)
    local = fly.local(own_ref, out_ref.at[y, x, core], local_sem.at[0])

    def place(ty, tx, rows):
        return out_ref.at[ty, tx, core, rows]

    fly.send(own_ref.at[top], place(y, x, top), send.at[0], recv.at[0], x_peer)
    fly.send(own_ref.at[low], place(y, x, low), send.at[1], recv.at[1], y_peer)
    fly.send(own_ref.at[low], place(y, x, low), send.at[2], recv.at[2], x_peer)
    fly.send(own_ref.at[top], place(y, x, top), send.at[3], recv.at[3], y_peer)
    fly.send(own_ref, out_ref.at[y, x, core], send.at[4], recv.at[4], core_peer)

    def arrive(index, ty, tx, rows, device):
        landed(place(ty, tx, rows), recv.at[index], device)
        fly.send(place(ty, tx, rows), place(ty, tx, rows), send.at[index + 5], recv.at[index + 5], core_peer)

    arrive(0, y, 1 - x, top, x_peer)
    fly.send(place(y, 1 - x, top), place(y, 1 - x, top), send.at[12], recv.at[12], y_peer)
    arrive(1, 1 - y, x, low, y_peer)
    fly.send(place(1 - y, x, low), place(1 - y, x, low), send.at[13], recv.at[13], x_peer)
    arrive(2, y, 1 - x, low, x_peer)
    arrive(3, 1 - y, x, top, y_peer)
    for index, rows, device in ((0, top, y_peer), (1, low, x_peer)):
        landed(place(1 - y, 1 - x, rows), recv.at[12 + index], device)
        fly.send(
            place(1 - y, 1 - x, rows), place(1 - y, 1 - x, rows), send.at[10 + index], recv.at[10 + index], core_peer
        )
    other = 1 - core
    landed(out_ref.at[y, x, other], recv.at[4], core_peer)
    for index, ty, tx, rows in (
        (5, y, 1 - x, top),
        (6, 1 - y, x, low),
        (7, y, 1 - x, low),
        (8, 1 - y, x, top),
        (10, 1 - y, 1 - x, top),
        (11, 1 - y, 1 - x, low),
    ):
        landed(out_ref.at[ty, tx, other, rows], recv.at[index], core_peer)
    local.wait()
    fly.drain()


def plane_gather(own):
    rows, width = own.shape
    dma = pltpu.SemaphoreType.DMA
    out = pl.pallas_call(
        plane_gather_kernel,
        out_shape=jax.ShapeDtypeStruct((2, 2, 2, rows, width), own.dtype),
        in_specs=[VM],
        out_specs=VM,
        scratch_shapes=[dma((1,)), dma((14,)), dma((14,))],
        compiler_params=pltpu.CompilerParams(collective_id=1, has_side_effects=True),
        name="plane_gather",
    )(own)
    return out.reshape(8 * rows, width)


def plane_sum_kernel(part_ref, out_ref, core_in, first, second, keep, send, recv):
    y, x, core = lax.axis_index("yb"), lax.axis_index("xc"), lax.axis_index("sp")
    x_peer, y_peer, core_peer = {"xc": 1 - x}, {"yb": 1 - y}, {"sp": 1 - core}
    fly = Flights()
    greet((x_peer, y_peer, core_peer))
    rows = part_ref.shape[3]
    size = rows // 2
    top, low = pl.ds(0, size), pl.ds(size, size)
    chips = ((1 - y, 1 - x), (1 - y, x), (y, 1 - x), (y, x))
    for index, (ty, tx) in enumerate(chips):
        fly.send(
            part_ref.at[ty, tx, 1 - core], core_in.at[index], send.at[index], recv.at[index], core_peer
        )

    def own_part(index):
        ty, tx = chips[index]
        return part_ref.at[ty, tx, core]

    def core_sum(index):
        landed(core_in.at[index], recv.at[index], core_peer)
        row_add(core_in.at[index], core_in.at[index], own_part(index), rows)

    core_sum(0)
    fly.send(core_in.at[0, top], first.at[0], send.at[4], recv.at[4], y_peer)
    fly.send(core_in.at[0, low], first.at[1], send.at[5], recv.at[5], x_peer)
    core_sum(1)
    fly.send(core_in.at[1, top], first.at[2], send.at[6], recv.at[6], y_peer)
    core_sum(2)
    fly.send(core_in.at[2, low], first.at[3], send.at[7], recv.at[7], x_peer)
    core_sum(3)
    landed(first.at[0], recv.at[4], y_peer)
    row_add(second.at[0], first.at[0], core_in.at[2, top], size)
    fly.send(second.at[0], second.at[2], send.at[8], recv.at[8], x_peer)
    landed(first.at[1], recv.at[5], x_peer)
    row_add(second.at[1], first.at[1], core_in.at[1, low], size)
    fly.send(second.at[1], second.at[3], send.at[9], recv.at[9], y_peer)
    landed(first.at[2], recv.at[6], y_peer)
    row_add(keep.at[top], first.at[2], core_in.at[3, top], size)
    landed(first.at[3], recv.at[7], x_peer)
    row_add(keep.at[low], first.at[3], core_in.at[3, low], size)
    landed(second.at[2], recv.at[8], x_peer)
    row_add(out_ref.at[top], keep.at[top], second.at[2], size)
    landed(second.at[3], recv.at[9], y_peer)
    row_add(out_ref.at[low], keep.at[low], second.at[3], size)
    fly.drain()


def plane_sum(partial):
    rows, width = partial.shape[0] // 8, partial.shape[1]
    dma = pltpu.SemaphoreType.DMA
    return pl.pallas_call(
        plane_sum_kernel,
        out_shape=jax.ShapeDtypeStruct((rows, width), F32),
        in_specs=[VM],
        out_specs=VM,
        scratch_shapes=[
            pltpu.VMEM((4, rows, width), BF),
            pltpu.VMEM((4, rows // 2, width), BF),
            pltpu.VMEM((4, rows // 2, width), BF),
            pltpu.VMEM((rows, width), F32),
            dma((10,)),
            dma((10,)),
        ],
        compiler_params=pltpu.CompilerParams(collective_id=2, has_side_effects=True),
        name="plane_sum",
    )(partial.reshape(2, 2, 2, rows, width))


AHEAD, LAG_PLANE, LAG_CHAIN = 6, 2, 4


def reduce_kernel(outer, kinds, *refs):
    count = len(kinds)
    shards = outer * PLANE
    gs, refs = refs[:count], refs[count:]
    frames_ref, small_ref, refs = refs[0], refs[1], refs[2:]
    outs, refs = refs[:count], refs[count:]
    frames_out, small_out, refs = refs[0], refs[1], refs[2:]
    near, refs = refs[:count], refs[count:]
    plane, refs = refs[:count], refs[count:]
    chain, refs = refs[:count], refs[count:]
    split = [i for i, kind in enumerate(kinds) if kind[1]]
    whole, refs = refs[: len(split)], refs[len(split) :]
    small_in, small_own, small_peer, refs = refs[0], refs[1], refs[2], refs[3:]
    e_s, e_r, e_l, s1, r1, s2, r2, zs, zr, o_s, o_r, f_s, f_r, m_s, m_r, l_s = refs
    z, y, x = (lax.axis_index(name) for name in FS)
    core = lax.axis_index("sp")
    here = (z * 2 + y) * 2 + x
    core_peer = {"sp": 1 - core}
    above, below = {"za": z + 1}, {"za": z - 1}
    fly = Flights()

    def chip(index):
        return {"za": index // 4, "yb": (index // 2) % 2, "xc": index % 2}

    others = [(here + j) % shards for j in range(1, shards)]
    greet((core_peer, *[chip(index) for index in others]))

    part = outer // 2
    source = list(gs)
    for j, i in enumerate(split):
        width = whole[j].shape[-1]
        mine = pl.ds(pl.multiple_of(core * width, width), width)
        theirs = pl.ds(pl.multiple_of((1 - core) * width, width), width)
        ours = pl.ds(core * part, part)
        fly.send(gs[i].at[:, :, :, :, theirs], whole[j].at[ours], e_s.at[j], e_r.at[j], core_peer)
        fly.local(gs[i].at[:, :, :, :, mine], whole[j].at[ours], e_l.at[j])
        source[i] = whole[j]

    def joined(i):
        j = split.index(i)
        width = whole[j].shape[-1]
        mine = pl.ds(pl.multiple_of(core * width, width), width)
        ours, other = pl.ds(core * part, part), pl.ds((1 - core) * part, part)
        pltpu.make_async_copy(gs[i].at[:, :, :, :, mine], whole[j].at[ours], e_l.at[j]).wait()
        landed(whole[j].at[other], e_r.at[j], core_peer)

    frame_copy = fly.local(frames_ref, frames_out.at[here], l_s.at[0])
    small_copy = fly.local(small_ref.at[here], small_in.at[here], l_s.at[1])
    for j, index in enumerate(others):
        fly.send(frames_ref, frames_out.at[here], f_s.at[j], f_r.at[here], chip(index))
        fly.send(small_ref.at[index], small_in.at[here], m_s.at[j], m_r.at[here], chip(index))

    def slot_at(step):
        if step == outer - 1:
            return z
        falling = outer - 1 - step
        falling = jnp.where(falling > z, falling, falling - 1)
        rising = jnp.where(step < z, step, step + 1)
        return jnp.where(z < part, falling, rising)

    units = [(slot_at(step), i) for step in range(outer) for i in range(count)]

    def turns(i, slot):
        turn = (slot + i) % 2
        first = ((y + 1 - turn) % 2, (x + turn) % 2)
        second = ((y + turn) % 2, (x + 1 - turn) % 2)
        return first, second

    def device(place):
        return {"yb": place[0], "xc": place[1]}

    def start(slot, i):
        first, _ = turns(i, slot)
        fly.send(
            source[i].at[slot, 1 - y, 1 - x], near[i].at[slot, 1], s1.at[i, slot, 1], r1.at[i, slot, 1], device(first)
        )
        fly.send(
            source[i].at[slot, first[0], first[1]], near[i].at[slot, 0], s1.at[i, slot, 0], r1.at[i, slot, 0], device(first)
        )

    def pass_on(slot, i):
        first, second = turns(i, slot)
        rows = near[i].shape[2]
        landed(near[i].at[slot, 1], r1.at[i, slot, 1], device(first))
        row_add(near[i].at[slot, 1], near[i].at[slot, 1], source[i].at[slot, second[0], second[1]], rows)
        fly.send(near[i].at[slot, 1], plane[i].at[slot], s2.at[i, slot], r2.at[i, slot], device(second))
        landed(near[i].at[slot, 0], r1.at[i, slot, 0], device(first))
        row_add(near[i].at[slot, 0], near[i].at[slot, 0], source[i].at[slot, y, x], rows)

    def plane_total(slot, i):
        _, second = turns(i, slot)
        rows = near[i].shape[2]
        landed(plane[i].at[slot], r2.at[i, slot], device(second))
        row_add(plane[i].at[slot], plane[i].at[slot], near[i].at[slot, 0], rows)

    def along(slot, i, last):
        rows = near[i].shape[2]
        if not last:
            for way, when, edge, ahead, behind in (
                (1, slot < z, z == outer - 1, below, above),
                (0, slot > z, z == 0, above, below),
            ):

                @pl.when(jnp.logical_and(when, jnp.logical_not(edge)))
                def _():
                    landed(chain[i].at[way, slot], zr.at[i, way, slot], behind)
                    row_add(plane[i].at[slot], plane[i].at[slot], chain[i].at[way, slot], rows)

                fly.send(
                    plane[i].at[slot], chain[i].at[way, slot], zs.at[i, way, slot], zr.at[i, way, slot], ahead, when
                )
            return
        parts = kinds[i][0]
        width = plane[i].shape[-1] // parts
        for way, when, behind in ((1, z < outer - 1, above), (0, z > 0, below)):

            @pl.when(when)
            def _():
                landed(chain[i].at[way, slot], zr.at[i, way, slot], behind)

        step = 16 if rows % 16 == 0 else rows
        has_above, has_below = z < outer - 1, z > 0

        def chunk(index, carry):
            at = pl.ds(pl.multiple_of(index * step, step), step)
            for part_no in range(parts):
                span = slice(part_no * width, (part_no + 1) * width)
                total = plane[i][slot, at, span].astype(F32)
                upper = chain[i][1, slot, at, span].astype(F32)
                lower = chain[i][0, slot, at, span].astype(F32)
                total = total + jnp.where(has_above, upper, 0.0) + jnp.where(has_below, lower, 0.0)
                column = pl.multiple_of((2 * part_no + core) * width, width)
                outs[i][at, pl.ds(column, width)] = total
            return carry

        lax.fori_loop(0, rows // step, chunk, 0)
        for part_no in range(parts):
            column = pl.multiple_of((2 * part_no + core) * width, width)
            block = outs[i].at[:, pl.ds(column, width)]
            fly.send(block, block, o_s.at[i, part_no], o_r.at[i, part_no], core_peer)

    waiting = set(split)

    def begin(unit):
        slot, i = units[unit]
        if i in waiting:
            joined(i)
            waiting.discard(i)
        start(slot, i)

    for unit in range(min(AHEAD, len(units))):
        begin(unit)
    for tick in range(len(units) + LAG_CHAIN):
        if tick < len(units):
            pass_on(*units[tick])
            if tick + AHEAD < len(units):
                begin(tick + AHEAD)
        if 0 <= tick - LAG_PLANE < len(units):
            plane_total(*units[tick - LAG_PLANE])
        if 0 <= tick - LAG_CHAIN < len(units):
            unit = tick - LAG_CHAIN
            along(*units[unit], unit >= (outer - 1) * count)

    small_copy.wait()
    frame_copy.wait()
    for index in others:
        landed(small_in.at[index], m_r.at[index], chip(index))
    small_own[...] = jnp.sum(small_in[...], axis=0)
    fly.send(small_own, small_peer, l_s.at[2], l_s.at[3], core_peer)
    for index in others:
        landed(frames_out.at[index], f_r.at[index], chip(index))
    landed(small_peer, l_s.at[3], core_peer)
    small_out[...] = small_own[...] + small_peer[...]
    for i in range(count):
        parts = kinds[i][0]
        width = plane[i].shape[-1] // parts
        for part_no in range(parts):
            column = pl.multiple_of((2 * part_no + 1 - core) * width, width)
            landed(outs[i].at[:, pl.ds(column, width)], o_r.at[i, part_no], core_peer)
    fly.drain()


def reduce_weights(outer, kinds, grads, frames, small):
    shards = outer * PLANE
    count = len(kinds)
    shaped, shapes, near, plane, chain, whole = [], [], [], [], [], []
    for (parts, split), grad in zip(kinds, grads, strict=True):
        lead = outer // 2 if split else outer
        rows = grad.shape[0] // (lead * PLANE)
        width = grad.shape[1] // 2 if split else grad.shape[1]
        shaped.append(grad.reshape(lead, 2, 2, rows, grad.shape[1]))
        shapes.append(jax.ShapeDtypeStruct((rows, 2 * width), F32))
        near.append(pltpu.VMEM((outer, 2, rows, width), BF))
        plane.append(pltpu.VMEM((outer, rows, width), BF))
        chain.append(pltpu.VMEM((2, outer, rows, width), BF))
        if split:
            whole.append(pltpu.VMEM((outer, 2, 2, rows, width), BF))
    shapes.append(jax.ShapeDtypeStruct((shards, *frames.shape), frames.dtype))
    shapes.append(jax.ShapeDtypeStruct(small.shape[1:], F32))
    dma = pltpu.SemaphoreType.DMA
    nsplit = len(whole)
    results = pl.pallas_call(
        functools.partial(reduce_kernel, outer, kinds),
        out_shape=shapes,
        in_specs=[VM] * (count + 2),
        out_specs=[VM] * count + [VM, VM],
        scratch_shapes=[
            *near,
            *plane,
            *chain,
            *whole,
            pltpu.VMEM(small.shape, F32),
            pltpu.VMEM(small.shape[1:], F32),
            pltpu.VMEM(small.shape[1:], F32),
            dma((nsplit,)),
            dma((nsplit,)),
            dma((nsplit,)),
            dma((count, outer, 2)),
            dma((count, outer, 2)),
            dma((count, outer)),
            dma((count, outer)),
            dma((count, 2, outer)),
            dma((count, 2, outer)),
            dma((count, 3)),
            dma((count, 3)),
            dma((shards,)),
            dma((shards,)),
            dma((shards,)),
            dma((shards,)),
            dma((4,)),
        ],
        compiler_params=pltpu.CompilerParams(
            collective_id=3, has_side_effects=True, vmem_limit_bytes=67043328
        ),
        name="reduce_weights",
    )(*shaped, frames, small)
    return results[:count], results[count], results[count + 1]


def gather(value, axes, axis=0):
    return lax.all_gather(value, axes, axis=axis, tiled=True)


def scatter(value, axes, axis=0):
    return lax.psum_scatter(value, axes, scatter_dimension=axis, tiled=True)


def swap(value, split_axis, concat_axis):
    return lax.all_to_all(value, "sp", split_axis=split_axis, concat_axis=concat_axis, tiled=True)


def rms_scale(total):
    return lax.rsqrt(total / D + EPSILON)


def square_sum(values):
    return jnp.sum(values * values, axis=1)


def rms_back(values, inverse, gain, grad):
    scaled = grad * gain
    return scaled, jnp.sum(scaled * values, axis=1)


def rms_finish(values, inverse, scaled, total):
    column = inverse[:, None]
    return scaled * column - values * (column * column * column) * (total / D)[:, None]


def body(
    tokens,
    text,
    clip_frames,
    timestep,
    mod_weight,
    mod_bias,
    qk_gains,
    self_in,
    self_out,
    cross_q,
    cross_kv,
    cross_out,
    mlp_in,
    mlp_out,
    cotangent,
):
    half = D // 2
    row_count = tokens.shape[0]
    frame_count = row_count // FRAME_TOK
    group_frames = timestep.shape[1]
    shards = D // self_in.shape[1]
    outer = shards // PLANE
    core = lax.axis_index("sp")
    chip = lax.axis_index(FS)
    own_frame = core * frame_count

    bias_len, gain_len = mod_bias.shape[1], qk_gains.shape[2]
    small_len = bias_len + 4 * gain_len
    small_rows = 8
    small_width = -(-(small_len + group_frames) // (small_rows * 128)) * 128
    small_room = small_rows * small_width

    def own_half(weight, parts):
        shaped = weight[0].reshape(weight.shape[1], parts, 2, -1)
        return lax.dynamic_index_in_dim(shaped, core, 2, keepdims=False).reshape(
            weight.shape[1], -1
        )

    small = jnp.concatenate(
        [
            mod_bias[0].astype(F32),
            qk_gains[0].reshape(-1).astype(F32),
            timestep[0].astype(F32),
            jnp.zeros((small_room - small_len - group_frames,), F32),
        ]
    ).reshape(small_rows, small_width)
    hid = mlp_out.shape[1] // 2
    in_rows = mlp_in.shape[1]
    up_part = lax.dynamic_index_in_dim(
        mlp_in[0].reshape(in_rows, outer, PLANE, 2, hid), core, 3, keepdims=False
    )
    up_part = up_part.transpose(2, 0, 1, 3).reshape(PLANE, in_rows, outer * hid)
    down_part = lax.dynamic_slice_in_dim(mlp_out[0], core * hid, hid, 0)
    gathered, raw = gather_weights(
        outer,
        [
            small,
            own_half(mod_weight, 1),
            own_half(self_in, 3),
            own_half(self_out, 1),
            own_half(cross_kv, 2),
            own_half(cross_q, 1),
            own_half(cross_out, 1),
        ],
        (3, 6),
        up_part,
        down_part,
    )
    small_all, mod_matrix, self_proj, self_back, cross_kvproj, cross_qproj, cross_back = gathered[:7]
    up_matrix, down_matrix = gathered[7:]
    small_all = small_all.reshape(shards, small_room)
    bias_all = small_all[:, :bias_len].reshape(-1)
    gain_all = (
        small_all[:, bias_len:small_len]
        .reshape(shards, 4, gain_len)
        .transpose(1, 0, 2)
        .reshape(4, 2, half)
    )
    gain_own = lax.dynamic_index_in_dim(gain_all, core, 1, keepdims=False)
    steps_all = small_all[:, small_len : small_len + group_frames].reshape(-1)

    live_keys = clip_frames * FRAME_TOK
    all_keys = jnp.full((1,), TXT, jnp.int32)
    own_steps = lax.dynamic_slice_in_dim(timestep[0], own_frame, frame_count)
    clip_pos = jnp.arange(group_frames, dtype=jnp.int32)
    cosine, sine = rotary_tables(
        jnp.repeat(clip_pos, FRAME_TOK),
        jnp.tile(jnp.arange(FRAME_TOK, dtype=jnp.int32), group_frames),
    )
    sinus = sinus_features(timestep[0]).astype(BF)

    mod_half = product(sinus, mod_matrix)
    mod_half = mod_half + lax.dynamic_slice_in_dim(bias_all, core * 3 * D, 3 * D)[None]
    modulation = swap(mod_half, 0, 1)
    shift_one, scale_one, gate_one, shift_two, scale_two, gate_two = jnp.split(
        modulation, 6, axis=1
    )

    text_all = gather(text, "sp")

    residual = tokens.astype(F32)
    attn_float, back_attn_input = jax.vjp(modulated, residual, shift_one, scale_one)
    attn_input = gather(attn_float.astype(BF), "sp")
    joined = product(attn_input, self_proj)
    raw_q, raw_k, raw_v = joined[:, :half], joined[:, half : 2 * half], joined[:, 2 * half :]
    totals = lax.psum(jnp.stack([square_sum(raw_q), square_sum(raw_k)]), "sp")
    inv_q, inv_k = rms_scale(totals[0]), rms_scale(totals[1])
    query = rotate(raw_q * inv_q[:, None] * gain_own[0], cosine, sine).astype(BF)
    key = rotate(raw_k * inv_k[:, None] * gain_own[1], cosine, sine).astype(BF)
    value = raw_v.astype(BF)
    self_mixed, self_lse = attend_forward(live_keys, query, key, value)
    self_branch = scatter(product(self_mixed, self_back), "sp")
    residual = residual + frame_scaled(self_branch, gate_one)

    text_raw = product(text_all, cross_kvproj)
    raw_ck, raw_cv = text_raw[:, :half], text_raw[:, half:]
    inv_ck = rms_scale(lax.psum(square_sum(raw_ck)[None], "sp")[0])
    cross_key = (raw_ck * inv_ck[:, None] * gain_own[3]).astype(BF)
    cross_value = raw_cv.astype(BF)

    cross_float, back_cross_norm = jax.vjp(layer_norm, residual)
    cross_input = gather(cross_float.astype(BF), "sp")
    cross_raw = product(cross_input, cross_qproj)
    inv_cq = rms_scale(lax.psum(square_sum(cross_raw)[None], "sp")[0])
    cross_query = (cross_raw * inv_cq[:, None] * gain_own[2]).astype(BF)
    cross_mixed, cross_lse = attend_forward(all_keys, cross_query, cross_key, cross_value)
    residual = residual + scatter(product(cross_mixed, cross_back), "sp")

    mlp_float, back_mlp_input = jax.vjp(modulated, residual, shift_two, scale_two)
    mlp_input = plane_gather(mlp_float.astype(BF))
    up_proj = product(mlp_input, up_matrix)
    activated_float, back_gelu = jax.vjp(
        lambda inner: jax.nn.gelu(inner, approximate=True), up_proj
    )
    activated = activated_float.astype(BF)

    mlp_branch = plane_sum(product(activated, down_matrix).astype(BF))
    output = (residual + frame_scaled(mlp_branch, gate_two)).astype(BF)

    grad_rows = cotangent.astype(F32)
    grad_branch = frame_scaled(grad_rows, gate_two).astype(BF)
    grad_gate_two = frame_sum(grad_rows * mlp_branch, frame_count)
    grad_branch_all = plane_gather(grad_branch)
    grad_down = product_tn(activated, grad_branch_all).astype(BF)
    down_owned = scatter(grad_down, "za")
    grad_up_low = back_gelu(product_nt(grad_branch_all, down_matrix))[0].astype(BF)
    grad_up = product_tn(mlp_input, grad_up_low).astype(BF)
    up_owned = scatter(grad_up, "za")
    grad_mlp_input = plane_sum(product_nt(grad_up_low, up_matrix).astype(BF))
    grad_from_mlp, grad_shift_two, grad_scale_two = back_mlp_input(grad_mlp_input)
    grad_rows = grad_rows + grad_from_mlp

    grad_low = gather(grad_rows.astype(BF), "sp")
    grad_cross_back = product_tn(cross_mixed, grad_low).astype(BF)
    grad_cross_mixed = product_nt(grad_low, cross_back).astype(BF)
    grad_cq, grad_ck, grad_cv = attend_backward(
        all_keys, cross_query, cross_key, cross_value, cross_lse, grad_cross_mixed
    )
    grad_cq, grad_ck = grad_cq.astype(F32), grad_ck.astype(F32)
    grad_gain_two = jnp.sum(grad_cq * cross_raw * inv_cq[:, None], axis=0)
    grad_gain_three = jnp.sum(grad_ck * raw_ck * inv_ck[:, None], axis=0)
    scaled_cq, dots_cq = rms_back(cross_raw, inv_cq, gain_own[2], grad_cq)
    scaled_ck, dots_ck = rms_back(raw_ck, inv_ck, gain_own[3], grad_ck)
    dots_cq = lax.psum(dots_cq[None], "sp")[0]
    dots_ck = lax.psum(dots_ck[None], "sp")[0]
    grad_cross_low = rms_finish(cross_raw, inv_cq, scaled_cq, dots_cq).astype(BF)
    grad_text_low = jnp.concatenate(
        [rms_finish(raw_ck, inv_ck, scaled_ck, dots_ck).astype(BF), grad_cv], axis=1
    )
    grad_cross_qproj = product_tn(cross_input, grad_cross_low).astype(BF)
    grad_cross_kvproj = product_tn(text_all, grad_text_low).astype(BF)
    grad_cross_input = scatter(product_nt(grad_cross_low, cross_qproj), "sp")
    grad_rows = grad_rows + back_cross_norm(grad_cross_input)[0]

    grad_gate_one = frame_sum(grad_rows * self_branch, frame_count)
    grad_self_low = gather(frame_scaled(grad_rows, gate_one).astype(BF), "sp")
    grad_self_back = product_tn(self_mixed, grad_self_low).astype(BF)
    grad_self_mixed = product_nt(grad_self_low, self_back).astype(BF)
    grad_q, grad_k, grad_v = attend_backward(
        live_keys, query, key, value, self_lse, grad_self_mixed
    )
    grad_q = rotate(grad_q.astype(F32), cosine, -sine)
    grad_k = rotate(grad_k.astype(F32), cosine, -sine)
    grad_gain_zero = jnp.sum(grad_q * raw_q * inv_q[:, None], axis=0)
    grad_gain_one = jnp.sum(grad_k * raw_k * inv_k[:, None], axis=0)
    scaled_q, dots_q = rms_back(raw_q, inv_q, gain_own[0], grad_q)
    scaled_k, dots_k = rms_back(raw_k, inv_k, gain_own[1], grad_k)
    dots = lax.psum(jnp.stack([dots_q, dots_k]), "sp")
    grad_joined_low = jnp.concatenate(
        [
            rms_finish(raw_q, inv_q, scaled_q, dots[0]).astype(BF),
            rms_finish(raw_k, inv_k, scaled_k, dots[1]).astype(BF),
            grad_v,
        ],
        axis=1,
    )
    grad_self_proj = product_tn(attn_input, grad_joined_low).astype(BF)
    grad_attn_input = scatter(product_nt(grad_joined_low, self_proj), "sp")
    grad_from_attn, grad_shift_one, grad_scale_one = back_attn_input(grad_attn_input)
    grad_rows = grad_rows + grad_from_attn

    grad_modulation = jnp.concatenate(
        [grad_shift_one, grad_scale_one, grad_gate_one, grad_shift_two, grad_scale_two, grad_gate_two],
        axis=1,
    )
    grad_mod_half = swap(grad_modulation, 1, 0)
    grad_gains = jnp.stack([grad_gain_zero, grad_gain_one, grad_gain_two, grad_gain_three])
    both = jnp.arange(2)[None, :, None] == core
    grad_gains = jnp.where(both, grad_gains[:, None, :], 0.0).reshape(4, shards, gain_len)
    grad_small = jnp.concatenate(
        [
            jnp.sum(grad_modulation, axis=0).reshape(shards, bias_len),
            grad_gains.transpose(1, 0, 2).reshape(shards, 4 * gain_len),
            jnp.zeros((shards, small_room - small_len), F32),
        ],
        axis=1,
    ).reshape(shards, small_rows, small_width)
    owned, grad_mod_all, small_owned = reduce_weights(
        outer,
        ((1, False), (2, False), (1, True), (1, True), (3, False)),
        [grad_cross_qproj, grad_cross_kvproj, grad_cross_back, grad_self_back, grad_self_proj],
        grad_mod_half.astype(BF),
        grad_small,
    )
    cross_q_grad, cross_kv_grad, cross_out_grad, self_out_grad, self_in_grad = owned
    small_owned = small_owned.reshape(-1)[:small_len]
    sinus_all = sinus_features(steps_all).astype(BF)
    own_features = mod_weight.shape[1]
    sinus_own = lax.dynamic_slice_in_dim(sinus_all, chip * own_features, own_features, 1)
    grad_mod_all = grad_mod_all.reshape(-1, grad_mod_half.shape[1])
    mod_weight_grad = gather(product_tn(sinus_own, grad_mod_all), "sp", 1)

    up_owned, down_owned, small_owned = lax.optimization_barrier((up_owned, down_owned, small_owned))
    up_rows = lax.all_to_all(up_owned, PL, split_axis=0, concat_axis=0, tiled=True)
    up_pair = gather(up_rows.reshape(1, PLANE, in_rows, outer, hid), "sp").astype(F32)
    mlp_in_grad = up_pair.transpose(2, 3, 1, 0, 4).reshape(1, in_rows, -1)
    return (
        output,
        grad_rows,
        mod_weight_grad[None],
        small_owned[None, :bias_len],
        small_owned[bias_len:].reshape(1, 4, gain_len),
        self_in_grad[None],
        self_out_grad[None],
        cross_q_grad[None],
        cross_kv_grad[None],
        cross_out_grad[None],
        mlp_in_grad,
        gather(down_owned, "sp").astype(F32)[None],
    )


def solution(mesh):
    chips, cores = mesh.shape["fsdp"], mesh.shape["sp"]
    grid = mesh.devices.reshape(chips // PLANE, 2, PLANE // 2, cores)
    inner = Mesh(grid, ALL)
    rows, second = P(ALL, None), P(None, FS, None)
    in_specs = (
        rows,
        rows,
        P(FS),
        P(FS, None),
        second,
        P(None, FS),
        P(None, None, FS),
        *([second] * 7),
        rows,
    )
    out_specs = (rows, rows, second, P(None, FS), P(None, None, FS), *([second] * 7))
    return jax.shard_map(body, mesh=inner, in_specs=in_specs, out_specs=out_specs, check_vma=False)
```

```python
import functools
import math

import jax
import jax.numpy as jnp
from jax import lax
from jax.experimental import pallas as pl
from jax.experimental.pallas import tpu as pltpu
from jax.sharding import Mesh
from jax.sharding import PartitionSpec as P

D = 1536
HD = 128
TXT = 512
FREQ = 256
WP = 8
FRAME_TOK = 64
PLANE = 4

EPSILON = 1e-06
NEGATIVE = -1e30

FS = ("za", "yb", "xc")
PL = ("yb", "xc")
ALL = ("za", "yb", "xc", "sp")
SCALE = 1.0 / math.sqrt(HD)
MESH = pl.DeviceIdType.MESH
BF = jnp.bfloat16
F32 = jnp.float32


def product(left, right):
    return jnp.dot(left, right, preferred_element_type=F32)


def product_tn(left, right):
    return lax.dot_general(left, right, (((0,), (0,)), ((), ())), preferred_element_type=F32)


def product_nt(left, right):
    return lax.dot_general(left, right, (((1,), (1,)), ((), ())), preferred_element_type=F32)


def layer_norm(values):
    centred = values - jnp.mean(values, axis=-1, keepdims=True)
    return centred * lax.rsqrt(jnp.mean(centred * centred, axis=-1, keepdims=True) + EPSILON)


def sinus_features(steps):
    half_dim = FREQ // 2
    rates = jnp.exp(jnp.arange(half_dim).astype(F32) * (-math.log(10000.0) / half_dim))
    angles = steps.astype(F32)[:, None] * rates[None, :]
    return jnp.concatenate([jnp.cos(angles), jnp.sin(angles)], axis=1)


def rotary_tables(frame_pos, token_spot):
    half_dim = HD // 2
    side_pairs = HD // 6
    lead_pairs = half_dim - 2 * side_pairs
    pair_index = jnp.arange(half_dim)
    log_base = -math.log(10000.0)
    lead_part = pair_index < lead_pairs
    side_part = jnp.logical_and(pair_index >= lead_pairs, pair_index < lead_pairs + side_pairs)
    last_part = pair_index >= lead_pairs + side_pairs
    frame_rate = jnp.where(
        lead_part, jnp.exp(log_base * pair_index.astype(F32) / lead_pairs), 0.0
    )
    row_rate = jnp.where(
        side_part, jnp.exp(log_base * (pair_index - lead_pairs).astype(F32) / side_pairs), 0.0
    )
    column_rate = jnp.where(
        last_part,
        jnp.exp(log_base * (pair_index - lead_pairs - side_pairs).astype(F32) / side_pairs),
        0.0,
    )
    patch_row = (token_spot // WP).astype(F32)
    patch_column = (token_spot % WP).astype(F32)
    angles = (
        frame_pos.astype(F32)[:, None] * frame_rate[None, :]
        + patch_row[:, None] * row_rate[None, :]
        + patch_column[:, None] * column_rate[None, :]
    )
    return (jnp.cos(angles), jnp.sin(angles))


def rotate(values, cosine, sine):
    row_count = values.shape[0]
    shaped = values.reshape(row_count, -1, HD)
    half_dim = HD // 2
    first_half = shaped[:, :, :half_dim]
    second_half = shaped[:, :, half_dim:]
    cos_rows = cosine[:, None, :]
    sin_rows = sine[:, None, :]
    turned = jnp.concatenate(
        [
            first_half * cos_rows - second_half * sin_rows,
            second_half * cos_rows + first_half * sin_rows,
        ],
        axis=2,
    )
    return turned.reshape(row_count, -1)


def modulated(residual, shift, scale):
    frames = shift.shape[0]
    normed = layer_norm(residual).reshape(frames, -1, residual.shape[1])
    return (normed * (1.0 + scale[:, None, :]) + shift[:, None, :]).reshape(residual.shape)


def frame_scaled(rows, gate):
    frames = gate.shape[0]
    return (rows.reshape(frames, -1, rows.shape[1]) * gate[:, None, :]).reshape(rows.shape)


def frame_sum(values, frames):
    return jnp.sum(values.reshape(frames, -1, values.shape[1]), axis=1)


def attend_forward_kernel(live_ref, q_ref, k_ref, v_ref, out_ref, lse_ref):
    rows, keys = q_ref.shape[0], k_ref.shape[0]
    spot = lax.broadcasted_iota(jnp.int32, (rows, keys), 1)
    allowed = spot < live_ref[0]
    for head in range(q_ref.shape[1] // HD):
        part = slice(head * HD, (head + 1) * HD)
        scores = jnp.where(allowed, product_nt(q_ref[:, part], k_ref[:, part]) * SCALE, NEGATIVE)
        row_max = jnp.max(scores, axis=1, keepdims=True)
        log_total = row_max + jnp.log(jnp.sum(jnp.exp(scores - row_max), axis=1, keepdims=True))
        weights = jnp.exp(scores - log_total).astype(BF)
        out_ref[:, part] = product(weights, v_ref[:, part]).astype(BF)
        lse_ref[:, part] = jnp.broadcast_to(log_total, (rows, HD))


def attend_backward_kernel(
    live_ref, q_ref, k_ref, v_ref, lse_ref, do_ref, dq_ref, dk_ref, dv_ref
):
    rows, keys = q_ref.shape[0], k_ref.shape[0]
    spot = lax.broadcasted_iota(jnp.int32, (rows, keys), 1)
    allowed = spot < live_ref[0]
    for head in range(q_ref.shape[1] // HD):
        part = slice(head * HD, (head + 1) * HD)
        query, key, value, grad = q_ref[:, part], k_ref[:, part], v_ref[:, part], do_ref[:, part]
        scores = jnp.where(allowed, product_nt(query, key) * SCALE, NEGATIVE)
        weights = jnp.exp(scores - lse_ref[:, head * HD : head * HD + 1])
        grad_weights = product_nt(grad, value)
        delta = jnp.sum(weights * grad_weights, axis=1, keepdims=True)
        grad_scores = (weights * (grad_weights - delta)).astype(BF)
        dq_ref[:, part] = (product(grad_scores, key) * SCALE).astype(BF)
        dk_ref[:, part] = (product_tn(grad_scores, query) * SCALE).astype(BF)
        dv_ref[:, part] = product_tn(weights.astype(BF), grad).astype(BF)


VM = pl.BlockSpec(memory_space=pltpu.VMEM)
SM = pl.BlockSpec(memory_space=pltpu.SMEM)
ANY = pl.BlockSpec(memory_space=pl.ANY)


def attend_forward(live, query, key, value):
    rows, width = query.shape
    keys = key.shape[0]
    heads = width // HD
    return pl.pallas_call(
        attend_forward_kernel,
        out_shape=(
            jax.ShapeDtypeStruct((rows, width), BF),
            jax.ShapeDtypeStruct((rows, width), F32),
        ),
        in_specs=[SM, VM, VM, VM],
        out_specs=(VM, VM),
        cost_estimate=pl.CostEstimate(
            flops=4 * rows * keys * width,
            bytes_accessed=8 * rows * width + 4 * keys * width,
            transcendentals=2 * rows * keys * heads,
        ),
    )(live, query, key, value)


def attend_backward(live, query, key, value, lse, grad):
    rows, width = query.shape
    keys = key.shape[0]
    heads = width // HD
    return pl.pallas_call(
        attend_backward_kernel,
        out_shape=(
            jax.ShapeDtypeStruct((rows, width), BF),
            jax.ShapeDtypeStruct((keys, width), BF),
            jax.ShapeDtypeStruct((keys, width), BF),
        ),
        in_specs=[SM, VM, VM, VM, VM, VM],
        out_specs=(VM, VM, VM),
        cost_estimate=pl.CostEstimate(
            flops=10 * rows * keys * width,
            bytes_accessed=10 * rows * width + 8 * keys * width,
            transcendentals=rows * keys * heads,
        ),
    )(live, query, key, value, lse, grad)


def row_add(target, left, right, rows):
    step = 32 if rows % 32 == 0 else rows

    def chunk(index, carry):
        at = pl.ds(pl.multiple_of(index * step, step), step)
        target[at, :] = left[at, :] + right[at, :]
        return carry

    lax.fori_loop(0, rows // step, chunk, 0)


def row_sum(target, left, right, rows):
    step = 16 if rows % 16 == 0 else rows

    def chunk(index, carry):
        at = pl.ds(pl.multiple_of(index * step, step), step)
        target[at, :] = left[at, :].astype(F32) + right[at, :].astype(F32)
        return carry

    lax.fori_loop(0, rows // step, chunk, 0)


class Flights:
    def __init__(self):
        self.sent = []

    def send(self, source, target, send_sem, recv_sem, device, when=None):
        copy = pltpu.make_async_remote_copy(
            src_ref=source,
            dst_ref=target,
            send_sem=send_sem,
            recv_sem=recv_sem,
            device_id=device,
            device_id_type=MESH,
        )
        if when is None:
            copy.start()
        else:
            pl.when(when)(copy.start)
        self.sent.append((when, copy))

    def local(self, source, target, sem):
        copy = pltpu.make_async_copy(source, target, sem)
        copy.start()
        return copy

    def drain(self):
        for when, copy in self.sent:
            if when is None:
                copy.wait_send()
            else:
                pl.when(when)(copy.wait_send)


def landed(target, sem, device):
    pltpu.make_async_remote_copy(
        src_ref=target,
        dst_ref=target,
        send_sem=sem,
        recv_sem=sem,
        device_id=device,
        device_id_type=MESH,
    ).wait_recv()


def greet(devices, optional=()):
    barrier = pltpu.get_barrier_semaphore()
    for device in devices:
        pl.semaphore_signal(barrier, inc=1, device_id=device, device_id_type=MESH)
    for when, device in optional:

        @pl.when(when)
        def _(device=device):
            pl.semaphore_signal(barrier, inc=1, device_id=device, device_id_type=MESH)

    count = len(devices)
    for when, _ in optional:
        count = count + when.astype(jnp.int32)
    pl.semaphore_wait(barrier, count)


def gather_kernel(outer, kinds, *refs):
    full = len(kinds)
    ins, refs = refs[:full], refs[full:]
    mlp_ref, text_ref, refs = refs[0], refs[1], refs[2:]
    outs, refs = list(refs[:full]), refs[full:]
    up_out, text_out, refs = refs[0], refs[1], refs[2:]
    own, refs = refs[:full], refs[full:]
    halves = [i for i, kind in enumerate(kinds) if kind[1]]
    whole, refs = refs[: len(halves)], refs[len(halves) :]
    up_own, local_sem, zs, zr, s1, r1, s2, r2, a_s, a_r, f_s, f_r, f_l, t_s = refs
    z, y, x = (lax.axis_index(name) for name in FS)
    core = lax.axis_index("sp")
    here = 2 * y + x
    up = full
    fins = {}
    for j, i in enumerate(halves):
        fins[i] = outs[i]
        outs[i] = whole[j]
    fly = Flights()
    x_peer, y_peer = {"xc": 1 - x}, {"yb": 1 - y}
    diagonal = {"yb": 1 - y, "xc": 1 - x}
    around = ((x_peer, y, 1 - x), (y_peer, 1 - y, x), (diagonal, 1 - y, 1 - x))
    above, below = {"za": z + 1}, {"za": z - 1}
    core_peer = {"sp": 1 - core}
    has_above, has_below = z + 1 < outer, z >= 1
    greet((x_peer, y_peer, diagonal, core_peer), ((has_above, above), (has_below, below)))

    for i, (parts, _) in enumerate(kinds):
        if parts == 0:
            own[i][...] = ins[i][...]
        for part in range(parts):
            width = ins[i].shape[1] // (2 * parts)
            column = pl.multiple_of((2 * part + core) * width, width)
            own[i][:, part * width : (part + 1) * width] = ins[i][:, pl.ds(column, width)]

    def shard(i, slot):
        return outs[i].at[slot, y, x] if i < full else up_out.at[slot]

    def z_send(i, way, hop, source=None):
        if hop > outer - 2:
            return
        slot = z - hop if way == 0 else z + hop
        when = jnp.logical_and(has_above, slot >= 0) if way == 0 else jnp.logical_and(has_below, slot < outer)
        fly.send(
            shard(i, slot) if source is None else source,
            shard(i, slot),
            zs.at[i, way, hop],
            zr.at[i, way, hop],
            above if way == 0 else below,
            when,
        )

    def z_slot(way, hop):
        slot = z - 1 - hop if way == 0 else z + 1 + hop
        return slot, (slot >= 0 if way == 0 else slot < outer)

    def z_wait(i, way, hop):
        slot, when = z_slot(way, hop)

        @pl.when(when)
        def _():
            landed(shard(i, slot), zr.at[i, way, hop], below if way == 0 else above)

    def turns(i, slot):
        turn = (slot + i) % 2
        first = ((y + turn) % 2, (x + 1 - turn) % 2)
        second = ((y + 1 - turn) % 2, (x + turn) % 2)
        return first, second

    def xy_own(i, slot, when=None, source=None):
        first, second = turns(i, slot)
        mine = outs[i].at[slot, y, x]
        source = mine if source is None else source
        fly.send(source, mine, s1.at[i, slot], r1.at[i, slot], {"yb": first[0], "xc": first[1]}, when)
        fly.send(source, mine, s2.at[i, slot, 0], r2.at[i, slot, 0], {"yb": second[0], "xc": second[1]}, when)

    def xy_pass(i, slot, when=None):
        first, second = turns(i, slot)
        theirs = outs[i].at[slot, first[0], first[1]]

        def wait():
            landed(theirs, r1.at[i, slot], {"yb": first[0], "xc": first[1]})

        if when is None:
            wait()
        else:
            pl.when(when)(wait)
        fly.send(theirs, theirs, s2.at[i, slot, 1], r2.at[i, slot, 1], {"yb": second[0], "xc": second[1]}, when)

    def xy_end(i, slot):
        _, second = turns(i, slot)
        device = {"yb": second[0], "xc": second[1]}
        landed(outs[i].at[slot, second[0], second[1]], r2.at[i, slot, 0], device)
        landed(outs[i].at[slot, 1 - y, 1 - x], r2.at[i, slot, 1], device)

    for i in range(full):
        for way in range(2):
            z_send(i, way, 0, own[i])
        xy_own(i, z, None, own[i])
    locals_ = [fly.local(own[i], outs[i].at[z, y, x], local_sem.at[i]) for i in range(full)]

    fly.send(text_ref, text_out.at[core], t_s.at[0], t_s.at[1], core_peer)
    locals_.append(fly.local(text_ref, text_out.at[core], t_s.at[2]))
    hid = mlp_ref.shape[1] // (outer * PLANE * 2)
    for own_core in range(2):

        @pl.when(core == own_core)
        def _(own_core=own_core):
            for place in range(PLANE):
                for slot in range(outer):
                    column = ((slot * PLANE + place) * 2 + own_core) * hid
                    up_own[place, :, slot * hid : (slot + 1) * hid] = mlp_ref[:, column : column + hid]

    for hop in range(outer - 1):
        for i in range(full):
            for way in range(2):
                slot, when = z_slot(way, hop)
                z_wait(i, way, hop)
                z_send(i, way, hop + 1)
                xy_own(i, slot, when)
        if hop == 0:
            locals_.append(fly.local(up_own.at[here], up_out.at[z, here], local_sem.at[up]))
            for turn, (device, ty, tx) in enumerate(around):
                fly.send(up_own.at[2 * ty + tx], up_out.at[z, here], a_s.at[turn], a_r.at[turn], device)
    for copy in locals_:
        copy.wait()
    for turn, (device, ty, tx) in enumerate(around):
        landed(up_out.at[z, 2 * ty + tx], a_r.at[turn], device)
    for way in range(2):
        z_send(up, way, 0)
    for i in range(full):
        xy_pass(i, z)
    for hop in range(outer - 1):
        for i in range(full):
            for way in range(2):
                slot, when = z_slot(way, hop)
                xy_pass(i, slot, when)
        for way in range(2):
            z_wait(up, way, hop)
            z_send(up, way, hop + 1)
    for i in (*halves, *(i for i in range(full) if i not in halves)):
        for slot in range(outer):
            xy_end(i, slot)
        if i not in halves:
            continue
        j, part = halves.index(i), outer // 2
        width = own[i].shape[-1]
        columns = pl.ds(pl.multiple_of(core * width, width), width)
        theirs, ours = pl.ds((1 - core) * part, part), pl.ds(core * part, part)
        fly.send(outs[i].at[theirs], fins[i].at[:, :, :, :, columns], f_s.at[j], f_r.at[j], core_peer)
        fly.local(outs[i].at[ours], fins[i].at[:, :, :, :, columns], f_l.at[j])
    for j, i in enumerate(halves):
        width = own[i].shape[-1]
        columns = pl.ds(pl.multiple_of(core * width, width), width)
        others = pl.ds(pl.multiple_of((1 - core) * width, width), width)
        ours = pl.ds(core * (outer // 2), outer // 2)
        pltpu.make_async_copy(outs[i].at[ours], fins[i].at[:, :, :, :, columns], f_l.at[j]).wait()
        landed(fins[i].at[:, :, :, :, others], f_r.at[j], core_peer)
    landed(text_out.at[1 - core], t_s.at[1], core_peer)
    fly.drain()


def gather_weights(outer, kinds, arrays, mlp, text):
    shapes, own, whole = [], [], []
    for (parts, keep), array in zip(kinds, arrays, strict=True):
        rows, width = array.shape
        half = width // 2 if parts else width
        own.append(pltpu.VMEM((rows, half), array.dtype))
        if keep:
            whole.append(pltpu.VMEM((outer, 2, 2, rows, half), array.dtype))
            shapes.append(jax.ShapeDtypeStruct((outer // 2, 2, 2, rows, width), array.dtype))
        else:
            shapes.append(jax.ShapeDtypeStruct((outer, 2, 2, rows, half), array.dtype))
    rows, units = mlp.shape
    mine = units // (2 * PLANE)
    shapes.append(jax.ShapeDtypeStruct((outer, PLANE, rows, mine), mlp.dtype))
    shapes.append(jax.ShapeDtypeStruct((2, *text.shape), text.dtype))
    dma = pltpu.SemaphoreType.DMA
    hops = outer - 1
    nf, nh = len(kinds), len(whole)
    results = pl.pallas_call(
        functools.partial(gather_kernel, outer, kinds),
        out_shape=shapes,
        in_specs=[VM] * (nf + 2),
        out_specs=[ANY] * len(shapes),
        scratch_shapes=[
            *own,
            *whole,
            pltpu.VMEM((PLANE, rows, mine), mlp.dtype),
            dma((nf + 1,)),
            dma((nf + 1, 2, hops)),
            dma((nf + 1, 2, hops)),
            dma((nf, outer)),
            dma((nf, outer)),
            dma((nf, outer, 2)),
            dma((nf, outer, 2)),
            dma((3,)),
            dma((3,)),
            dma((nh,)),
            dma((nh,)),
            dma((nh,)),
            dma((3,)),
        ],
        compiler_params=pltpu.CompilerParams(
            collective_id=0, has_side_effects=True, vmem_limit_bytes=40 * 1024 * 1024
        ),
        cost_estimate=pl.CostEstimate(flops=10**11, bytes_accessed=10**8, transcendentals=0),
        name="gather_weights",
    )(*arrays, mlp, text)
    return [value.reshape(-1, value.shape[-1]) for value in results]


def plane_gather_kernel(own_ref, out_ref, local_sem, send, recv):
    y, x, core = lax.axis_index("yb"), lax.axis_index("xc"), lax.axis_index("sp")
    x_peer, y_peer, core_peer = {"xc": 1 - x}, {"yb": 1 - y}, {"sp": 1 - core}
    fly = Flights()
    greet((x_peer, y_peer, core_peer))
    size = own_ref.shape[0] // 2
    top, low = pl.ds(0, size), pl.ds(size, size)
    fly.send(own_ref.at[top], out_ref.at[0, 1, 0, top], send.at[0], recv.at[0], x_peer)
    fly.send(own_ref.at[low], out_ref.at[1, 0, 0, low], send.at[1], recv.at[1], y_peer)
    fly.send(own_ref.at[low], out_ref.at[0, 1, 0, low], send.at[2], recv.at[2], x_peer)
    fly.send(own_ref.at[top], out_ref.at[1, 0, 0, top], send.at[3], recv.at[3], y_peer)
    fly.send(own_ref, out_ref.at[0, 0, 1], send.at[4], recv.at[4], core_peer)
    local = fly.local(own_ref, out_ref.at[0, 0, 0], local_sem.at[0])
    across = []

    def arrive(index, dy, dx, rows, device, onward=None):
        block = out_ref.at[dy, dx, 0, rows]
        landed(block, recv.at[index], device)
        if onward is not None:
            to, number = onward
            fly.send(block, out_ref.at[1, 1, 0, rows], send.at[number], recv.at[number], to)
        fly.send(block, out_ref.at[dy, dx, 1, rows], send.at[index + 7], recv.at[index + 7], core_peer)
        across.append((index + 7, dy, dx, rows))

    arrive(0, 0, 1, top, x_peer, (y_peer, 5))
    arrive(1, 1, 0, low, y_peer, (x_peer, 6))
    arrive(2, 0, 1, low, x_peer)
    arrive(3, 1, 0, top, y_peer)
    arrive(5, 1, 1, top, y_peer)
    arrive(6, 1, 1, low, x_peer)
    landed(out_ref.at[0, 0, 1], recv.at[4], core_peer)
    for index, dy, dx, rows in across:
        landed(out_ref.at[dy, dx, 1, rows], recv.at[index], core_peer)
    local.wait()
    fly.drain()


def plane_gather(own):
    rows, width = own.shape
    dma = pltpu.SemaphoreType.DMA
    out = pl.pallas_call(
        plane_gather_kernel,
        out_shape=jax.ShapeDtypeStruct((2, 2, 2, rows, width), own.dtype),
        in_specs=[VM],
        out_specs=VM,
        scratch_shapes=[dma((1,)), dma((14,)), dma((14,))],
        compiler_params=pltpu.CompilerParams(collective_id=1, has_side_effects=True),
        cost_estimate=pl.CostEstimate(flops=10**10, bytes_accessed=10**7, transcendentals=0),
        name="plane_gather",
    )(own)
    return out.reshape(8 * rows, width)


def plane_sum_kernel(part_ref, out_ref, core_in, first, second, keep, send, recv):
    y, x, core = lax.axis_index("yb"), lax.axis_index("xc"), lax.axis_index("sp")
    x_peer, y_peer, core_peer = {"xc": 1 - x}, {"yb": 1 - y}, {"sp": 1 - core}
    fly = Flights()
    greet((x_peer, y_peer, core_peer))
    rows = part_ref.shape[3]
    size = rows // 2
    top, low = pl.ds(0, size), pl.ds(size, size)
    chips = ((1, 1), (1, 0), (0, 1), (0, 0))
    for index, (dy, dx) in enumerate(chips):
        fly.send(part_ref.at[dy, dx, 1], core_in.at[index], send.at[index], recv.at[index], core_peer)

    def core_sum(index):
        dy, dx = chips[index]
        landed(core_in.at[index], recv.at[index], core_peer)
        row_add(core_in.at[index], core_in.at[index], part_ref.at[dy, dx, 0], rows)

    core_sum(0)
    fly.send(core_in.at[0, top], first.at[0], send.at[4], recv.at[4], y_peer)
    fly.send(core_in.at[0, low], first.at[1], send.at[5], recv.at[5], x_peer)
    core_sum(1)
    fly.send(core_in.at[1, top], first.at[2], send.at[6], recv.at[6], y_peer)
    core_sum(2)
    fly.send(core_in.at[2, low], first.at[3], send.at[7], recv.at[7], x_peer)
    core_sum(3)
    landed(first.at[0], recv.at[4], y_peer)
    row_add(second.at[0], first.at[0], core_in.at[2, top], size)
    fly.send(second.at[0], second.at[2], send.at[8], recv.at[8], x_peer)
    landed(first.at[1], recv.at[5], x_peer)
    row_add(second.at[1], first.at[1], core_in.at[1, low], size)
    fly.send(second.at[1], second.at[3], send.at[9], recv.at[9], y_peer)
    landed(first.at[2], recv.at[6], y_peer)
    row_sum(keep.at[top], first.at[2], core_in.at[3, top], size)
    landed(first.at[3], recv.at[7], x_peer)
    row_sum(keep.at[low], first.at[3], core_in.at[3, low], size)
    landed(second.at[2], recv.at[8], x_peer)
    row_sum(out_ref.at[top], keep.at[top], second.at[2], size)
    landed(second.at[3], recv.at[9], y_peer)
    row_sum(out_ref.at[low], keep.at[low], second.at[3], size)
    fly.drain()


def plane_sum(partial):
    rows, width = partial.shape[0] // 8, partial.shape[1]
    dma = pltpu.SemaphoreType.DMA
    return pl.pallas_call(
        plane_sum_kernel,
        out_shape=jax.ShapeDtypeStruct((rows, width), F32),
        in_specs=[VM],
        out_specs=VM,
        scratch_shapes=[
            pltpu.VMEM((4, rows, width), BF),
            pltpu.VMEM((4, rows // 2, width), BF),
            pltpu.VMEM((4, rows // 2, width), BF),
            pltpu.VMEM((rows, width), F32),
            dma((10,)),
            dma((10,)),
        ],
        compiler_params=pltpu.CompilerParams(collective_id=2, has_side_effects=True),
        cost_estimate=pl.CostEstimate(flops=10**10, bytes_accessed=10**7, transcendentals=0),
        name="plane_sum",
    )(partial.reshape(2, 2, 2, rows, width))


def pair_sum_kernel(part_ref, out_ref, peer_in, send, recv):
    core = lax.axis_index("sp")
    core_peer = {"sp": 1 - core}
    fly = Flights()
    greet((core_peer,))
    size = part_ref.shape[1] // 2
    for index in range(2):
        rows = pl.ds(index * size, size)
        fly.send(part_ref.at[1 - core, rows], peer_in.at[rows], send.at[index], recv.at[index], core_peer)
    for index in range(2):
        rows = pl.ds(index * size, size)
        landed(peer_in.at[rows], recv.at[index], core_peer)
        row_sum(out_ref.at[rows], part_ref.at[core, rows], peer_in.at[rows], size)
    fly.drain()


def pair_sum(partial):
    rows, width = partial.shape[0] // 2, partial.shape[1]
    dma = pltpu.SemaphoreType.DMA
    return pl.pallas_call(
        pair_sum_kernel,
        out_shape=jax.ShapeDtypeStruct((rows, width), F32),
        in_specs=[VM],
        out_specs=VM,
        scratch_shapes=[pltpu.VMEM((rows, width), F32), dma((2,)), dma((2,))],
        compiler_params=pltpu.CompilerParams(collective_id=4, has_side_effects=True),
        cost_estimate=pl.CostEstimate(flops=10**9, bytes_accessed=10**7, transcendentals=0),
        name="pair_sum",
    )(partial.reshape(2, rows, width))


AHEAD, LAG_PLANE, LAG_CHAIN = 6, 2, 4


def reduce_kernel(outer, kinds, *refs):
    count = len(kinds)
    shards = outer * PLANE
    gs, refs = refs[:count], refs[count:]
    frames_ref, small_ref, up_ref, down_ref, refs = *refs[:4], refs[4:]
    outs, refs = refs[:count], refs[count:]
    frames_out, small_out, up_out, down_out, refs = *refs[:4], refs[4:]
    near, refs = refs[:count], refs[count:]
    plane, refs = refs[:count], refs[count:]
    chain, refs = refs[:count], refs[count:]
    split = [i for i, kind in enumerate(kinds) if kind[1]]
    whole, refs = refs[: len(split)], refs[len(split) :]
    small_in, small_own, small_peer, up_in, down_in, refs = *refs[:5], refs[5:]
    e_s, e_r, e_l, s1, r1, s2, r2, zs, zr, o_s, o_r, f_s, f_r, m_s, m_r, l_s, p_s, p_r = refs
    z, y, x = (lax.axis_index(name) for name in FS)
    core = lax.axis_index("sp")
    here = (z * 2 + y) * 2 + x
    core_peer = {"sp": 1 - core}
    above, below = {"za": z + 1}, {"za": z - 1}
    fly = Flights()

    def chip(index):
        return {"za": index // 4, "yb": (index // 2) % 2, "xc": index % 2}

    others = [(here + j) % shards for j in range(1, shards)]
    greet((core_peer, *[chip(index) for index in others]))

    part = outer // 2
    source = list(gs)
    for j, i in enumerate(split):
        width = whole[j].shape[-1]
        mine = pl.ds(pl.multiple_of(core * width, width), width)
        theirs = pl.ds(pl.multiple_of((1 - core) * width, width), width)
        ours = pl.ds(core * part, part)
        fly.send(gs[i].at[:, :, :, :, theirs], whole[j].at[ours], e_s.at[j], e_r.at[j], core_peer)
        fly.local(gs[i].at[:, :, :, :, mine], whole[j].at[ours], e_l.at[j])
        source[i] = whole[j]

    def joined(i):
        j = split.index(i)
        width = whole[j].shape[-1]
        mine = pl.ds(pl.multiple_of(core * width, width), width)
        ours, other = pl.ds(core * part, part), pl.ds((1 - core) * part, part)
        pltpu.make_async_copy(gs[i].at[:, :, :, :, mine], whole[j].at[ours], e_l.at[j]).wait()
        landed(whole[j].at[other], e_r.at[j], core_peer)

    frame_width = frames_ref.shape[1]
    frame_mine = pl.ds(pl.multiple_of(core * frame_width, frame_width), frame_width)
    frame_other = pl.ds(pl.multiple_of((1 - core) * frame_width, frame_width), frame_width)
    frame_copy = fly.local(frames_ref, frames_out.at[here, :, frame_mine], l_s.at[0])
    small_copy = fly.local(small_ref.at[here], small_in.at[here], l_s.at[1])
    for j, index in enumerate(others):
        fly.send(frames_ref, frames_out.at[here, :, frame_mine], f_s.at[j], f_r.at[here], chip(index))
        fly.send(small_ref.at[index], small_in.at[here], m_s.at[j], m_r.at[here], chip(index))

    near_by = ((y, 1 - x), (1 - y, x), (1 - y, 1 - x))
    up_copy = fly.local(up_ref.at[2 * y + x], up_in.at[core, 2 * y + x], p_s.at[0])
    for j, (ty, tx) in enumerate(near_by):
        fly.send(
            up_ref.at[2 * ty + tx],
            up_in.at[core, 2 * y + x],
            p_s.at[j + 1],
            p_r.at[j + 1],
            {"yb": ty, "xc": tx},
        )
    fly.send(down_ref, down_in, p_s.at[4], p_r.at[4], core_peer)

    def feed_forward_landed():
        up_copy.wait()
        for j, (ty, tx) in enumerate(near_by):
            landed(up_in.at[core, 2 * ty + tx], p_r.at[j + 1], {"yb": ty, "xc": tx})
        fly.send(up_in.at[core], up_in.at[core], p_s.at[5], p_r.at[5], core_peer)
        hid = down_ref.shape[0]
        landed(down_in, p_r.at[4], core_peer)
        for side in range(2):

            @pl.when(core == side)
            def _(side=side):
                down_out[side * hid : (side + 1) * hid, :] = down_ref[...].astype(F32)
                down_out[(1 - side) * hid : (2 - side) * hid, :] = down_in[...].astype(F32)

    def feed_forward_rows():
        hid = down_ref.shape[0]
        landed(up_in.at[1 - core], p_r.at[5], core_peer)
        for slot in range(outer):
            for place in range(PLANE):
                for side in range(2):
                    column = ((slot * PLANE + place) * 2 + side) * hid
                    up_out[:, column : column + hid] = up_in[side, place, :, slot * hid : (slot + 1) * hid].astype(F32)

    def slot_at(step):
        if step == outer - 1:
            return z
        falling = outer - 1 - step
        falling = jnp.where(falling > z, falling, falling - 1)
        rising = jnp.where(step < z, step, step + 1)
        return jnp.where(z < part, falling, rising)

    units = [(slot_at(step), i) for step in range(outer) for i in range(count)]

    def turns(i, slot):
        turn = (slot + i) % 2
        first = ((y + 1 - turn) % 2, (x + turn) % 2)
        second = ((y + turn) % 2, (x + 1 - turn) % 2)
        return first, second

    def device(place):
        return {"yb": place[0], "xc": place[1]}

    def start(slot, i):
        first, _ = turns(i, slot)
        fly.send(
            source[i].at[slot, 1 - y, 1 - x], near[i].at[slot, 1], s1.at[i, slot, 1], r1.at[i, slot, 1], device(first)
        )
        fly.send(
            source[i].at[slot, first[0], first[1]], near[i].at[slot, 0], s1.at[i, slot, 0], r1.at[i, slot, 0], device(first)
        )

    def pass_on(slot, i):
        first, second = turns(i, slot)
        rows = near[i].shape[2]
        landed(near[i].at[slot, 1], r1.at[i, slot, 1], device(first))
        row_add(near[i].at[slot, 1], near[i].at[slot, 1], source[i].at[slot, second[0], second[1]], rows)
        fly.send(near[i].at[slot, 1], plane[i].at[slot], s2.at[i, slot], r2.at[i, slot], device(second))
        landed(near[i].at[slot, 0], r1.at[i, slot, 0], device(first))
        row_add(near[i].at[slot, 0], near[i].at[slot, 0], source[i].at[slot, y, x], rows)

    def plane_total(slot, i):
        _, second = turns(i, slot)
        rows = near[i].shape[2]
        landed(plane[i].at[slot], r2.at[i, slot], device(second))
        row_add(plane[i].at[slot], plane[i].at[slot], near[i].at[slot, 0], rows)

    def along(slot, i, last):
        rows = near[i].shape[2]
        if not last:
            for way, when, edge, ahead, behind in (
                (1, slot < z, z == outer - 1, below, above),
                (0, slot > z, z == 0, above, below),
            ):

                @pl.when(jnp.logical_and(when, jnp.logical_not(edge)))
                def _():
                    landed(chain[i].at[slot + 1 - way], zr.at[i, way, slot], behind)
                    row_add(plane[i].at[slot], plane[i].at[slot], chain[i].at[slot + 1 - way], rows)

                fly.send(
                    plane[i].at[slot], chain[i].at[slot + 1 - way], zs.at[i, way, slot], zr.at[i, way, slot], ahead, when
                )
            return
        parts = kinds[i][0]
        width = plane[i].shape[-1] // parts
        for way, when, behind in ((1, z < outer - 1, above), (0, z > 0, below)):

            @pl.when(when)
            def _():
                landed(chain[i].at[slot + 1 - way], zr.at[i, way, slot], behind)

        step = 16 if rows % 16 == 0 else rows
        has_above, has_below = z < outer - 1, z > 0

        def chunk(index, carry):
            at = pl.ds(pl.multiple_of(index * step, step), step)
            for part_no in range(parts):
                span = slice(part_no * width, (part_no + 1) * width)
                total = plane[i][slot, at, span].astype(F32)
                upper = chain[i][slot, at, span].astype(F32)
                lower = chain[i][slot + 1, at, span].astype(F32)
                total = total + jnp.where(has_above, upper, 0.0) + jnp.where(has_below, lower, 0.0)
                column = pl.multiple_of((2 * part_no + core) * width, width)
                outs[i][at, pl.ds(column, width)] = total
            return carry

        lax.fori_loop(0, rows // step, chunk, 0)
        for part_no in range(parts):
            column = pl.multiple_of((2 * part_no + core) * width, width)
            block = outs[i].at[:, pl.ds(column, width)]
            fly.send(block, block, o_s.at[i, part_no], o_r.at[i, part_no], core_peer)

    waiting = set(split)

    def begin(unit):
        slot, i = units[unit]
        if i in waiting:
            joined(i)
            waiting.discard(i)
        start(slot, i)

    for unit in range(min(AHEAD, len(units))):
        begin(unit)
    for tick in range(len(units) + LAG_CHAIN):
        if tick < len(units):
            pass_on(*units[tick])
            if tick + AHEAD < len(units):
                begin(tick + AHEAD)
        if 0 <= tick - LAG_PLANE < len(units):
            plane_total(*units[tick - LAG_PLANE])
        if tick == 2:
            feed_forward_landed()
        if tick == 6:
            feed_forward_rows()
        if 0 <= tick - LAG_CHAIN < len(units):
            unit = tick - LAG_CHAIN
            along(*units[unit], unit >= (outer - 1) * count)

    small_copy.wait()
    frame_copy.wait()
    for index in others:
        landed(small_in.at[index], m_r.at[index], chip(index))
    small_own[...] = jnp.sum(small_in[...], axis=0)
    fly.send(small_own, small_peer, l_s.at[2], l_s.at[3], core_peer)
    for index in others:
        landed(frames_out.at[index, :, frame_mine], f_r.at[index], chip(index))
    fly.send(frames_out.at[:, :, frame_mine], frames_out.at[:, :, frame_mine], p_s.at[6], p_r.at[6], core_peer)
    landed(frames_out.at[:, :, frame_other], p_r.at[6], core_peer)
    landed(small_peer, l_s.at[3], core_peer)
    small_out[...] = small_own[...] + small_peer[...]
    for i in range(count):
        parts = kinds[i][0]
        width = plane[i].shape[-1] // parts
        for part_no in range(parts):
            column = pl.multiple_of((2 * part_no + 1 - core) * width, width)
            landed(outs[i].at[:, pl.ds(column, width)], o_r.at[i, part_no], core_peer)
    fly.drain()


def reduce_weights(outer, kinds, grads, frames, small, up, down):
    shards = outer * PLANE
    count = len(kinds)
    shaped, shapes, near, plane, chain, whole = [], [], [], [], [], []
    for (parts, split), grad in zip(kinds, grads, strict=True):
        lead = outer // 2 if split else outer
        rows = grad.shape[0] // (lead * PLANE)
        width = grad.shape[1] // 2 if split else grad.shape[1]
        shaped.append(grad.reshape(lead, 2, 2, rows, grad.shape[1]))
        shapes.append(jax.ShapeDtypeStruct((rows, 2 * width), F32))
        near.append(pltpu.VMEM((outer, 2, rows, width), BF))
        plane.append(pltpu.VMEM((outer, rows, width), BF))
        chain.append(pltpu.VMEM((outer + 1, rows, width), BF))
        if split:
            whole.append(pltpu.VMEM((outer, 2, 2, rows, width), BF))
    shapes.append(jax.ShapeDtypeStruct((shards, frames.shape[0], 2 * frames.shape[1]), frames.dtype))
    shapes.append(jax.ShapeDtypeStruct(small.shape[1:], F32))
    shapes.append(jax.ShapeDtypeStruct((up.shape[1], 2 * PLANE * up.shape[2]), F32))
    shapes.append(jax.ShapeDtypeStruct((2 * down.shape[0], down.shape[1]), F32))
    dma = pltpu.SemaphoreType.DMA
    nsplit = len(whole)
    results = pl.pallas_call(
        functools.partial(reduce_kernel, outer, kinds),
        out_shape=shapes,
        in_specs=[VM] * (count + 4),
        out_specs=[VM] * (count + 4),
        scratch_shapes=[
            *near,
            *plane,
            *chain,
            *whole,
            pltpu.VMEM(small.shape, F32),
            pltpu.VMEM(small.shape[1:], F32),
            pltpu.VMEM(small.shape[1:], F32),
            pltpu.VMEM((2, *up.shape), up.dtype),
            pltpu.VMEM(down.shape, down.dtype),
            dma((nsplit,)),
            dma((nsplit,)),
            dma((nsplit,)),
            dma((count, outer, 2)),
            dma((count, outer, 2)),
            dma((count, outer)),
            dma((count, outer)),
            dma((count, 2, outer)),
            dma((count, 2, outer)),
            dma((count, 3)),
            dma((count, 3)),
            dma((shards,)),
            dma((shards,)),
            dma((shards,)),
            dma((shards,)),
            dma((4,)),
            dma((7,)),
            dma((7,)),
        ],
        cost_estimate=pl.CostEstimate(flops=10**11, bytes_accessed=10**8, transcendentals=0),
        compiler_params=pltpu.CompilerParams(
            collective_id=3, has_side_effects=True, vmem_limit_bytes=67043328
        ),
        name="reduce_weights",
    )(*shaped, frames, small, up, down)
    return results[:count], *results[count:]


def gather(value, axes, axis=0):
    return lax.all_gather(value, axes, axis=axis, tiled=True)


def scatter(value, axes, axis=0):
    return lax.psum_scatter(value, axes, scatter_dimension=axis, tiled=True)


def swap(value, split_axis, concat_axis):
    return lax.all_to_all(value, "sp", split_axis=split_axis, concat_axis=concat_axis, tiled=True)


def rms_scale(total):
    return lax.rsqrt(total / D + EPSILON)


def square_sum(values):
    return jnp.sum(values * values, axis=1)


def rms_back(values, inverse, gain, grad):
    scaled = grad * gain
    return scaled, jnp.sum(scaled * values, axis=1)


def rms_finish(values, inverse, scaled, total):
    column = inverse[:, None]
    return scaled * column - values * (column * column * column) * (total / D)[:, None]


def body(
    tokens,
    text,
    clip_frames,
    timestep,
    mod_weight,
    mod_bias,
    qk_gains,
    self_in,
    self_out,
    cross_q,
    cross_kv,
    cross_out,
    mlp_in,
    mlp_out,
    cotangent,
):
    half = D // 2
    row_count = tokens.shape[0]
    frame_count = row_count // FRAME_TOK
    group_frames = timestep.shape[1]
    shards = D // self_in.shape[1]
    outer = shards // PLANE
    core = lax.axis_index("sp")
    chip = lax.axis_index(FS)
    own_frame = core * frame_count

    bias_len, gain_len = mod_bias.shape[1], qk_gains.shape[2]
    small_len = bias_len + 4 * gain_len
    small_rows = 8
    small_width = -(-(small_len + group_frames) // (small_rows * 128)) * 128
    small_room = small_rows * small_width

    small = jnp.concatenate(
        [
            mod_bias[0].astype(F32),
            qk_gains[0].reshape(-1).astype(F32),
            timestep[0].astype(F32),
            jnp.zeros((small_room - small_len - group_frames,), F32),
        ]
    ).reshape(small_rows, small_width)
    gathered = gather_weights(
        outer,
        ((0, False), (1, False), (3, False), (1, True), (2, False), (1, False), (1, True)),
        [small, *(w[0] for w in (mod_weight, self_in, self_out, cross_kv, cross_q, cross_out))],
        mlp_in[0],
        text,
    )
    small_all, mod_matrix, self_proj, self_back, cross_kvproj, cross_qproj, cross_back = gathered[:7]
    up_matrix, text_all = gathered[7:]
    hid = mlp_out.shape[1] // 2
    down_part = lax.dynamic_slice_in_dim(mlp_out[0], core * hid, hid, 0)
    down_part, small_all = lax.optimization_barrier((down_part, small_all))
    down_matrix = gather(down_part, "za")
    small_all = small_all.reshape(shards, small_room)
    bias_all = small_all[:, :bias_len].reshape(-1)
    gain_all = (
        small_all[:, bias_len:small_len]
        .reshape(shards, 4, gain_len)
        .transpose(1, 0, 2)
        .reshape(4, 2, half)
    )
    gain_own = lax.dynamic_index_in_dim(gain_all, core, 1, keepdims=False)
    steps_all = small_all[:, small_len : small_len + group_frames].reshape(-1)

    live_keys = clip_frames * FRAME_TOK
    all_keys = jnp.full((1,), TXT, jnp.int32)
    own_steps = lax.dynamic_slice_in_dim(timestep[0], own_frame, frame_count)
    clip_pos = jnp.arange(group_frames, dtype=jnp.int32)
    cosine, sine = rotary_tables(
        jnp.repeat(clip_pos, FRAME_TOK),
        jnp.tile(jnp.arange(FRAME_TOK, dtype=jnp.int32), group_frames),
    )
    sinus = sinus_features(timestep[0]).astype(BF)

    mod_half = product(sinus, mod_matrix)
    mod_half = mod_half + lax.dynamic_slice_in_dim(bias_all, core * 3 * D, 3 * D)[None]
    modulation = swap(mod_half, 0, 1)
    shift_one, scale_one, gate_one, shift_two, scale_two, gate_two = jnp.split(
        modulation, 6, axis=1
    )

    grad_branch = frame_scaled(cotangent.astype(F32), gate_two).astype(BF)
    exchange = [(0, 1), (1, 0)]
    beside = jnp.stack([grad_branch, lax.ppermute(grad_branch, "xc", exchange)])
    beside = jnp.stack([beside, lax.ppermute(beside, "yb", exchange)])
    beside = jnp.stack([beside, lax.ppermute(beside, "sp", exchange)], axis=2)
    grad_branch_all = beside.reshape(-1, D)

    residual = tokens.astype(F32)
    attn_float, back_attn_input = jax.vjp(modulated, residual, shift_one, scale_one)
    attn_input = gather(attn_float.astype(BF), "sp")
    joined = product(attn_input, self_proj)
    raw_q, raw_k, raw_v = joined[:, :half], joined[:, half : 2 * half], joined[:, 2 * half :]
    totals = lax.psum(jnp.stack([square_sum(raw_q), square_sum(raw_k)]), "sp")
    inv_q, inv_k = rms_scale(totals[0]), rms_scale(totals[1])
    query = rotate(raw_q * inv_q[:, None] * gain_own[0], cosine, sine).astype(BF)
    key = rotate(raw_k * inv_k[:, None] * gain_own[1], cosine, sine).astype(BF)
    value = raw_v.astype(BF)
    self_mixed, self_lse = attend_forward(live_keys, query, key, value)
    self_branch = pair_sum(product(self_mixed, self_back))
    residual = residual + frame_scaled(self_branch, gate_one)

    text_raw = product(text_all, cross_kvproj)
    raw_ck, raw_cv = text_raw[:, :half], text_raw[:, half:]
    inv_ck = rms_scale(lax.psum(square_sum(raw_ck)[None], "sp")[0])
    cross_key = (raw_ck * inv_ck[:, None] * gain_own[3]).astype(BF)
    cross_value = raw_cv.astype(BF)

    cross_float, back_cross_norm = jax.vjp(layer_norm, residual)
    cross_input = gather(cross_float.astype(BF), "sp")
    cross_raw = product(cross_input, cross_qproj)
    inv_cq = rms_scale(lax.psum(square_sum(cross_raw)[None], "sp")[0])
    cross_query = (cross_raw * inv_cq[:, None] * gain_own[2]).astype(BF)
    cross_mixed, cross_lse = attend_forward(all_keys, cross_query, cross_key, cross_value)
    residual = residual + pair_sum(product(cross_mixed, cross_back))

    mlp_float, back_mlp_input = jax.vjp(modulated, residual, shift_two, scale_two)
    mlp_input = plane_gather(mlp_float.astype(BF))
    up_proj = product(mlp_input, up_matrix)
    activated_float, back_gelu = jax.vjp(
        lambda inner: jax.nn.gelu(inner, approximate=True), up_proj
    )
    activated = activated_float.astype(BF)

    mlp_branch = plane_sum(product(activated, down_matrix).astype(BF))
    output = (residual + frame_scaled(mlp_branch, gate_two)).astype(BF)

    grad_rows = cotangent.astype(F32)
    grad_gate_two = frame_sum(grad_rows * mlp_branch, frame_count)
    grad_down = product_tn(activated, grad_branch_all).astype(BF)
    grad_up_low = back_gelu(product_nt(grad_branch_all, down_matrix))[0].astype(BF)
    grad_up = product_tn(mlp_input, grad_up_low).astype(BF)
    grad_mlp_part = product_nt(grad_up_low, up_matrix).astype(BF)
    grad_mlp_part, grad_up, grad_down = lax.optimization_barrier((grad_mlp_part, grad_up, grad_down))
    down_owned = scatter(grad_down, "za")
    up_owned = scatter(grad_up, "za")
    grad_mlp_input = plane_sum(grad_mlp_part)
    grad_from_mlp, grad_shift_two, grad_scale_two = back_mlp_input(grad_mlp_input)
    grad_rows = grad_rows + grad_from_mlp

    grad_low = gather(grad_rows.astype(BF), "sp")
    grad_cross_back = product_tn(cross_mixed, grad_low).astype(BF)
    grad_cross_mixed = product_nt(grad_low, cross_back).astype(BF)
    grad_cq, grad_ck, grad_cv = attend_backward(
        all_keys, cross_query, cross_key, cross_value, cross_lse, grad_cross_mixed
    )
    grad_cq, grad_ck = grad_cq.astype(F32), grad_ck.astype(F32)
    grad_gain_two = jnp.sum(grad_cq * cross_raw * inv_cq[:, None], axis=0)
    grad_gain_three = jnp.sum(grad_ck * raw_ck * inv_ck[:, None], axis=0)
    scaled_cq, dots_cq = rms_back(cross_raw, inv_cq, gain_own[2], grad_cq)
    scaled_ck, dots_ck = rms_back(raw_ck, inv_ck, gain_own[3], grad_ck)
    dots_cq = lax.psum(dots_cq[None], "sp")[0]
    dots_ck = lax.psum(dots_ck[None], "sp")[0]
    grad_cross_low = rms_finish(cross_raw, inv_cq, scaled_cq, dots_cq).astype(BF)
    grad_text_low = jnp.concatenate(
        [rms_finish(raw_ck, inv_ck, scaled_ck, dots_ck).astype(BF), grad_cv], axis=1
    )
    grad_cross_qproj = product_tn(cross_input, grad_cross_low).astype(BF)
    grad_cross_kvproj = product_tn(text_all, grad_text_low).astype(BF)
    grad_cross_input = pair_sum(product_nt(grad_cross_low, cross_qproj))
    grad_rows = grad_rows + back_cross_norm(grad_cross_input)[0]

    grad_gate_one = frame_sum(grad_rows * self_branch, frame_count)
    grad_self_low = gather(frame_scaled(grad_rows, gate_one).astype(BF), "sp")
    grad_self_back = product_tn(self_mixed, grad_self_low).astype(BF)
    grad_self_mixed = product_nt(grad_self_low, self_back).astype(BF)
    grad_q, grad_k, grad_v = attend_backward(
        live_keys, query, key, value, self_lse, grad_self_mixed
    )
    grad_q = rotate(grad_q.astype(F32), cosine, -sine)
    grad_k = rotate(grad_k.astype(F32), cosine, -sine)
    grad_gain_zero = jnp.sum(grad_q * raw_q * inv_q[:, None], axis=0)
    grad_gain_one = jnp.sum(grad_k * raw_k * inv_k[:, None], axis=0)
    scaled_q, dots_q = rms_back(raw_q, inv_q, gain_own[0], grad_q)
    scaled_k, dots_k = rms_back(raw_k, inv_k, gain_own[1], grad_k)
    dots = lax.psum(jnp.stack([dots_q, dots_k]), "sp")
    grad_joined_low = jnp.concatenate(
        [
            rms_finish(raw_q, inv_q, scaled_q, dots[0]).astype(BF),
            rms_finish(raw_k, inv_k, scaled_k, dots[1]).astype(BF),
            grad_v,
        ],
        axis=1,
    )
    grad_self_proj = product_tn(attn_input, grad_joined_low).astype(BF)
    grad_attn_input = pair_sum(product_nt(grad_joined_low, self_proj))
    grad_from_attn, grad_shift_one, grad_scale_one = back_attn_input(grad_attn_input)
    grad_rows = grad_rows + grad_from_attn

    grad_modulation = jnp.concatenate(
        [grad_shift_one, grad_scale_one, grad_gate_one, grad_shift_two, grad_scale_two, grad_gate_two],
        axis=1,
    )
    grad_mod_half = swap(grad_modulation, 1, 0)
    grad_gains = jnp.stack([grad_gain_zero, grad_gain_one, grad_gain_two, grad_gain_three])
    both = jnp.arange(2)[None, :, None] == core
    grad_gains = jnp.where(both, grad_gains[:, None, :], 0.0).reshape(4, shards, gain_len)
    grad_small = jnp.concatenate(
        [
            jnp.sum(grad_modulation, axis=0).reshape(shards, bias_len),
            grad_gains.transpose(1, 0, 2).reshape(shards, 4 * gain_len),
            jnp.zeros((shards, small_room - small_len), F32),
        ],
        axis=1,
    ).reshape(shards, small_rows, small_width)
    owned, grad_mod_all, small_owned, mlp_in_grad, mlp_out_grad = reduce_weights(
        outer,
        ((1, False), (2, False), (1, True), (1, True), (3, False)),
        [grad_cross_qproj, grad_cross_kvproj, grad_cross_back, grad_self_back, grad_self_proj],
        grad_mod_half.astype(BF),
        grad_small,
        up_owned.reshape(PLANE, -1, up_owned.shape[1]),
        down_owned,
    )
    cross_q_grad, cross_kv_grad, cross_out_grad, self_out_grad, self_in_grad = owned
    small_owned = small_owned.reshape(-1)[:small_len]
    sinus_all = sinus_features(steps_all).astype(BF)
    own_features = mod_weight.shape[1]
    sinus_own = lax.dynamic_slice_in_dim(sinus_all, chip * own_features, own_features, 1)
    mod_weight_grad = product_tn(sinus_own, grad_mod_all.reshape(-1, 6 * D))
    return (
        output,
        grad_rows,
        mod_weight_grad[None],
        small_owned[None, :bias_len],
        small_owned[bias_len:].reshape(1, 4, gain_len),
        self_in_grad[None],
        self_out_grad[None],
        cross_q_grad[None],
        cross_kv_grad[None],
        cross_out_grad[None],
        mlp_in_grad[None],
        mlp_out_grad[None],
    )


def solution(mesh):
    chips, cores = mesh.shape["fsdp"], mesh.shape["sp"]
    grid = mesh.devices.reshape(chips // PLANE, 2, PLANE // 2, cores)
    inner = Mesh(grid, ALL)
    rows, second = P(ALL, None), P(None, FS, None)
    in_specs = (
        rows,
        rows,
        P(FS),
        P(FS, None),
        second,
        P(None, FS),
        P(None, None, FS),
        *([second] * 7),
        rows,
    )
    out_specs = (rows, rows, second, P(None, FS), P(None, None, FS), *([second] * 7))
    return jax.shard_map(body, mesh=inner, in_specs=in_specs, out_specs=out_specs, check_vma=False)
```

```python
import functools
import math

import jax
import jax.numpy as jnp
from jax import lax
from jax.experimental import pallas as pl
from jax.experimental.pallas import tpu as pltpu
from jax.sharding import Mesh
from jax.sharding import PartitionSpec as P


D = 1536
HD = 128
TXT = 512
FREQ = 256
WP = 8
FRAME_TOK = 64
PLANE = 4

EPSILON = 1e-06
NEGATIVE = -1e30

FS = ("za", "yb", "xc")
PL = ("yb", "xc")
ALL = ("za", "yb", "xc", "sp")
SCALE = 1.0 / math.sqrt(HD)
MESH = pl.DeviceIdType.MESH
BF = jnp.bfloat16
F32 = jnp.float32


def product(left, right):
    return jnp.dot(left, right, preferred_element_type=F32)


def product_tn(left, right):
    return lax.dot_general(left, right, (((0,), (0,)), ((), ())), preferred_element_type=F32)


def product_nt(left, right):
    return lax.dot_general(left, right, (((1,), (1,)), ((), ())), preferred_element_type=F32)


def layer_norm(values):
    centred = values - jnp.mean(values, axis=-1, keepdims=True)
    return centred * lax.rsqrt(jnp.mean(centred * centred, axis=-1, keepdims=True) + EPSILON)


def sinus_features(steps):
    half_dim = FREQ // 2
    rates = jnp.exp(jnp.arange(half_dim).astype(F32) * (-math.log(10000.0) / half_dim))
    angles = steps.astype(F32)[:, None] * rates[None, :]
    return jnp.concatenate([jnp.cos(angles), jnp.sin(angles)], axis=1)


def rotary_tables(frame_pos, token_spot):
    half_dim = HD // 2
    side_pairs = HD // 6
    lead_pairs = half_dim - 2 * side_pairs
    pair_index = jnp.arange(half_dim)
    log_base = -math.log(10000.0)
    lead_part = pair_index < lead_pairs
    side_part = jnp.logical_and(pair_index >= lead_pairs, pair_index < lead_pairs + side_pairs)
    last_part = pair_index >= lead_pairs + side_pairs
    frame_rate = jnp.where(
        lead_part, jnp.exp(log_base * pair_index.astype(F32) / lead_pairs), 0.0
    )
    row_rate = jnp.where(
        side_part, jnp.exp(log_base * (pair_index - lead_pairs).astype(F32) / side_pairs), 0.0
    )
    column_rate = jnp.where(
        last_part,
        jnp.exp(log_base * (pair_index - lead_pairs - side_pairs).astype(F32) / side_pairs),
        0.0,
    )
    patch_row = (token_spot // WP).astype(F32)
    patch_column = (token_spot % WP).astype(F32)
    angles = (
        frame_pos.astype(F32)[:, None] * frame_rate[None, :]
        + patch_row[:, None] * row_rate[None, :]
        + patch_column[:, None] * column_rate[None, :]
    )
    return (jnp.cos(angles), jnp.sin(angles))


def rotate(values, cosine, sine):
    row_count = values.shape[0]
    shaped = values.reshape(row_count, -1, HD)
    half_dim = HD // 2
    first_half = shaped[:, :, :half_dim]
    second_half = shaped[:, :, half_dim:]
    cos_rows = cosine[:, None, :]
    sin_rows = sine[:, None, :]
    turned = jnp.concatenate(
        [
            first_half * cos_rows - second_half * sin_rows,
            second_half * cos_rows + first_half * sin_rows,
        ],
        axis=2,
    )
    return turned.reshape(row_count, -1)


def modulated(residual, shift, scale):
    frames = shift.shape[0]
    normed = layer_norm(residual).reshape(frames, -1, residual.shape[1])
    return (normed * (1.0 + scale[:, None, :]) + shift[:, None, :]).reshape(residual.shape)


def frame_scaled(rows, gate):
    frames = gate.shape[0]
    return (rows.reshape(frames, -1, rows.shape[1]) * gate[:, None, :]).reshape(rows.shape)


def frame_sum(values, frames):
    return jnp.sum(values.reshape(frames, -1, values.shape[1]), axis=1)


def attend_forward_kernel(live_ref, q_ref, k_ref, v_ref, out_ref, lse_ref):
    rows, keys = q_ref.shape[0], k_ref.shape[0]
    spot = lax.broadcasted_iota(jnp.int32, (rows, keys), 1)
    allowed = spot < live_ref[0]
    for head in range(q_ref.shape[1] // HD):
        part = slice(head * HD, (head + 1) * HD)
        scores = jnp.where(allowed, product_nt(q_ref[:, part], k_ref[:, part]) * SCALE, NEGATIVE)
        row_max = jnp.max(scores, axis=1, keepdims=True)
        log_total = row_max + jnp.log(jnp.sum(jnp.exp(scores - row_max), axis=1, keepdims=True))
        weights = jnp.exp(scores - log_total).astype(BF)
        out_ref[:, part] = product(weights, v_ref[:, part]).astype(BF)
        lse_ref[:, part] = jnp.broadcast_to(log_total, (rows, HD))


def attend_backward_kernel(
    live_ref, q_ref, k_ref, v_ref, lse_ref, do_ref, dq_ref, dk_ref, dv_ref
):
    rows, keys = q_ref.shape[0], k_ref.shape[0]
    spot = lax.broadcasted_iota(jnp.int32, (rows, keys), 1)
    allowed = spot < live_ref[0]
    for head in range(q_ref.shape[1] // HD):
        part = slice(head * HD, (head + 1) * HD)
        query, key, value, grad = q_ref[:, part], k_ref[:, part], v_ref[:, part], do_ref[:, part]
        scores = jnp.where(allowed, product_nt(query, key) * SCALE, NEGATIVE)
        weights = jnp.exp(scores - lse_ref[:, head * HD : head * HD + 1])
        grad_weights = product_nt(grad, value)
        delta = jnp.sum(weights * grad_weights, axis=1, keepdims=True)
        grad_scores = (weights * (grad_weights - delta)).astype(BF)
        dq_ref[:, part] = (product(grad_scores, key) * SCALE).astype(BF)
        dk_ref[:, part] = (product_tn(grad_scores, query) * SCALE).astype(BF)
        dv_ref[:, part] = product_tn(weights.astype(BF), grad).astype(BF)


VM = pl.BlockSpec(memory_space=pltpu.VMEM)
SM = pl.BlockSpec(memory_space=pltpu.SMEM)
ANY = pl.BlockSpec(memory_space=pl.ANY)


def attend_forward(live, query, key, value):
    rows, width = query.shape
    keys = key.shape[0]
    heads = width // HD
    return pl.pallas_call(
        attend_forward_kernel,
        out_shape=(
            jax.ShapeDtypeStruct((rows, width), BF),
            jax.ShapeDtypeStruct((rows, width), F32),
        ),
        in_specs=[SM, VM, VM, VM],
        out_specs=(VM, VM),
        cost_estimate=pl.CostEstimate(
            flops=4 * rows * keys * width,
            bytes_accessed=8 * rows * width + 4 * keys * width,
            transcendentals=2 * rows * keys * heads,
        ),
    )(live, query, key, value)


def attend_backward(live, query, key, value, lse, grad):
    rows, width = query.shape
    keys = key.shape[0]
    heads = width // HD
    return pl.pallas_call(
        attend_backward_kernel,
        out_shape=(
            jax.ShapeDtypeStruct((rows, width), BF),
            jax.ShapeDtypeStruct((keys, width), BF),
            jax.ShapeDtypeStruct((keys, width), BF),
        ),
        in_specs=[SM, VM, VM, VM, VM, VM],
        out_specs=(VM, VM, VM),
        cost_estimate=pl.CostEstimate(
            flops=10 * rows * keys * width,
            bytes_accessed=10 * rows * width + 8 * keys * width,
            transcendentals=rows * keys * heads,
        ),
    )(live, query, key, value, lse, grad)


def row_add(target, left, right, rows):
    step = 32 if rows % 32 == 0 else rows

    def chunk(index, carry):
        at = pl.ds(pl.multiple_of(index * step, step), step)
        target[at, :] = left[at, :] + right[at, :]
        return carry

    lax.fori_loop(0, rows // step, chunk, 0)


def row_sum(target, left, right, rows):
    step = 16 if rows % 16 == 0 else rows

    def chunk(index, carry):
        at = pl.ds(pl.multiple_of(index * step, step), step)
        target[at, :] = left[at, :].astype(F32) + right[at, :].astype(F32)
        return carry

    lax.fori_loop(0, rows // step, chunk, 0)


class Flights:
    def __init__(self):
        self.sent = []

    def send(self, source, target, send_sem, recv_sem, device, when=None):
        copy = pltpu.make_async_remote_copy(
            src_ref=source,
            dst_ref=target,
            send_sem=send_sem,
            recv_sem=recv_sem,
            device_id=device,
            device_id_type=MESH,
        )
        if when is None:
            copy.start()
        else:
            pl.when(when)(copy.start)
        self.sent.append((when, copy))

    def local(self, source, target, sem):
        copy = pltpu.make_async_copy(source, target, sem)
        copy.start()
        return copy

    def drain(self):
        for when, copy in self.sent:
            if when is None:
                copy.wait_send()
            else:
                pl.when(when)(copy.wait_send)


def landed(target, sem, device):
    pltpu.make_async_remote_copy(
        src_ref=target,
        dst_ref=target,
        send_sem=sem,
        recv_sem=sem,
        device_id=device,
        device_id_type=MESH,
    ).wait_recv()


def greet(devices, optional=()):
    barrier = pltpu.get_barrier_semaphore()
    for device in devices:
        pl.semaphore_signal(barrier, inc=1, device_id=device, device_id_type=MESH)
    for when, device in optional:

        @pl.when(when)
        def _(device=device):
            pl.semaphore_signal(barrier, inc=1, device_id=device, device_id_type=MESH)

    count = len(devices)
    for when, _ in optional:
        count = count + when.astype(jnp.int32)
    pl.semaphore_wait(barrier, count)


def gather_kernel(outer, kinds, *refs):
    full = len(kinds)
    ins, refs = refs[:full], refs[full:]
    mlp_ref, text_ref, refs = refs[0], refs[1], refs[2:]
    outs, refs = list(refs[:full]), refs[full:]
    up_out, text_out, refs = refs[0], refs[1], refs[2:]
    own, refs = refs[:full], refs[full:]
    halves = [i for i, kind in enumerate(kinds) if kind[1]]
    whole, refs = refs[: len(halves)], refs[len(halves) :]
    up_own, local_sem, zs, zr, s1, r1, s2, r2, a_s, a_r, f_s, f_r, f_l, t_s = refs
    z, y, x = (lax.axis_index(name) for name in FS)
    core = lax.axis_index("sp")
    here = 2 * y + x
    up = full
    fins = {}
    for j, i in enumerate(halves):
        fins[i] = outs[i]
        outs[i] = whole[j]
    fly = Flights()
    x_peer, y_peer = {"xc": 1 - x}, {"yb": 1 - y}
    diagonal = {"yb": 1 - y, "xc": 1 - x}
    around = ((x_peer, y, 1 - x), (y_peer, 1 - y, x), (diagonal, 1 - y, 1 - x))
    above, below = {"za": z + 1}, {"za": z - 1}
    core_peer = {"sp": 1 - core}
    has_above, has_below = z + 1 < outer, z >= 1
    greet((x_peer, y_peer, diagonal, core_peer), ((has_above, above), (has_below, below)))

    for i, (parts, _) in enumerate(kinds):
        if parts == 0:
            own[i][...] = ins[i][...]
        for part in range(parts):
            width = ins[i].shape[1] // (2 * parts)
            column = pl.multiple_of((2 * part + core) * width, width)
            own[i][:, part * width : (part + 1) * width] = ins[i][:, pl.ds(column, width)]

    def shard(i, slot):
        return outs[i].at[slot, y, x] if i < full else up_out.at[slot]

    def z_send(i, way, hop, source=None):
        if hop > outer - 2:
            return
        slot = z - hop if way == 0 else z + hop
        when = jnp.logical_and(has_above, slot >= 0) if way == 0 else jnp.logical_and(has_below, slot < outer)
        fly.send(
            shard(i, slot) if source is None else source,
            shard(i, slot),
            zs.at[i, way, hop],
            zr.at[i, way, hop],
            above if way == 0 else below,
            when,
        )

    def z_slot(way, hop):
        slot = z - 1 - hop if way == 0 else z + 1 + hop
        return slot, (slot >= 0 if way == 0 else slot < outer)

    def z_wait(i, way, hop):
        slot, when = z_slot(way, hop)

        @pl.when(when)
        def _():
            landed(shard(i, slot), zr.at[i, way, hop], below if way == 0 else above)

    def turns(i, slot):
        turn = (slot + i) % 2
        first = ((y + turn) % 2, (x + 1 - turn) % 2)
        second = ((y + 1 - turn) % 2, (x + turn) % 2)
        return first, second

    def xy_own(i, slot, when=None, source=None):
        first, second = turns(i, slot)
        mine = outs[i].at[slot, y, x]
        source = mine if source is None else source
        fly.send(source, mine, s1.at[i, slot], r1.at[i, slot], {"yb": first[0], "xc": first[1]}, when)
        fly.send(source, mine, s2.at[i, slot, 0], r2.at[i, slot, 0], {"yb": second[0], "xc": second[1]}, when)

    def xy_pass(i, slot, when=None):
        first, second = turns(i, slot)
        theirs = outs[i].at[slot, first[0], first[1]]

        def wait():
            landed(theirs, r1.at[i, slot], {"yb": first[0], "xc": first[1]})

        if when is None:
            wait()
        else:
            pl.when(when)(wait)
        fly.send(theirs, theirs, s2.at[i, slot, 1], r2.at[i, slot, 1], {"yb": second[0], "xc": second[1]}, when)

    def xy_end(i, slot):
        _, second = turns(i, slot)
        device = {"yb": second[0], "xc": second[1]}
        landed(outs[i].at[slot, second[0], second[1]], r2.at[i, slot, 0], device)
        landed(outs[i].at[slot, 1 - y, 1 - x], r2.at[i, slot, 1], device)

    for i in range(full):
        for way in range(2):
            z_send(i, way, 0, own[i])
        xy_own(i, z, None, own[i])
    locals_ = [fly.local(own[i], outs[i].at[z, y, x], local_sem.at[i]) for i in range(full)]

    fly.send(text_ref, text_out.at[core], t_s.at[0], t_s.at[1], core_peer)
    locals_.append(fly.local(text_ref, text_out.at[core], t_s.at[2]))
    hid = mlp_ref.shape[1] // (outer * PLANE * 2)
    for own_core in range(2):

        @pl.when(core == own_core)
        def _(own_core=own_core):
            for place in range(PLANE):
                for slot in range(outer):
                    column = ((slot * PLANE + place) * 2 + own_core) * hid
                    up_own[place, :, slot * hid : (slot + 1) * hid] = mlp_ref[:, column : column + hid]

    for hop in range(outer - 1):
        for i in range(full):
            for way in range(2):
                slot, when = z_slot(way, hop)
                z_wait(i, way, hop)
                z_send(i, way, hop + 1)
                xy_own(i, slot, when)
        if hop == 0:
            locals_.append(fly.local(up_own.at[here], up_out.at[z, here], local_sem.at[up]))
            for turn, (device, ty, tx) in enumerate(around):
                fly.send(up_own.at[2 * ty + tx], up_out.at[z, here], a_s.at[turn], a_r.at[turn], device)
    for copy in locals_:
        copy.wait()
    for turn, (device, ty, tx) in enumerate(around):
        landed(up_out.at[z, 2 * ty + tx], a_r.at[turn], device)
    for way in range(2):
        z_send(up, way, 0)
    for i in range(full):
        xy_pass(i, z)
    for hop in range(outer - 1):
        for i in range(full):
            for way in range(2):
                slot, when = z_slot(way, hop)
                xy_pass(i, slot, when)
        for way in range(2):
            z_wait(up, way, hop)
            z_send(up, way, hop + 1)
    for i in (*halves, *(i for i in range(full) if i not in halves)):
        for slot in range(outer):
            xy_end(i, slot)
        if i not in halves:
            continue
        j, part = halves.index(i), outer // 2
        width = own[i].shape[-1]
        columns = pl.ds(pl.multiple_of(core * width, width), width)
        theirs, ours = pl.ds((1 - core) * part, part), pl.ds(core * part, part)
        fly.send(outs[i].at[theirs], fins[i].at[:, :, :, :, columns], f_s.at[j], f_r.at[j], core_peer)
        fly.local(outs[i].at[ours], fins[i].at[:, :, :, :, columns], f_l.at[j])
    for j, i in enumerate(halves):
        width = own[i].shape[-1]
        columns = pl.ds(pl.multiple_of(core * width, width), width)
        others = pl.ds(pl.multiple_of((1 - core) * width, width), width)
        ours = pl.ds(core * (outer // 2), outer // 2)
        pltpu.make_async_copy(outs[i].at[ours], fins[i].at[:, :, :, :, columns], f_l.at[j]).wait()
        landed(fins[i].at[:, :, :, :, others], f_r.at[j], core_peer)
    landed(text_out.at[1 - core], t_s.at[1], core_peer)
    fly.drain()


def gather_weights(outer, kinds, arrays, mlp, text):
    shapes, own, whole = [], [], []
    for (parts, keep), array in zip(kinds, arrays, strict=True):
        rows, width = array.shape
        half = width // 2 if parts else width
        own.append(pltpu.VMEM((rows, half), array.dtype))
        if keep:
            whole.append(pltpu.VMEM((outer, 2, 2, rows, half), array.dtype))
            shapes.append(jax.ShapeDtypeStruct((outer // 2, 2, 2, rows, width), array.dtype))
        else:
            shapes.append(jax.ShapeDtypeStruct((outer, 2, 2, rows, half), array.dtype))
    rows, units = mlp.shape
    mine = units // (2 * PLANE)
    shapes.append(jax.ShapeDtypeStruct((outer, PLANE, rows, mine), mlp.dtype))
    shapes.append(jax.ShapeDtypeStruct((2, *text.shape), text.dtype))
    dma = pltpu.SemaphoreType.DMA
    hops = outer - 1
    nf, nh = len(kinds), len(whole)
    results = pl.pallas_call(
        functools.partial(gather_kernel, outer, kinds),
        out_shape=shapes,
        in_specs=[VM] * (nf + 2),
        out_specs=[ANY] * len(shapes),
        scratch_shapes=[
            *own,
            *whole,
            pltpu.VMEM((PLANE, rows, mine), mlp.dtype),
            dma((nf + 1,)),
            dma((nf + 1, 2, hops)),
            dma((nf + 1, 2, hops)),
            dma((nf, outer)),
            dma((nf, outer)),
            dma((nf, outer, 2)),
            dma((nf, outer, 2)),
            dma((3,)),
            dma((3,)),
            dma((nh,)),
            dma((nh,)),
            dma((nh,)),
            dma((3,)),
        ],
        compiler_params=pltpu.CompilerParams(
            collective_id=0, has_side_effects=True, vmem_limit_bytes=40 * 1024 * 1024
        ),
        cost_estimate=pl.CostEstimate(flops=10**11, bytes_accessed=10**8, transcendentals=0),
        name="gather_weights",
    )(*arrays, mlp, text)
    return [value.reshape(-1, value.shape[-1]) for value in results]


def plane_gather_kernel(own_ref, out_ref, local_sem, send, recv):
    y, x, core = lax.axis_index("yb"), lax.axis_index("xc"), lax.axis_index("sp")
    x_peer, y_peer, core_peer = {"xc": 1 - x}, {"yb": 1 - y}, {"sp": 1 - core}
    fly = Flights()
    greet((x_peer, y_peer, core_peer))
    size = own_ref.shape[0] // 2
    top, low = pl.ds(0, size), pl.ds(size, size)
    fly.send(own_ref.at[top], out_ref.at[0, 1, 0, top], send.at[0], recv.at[0], x_peer)
    fly.send(own_ref.at[low], out_ref.at[1, 0, 0, low], send.at[1], recv.at[1], y_peer)
    fly.send(own_ref.at[low], out_ref.at[0, 1, 0, low], send.at[2], recv.at[2], x_peer)
    fly.send(own_ref.at[top], out_ref.at[1, 0, 0, top], send.at[3], recv.at[3], y_peer)
    fly.send(own_ref, out_ref.at[0, 0, 1], send.at[4], recv.at[4], core_peer)
    local = fly.local(own_ref, out_ref.at[0, 0, 0], local_sem.at[0])
    across = []

    def arrive(index, dy, dx, rows, device, onward=None):
        block = out_ref.at[dy, dx, 0, rows]
        landed(block, recv.at[index], device)
        if onward is not None:
            to, number = onward
            fly.send(block, out_ref.at[1, 1, 0, rows], send.at[number], recv.at[number], to)
        fly.send(block, out_ref.at[dy, dx, 1, rows], send.at[index + 7], recv.at[index + 7], core_peer)
        across.append((index + 7, dy, dx, rows))

    arrive(0, 0, 1, top, x_peer, (y_peer, 5))
    arrive(1, 1, 0, low, y_peer, (x_peer, 6))
    arrive(2, 0, 1, low, x_peer)
    arrive(3, 1, 0, top, y_peer)
    arrive(5, 1, 1, top, y_peer)
    arrive(6, 1, 1, low, x_peer)
    landed(out_ref.at[0, 0, 1], recv.at[4], core_peer)
    for index, dy, dx, rows in across:
        landed(out_ref.at[dy, dx, 1, rows], recv.at[index], core_peer)
    local.wait()
    fly.drain()


def plane_gather(own):
    rows, width = own.shape
    dma = pltpu.SemaphoreType.DMA
    out = pl.pallas_call(
        plane_gather_kernel,
        out_shape=jax.ShapeDtypeStruct((2, 2, 2, rows, width), own.dtype),
        in_specs=[VM],
        out_specs=VM,
        scratch_shapes=[dma((1,)), dma((14,)), dma((14,))],
        compiler_params=pltpu.CompilerParams(collective_id=1, has_side_effects=True),
        cost_estimate=pl.CostEstimate(flops=10**10, bytes_accessed=10**7, transcendentals=0),
        name="plane_gather",
    )(own)
    return out.reshape(8 * rows, width)


def plane_sum_kernel(part_a, part_b, out_a, out_b, core_in, first, second, keep, send, recv):
    y, x, core = lax.axis_index("yb"), lax.axis_index("xc"), lax.axis_index("sp")
    x_peer, y_peer, core_peer = {"xc": 1 - x}, {"yb": 1 - y}, {"sp": 1 - core}
    fly = Flights()
    greet((x_peer, y_peer, core_peer))
    rows = part_a.shape[3]
    chips = (((1, 1), (1, 0), (0, 1), (0, 0)), ((1, 1), (0, 1), (1, 0), (0, 0)))
    parts, outs, peers = (part_a, part_b), (out_a, out_b), ((y_peer, x_peer), (x_peer, y_peer))
    for index in range(4):
        for n in range(2):
            dy, dx = chips[n][index]
            fly.send(
                parts[n].at[dy, dx, 1], core_in.at[n, index], send.at[n, index], recv.at[n, index], core_peer
            )

    def core_sum(n, index):
        dy, dx = chips[n][index]
        landed(core_in.at[n, index], recv.at[n, index], core_peer)
        row_add(core_in.at[n, index], core_in.at[n, index], parts[n].at[dy, dx, 0], rows)

    for index in range(2):
        for n in range(2):
            core_sum(n, index)
            fly.send(
                core_in.at[n, index], first.at[n, index], send.at[n, index + 4], recv.at[n, index + 4], peers[n][0]
            )
    for index in (2, 3):
        for n in range(2):
            core_sum(n, index)
    for n in range(2):
        landed(first.at[n, 0], recv.at[n, 4], peers[n][0])
        row_add(second.at[n, 0], first.at[n, 0], core_in.at[n, 2], rows)
        fly.send(second.at[n, 0], second.at[n, 1], send.at[n, 6], recv.at[n, 6], peers[n][1])
    for n in range(2):
        landed(first.at[n, 1], recv.at[n, 5], peers[n][0])
        row_sum(keep.at[n], first.at[n, 1], core_in.at[n, 3], rows)
    for n in range(2):
        landed(second.at[n, 1], recv.at[n, 6], peers[n][1])
        row_sum(outs[n], keep.at[n], second.at[n, 1], rows)
    fly.drain()


def plane_sum(one, other):
    rows, width = one.shape[0] // 8, one.shape[1]
    dma = pltpu.SemaphoreType.DMA
    shape = jax.ShapeDtypeStruct((rows, width), F32)
    return pl.pallas_call(
        plane_sum_kernel,
        out_shape=(shape, shape),
        in_specs=[VM, VM],
        out_specs=(VM, VM),
        scratch_shapes=[
            pltpu.VMEM((2, 4, rows, width), BF),
            pltpu.VMEM((2, 2, rows, width), BF),
            pltpu.VMEM((2, 2, rows, width), BF),
            pltpu.VMEM((2, rows, width), F32),
            dma((2, 7)),
            dma((2, 7)),
        ],
        compiler_params=pltpu.CompilerParams(collective_id=2, has_side_effects=True),
        cost_estimate=pl.CostEstimate(flops=10**10, bytes_accessed=10**7, transcendentals=0),
        name="plane_sum",
    )(one.reshape(2, 2, 2, rows, width), other.reshape(2, 2, 2, rows, width))


def pair_sum_kernel(part_ref, out_ref, peer_in, send, recv):
    core = lax.axis_index("sp")
    core_peer = {"sp": 1 - core}
    fly = Flights()
    greet((core_peer,))
    size = part_ref.shape[1] // 2
    for index in range(2):
        rows = pl.ds(index * size, size)
        fly.send(part_ref.at[1 - core, rows], peer_in.at[rows], send.at[index], recv.at[index], core_peer)
    for index in range(2):
        rows = pl.ds(index * size, size)
        landed(peer_in.at[rows], recv.at[index], core_peer)
        row_sum(out_ref.at[rows], part_ref.at[core, rows], peer_in.at[rows], size)
    fly.drain()


def pair_sum(partial):
    rows, width = partial.shape[0] // 2, partial.shape[1]
    dma = pltpu.SemaphoreType.DMA
    return pl.pallas_call(
        pair_sum_kernel,
        out_shape=jax.ShapeDtypeStruct((rows, width), F32),
        in_specs=[VM],
        out_specs=VM,
        scratch_shapes=[pltpu.VMEM((rows, width), F32), dma((2,)), dma((2,))],
        compiler_params=pltpu.CompilerParams(collective_id=4, has_side_effects=True),
        cost_estimate=pl.CostEstimate(flops=10**9, bytes_accessed=10**7, transcendentals=0),
        name="pair_sum",
    )(partial.reshape(2, rows, width))


AHEAD, LAG_PLANE, LAG_CHAIN = 6, 2, 4
PLAIN, SPLIT, OVER_X, OVER_Y = range(4)


def reduce_kernel(outer, kinds, *refs):
    count = len(kinds)
    shards = outer * PLANE
    gs, refs = refs[:count], refs[count:]
    frames_ref, small_ref, up_ref, down_ref, refs = *refs[:4], refs[4:]
    outs, refs = refs[:count], refs[count:]
    frames_out, small_out, up_out, down_out, refs = *refs[:4], refs[4:]
    pieces = [(i, part) for i, (parts, _) in enumerate(kinds) for part in range(parts)]
    total = len(pieces)
    forms = [kinds[i][1] for i, _ in pieces]
    near_refs, near = list(refs), {}
    for p in range(total):
        if forms[p] in (PLAIN, SPLIT):
            near[p] = near_refs.pop(0)
    refs = near_refs
    plane, refs = refs[:total], refs[total:]
    chain, refs = refs[:total], refs[total:]
    split = [i for i, kind in enumerate(kinds) if kind[1] == SPLIT]
    whole, refs = refs[: len(split)], refs[len(split) :]
    small_in, small_own, small_peer, up_in, down_in, refs = *refs[:5], refs[5:]
    e_s, e_r, e_l, s1, r1, s2, r2, zs, zr, o_s, o_r, f_s, f_r, m_s, m_r, l_s, p_s, p_r = refs
    z, y, x = (lax.axis_index(name) for name in FS)
    core = lax.axis_index("sp")
    here = (z * 2 + y) * 2 + x
    core_peer = {"sp": 1 - core}
    above, below = {"za": z + 1}, {"za": z - 1}
    fly = Flights()

    def chip(index):
        return {"za": index // 4, "yb": (index // 2) % 2, "xc": index % 2}

    others = [(here + j) % shards for j in range(1, shards)]
    greet((core_peer, *[chip(index) for index in others]))

    part_slots = outer // 2
    ours, other_slots = pl.ds(core * part_slots, part_slots), pl.ds((1 - core) * part_slots, part_slots)
    for j, i in enumerate(split):
        width = whole[j].shape[-1]
        mine = pl.ds(pl.multiple_of(core * width, width), width)
        theirs = pl.ds(pl.multiple_of((1 - core) * width, width), width)
        fly.send(gs[i].at[:, :, :, :, theirs], whole[j].at[ours], e_s.at[j], e_r.at[j], core_peer)
        fly.local(gs[i].at[:, :, :, :, mine], whole[j].at[ours], e_l.at[j])

    def joined(i):
        j = split.index(i)
        width = whole[j].shape[-1]
        mine = pl.ds(pl.multiple_of(core * width, width), width)
        pltpu.make_async_copy(gs[i].at[:, :, :, :, mine], whole[j].at[ours], e_l.at[j]).wait()
        landed(whole[j].at[other_slots], e_r.at[j], core_peer)

    def width_of(p):
        return plane[p].shape[-1]

    def source(p, *place):
        i, part = pieces[p]
        held = whole[split.index(i)] if forms[p] == SPLIT else gs[i]
        width = width_of(p)
        return held.at[(*place, slice(None), pl.ds(part * width, width))]

    frame_width = frames_ref.shape[1]
    frame_mine = pl.ds(pl.multiple_of(core * frame_width, frame_width), frame_width)
    frame_other = pl.ds(pl.multiple_of((1 - core) * frame_width, frame_width), frame_width)
    frame_copy = fly.local(frames_ref, frames_out.at[here, :, frame_mine], l_s.at[0])
    small_copy = fly.local(small_ref.at[here], small_in.at[here], l_s.at[1])
    for j, index in enumerate(others):
        fly.send(frames_ref, frames_out.at[here, :, frame_mine], f_s.at[j], f_r.at[here], chip(index))
        fly.send(small_ref.at[index], small_in.at[here], m_s.at[j], m_r.at[here], chip(index))

    near_by = ((y, 1 - x), (1 - y, x), (1 - y, 1 - x))
    up_copy = fly.local(up_ref.at[2 * y + x], up_in.at[core, 2 * y + x], p_s.at[0])
    for j, (ty, tx) in enumerate(near_by):
        fly.send(
            up_ref.at[2 * ty + tx],
            up_in.at[core, 2 * y + x],
            p_s.at[j + 1],
            p_r.at[j + 1],
            {"yb": ty, "xc": tx},
        )
    fly.send(down_ref, down_in, p_s.at[4], p_r.at[4], core_peer)

    def feed_forward_landed():
        up_copy.wait()
        for j, (ty, tx) in enumerate(near_by):
            landed(up_in.at[core, 2 * ty + tx], p_r.at[j + 1], {"yb": ty, "xc": tx})
        fly.send(up_in.at[core], up_in.at[core], p_s.at[5], p_r.at[5], core_peer)
        hid = down_ref.shape[0]
        landed(down_in, p_r.at[4], core_peer)
        for side in range(2):

            @pl.when(core == side)
            def _(side=side):
                down_out[side * hid : (side + 1) * hid, :] = down_ref[...].astype(F32)
                down_out[(1 - side) * hid : (2 - side) * hid, :] = down_in[...].astype(F32)

    def feed_forward_rows():
        hid = down_ref.shape[0]
        landed(up_in.at[1 - core], p_r.at[5], core_peer)
        for slot in range(outer):
            for place in range(PLANE):
                for side in range(2):
                    column = ((slot * PLANE + place) * 2 + side) * hid
                    up_out[:, column : column + hid] = up_in[side, place, :, slot * hid : (slot + 1) * hid].astype(F32)

    def slot_at(step):
        if step == outer - 1:
            return z
        falling = outer - 1 - step
        falling = jnp.where(falling > z, falling, falling - 1)
        rising = jnp.where(step < z, step, step + 1)
        return jnp.where(z < part_slots, falling, rising)

    units = [(slot_at(step), p) for step in range(outer) for p in range(total)]

    def turns(p, slot):
        turn = (slot + p) % 2
        first = ((y + 1 - turn) % 2, (x + turn) % 2)
        second = ((y + turn) % 2, (x + 1 - turn) % 2)
        return first, second

    def device(place):
        return {"yb": place[0], "xc": place[1]}

    def start(slot, p):
        first, _ = turns(p, slot)
        fly.send(
            source(p, slot, 1 - y, 1 - x), near[p].at[slot, 1], s1.at[p, slot, 1], r1.at[p, slot, 1], device(first)
        )
        fly.send(
            source(p, slot, first[0], first[1]), near[p].at[slot, 0], s1.at[p, slot, 0], r1.at[p, slot, 0], device(first)
        )

    def summed_over(p):
        return (x, {"xc": 1 - x}) if forms[p] == OVER_X else (y, {"yb": 1 - y})

    def pass_on(slot, p):
        rows = plane[p].shape[1]
        if p not in near:
            index, peer = summed_over(p)
            fly.send(source(p, slot, 1 - index), plane[p].at[slot], s2.at[p, slot], r2.at[p, slot], peer)
            return
        first, second = turns(p, slot)
        landed(near[p].at[slot, 1], r1.at[p, slot, 1], device(first))
        row_add(near[p].at[slot, 1], near[p].at[slot, 1], source(p, slot, second[0], second[1]), rows)
        fly.send(near[p].at[slot, 1], plane[p].at[slot], s2.at[p, slot], r2.at[p, slot], device(second))
        landed(near[p].at[slot, 0], r1.at[p, slot, 0], device(first))
        row_add(near[p].at[slot, 0], near[p].at[slot, 0], source(p, slot, y, x), rows)

    def plane_total(slot, p):
        rows = plane[p].shape[1]
        if p not in near:
            index, peer = summed_over(p)
            landed(plane[p].at[slot], r2.at[p, slot], peer)
            row_add(plane[p].at[slot], plane[p].at[slot], source(p, slot, index), rows)
            return
        _, second = turns(p, slot)
        landed(plane[p].at[slot], r2.at[p, slot], device(second))
        row_add(plane[p].at[slot], plane[p].at[slot], near[p].at[slot, 0], rows)

    def along(slot, p, last):
        rows, width = plane[p].shape[1:]
        if not last:
            for way, when, edge, ahead, behind in (
                (1, slot < z, z == outer - 1, below, above),
                (0, slot > z, z == 0, above, below),
            ):
                link = chain[p].at[slot + 1 - way]

                @pl.when(jnp.logical_and(when, jnp.logical_not(edge)))
                def _(way=way, link=link, behind=behind):
                    landed(link, zr.at[p, way, slot], behind)
                    row_add(plane[p].at[slot], plane[p].at[slot], link, rows)

                fly.send(plane[p].at[slot], link, zs.at[p, way, slot], zr.at[p, way, slot], ahead, when)
            return
        has_above, has_below = z < outer - 1, z > 0
        for way, when, behind in ((1, has_above, above), (0, has_below, below)):

            @pl.when(when)
            def _(way=way, behind=behind):
                landed(chain[p].at[slot + 1 - way], zr.at[p, way, slot], behind)

        step = 16 if rows % 16 == 0 else rows
        i, part = pieces[p]
        column = pl.multiple_of((2 * part + core) * width, width)

        def chunk(index, carry):
            at = pl.ds(pl.multiple_of(index * step, step), step)
            upper = jnp.where(has_above, chain[p][slot, at, :].astype(F32), 0.0)
            lower = jnp.where(has_below, chain[p][slot + 1, at, :].astype(F32), 0.0)
            outs[i][at, pl.ds(column, width)] = plane[p][slot, at, :].astype(F32) + upper + lower
            return carry

        lax.fori_loop(0, rows // step, chunk, 0)
        block = outs[i].at[:, pl.ds(column, width)]
        fly.send(block, block, o_s.at[p], o_r.at[p], core_peer)

    waiting = set(split)

    def begin(unit):
        slot, p = units[unit]
        if p not in near:
            return
        if pieces[p][0] in waiting:
            joined(pieces[p][0])
            waiting.discard(pieces[p][0])
        start(slot, p)

    for unit in range(min(AHEAD, len(units))):
        begin(unit)
    for tick in range(len(units) + LAG_CHAIN):
        if tick < len(units):
            pass_on(*units[tick])
            if tick + AHEAD < len(units):
                begin(tick + AHEAD)
        if 0 <= tick - LAG_PLANE < len(units):
            plane_total(*units[tick - LAG_PLANE])
        if tick == 4:
            feed_forward_landed()
        if tick == 10:
            feed_forward_rows()
        if 0 <= tick - LAG_CHAIN < len(units):
            unit = tick - LAG_CHAIN
            along(*units[unit], unit >= (outer - 1) * total)
        if tick == total:
            frame_copy.wait()
            for index in others:
                landed(frames_out.at[index, :, frame_mine], f_r.at[index], chip(index))
            fly.send(frames_out.at[:, :, frame_mine], frames_out.at[:, :, frame_mine], p_s.at[6], p_r.at[6], core_peer)
            small_copy.wait()
            for index in others:
                landed(small_in.at[index], m_r.at[index], chip(index))
            small_own[...] = jnp.sum(small_in[...], axis=0)
            fly.send(small_own, small_peer, l_s.at[2], l_s.at[3], core_peer)

    landed(frames_out.at[:, :, frame_other], p_r.at[6], core_peer)
    landed(small_peer, l_s.at[3], core_peer)
    small_out[...] = small_own[...] + small_peer[...]
    for p, (i, part) in enumerate(pieces):
        width = width_of(p)
        column = pl.multiple_of((2 * part + 1 - core) * width, width)
        landed(outs[i].at[:, pl.ds(column, width)], o_r.at[p], core_peer)
    fly.drain()


def reduce_weights(outer, kinds, grads, frames, small, up, down):
    shards = outer * PLANE
    shaped, shapes, near, plane, chain, whole = [], [], [], [], [], []
    for (parts, form), grad in zip(kinds, grads, strict=True):
        full_width = grad.shape[-1] // 2 if form == SPLIT else grad.shape[-1]
        if form in (PLAIN, SPLIT):
            lead = outer // 2 if form == SPLIT else outer
            grad = grad.reshape(lead, 2, 2, -1, grad.shape[-1])
        rows, width = grad.shape[-2], full_width // parts
        shaped.append(grad)
        shapes.append(jax.ShapeDtypeStruct((rows, 2 * full_width), F32))
        for _ in range(parts):
            if form in (PLAIN, SPLIT):
                near.append(pltpu.VMEM((outer, 2, rows, width), BF))
            plane.append(pltpu.VMEM((outer, rows, width), BF))
            chain.append(pltpu.VMEM((outer + 1, rows, width), BF))
        if form == SPLIT:
            whole.append(pltpu.VMEM((outer, 2, 2, rows, full_width), BF))
    shapes.append(jax.ShapeDtypeStruct((shards, frames.shape[0], 2 * frames.shape[1]), frames.dtype))
    shapes.append(jax.ShapeDtypeStruct(small.shape[1:], F32))
    shapes.append(jax.ShapeDtypeStruct((up.shape[1], 2 * PLANE * up.shape[2]), F32))
    shapes.append(jax.ShapeDtypeStruct((2 * down.shape[0], down.shape[1]), F32))
    dma = pltpu.SemaphoreType.DMA
    count, total, nsplit = len(kinds), len(plane), len(whole)
    results = pl.pallas_call(
        functools.partial(reduce_kernel, outer, kinds),
        out_shape=shapes,
        in_specs=[VM] * (count + 4),
        out_specs=[VM] * (count + 4),
        scratch_shapes=[
            *near,
            *plane,
            *chain,
            *whole,
            pltpu.VMEM(small.shape, F32),
            pltpu.VMEM(small.shape[1:], F32),
            pltpu.VMEM(small.shape[1:], F32),
            pltpu.VMEM((2, *up.shape), up.dtype),
            pltpu.VMEM(down.shape, down.dtype),
            dma((nsplit,)),
            dma((nsplit,)),
            dma((nsplit,)),
            dma((total, outer, 2)),
            dma((total, outer, 2)),
            dma((total, outer)),
            dma((total, outer)),
            dma((total, 2, outer)),
            dma((total, 2, outer)),
            dma((total,)),
            dma((total,)),
            dma((shards,)),
            dma((shards,)),
            dma((shards,)),
            dma((shards,)),
            dma((4,)),
            dma((7,)),
            dma((7,)),
        ],
        cost_estimate=pl.CostEstimate(flops=10**11, bytes_accessed=10**8, transcendentals=0),
        compiler_params=pltpu.CompilerParams(
            collective_id=3, has_side_effects=True, vmem_limit_bytes=67043328
        ),
        name="reduce_weights",
    )(*shaped, frames, small, up, down)
    return results[:count], *results[count:]


def gather(value, axes, axis=0):
    return lax.all_gather(value, axes, axis=axis, tiled=True)


def scatter(value, axes, axis=0):
    return lax.psum_scatter(value, axes, scatter_dimension=axis, tiled=True)


def swap(value, split_axis, concat_axis):
    return lax.all_to_all(value, "sp", split_axis=split_axis, concat_axis=concat_axis, tiled=True)


def rms_scale(total):
    return lax.rsqrt(total / D + EPSILON)


def square_sum(values):
    return jnp.sum(values * values, axis=1)


def rms_back(values, gain, grad):
    scaled = grad * gain
    return scaled, jnp.sum(scaled * values, axis=1)


def rms_finish(values, inverse, scaled, total):
    column = inverse[:, None]
    return scaled * column - values * (column * column * column) * (total / D)[:, None]


def body(
    tokens,
    text,
    clip_frames,
    timestep,
    mod_weight,
    mod_bias,
    qk_gains,
    self_in,
    self_out,
    cross_q,
    cross_kv,
    cross_out,
    mlp_in,
    mlp_out,
    cotangent,
):
    half = D // 2
    row_count = tokens.shape[0]
    frame_count = row_count // FRAME_TOK
    group_frames = timestep.shape[1]
    shards = D // self_in.shape[1]
    outer = shards // PLANE
    core = lax.axis_index("sp")
    chip = lax.axis_index(FS)
    in_rows = self_in.shape[1]
    own_frame = core * frame_count

    bias_len, gain_len = mod_bias.shape[1], qk_gains.shape[2]
    small_len = bias_len + 4 * gain_len
    small_rows = 8
    small_width = -(-(small_len + group_frames) // (small_rows * 128)) * 128
    small_room = small_rows * small_width

    small = jnp.concatenate(
        [
            mod_bias[0].astype(F32),
            qk_gains[0].reshape(-1).astype(F32),
            timestep[0].astype(F32),
            jnp.zeros((small_room - small_len - group_frames,), F32),
        ]
    ).reshape(small_rows, small_width)
    gathered = gather_weights(
        outer,
        ((0, False), (1, False), (3, False), (1, True), (2, False), (1, False), (1, True)),
        [small, *(w[0] for w in (mod_weight, self_in, self_out, cross_kv, cross_q, cross_out))],
        mlp_in[0],
        text,
    )
    small_all, mod_matrix, self_proj, self_back, cross_kvproj, cross_qproj, cross_back = gathered[:7]
    up_matrix, text_all = gathered[7:]
    hid = mlp_out.shape[1] // 2
    down_part = lax.dynamic_slice_in_dim(mlp_out[0], core * hid, hid, 0)
    down_part, small_all = lax.optimization_barrier((down_part, small_all))
    down_matrix = gather(down_part, "za")
    small_all = small_all.reshape(shards, small_room)
    bias_all = small_all[:, :bias_len].reshape(-1)
    gain_all = (
        small_all[:, bias_len:small_len]
        .reshape(shards, 4, gain_len)
        .transpose(1, 0, 2)
        .reshape(4, 2, half)
    )
    gain_own = lax.dynamic_index_in_dim(gain_all, core, 1, keepdims=False)
    steps_all = small_all[:, small_len : small_len + group_frames].reshape(-1)

    live_keys = clip_frames * FRAME_TOK
    all_keys = jnp.full((1,), TXT, jnp.int32)
    own_steps = lax.dynamic_slice_in_dim(timestep[0], own_frame, frame_count)
    clip_pos = jnp.arange(group_frames, dtype=jnp.int32)
    cosine, sine = rotary_tables(
        jnp.repeat(clip_pos, FRAME_TOK),
        jnp.tile(jnp.arange(FRAME_TOK, dtype=jnp.int32), group_frames),
    )
    sinus = sinus_features(timestep[0]).astype(BF)

    mod_half = product(sinus, mod_matrix)
    mod_half = mod_half + lax.dynamic_slice_in_dim(bias_all, core * 3 * D, 3 * D)[None]
    modulation = swap(mod_half, 0, 1)
    shift_one, scale_one, gate_one, shift_two, scale_two, gate_two = jnp.split(
        modulation, 6, axis=1
    )

    grad_branch = frame_scaled(cotangent.astype(F32), gate_two).astype(BF)
    exchange = [(0, 1), (1, 0)]
    beside = [
        grad_branch,
        lax.ppermute(grad_branch, "xc", exchange),
        lax.ppermute(grad_branch, "yb", exchange),
        lax.ppermute(grad_branch, PL, [(0, 3), (1, 2), (2, 1), (3, 0)]),
    ]

    residual = tokens.astype(F32)
    attn_float, back_attn_input = jax.vjp(modulated, residual, shift_one, scale_one)
    attn_input = gather(attn_float.astype(BF), "sp")
    joined = product(attn_input, self_proj)
    raw_q, raw_k, raw_v = joined[:, :half], joined[:, half : 2 * half], joined[:, 2 * half :]
    totals = lax.psum(jnp.stack([square_sum(raw_q), square_sum(raw_k)]), "sp")
    inv_q, inv_k = rms_scale(totals[0]), rms_scale(totals[1])
    query = rotate(raw_q * inv_q[:, None] * gain_own[0], cosine, sine).astype(BF)
    key = rotate(raw_k * inv_k[:, None] * gain_own[1], cosine, sine).astype(BF)
    value = raw_v.astype(BF)
    self_mixed, self_lse = attend_forward(live_keys, query, key, value)
    self_branch = pair_sum(product(self_mixed, self_back))
    residual = residual + frame_scaled(self_branch, gate_one)
    residual, *beside = lax.optimization_barrier((residual, *beside))
    beside = jnp.stack(beside)
    grad_branch_all = jnp.stack([beside, lax.ppermute(beside, "sp", exchange)], axis=1).reshape(-1, D)

    text_raw = product(text_all, cross_kvproj)
    raw_ck, raw_cv = text_raw[:, :half], text_raw[:, half:]
    inv_ck = rms_scale(lax.psum(square_sum(raw_ck)[None], "sp")[0])
    cross_key = (raw_ck * inv_ck[:, None] * gain_own[3]).astype(BF)
    cross_value = raw_cv.astype(BF)

    cross_float, back_cross_norm = jax.vjp(layer_norm, residual)
    cross_input = gather(cross_float.astype(BF), "sp")
    cross_raw = product(cross_input, cross_qproj)
    inv_cq = rms_scale(lax.psum(square_sum(cross_raw)[None], "sp")[0])
    cross_query = (cross_raw * inv_cq[:, None] * gain_own[2]).astype(BF)
    cross_mixed, cross_lse = attend_forward(all_keys, cross_query, cross_key, cross_value)
    residual = residual + pair_sum(product(cross_mixed, cross_back))

    mlp_float, back_mlp_input = jax.vjp(modulated, residual, shift_two, scale_two)
    mlp_input = plane_gather(mlp_float.astype(BF))
    up_proj = product(mlp_input, up_matrix)
    activated_float, back_gelu = jax.vjp(
        lambda inner: jax.nn.gelu(inner, approximate=True), up_proj
    )
    activated = activated_float.astype(BF)

    mlp_part = product(activated, down_matrix).astype(BF)

    grad_rows = cotangent.astype(F32)
    grad_down = product_tn(activated, grad_branch_all).astype(BF)
    grad_up_low = back_gelu(product_nt(grad_branch_all, down_matrix))[0].astype(BF)
    grad_up = product_tn(mlp_input, grad_up_low).astype(BF)
    grad_mlp_part = product_nt(grad_up_low, up_matrix).astype(BF)
    grad_mlp_part, grad_up, grad_down = lax.optimization_barrier((grad_mlp_part, grad_up, grad_down))
    down_owned = scatter(grad_down, "za")
    up_owned = scatter(grad_up, "za")
    mlp_branch, grad_mlp_input = plane_sum(mlp_part, grad_mlp_part)
    output = (residual + frame_scaled(mlp_branch, gate_two)).astype(BF)
    grad_gate_two = frame_sum(grad_rows * mlp_branch, frame_count)
    grad_from_mlp, grad_shift_two, grad_scale_two = back_mlp_input(grad_mlp_input)
    grad_rows = grad_rows + grad_from_mlp

    grad_low = gather(grad_rows.astype(BF), "sp")
    grad_cross_back = product_tn(cross_mixed, grad_low).astype(BF)
    grad_cross_mixed = product_nt(grad_low, cross_back).astype(BF)
    grad_cq, grad_ck, grad_cv = attend_backward(
        all_keys, cross_query, cross_key, cross_value, cross_lse, grad_cross_mixed
    )
    grad_cq, grad_ck = grad_cq.astype(F32), grad_ck.astype(F32)
    grad_gain_two = jnp.sum(grad_cq * cross_raw * inv_cq[:, None], axis=0)
    grad_gain_three = jnp.sum(grad_ck * raw_ck * inv_ck[:, None], axis=0)
    scaled_cq, dots_cq = rms_back(cross_raw, gain_own[2], grad_cq)
    scaled_ck, dots_ck = rms_back(raw_ck, gain_own[3], grad_ck)
    dots = lax.psum(jnp.concatenate([dots_cq, dots_ck])[None], "sp")[0]
    dots_cq, dots_ck = dots[: dots_cq.shape[0]], dots[dots_cq.shape[0] :]
    grad_cross_low = rms_finish(cross_raw, inv_cq, scaled_cq, dots_cq).astype(BF)
    grad_text_low = jnp.concatenate(
        [rms_finish(raw_ck, inv_ck, scaled_ck, dots_ck).astype(BF), grad_cv], axis=1
    )
    grad_cross_qproj = product_tn(cross_input, grad_cross_low).astype(BF)
    grad_cross_kvproj = product_tn(text_all, grad_text_low).astype(BF)
    place_y, place_x = lax.axis_index("yb"), lax.axis_index("xc")
    kv_parts = grad_cross_kvproj.reshape(outer, 2, 2, in_rows, -1)
    q_parts = grad_cross_qproj.reshape(outer, 2, 2, in_rows, -1)
    kv_sent = lax.ppermute(lax.dynamic_index_in_dim(kv_parts, 1 - place_y, 1, False), "yb", exchange)
    q_sent = lax.ppermute(lax.dynamic_index_in_dim(q_parts, 1 - place_x, 2, False), "xc", exchange)
    grad_cross_input = pair_sum(product_nt(grad_cross_low, cross_qproj))
    grad_rows = grad_rows + back_cross_norm(grad_cross_input)[0]

    grad_gate_one = frame_sum(grad_rows * self_branch, frame_count)
    grad_self_low = gather(frame_scaled(grad_rows, gate_one).astype(BF), "sp")
    grad_self_back = product_tn(self_mixed, grad_self_low).astype(BF)
    grad_self_mixed = product_nt(grad_self_low, self_back).astype(BF)
    grad_q, grad_k, grad_v = attend_backward(
        live_keys, query, key, value, self_lse, grad_self_mixed
    )
    grad_q = rotate(grad_q.astype(F32), cosine, -sine)
    grad_k = rotate(grad_k.astype(F32), cosine, -sine)
    grad_gain_zero = jnp.sum(grad_q * raw_q * inv_q[:, None], axis=0)
    grad_gain_one = jnp.sum(grad_k * raw_k * inv_k[:, None], axis=0)
    scaled_q, dots_q = rms_back(raw_q, gain_own[0], grad_q)
    scaled_k, dots_k = rms_back(raw_k, gain_own[1], grad_k)
    dots = lax.psum(jnp.stack([dots_q, dots_k]), "sp")
    grad_joined_low = jnp.concatenate(
        [
            rms_finish(raw_q, inv_q, scaled_q, dots[0]).astype(BF),
            rms_finish(raw_k, inv_k, scaled_k, dots[1]).astype(BF),
            grad_v,
        ],
        axis=1,
    )
    grad_self_proj = product_tn(attn_input, grad_joined_low).astype(BF)
    grad_attn_input = pair_sum(product_nt(grad_joined_low, self_proj))
    grad_from_attn, grad_shift_one, grad_scale_one = back_attn_input(grad_attn_input)
    grad_rows = grad_rows + grad_from_attn

    grad_modulation = jnp.concatenate(
        [grad_shift_one, grad_scale_one, grad_gate_one, grad_shift_two, grad_scale_two, grad_gate_two],
        axis=1,
    )
    grad_mod_half = swap(grad_modulation, 1, 0)
    grad_gains = jnp.stack([grad_gain_zero, grad_gain_one, grad_gain_two, grad_gain_three])
    both = jnp.arange(2)[None, :, None] == core
    grad_gains = jnp.where(both, grad_gains[:, None, :], 0.0).reshape(4, shards, gain_len)
    grad_small = jnp.concatenate(
        [
            jnp.sum(grad_modulation, axis=0).reshape(shards, bias_len),
            grad_gains.transpose(1, 0, 2).reshape(shards, 4 * gain_len),
            jnp.zeros((shards, small_room - small_len), F32),
        ],
        axis=1,
    ).reshape(shards, small_rows, small_width)
    kv_near = lax.dynamic_index_in_dim(kv_parts, place_y, 1, False) + kv_sent
    q_near = lax.dynamic_index_in_dim(q_parts, place_x, 2, False) + q_sent
    owned, grad_mod_all, small_owned, mlp_in_grad, mlp_out_grad = reduce_weights(
        outer,
        ((1, OVER_Y), (2, OVER_X), (1, SPLIT), (1, SPLIT), (3, PLAIN)),
        [q_near, kv_near, grad_cross_back, grad_self_back, grad_self_proj],
        grad_mod_half.astype(BF),
        grad_small,
        up_owned.reshape(PLANE, -1, up_owned.shape[1]),
        down_owned,
    )
    cross_q_grad, cross_kv_grad, cross_out_grad, self_out_grad, self_in_grad = owned
    small_owned = small_owned.reshape(-1)[:small_len]
    sinus_all = sinus_features(steps_all).astype(BF)
    own_features = mod_weight.shape[1]
    sinus_own = lax.dynamic_slice_in_dim(sinus_all, chip * own_features, own_features, 1)
    mod_weight_grad = product_tn(sinus_own, grad_mod_all.reshape(-1, 6 * D))
    return (
        output,
        grad_rows,
        mod_weight_grad[None],
        small_owned[None, :bias_len],
        small_owned[bias_len:].reshape(1, 4, gain_len),
        self_in_grad[None],
        self_out_grad[None],
        cross_q_grad[None],
        cross_kv_grad[None],
        cross_out_grad[None],
        mlp_in_grad[None],
        mlp_out_grad[None],
    )


def solution(mesh):
    chips, cores = mesh.shape["fsdp"], mesh.shape["sp"]
    grid = mesh.devices.reshape(chips // PLANE, 2, PLANE // 2, cores)
    inner = Mesh(grid, ALL)
    rows, second = P(ALL, None), P(None, FS, None)
    in_specs = (
        rows,
        rows,
        P(FS),
        P(FS, None),
        second,
        P(None, FS),
        P(None, None, FS),
        *([second] * 7),
        rows,
    )
    out_specs = (rows, rows, second, P(None, FS), P(None, None, FS), *([second] * 7))

    return jax.shard_map(body, mesh=inner, in_specs=in_specs, out_specs=out_specs, check_vma=False)
```

```python
import functools
import math

import jax
import jax.numpy as jnp
from jax import lax
from jax.experimental import pallas as pl
from jax.experimental.pallas import tpu as pltpu
from jax.sharding import Mesh
from jax.sharding import PartitionSpec as P


D = 1536
HD = 128
TXT = 512
FREQ = 256
WP = 8
FRAME_TOK = 64
PLANE = 4

EPSILON = 1e-06
NEGATIVE = -1e30

FS = ("za", "yb", "xc")
PL = ("yb", "xc")
ALL = ("za", "yb", "xc", "sp")
SCALE = 1.0 / math.sqrt(HD)
MESH = pl.DeviceIdType.MESH
BF = jnp.bfloat16
F32 = jnp.float32


def product(left, right):
    return jnp.dot(left, right, preferred_element_type=F32)


def product_tn(left, right):
    return lax.dot_general(left, right, (((0,), (0,)), ((), ())), preferred_element_type=F32)


def product_nt(left, right):
    return lax.dot_general(left, right, (((1,), (1,)), ((), ())), preferred_element_type=F32)


def layer_norm(values):
    centred = values - jnp.mean(values, axis=-1, keepdims=True)
    return centred * lax.rsqrt(jnp.mean(centred * centred, axis=-1, keepdims=True) + EPSILON)


def sinus_features(steps):
    half_dim = FREQ // 2
    rates = jnp.exp(jnp.arange(half_dim).astype(F32) * (-math.log(10000.0) / half_dim))
    angles = steps.astype(F32)[:, None] * rates[None, :]
    return jnp.concatenate([jnp.cos(angles), jnp.sin(angles)], axis=1)


def rotary_tables(frame_pos, token_spot):
    half_dim = HD // 2
    side_pairs = HD // 6
    lead_pairs = half_dim - 2 * side_pairs
    pair_index = jnp.arange(half_dim)
    log_base = -math.log(10000.0)
    lead_part = pair_index < lead_pairs
    side_part = jnp.logical_and(pair_index >= lead_pairs, pair_index < lead_pairs + side_pairs)
    last_part = pair_index >= lead_pairs + side_pairs
    frame_rate = jnp.where(
        lead_part, jnp.exp(log_base * pair_index.astype(F32) / lead_pairs), 0.0
    )
    row_rate = jnp.where(
        side_part, jnp.exp(log_base * (pair_index - lead_pairs).astype(F32) / side_pairs), 0.0
    )
    column_rate = jnp.where(
        last_part,
        jnp.exp(log_base * (pair_index - lead_pairs - side_pairs).astype(F32) / side_pairs),
        0.0,
    )
    patch_row = (token_spot // WP).astype(F32)
    patch_column = (token_spot % WP).astype(F32)
    angles = (
        frame_pos.astype(F32)[:, None] * frame_rate[None, :]
        + patch_row[:, None] * row_rate[None, :]
        + patch_column[:, None] * column_rate[None, :]
    )
    return (jnp.cos(angles), jnp.sin(angles))


def modulated(residual, shift, scale):
    frames = shift.shape[0]
    normed = layer_norm(residual).reshape(frames, -1, residual.shape[1])
    return (normed * (1.0 + scale[:, None, :]) + shift[:, None, :]).reshape(residual.shape)


def frame_scaled(rows, gate):
    frames = gate.shape[0]
    return (rows.reshape(frames, -1, rows.shape[1]) * gate[:, None, :]).reshape(rows.shape)


def frame_sum(values, frames):
    return jnp.sum(values.reshape(frames, -1, values.shape[1]), axis=1)


VM = pl.BlockSpec(memory_space=pltpu.VMEM)
SM = pl.BlockSpec(memory_space=pltpu.SMEM)
ANY = pl.BlockSpec(memory_space=pl.ANY)


def row_add(target, left, right, rows):
    step = 32 if rows % 32 == 0 else rows

    def chunk(index, carry):
        at = pl.ds(pl.multiple_of(index * step, step), step)
        target[at, :] = left[at, :] + right[at, :]
        return carry

    lax.fori_loop(0, rows // step, chunk, 0)


def row_sum(target, left, right, rows):
    step = 16 if rows % 16 == 0 else rows

    def chunk(index, carry):
        at = pl.ds(pl.multiple_of(index * step, step), step)
        target[at, :] = left[at, :].astype(F32) + right[at, :].astype(F32)
        return carry

    lax.fori_loop(0, rows // step, chunk, 0)


class Flights:
    def __init__(self):
        self.sent = []

    def send(self, source, target, send_sem, recv_sem, device, when=None):
        copy = pltpu.make_async_remote_copy(
            src_ref=source,
            dst_ref=target,
            send_sem=send_sem,
            recv_sem=recv_sem,
            device_id=device,
            device_id_type=MESH,
        )
        if when is None:
            copy.start()
        else:
            pl.when(when)(copy.start)
        self.sent.append((when, copy))

    def local(self, source, target, sem):
        copy = pltpu.make_async_copy(source, target, sem)
        copy.start()
        return copy

    def drain(self):
        for when, copy in self.sent:
            if when is None:
                copy.wait_send()
            else:
                pl.when(when)(copy.wait_send)


def landed(target, sem, device):
    pltpu.make_async_remote_copy(
        src_ref=target,
        dst_ref=target,
        send_sem=sem,
        recv_sem=sem,
        device_id=device,
        device_id_type=MESH,
    ).wait_recv()


def greet(devices, optional=()):
    barrier = pltpu.get_barrier_semaphore()
    for device in devices:
        pl.semaphore_signal(barrier, inc=1, device_id=device, device_id_type=MESH)
    for when, device in optional:

        @pl.when(when)
        def _(device=device):
            pl.semaphore_signal(barrier, inc=1, device_id=device, device_id_type=MESH)

    count = len(devices)
    for when, _ in optional:
        count = count + when.astype(jnp.int32)
    pl.semaphore_wait(barrier, count)


def raw_views(joint, refs):
    if joint:
        rows_ref, rest = refs[0], refs[1:]
        width = rows_ref.shape[1] // 3
        spans = ((rows_ref, 0), (rows_ref, width), (rows_ref, 2 * width))
    else:
        rows_ref, keys_ref, rest = refs[0], refs[1], refs[2:]
        width = rows_ref.shape[1]
        spans = ((rows_ref, 0), (keys_ref, 0), (keys_ref, width))

    def view(which, head):
        ref, base = spans[which]
        return ref[:, base + head * HD : base + (head + 1) * HD]

    return view, width, rest


def turned(values, cos_ref, sin_ref, sign):
    return values * cos_ref[...] + sign * (pltpu.roll(values, HD // 2, 1) * sin_ref[...])


def attend_forward_kernel(joint, rotary, live_ref, *refs):
    view, width, refs = raw_views(joint, refs)
    gain_ref, cos_ref, sin_ref, refs = *refs[:3], refs[3:]
    out_ref, lse_ref, query_ref, key_ref, inv_q_ref, inv_k_ref, refs = *refs[:6], refs[6:]
    q_sum, k_sum, q_peer, k_peer, send, recv = refs
    heads = width // HD
    core_peer = {"sp": 1 - lax.axis_index("sp")}
    fly = Flights()
    greet((core_peer,))
    for which, own, peer in ((0, q_sum, q_peer), (1, k_sum, k_peer)):
        total = view(which, 0) * view(which, 0)
        for head in range(1, heads):
            total = total + view(which, head) * view(which, head)
        own[...] = jnp.broadcast_to(jnp.sum(total, axis=1, keepdims=True), own.shape)
        fly.send(own, peer, send.at[which], recv.at[which], core_peer)
    for which, own, peer, kept in ((0, q_sum, q_peer, inv_q_ref), (1, k_sum, k_peer, inv_k_ref)):
        landed(peer, recv.at[which], core_peer)
        kept[...] = lax.rsqrt((own[...] + peer[...]) / D + EPSILON)
    rows, keys = query_ref.shape[0], key_ref.shape[0]
    spot = lax.broadcasted_iota(jnp.int32, (rows, keys), 1)
    allowed = spot < live_ref[0]
    for head in range(heads):
        part = slice(head * HD, (head + 1) * HD)
        query = view(0, head) * inv_q_ref[...] * gain_ref[0:1, part]
        key = view(1, head) * inv_k_ref[...] * gain_ref[1:2, part]
        if rotary:
            query, key = turned(query, cos_ref, sin_ref, 1.0), turned(key, cos_ref, sin_ref, 1.0)
        query, key, value = query.astype(BF), key.astype(BF), view(2, head).astype(BF)
        query_ref[:, part], key_ref[:, part] = query, key
        scores = jnp.where(allowed, product_nt(query, key) * SCALE, NEGATIVE)
        row_max = jnp.max(scores, axis=1, keepdims=True)
        log_total = row_max + jnp.log(jnp.sum(jnp.exp(scores - row_max), axis=1, keepdims=True))
        weights = jnp.exp(scores - log_total).astype(BF)
        out_ref[:, part] = product(weights, value).astype(BF)
        lse_ref[:, part] = jnp.broadcast_to(log_total, (rows, HD))
    fly.drain()


def attend_backward_kernel(joint, rotary, live_ref, *refs):
    view, width, refs = raw_views(joint, refs)
    gain_ref, cos_ref, sin_ref, refs = *refs[:3], refs[3:]
    query_ref, key_ref, lse_ref, inv_q_ref, inv_k_ref, do_ref, refs = *refs[:6], refs[6:]
    if joint:
        grad_refs, refs = ((refs[0], 0), (refs[0], width), (refs[0], 2 * width)), refs[1:]
    else:
        grad_refs, refs = ((refs[0], 0), (refs[1], 0), (refs[1], width)), refs[2:]
    gain_out, scaled_q, scaled_k, q_dot, k_dot, q_peer, k_peer, send, recv = refs
    heads = width // HD
    core_peer = {"sp": 1 - lax.axis_index("sp")}
    fly = Flights()
    greet((core_peer,))
    rows, keys = query_ref.shape[0], key_ref.shape[0]
    spot = lax.broadcasted_iota(jnp.int32, (rows, keys), 1)
    allowed = spot < live_ref[0]
    dots = [None, None]
    gain_out[...] = jnp.zeros_like(gain_out)
    for head in range(heads):
        part = slice(head * HD, (head + 1) * HD)
        query, key, grad = query_ref[:, part], key_ref[:, part], do_ref[:, part]
        value = view(2, head).astype(BF)
        scores = jnp.where(allowed, product_nt(query, key) * SCALE, NEGATIVE)
        weights = jnp.exp(scores - lse_ref[:, head * HD : head * HD + 1])
        grad_weights = product_nt(grad, value)
        delta = jnp.sum(weights * grad_weights, axis=1, keepdims=True)
        grad_scores = (weights * (grad_weights - delta)).astype(BF)
        grad_query = (product(grad_scores, key) * SCALE).astype(BF).astype(F32)
        grad_key = (product_tn(grad_scores, query) * SCALE).astype(BF).astype(F32)
        grad_value = product_tn(weights.astype(BF), grad).astype(BF)
        ref, base = grad_refs[2]
        ref[:, base + head * HD : base + (head + 1) * HD] = grad_value
        for which, grad_rows, inverse, held in ((0, grad_query, inv_q_ref, scaled_q), (1, grad_key, inv_k_ref, scaled_k)):
            if rotary:
                grad_rows = turned(grad_rows, cos_ref, sin_ref, -1.0)
            raw = view(which, head)
            gain_out[which : which + 1, part] = jnp.sum(grad_rows * raw * inverse[...], axis=0, keepdims=True)
            scaled = grad_rows * gain_ref[which : which + 1, part]
            held[:, part] = scaled
            dots[which] = scaled * raw if head == 0 else dots[which] + scaled * raw
    for which, own, peer in ((0, q_dot, q_peer), (1, k_dot, k_peer)):
        own[...] = jnp.broadcast_to(jnp.sum(dots[which], axis=1, keepdims=True), own.shape)
        fly.send(own, peer, send.at[which], recv.at[which], core_peer)
    for which, own, peer, inverse, held in (
        (0, q_dot, q_peer, inv_q_ref, scaled_q),
        (1, k_dot, k_peer, inv_k_ref, scaled_k),
    ):
        landed(peer, recv.at[which], core_peer)
        column = inverse[...]
        slope = column * column * column * ((own[...] + peer[...]) / D)
        ref, base = grad_refs[which]
        for head in range(heads):
            part = slice(head * HD, (head + 1) * HD)
            out = held[:, part] * column - view(which, head) * slope
            ref[:, base + head * HD : base + (head + 1) * HD] = out.astype(BF)
    fly.drain()


def attend_call(kernel, joint, rotary, number, live, raws, others, shapes, scratch, flops, exps):
    dma = pltpu.SemaphoreType.DMA
    arrays = [*raws, *others]
    moved = sum(v.size * v.dtype.itemsize for v in [*arrays, *shapes])
    return pl.pallas_call(
        functools.partial(kernel, joint, rotary),
        out_shape=shapes,
        in_specs=[SM] + [VM] * len(arrays),
        out_specs=[VM] * len(shapes),
        scratch_shapes=[*scratch, dma((2,)), dma((2,))],
        compiler_params=pltpu.CompilerParams(collective_id=number, has_side_effects=True),
        cost_estimate=pl.CostEstimate(flops=flops, bytes_accessed=moved, transcendentals=exps),
    )(live, *arrays)


def attend_sizes(raws):
    joint = len(raws) == 1
    rows, keys = raws[0].shape[0], raws[-1].shape[0]
    return joint, rows, keys, raws[0].shape[1] // 3 if joint else raws[0].shape[1]


def attend_forward(live, raws, gains, cosine, sine, rotary, number):
    joint, rows, keys, width = attend_sizes(raws)
    shape = jax.ShapeDtypeStruct
    shapes = [
        shape((rows, width), BF),
        shape((rows, width), F32),
        shape((rows, width), BF),
        shape((keys, width), BF),
        shape((rows, HD), F32),
        shape((keys, HD), F32),
    ]
    scratch = [pltpu.VMEM((n, HD), F32) for n in (rows, keys, rows, keys)]
    work = rows * keys * width
    return attend_call(
        attend_forward_kernel, joint, rotary, number, live, raws, [gains, cosine, sine],
        shapes, scratch, 4 * work, 2 * work // HD,
    )


def attend_backward(live, raws, gains, cosine, sine, rotary, number, saved, grad):
    joint, rows, keys, width = attend_sizes(raws)
    shape = jax.ShapeDtypeStruct
    shapes = [shape(raw.shape, BF) for raw in raws] + [shape((8, width), F32)]
    scratch = [pltpu.VMEM((rows, width), F32), pltpu.VMEM((keys, width), F32)]
    scratch += [pltpu.VMEM((n, HD), F32) for n in (rows, keys, rows, keys)]
    work = rows * keys * width
    return attend_call(
        attend_backward_kernel, joint, rotary, number, live, raws,
        [gains, cosine, sine, *saved, grad], shapes, scratch, 10 * work, work // HD,
    )


ALL_CHIPS, KEEP, HALF_X, HALF_Y = range(4)


def gather_kernel(outer, kinds, *refs):
    full = len(kinds)
    ins, refs = refs[:full], refs[full:]
    mlp_ref, text_ref, refs = refs[0], refs[1], refs[2:]
    outs, refs = list(refs[:full]), refs[full:]
    up_out, text_out, refs = refs[0], refs[1], refs[2:]
    own, refs = refs[:full], refs[full:]
    halves = [i for i, kind in enumerate(kinds) if kind[1] == KEEP]
    form = [kind[1] for kind in kinds]
    whole, refs = refs[: len(halves)], refs[len(halves) :]
    up_own, local_sem, zs, zr, s1, r1, s2, r2, a_s, a_r, f_s, f_r, f_l, t_s = refs
    z, y, x = (lax.axis_index(name) for name in FS)
    core = lax.axis_index("sp")
    here = 2 * y + x
    up = full
    fins = {}
    for j, i in enumerate(halves):
        fins[i] = outs[i]
        outs[i] = whole[j]
    fly = Flights()
    x_peer, y_peer = {"xc": 1 - x}, {"yb": 1 - y}
    diagonal = {"yb": 1 - y, "xc": 1 - x}
    around = ((x_peer, y, 1 - x), (y_peer, 1 - y, x), (diagonal, 1 - y, 1 - x))
    above, below = {"za": z + 1}, {"za": z - 1}
    core_peer = {"sp": 1 - core}
    has_above, has_below = z + 1 < outer, z >= 1
    greet((x_peer, y_peer, diagonal, core_peer), ((has_above, above), (has_below, below)))

    for i, (parts, _) in enumerate(kinds):
        if parts == 0:
            own[i][...] = ins[i][...]
        for part in range(parts):
            width = ins[i].shape[1] // (2 * parts)
            column = pl.multiple_of((2 * part + core) * width, width)
            own[i][:, part * width : (part + 1) * width] = ins[i][:, pl.ds(column, width)]

    def spot(i, slot, ty, tx):
        if form[i] == HALF_X:
            return outs[i].at[slot, tx]
        if form[i] == HALF_Y:
            return outs[i].at[slot, ty]
        return outs[i].at[slot, ty, tx]

    def shard(i, slot):
        return spot(i, slot, y, x) if i < full else up_out.at[slot]

    def z_send(i, way, hop, source=None):
        if hop > outer - 2:
            return
        slot = z - hop if way == 0 else z + hop
        when = jnp.logical_and(has_above, slot >= 0) if way == 0 else jnp.logical_and(has_below, slot < outer)
        fly.send(
            shard(i, slot) if source is None else source,
            shard(i, slot),
            zs.at[i, way, hop],
            zr.at[i, way, hop],
            above if way == 0 else below,
            when,
        )

    def z_slot(way, hop):
        slot = z - 1 - hop if way == 0 else z + 1 + hop
        return slot, (slot >= 0 if way == 0 else slot < outer)

    def z_wait(i, way, hop):
        slot, when = z_slot(way, hop)

        @pl.when(when)
        def _():
            landed(shard(i, slot), zr.at[i, way, hop], below if way == 0 else above)

    def turns(i, slot):
        turn = (slot + i) % 2
        first = ((y + turn) % 2, (x + 1 - turn) % 2)
        second = ((y + 1 - turn) % 2, (x + turn) % 2)
        return first, second

    def xy_own(i, slot, when=None, source=None):
        mine = spot(i, slot, y, x)
        source = mine if source is None else source
        if form[i] in (HALF_X, HALF_Y):
            peer = x_peer if form[i] == HALF_X else y_peer
            fly.send(source, mine, s1.at[i, slot], r1.at[i, slot], peer, when)
            return
        first, second = turns(i, slot)
        fly.send(source, mine, s1.at[i, slot], r1.at[i, slot], {"yb": first[0], "xc": first[1]}, when)
        fly.send(source, mine, s2.at[i, slot, 0], r2.at[i, slot, 0], {"yb": second[0], "xc": second[1]}, when)

    def xy_pass(i, slot, when=None):
        if form[i] in (HALF_X, HALF_Y):
            return
        first, second = turns(i, slot)
        theirs = outs[i].at[slot, first[0], first[1]]

        def wait():
            landed(theirs, r1.at[i, slot], {"yb": first[0], "xc": first[1]})

        if when is None:
            wait()
        else:
            pl.when(when)(wait)
        fly.send(theirs, theirs, s2.at[i, slot, 1], r2.at[i, slot, 1], {"yb": second[0], "xc": second[1]}, when)

    def xy_end(i, slot):
        if form[i] == HALF_X:
            landed(spot(i, slot, y, 1 - x), r1.at[i, slot], x_peer)
            return
        if form[i] == HALF_Y:
            landed(spot(i, slot, 1 - y, x), r1.at[i, slot], y_peer)
            return
        _, second = turns(i, slot)
        device = {"yb": second[0], "xc": second[1]}
        landed(outs[i].at[slot, second[0], second[1]], r2.at[i, slot, 0], device)
        landed(outs[i].at[slot, 1 - y, 1 - x], r2.at[i, slot, 1], device)

    for i in range(full):
        for way in range(2):
            z_send(i, way, 0, own[i])
        xy_own(i, z, None, own[i])
    locals_ = [fly.local(own[i], spot(i, z, y, x), local_sem.at[i]) for i in range(full)]

    fly.send(text_ref, text_out.at[core], t_s.at[0], t_s.at[1], core_peer)
    locals_.append(fly.local(text_ref, text_out.at[core], t_s.at[2]))
    hid = mlp_ref.shape[1] // (outer * PLANE * 2)
    for own_core in range(2):

        @pl.when(core == own_core)
        def _(own_core=own_core):
            for place in range(PLANE):
                for slot in range(outer):
                    column = ((slot * PLANE + place) * 2 + own_core) * hid
                    up_own[place, :, slot * hid : (slot + 1) * hid] = mlp_ref[:, column : column + hid]

    for hop in range(outer - 1):
        for i in range(full):
            for way in range(2):
                slot, when = z_slot(way, hop)
                z_wait(i, way, hop)
                z_send(i, way, hop + 1)
                xy_own(i, slot, when)
        if hop == 0:
            locals_.append(fly.local(up_own.at[here], up_out.at[z, here], local_sem.at[up]))
            for turn, (device, ty, tx) in enumerate(around):
                fly.send(up_own.at[2 * ty + tx], up_out.at[z, here], a_s.at[turn], a_r.at[turn], device)
    for copy in locals_:
        copy.wait()
    for turn, (device, ty, tx) in enumerate(around):
        landed(up_out.at[z, 2 * ty + tx], a_r.at[turn], device)
    for way in range(2):
        z_send(up, way, 0)
    for i in range(full):
        xy_pass(i, z)
    for hop in range(outer - 1):
        for i in range(full):
            for way in range(2):
                slot, when = z_slot(way, hop)
                xy_pass(i, slot, when)
        for way in range(2):
            z_wait(up, way, hop)
            z_send(up, way, hop + 1)
    for i in (*halves, *(i for i in range(full) if i not in halves)):
        for slot in range(outer):
            xy_end(i, slot)
        if i not in halves:
            continue
        j, part = halves.index(i), outer // 2
        width = own[i].shape[-1]
        columns = pl.ds(pl.multiple_of(core * width, width), width)
        theirs, ours = pl.ds((1 - core) * part, part), pl.ds(core * part, part)
        fly.send(outs[i].at[theirs], fins[i].at[:, :, :, :, columns], f_s.at[j], f_r.at[j], core_peer)
        fly.local(outs[i].at[ours], fins[i].at[:, :, :, :, columns], f_l.at[j])
    for j, i in enumerate(halves):
        width = own[i].shape[-1]
        columns = pl.ds(pl.multiple_of(core * width, width), width)
        others = pl.ds(pl.multiple_of((1 - core) * width, width), width)
        ours = pl.ds(core * (outer // 2), outer // 2)
        pltpu.make_async_copy(outs[i].at[ours], fins[i].at[:, :, :, :, columns], f_l.at[j]).wait()
        landed(fins[i].at[:, :, :, :, others], f_r.at[j], core_peer)
    landed(text_out.at[1 - core], t_s.at[1], core_peer)
    fly.drain()


def gather_weights(outer, kinds, arrays, mlp, text):
    shapes, own, whole = [], [], []
    for (parts, form), array in zip(kinds, arrays, strict=True):
        rows, width = array.shape
        half = width // 2 if parts else width
        own.append(pltpu.VMEM((rows, half), array.dtype))
        if form in (HALF_X, HALF_Y):
            shapes.append(jax.ShapeDtypeStruct((outer, 2, rows, half), array.dtype))
        elif form == KEEP:
            whole.append(pltpu.VMEM((outer, 2, 2, rows, half), array.dtype))
            shapes.append(jax.ShapeDtypeStruct((outer // 2, 2, 2, rows, width), array.dtype))
        else:
            shapes.append(jax.ShapeDtypeStruct((outer, 2, 2, rows, half), array.dtype))
    rows, units = mlp.shape
    mine = units // (2 * PLANE)
    shapes.append(jax.ShapeDtypeStruct((outer, PLANE, rows, mine), mlp.dtype))
    shapes.append(jax.ShapeDtypeStruct((2, *text.shape), text.dtype))
    dma = pltpu.SemaphoreType.DMA
    hops = outer - 1
    nf, nh = len(kinds), len(whole)
    results = pl.pallas_call(
        functools.partial(gather_kernel, outer, kinds),
        out_shape=shapes,
        in_specs=[VM] * (nf + 2),
        out_specs=[ANY] * len(shapes),
        scratch_shapes=[
            *own,
            *whole,
            pltpu.VMEM((PLANE, rows, mine), mlp.dtype),
            dma((nf + 1,)),
            dma((nf + 1, 2, hops)),
            dma((nf + 1, 2, hops)),
            dma((nf, outer)),
            dma((nf, outer)),
            dma((nf, outer, 2)),
            dma((nf, outer, 2)),
            dma((3,)),
            dma((3,)),
            dma((nh,)),
            dma((nh,)),
            dma((nh,)),
            dma((3,)),
        ],
        compiler_params=pltpu.CompilerParams(
            collective_id=0, has_side_effects=True, vmem_limit_bytes=40 * 1024 * 1024
        ),
        cost_estimate=pl.CostEstimate(flops=10**11, bytes_accessed=10**8, transcendentals=0),
        name="gather_weights",
    )(*arrays, mlp, text)
    return [value.reshape(-1, value.shape[-1]) if value.ndim != 4 or i >= nf else value for i, value in enumerate(results)]


def plane_gather_kernel(own_ref, out_ref, local_sem, send, recv):
    y, x, core = lax.axis_index("yb"), lax.axis_index("xc"), lax.axis_index("sp")
    x_peer, y_peer, core_peer = {"xc": 1 - x}, {"yb": 1 - y}, {"sp": 1 - core}
    fly = Flights()
    greet((x_peer, y_peer, core_peer))
    size = own_ref.shape[0] // 2
    top, low = pl.ds(0, size), pl.ds(size, size)
    fly.send(own_ref.at[top], out_ref.at[0, 1, 0, top], send.at[0], recv.at[0], x_peer)
    fly.send(own_ref.at[low], out_ref.at[1, 0, 0, low], send.at[1], recv.at[1], y_peer)
    fly.send(own_ref.at[low], out_ref.at[0, 1, 0, low], send.at[2], recv.at[2], x_peer)
    fly.send(own_ref.at[top], out_ref.at[1, 0, 0, top], send.at[3], recv.at[3], y_peer)
    fly.send(own_ref, out_ref.at[0, 0, 1], send.at[4], recv.at[4], core_peer)
    local = fly.local(own_ref, out_ref.at[0, 0, 0], local_sem.at[0])
    across = []

    def arrive(index, dy, dx, rows, device, onward=None):
        block = out_ref.at[dy, dx, 0, rows]
        landed(block, recv.at[index], device)
        if onward is not None:
            to, number = onward
            fly.send(block, out_ref.at[1, 1, 0, rows], send.at[number], recv.at[number], to)
        fly.send(block, out_ref.at[dy, dx, 1, rows], send.at[index + 7], recv.at[index + 7], core_peer)
        across.append((index + 7, dy, dx, rows))

    arrive(0, 0, 1, top, x_peer, (y_peer, 5))
    arrive(1, 1, 0, low, y_peer, (x_peer, 6))
    arrive(2, 0, 1, low, x_peer)
    arrive(3, 1, 0, top, y_peer)
    arrive(5, 1, 1, top, y_peer)
    arrive(6, 1, 1, low, x_peer)
    landed(out_ref.at[0, 0, 1], recv.at[4], core_peer)
    for index, dy, dx, rows in across:
        landed(out_ref.at[dy, dx, 1, rows], recv.at[index], core_peer)
    local.wait()
    fly.drain()


def plane_gather(own):
    rows, width = own.shape
    dma = pltpu.SemaphoreType.DMA
    out = pl.pallas_call(
        plane_gather_kernel,
        out_shape=jax.ShapeDtypeStruct((2, 2, 2, rows, width), own.dtype),
        in_specs=[VM],
        out_specs=VM,
        scratch_shapes=[dma((1,)), dma((14,)), dma((14,))],
        compiler_params=pltpu.CompilerParams(collective_id=1, has_side_effects=True),
        cost_estimate=pl.CostEstimate(flops=10**10, bytes_accessed=10**7, transcendentals=0),
        name="plane_gather",
    )(own)
    return out.reshape(8 * rows, width)


def plane_sum_kernel(part_a, part_b, out_a, out_b, core_in, first, second, keep, send, recv):
    y, x, core = lax.axis_index("yb"), lax.axis_index("xc"), lax.axis_index("sp")
    x_peer, y_peer, core_peer = {"xc": 1 - x}, {"yb": 1 - y}, {"sp": 1 - core}
    fly = Flights()
    greet((x_peer, y_peer, core_peer))
    rows = part_a.shape[3]
    chips = (((1, 1), (1, 0), (0, 1), (0, 0)), ((1, 1), (0, 1), (1, 0), (0, 0)))
    parts, outs, peers = (part_a, part_b), (out_a, out_b), ((y_peer, x_peer), (x_peer, y_peer))
    for index in range(4):
        for n in range(2):
            dy, dx = chips[n][index]
            fly.send(
                parts[n].at[dy, dx, 1], core_in.at[n, index], send.at[n, index], recv.at[n, index], core_peer
            )

    def core_sum(n, index):
        dy, dx = chips[n][index]
        landed(core_in.at[n, index], recv.at[n, index], core_peer)
        row_add(core_in.at[n, index], core_in.at[n, index], parts[n].at[dy, dx, 0], rows)

    for index in range(2):
        for n in range(2):
            core_sum(n, index)
            fly.send(
                core_in.at[n, index], first.at[n, index], send.at[n, index + 4], recv.at[n, index + 4], peers[n][0]
            )
    for index in (2, 3):
        for n in range(2):
            core_sum(n, index)
    for n in range(2):
        landed(first.at[n, 0], recv.at[n, 4], peers[n][0])
        row_add(second.at[n, 0], first.at[n, 0], core_in.at[n, 2], rows)
        fly.send(second.at[n, 0], second.at[n, 1], send.at[n, 6], recv.at[n, 6], peers[n][1])
    for n in range(2):
        landed(first.at[n, 1], recv.at[n, 5], peers[n][0])
        row_sum(keep.at[n], first.at[n, 1], core_in.at[n, 3], rows)
    for n in range(2):
        landed(second.at[n, 1], recv.at[n, 6], peers[n][1])
        row_sum(outs[n], keep.at[n], second.at[n, 1], rows)
    fly.drain()


def plane_sum(one, other):
    rows, width = one.shape[0] // 8, one.shape[1]
    dma = pltpu.SemaphoreType.DMA
    shape = jax.ShapeDtypeStruct((rows, width), F32)
    return pl.pallas_call(
        plane_sum_kernel,
        out_shape=(shape, shape),
        in_specs=[VM, VM],
        out_specs=(VM, VM),
        scratch_shapes=[
            pltpu.VMEM((2, 4, rows, width), BF),
            pltpu.VMEM((2, 2, rows, width), BF),
            pltpu.VMEM((2, 2, rows, width), BF),
            pltpu.VMEM((2, rows, width), F32),
            dma((2, 7)),
            dma((2, 7)),
        ],
        compiler_params=pltpu.CompilerParams(collective_id=2, has_side_effects=True),
        cost_estimate=pl.CostEstimate(flops=10**10, bytes_accessed=10**7, transcendentals=0),
        name="plane_sum",
    )(one.reshape(2, 2, 2, rows, width), other.reshape(2, 2, 2, rows, width))


def pair_sum_kernel(part_ref, out_ref, peer_in, send, recv):
    core = lax.axis_index("sp")
    core_peer = {"sp": 1 - core}
    fly = Flights()
    greet((core_peer,))
    size = part_ref.shape[1] // 2
    for index in range(2):
        rows = pl.ds(index * size, size)
        fly.send(part_ref.at[1 - core, rows], peer_in.at[rows], send.at[index], recv.at[index], core_peer)
    for index in range(2):
        rows = pl.ds(index * size, size)
        landed(peer_in.at[rows], recv.at[index], core_peer)
        row_sum(out_ref.at[rows], part_ref.at[core, rows], peer_in.at[rows], size)
    fly.drain()


def pair_sum(partial):
    rows, width = partial.shape[0] // 2, partial.shape[1]
    dma = pltpu.SemaphoreType.DMA
    return pl.pallas_call(
        pair_sum_kernel,
        out_shape=jax.ShapeDtypeStruct((rows, width), F32),
        in_specs=[VM],
        out_specs=VM,
        scratch_shapes=[pltpu.VMEM((rows, width), F32), dma((2,)), dma((2,))],
        compiler_params=pltpu.CompilerParams(collective_id=4, has_side_effects=True),
        cost_estimate=pl.CostEstimate(flops=10**9, bytes_accessed=10**7, transcendentals=0),
        name="pair_sum",
    )(partial.reshape(2, rows, width))


AHEAD, LAG_PLANE, LAG_CHAIN = 6, 2, 4
PLAIN, SPLIT, OVER_X, OVER_Y = range(4)


def reduce_kernel(outer, kinds, *refs):
    count = len(kinds)
    shards = outer * PLANE
    gs, refs = refs[:count], refs[count:]
    frames_ref, small_ref, up_ref, down_ref, refs = *refs[:4], refs[4:]
    outs, refs = refs[:count], refs[count:]
    frames_out, small_out, up_out, down_out, refs = *refs[:4], refs[4:]
    pieces = [(i, part) for i, (parts, _) in enumerate(kinds) for part in range(parts)]
    total = len(pieces)
    forms = [kinds[i][1] for i, _ in pieces]
    near_refs, near = list(refs), {}
    for p in range(total):
        if forms[p] in (PLAIN, SPLIT):
            near[p] = near_refs.pop(0)
    refs = near_refs
    plane, refs = refs[:total], refs[total:]
    chain, refs = refs[:total], refs[total:]
    split = [i for i, kind in enumerate(kinds) if kind[1] == SPLIT]
    whole, refs = refs[: len(split)], refs[len(split) :]
    small_in, small_own, small_peer, up_in, down_in, refs = *refs[:5], refs[5:]
    e_s, e_r, e_l, s1, r1, s2, r2, zs, zr, o_s, o_r, f_s, f_r, m_s, m_r, l_s, p_s, p_r = refs
    z, y, x = (lax.axis_index(name) for name in FS)
    core = lax.axis_index("sp")
    here = (z * 2 + y) * 2 + x
    core_peer = {"sp": 1 - core}
    above, below = {"za": z + 1}, {"za": z - 1}
    fly = Flights()

    def chip(index):
        return {"za": index // 4, "yb": (index // 2) % 2, "xc": index % 2}

    others = [(here + j) % shards for j in range(1, shards)]
    greet((core_peer, *[chip(index) for index in others]))

    part_slots = outer // 2
    ours, other_slots = pl.ds(core * part_slots, part_slots), pl.ds((1 - core) * part_slots, part_slots)
    for j, i in enumerate(split):
        width = whole[j].shape[-1]
        mine = pl.ds(pl.multiple_of(core * width, width), width)
        theirs = pl.ds(pl.multiple_of((1 - core) * width, width), width)
        fly.send(gs[i].at[:, :, :, :, theirs], whole[j].at[ours], e_s.at[j], e_r.at[j], core_peer)
        fly.local(gs[i].at[:, :, :, :, mine], whole[j].at[ours], e_l.at[j])

    def joined(i):
        j = split.index(i)
        width = whole[j].shape[-1]
        mine = pl.ds(pl.multiple_of(core * width, width), width)
        pltpu.make_async_copy(gs[i].at[:, :, :, :, mine], whole[j].at[ours], e_l.at[j]).wait()
        landed(whole[j].at[other_slots], e_r.at[j], core_peer)

    def width_of(p):
        return plane[p].shape[-1]

    def source(p, *place):
        i, part = pieces[p]
        held = whole[split.index(i)] if forms[p] == SPLIT else gs[i]
        width = width_of(p)
        return held.at[(*place, slice(None), pl.ds(part * width, width))]

    frame_width = frames_ref.shape[1]
    frame_mine = pl.ds(pl.multiple_of(core * frame_width, frame_width), frame_width)
    frame_other = pl.ds(pl.multiple_of((1 - core) * frame_width, frame_width), frame_width)
    frame_copy = fly.local(frames_ref, frames_out.at[here, :, frame_mine], l_s.at[0])
    small_copy = fly.local(small_ref.at[here], small_in.at[here], l_s.at[1])
    for j, index in enumerate(others):
        fly.send(frames_ref, frames_out.at[here, :, frame_mine], f_s.at[j], f_r.at[here], chip(index))
        fly.send(small_ref.at[index], small_in.at[here], m_s.at[j], m_r.at[here], chip(index))

    near_by = ((y, 1 - x), (1 - y, x), (1 - y, 1 - x))
    up_copy = fly.local(up_ref.at[2 * y + x], up_in.at[core, 2 * y + x], p_s.at[0])
    for j, (ty, tx) in enumerate(near_by):
        fly.send(
            up_ref.at[2 * ty + tx],
            up_in.at[core, 2 * y + x],
            p_s.at[j + 1],
            p_r.at[j + 1],
            {"yb": ty, "xc": tx},
        )
    fly.send(down_ref, down_in, p_s.at[4], p_r.at[4], core_peer)

    def feed_forward_landed():
        up_copy.wait()
        for j, (ty, tx) in enumerate(near_by):
            landed(up_in.at[core, 2 * ty + tx], p_r.at[j + 1], {"yb": ty, "xc": tx})
        fly.send(up_in.at[core], up_in.at[core], p_s.at[5], p_r.at[5], core_peer)
        hid = down_ref.shape[0]
        landed(down_in, p_r.at[4], core_peer)
        for side in range(2):

            @pl.when(core == side)
            def _(side=side):
                down_out[side * hid : (side + 1) * hid, :] = down_ref[...].astype(F32)
                down_out[(1 - side) * hid : (2 - side) * hid, :] = down_in[...].astype(F32)

    def feed_forward_rows():
        hid = down_ref.shape[0]
        landed(up_in.at[1 - core], p_r.at[5], core_peer)
        for slot in range(outer):
            for place in range(PLANE):
                for side in range(2):
                    column = ((slot * PLANE + place) * 2 + side) * hid
                    up_out[:, column : column + hid] = up_in[side, place, :, slot * hid : (slot + 1) * hid].astype(F32)

    def slot_at(step):
        if step == outer - 1:
            return z
        falling = outer - 1 - step
        falling = jnp.where(falling > z, falling, falling - 1)
        rising = jnp.where(step < z, step, step + 1)
        return jnp.where(z < part_slots, falling, rising)

    units = [(slot_at(step), p) for step in range(outer) for p in range(total)]

    def turns(p, slot):
        turn = (slot + p) % 2
        first = ((y + 1 - turn) % 2, (x + turn) % 2)
        second = ((y + turn) % 2, (x + 1 - turn) % 2)
        return first, second

    def device(place):
        return {"yb": place[0], "xc": place[1]}

    def start(slot, p):
        first, _ = turns(p, slot)
        fly.send(
            source(p, slot, 1 - y, 1 - x), near[p].at[slot, 1], s1.at[p, slot, 1], r1.at[p, slot, 1], device(first)
        )
        fly.send(
            source(p, slot, first[0], first[1]), near[p].at[slot, 0], s1.at[p, slot, 0], r1.at[p, slot, 0], device(first)
        )

    def summed_over(p):
        return (x, {"xc": 1 - x}) if forms[p] == OVER_X else (y, {"yb": 1 - y})

    def pass_on(slot, p):
        rows = plane[p].shape[1]
        if p not in near:
            index, peer = summed_over(p)
            fly.send(source(p, slot, 1 - index), plane[p].at[slot], s2.at[p, slot], r2.at[p, slot], peer)
            return
        first, second = turns(p, slot)
        landed(near[p].at[slot, 1], r1.at[p, slot, 1], device(first))
        row_add(near[p].at[slot, 1], near[p].at[slot, 1], source(p, slot, second[0], second[1]), rows)
        fly.send(near[p].at[slot, 1], plane[p].at[slot], s2.at[p, slot], r2.at[p, slot], device(second))
        landed(near[p].at[slot, 0], r1.at[p, slot, 0], device(first))
        row_add(near[p].at[slot, 0], near[p].at[slot, 0], source(p, slot, y, x), rows)

    def plane_total(slot, p):
        rows = plane[p].shape[1]
        if p not in near:
            index, peer = summed_over(p)
            landed(plane[p].at[slot], r2.at[p, slot], peer)
            row_add(plane[p].at[slot], plane[p].at[slot], source(p, slot, index), rows)
            return
        _, second = turns(p, slot)
        landed(plane[p].at[slot], r2.at[p, slot], device(second))
        row_add(plane[p].at[slot], plane[p].at[slot], near[p].at[slot, 0], rows)

    def along(slot, p, last):
        rows, width = plane[p].shape[1:]
        if not last:
            for way, when, edge, ahead, behind in (
                (1, slot < z, z == outer - 1, below, above),
                (0, slot > z, z == 0, above, below),
            ):
                link = chain[p].at[slot + 1 - way]

                @pl.when(jnp.logical_and(when, jnp.logical_not(edge)))
                def _(way=way, link=link, behind=behind):
                    landed(link, zr.at[p, way, slot], behind)
                    row_add(plane[p].at[slot], plane[p].at[slot], link, rows)

                fly.send(plane[p].at[slot], link, zs.at[p, way, slot], zr.at[p, way, slot], ahead, when)
            return
        has_above, has_below = z < outer - 1, z > 0
        for way, when, behind in ((1, has_above, above), (0, has_below, below)):

            @pl.when(when)
            def _(way=way, behind=behind):
                landed(chain[p].at[slot + 1 - way], zr.at[p, way, slot], behind)

        step = 16 if rows % 16 == 0 else rows
        i, part = pieces[p]
        column = pl.multiple_of((2 * part + core) * width, width)

        def chunk(index, carry):
            at = pl.ds(pl.multiple_of(index * step, step), step)
            upper = jnp.where(has_above, chain[p][slot, at, :].astype(F32), 0.0)
            lower = jnp.where(has_below, chain[p][slot + 1, at, :].astype(F32), 0.0)
            outs[i][at, pl.ds(column, width)] = plane[p][slot, at, :].astype(F32) + upper + lower
            return carry

        lax.fori_loop(0, rows // step, chunk, 0)
        block = outs[i].at[:, pl.ds(column, width)]
        fly.send(block, block, o_s.at[p], o_r.at[p], core_peer)

    waiting = set(split)

    def begin(unit):
        slot, p = units[unit]
        if p not in near:
            return
        if pieces[p][0] in waiting:
            joined(pieces[p][0])
            waiting.discard(pieces[p][0])
        start(slot, p)

    for unit in range(min(AHEAD, len(units))):
        begin(unit)
    for tick in range(len(units) + LAG_CHAIN):
        if tick < len(units):
            pass_on(*units[tick])
            if tick + AHEAD < len(units):
                begin(tick + AHEAD)
        if 0 <= tick - LAG_PLANE < len(units):
            plane_total(*units[tick - LAG_PLANE])
        if tick == 4:
            feed_forward_landed()
        if tick == 10:
            feed_forward_rows()
        if 0 <= tick - LAG_CHAIN < len(units):
            unit = tick - LAG_CHAIN
            along(*units[unit], unit >= (outer - 1) * total)
        if tick == total:
            frame_copy.wait()
            for index in others:
                landed(frames_out.at[index, :, frame_mine], f_r.at[index], chip(index))
            fly.send(frames_out.at[:, :, frame_mine], frames_out.at[:, :, frame_mine], p_s.at[6], p_r.at[6], core_peer)
            small_copy.wait()
            for index in others:
                landed(small_in.at[index], m_r.at[index], chip(index))
            small_own[...] = jnp.sum(small_in[...], axis=0)
            fly.send(small_own, small_peer, l_s.at[2], l_s.at[3], core_peer)

    landed(frames_out.at[:, :, frame_other], p_r.at[6], core_peer)
    landed(small_peer, l_s.at[3], core_peer)
    small_out[...] = small_own[...] + small_peer[...]
    for p, (i, part) in enumerate(pieces):
        width = width_of(p)
        column = pl.multiple_of((2 * part + 1 - core) * width, width)
        landed(outs[i].at[:, pl.ds(column, width)], o_r.at[p], core_peer)
    fly.drain()


def reduce_weights(outer, kinds, grads, frames, small, up, down):
    shards = outer * PLANE
    shaped, shapes, near, plane, chain, whole = [], [], [], [], [], []
    for (parts, form), grad in zip(kinds, grads, strict=True):
        full_width = grad.shape[-1] // 2 if form == SPLIT else grad.shape[-1]
        if form in (PLAIN, SPLIT):
            lead = outer // 2 if form == SPLIT else outer
            grad = grad.reshape(lead, 2, 2, -1, grad.shape[-1])
        rows, width = grad.shape[-2], full_width // parts
        shaped.append(grad)
        shapes.append(jax.ShapeDtypeStruct((rows, 2 * full_width), F32))
        for _ in range(parts):
            if form in (PLAIN, SPLIT):
                near.append(pltpu.VMEM((outer, 2, rows, width), BF))
            plane.append(pltpu.VMEM((outer, rows, width), BF))
            chain.append(pltpu.VMEM((outer + 1, rows, width), BF))
        if form == SPLIT:
            whole.append(pltpu.VMEM((outer, 2, 2, rows, full_width), BF))
    shapes.append(jax.ShapeDtypeStruct((shards, frames.shape[0], 2 * frames.shape[1]), frames.dtype))
    shapes.append(jax.ShapeDtypeStruct(small.shape[1:], F32))
    shapes.append(jax.ShapeDtypeStruct((up.shape[1], 2 * PLANE * up.shape[2]), F32))
    shapes.append(jax.ShapeDtypeStruct((2 * down.shape[0], down.shape[1]), F32))
    dma = pltpu.SemaphoreType.DMA
    count, total, nsplit = len(kinds), len(plane), len(whole)
    results = pl.pallas_call(
        functools.partial(reduce_kernel, outer, kinds),
        out_shape=shapes,
        in_specs=[VM] * (count + 4),
        out_specs=[VM] * (count + 4),
        scratch_shapes=[
            *near,
            *plane,
            *chain,
            *whole,
            pltpu.VMEM(small.shape, F32),
            pltpu.VMEM(small.shape[1:], F32),
            pltpu.VMEM(small.shape[1:], F32),
            pltpu.VMEM((2, *up.shape), up.dtype),
            pltpu.VMEM(down.shape, down.dtype),
            dma((nsplit,)),
            dma((nsplit,)),
            dma((nsplit,)),
            dma((total, outer, 2)),
            dma((total, outer, 2)),
            dma((total, outer)),
            dma((total, outer)),
            dma((total, 2, outer)),
            dma((total, 2, outer)),
            dma((total,)),
            dma((total,)),
            dma((shards,)),
            dma((shards,)),
            dma((shards,)),
            dma((shards,)),
            dma((4,)),
            dma((7,)),
            dma((7,)),
        ],
        cost_estimate=pl.CostEstimate(flops=10**11, bytes_accessed=10**8, transcendentals=0),
        compiler_params=pltpu.CompilerParams(
            collective_id=3, has_side_effects=True, vmem_limit_bytes=67043328
        ),
        name="reduce_weights",
    )(*shaped, frames, small, up, down)
    return results[:count], *results[count:]


def gather(value, axes, axis=0):
    return lax.all_gather(value, axes, axis=axis, tiled=True)


def scatter(value, axes, axis=0):
    return lax.psum_scatter(value, axes, scatter_dimension=axis, tiled=True)


def swap(value, split_axis, concat_axis):
    return lax.all_to_all(value, "sp", split_axis=split_axis, concat_axis=concat_axis, tiled=True)


def body(
    tokens,
    text,
    clip_frames,
    timestep,
    mod_weight,
    mod_bias,
    qk_gains,
    self_in,
    self_out,
    cross_q,
    cross_kv,
    cross_out,
    mlp_in,
    mlp_out,
    cotangent,
):
    half = D // 2
    row_count = tokens.shape[0]
    frame_count = row_count // FRAME_TOK
    group_frames = timestep.shape[1]
    shards = D // self_in.shape[1]
    outer = shards // PLANE
    core = lax.axis_index("sp")
    chip = lax.axis_index(FS)
    in_rows = self_in.shape[1]
    own_frame = core * frame_count

    bias_len, gain_len = mod_bias.shape[1], qk_gains.shape[2]
    small_len = bias_len + 4 * gain_len
    small_rows = 8
    small_width = -(-(small_len + group_frames) // (small_rows * 128)) * 128
    small_room = small_rows * small_width

    small = jnp.concatenate(
        [
            mod_bias[0].astype(F32),
            qk_gains[0].reshape(-1).astype(F32),
            timestep[0].astype(F32),
            jnp.zeros((small_room - small_len - group_frames,), F32),
        ]
    ).reshape(small_rows, small_width)
    gathered = gather_weights(
        outer,
        ((0, ALL_CHIPS), (1, ALL_CHIPS), (3, ALL_CHIPS), (1, KEEP), (2, HALF_X), (1, HALF_Y), (1, KEEP)),
        [small, *(w[0] for w in (mod_weight, self_in, self_out, cross_kv, cross_q, cross_out))],
        mlp_in[0],
        text,
    )
    small_all, mod_matrix, self_proj, self_back, kv_half, q_half, cross_back = gathered[:7]
    up_matrix, text_all = gathered[7:]
    hid = mlp_out.shape[1] // 2
    down_part = lax.dynamic_slice_in_dim(mlp_out[0], core * hid, hid, 0)
    down_part, small_all = lax.optimization_barrier((down_part, small_all))
    down_matrix = gather(down_part, "za")
    small_all = small_all.reshape(shards, small_room)
    bias_all = small_all[:, :bias_len].reshape(-1)
    gain_all = (
        small_all[:, bias_len:small_len]
        .reshape(shards, 4, gain_len)
        .transpose(1, 0, 2)
        .reshape(4, 2, half)
    )
    gain_own = lax.dynamic_index_in_dim(gain_all, core, 1, keepdims=False)
    steps_all = small_all[:, small_len : small_len + group_frames].reshape(-1)

    live_keys = clip_frames * FRAME_TOK
    all_keys = jnp.full((1,), TXT, jnp.int32)
    own_steps = lax.dynamic_slice_in_dim(timestep[0], own_frame, frame_count)
    clip_pos = jnp.arange(group_frames, dtype=jnp.int32)
    cosine, sine = rotary_tables(
        jnp.repeat(clip_pos, FRAME_TOK),
        jnp.tile(jnp.arange(FRAME_TOK, dtype=jnp.int32), group_frames),
    )
    cosine, sine = jnp.concatenate([cosine, cosine], axis=1), jnp.concatenate([-sine, sine], axis=1)
    sinus = sinus_features(timestep[0]).astype(BF)

    mod_half = product(sinus, mod_matrix)
    mod_half = mod_half + lax.dynamic_slice_in_dim(bias_all, core * 3 * D, 3 * D)[None]
    modulation = swap(mod_half, 0, 1)
    shift_one, scale_one, gate_one, shift_two, scale_two, gate_two = jnp.split(
        modulation, 6, axis=1
    )

    grad_branch = frame_scaled(cotangent.astype(F32), gate_two).astype(BF)
    exchange = [(0, 1), (1, 0)]
    place_y, place_x = lax.axis_index("yb"), lax.axis_index("xc")
    kv_other = lax.ppermute(kv_half, "yb", exchange)
    q_other = lax.ppermute(q_half, "xc", exchange)
    beside = [
        grad_branch,
        lax.ppermute(grad_branch, "xc", exchange),
        lax.ppermute(grad_branch, "yb", exchange),
        lax.ppermute(grad_branch, PL, [(0, 3), (1, 2), (2, 1), (3, 0)]),
    ]

    residual = tokens.astype(F32)
    attn_float, back_attn_input = jax.vjp(modulated, residual, shift_one, scale_one)
    attn_input = gather(attn_float.astype(BF), "sp")
    joined = product(attn_input, self_proj)
    self_mixed, self_lse, *self_kept = attend_forward(
        live_keys, [joined], gain_own[:2], cosine, sine, True, 5
    )
    self_branch = pair_sum(product(self_mixed, self_back))
    residual = residual + frame_scaled(self_branch, gate_one)

    def beside_own(own, other, place, axis):
        pair = jnp.where(place == 0, jnp.stack([own, other], axis), jnp.stack([other, own], axis))
        return pair.reshape(-1, own.shape[-1])

    cross_kvproj = beside_own(kv_half, kv_other, place_y, 1)
    cross_qproj = beside_own(q_half, q_other, place_x, 2)
    text_raw = product(text_all, cross_kvproj)
    cross_float, back_cross_norm = jax.vjp(layer_norm, residual)
    cross_input = gather(cross_float.astype(BF), "sp")
    cross_raw = product(cross_input, cross_qproj)
    cross_mixed, cross_lse, *cross_kept = attend_forward(
        all_keys, [cross_raw, text_raw], gain_own[2:], cosine, sine, False, 6
    )
    cross_branch = pair_sum(product(cross_mixed, cross_back))
    residual = residual + cross_branch
    residual, *beside = lax.optimization_barrier((residual, *beside))
    beside = jnp.stack(beside)
    grad_branch_all = jnp.stack([beside, lax.ppermute(beside, "sp", exchange)], axis=1).reshape(-1, D)


    mlp_float, back_mlp_input = jax.vjp(modulated, residual, shift_two, scale_two)
    mlp_input = plane_gather(mlp_float.astype(BF))
    up_proj = product(mlp_input, up_matrix)
    activated_float, back_gelu = jax.vjp(
        lambda inner: jax.nn.gelu(inner, approximate=True), up_proj
    )
    activated = activated_float.astype(BF)

    mlp_part = product(activated, down_matrix).astype(BF)

    grad_rows = cotangent.astype(F32)
    grad_down = product_tn(activated, grad_branch_all).astype(BF)
    grad_up_low = back_gelu(product_nt(grad_branch_all, down_matrix))[0].astype(BF)
    grad_up = product_tn(mlp_input, grad_up_low).astype(BF)
    grad_mlp_part = product_nt(grad_up_low, up_matrix).astype(BF)
    grad_mlp_part, grad_up, grad_down = lax.optimization_barrier((grad_mlp_part, grad_up, grad_down))
    down_owned = scatter(grad_down, "za")
    up_owned = scatter(grad_up, "za")
    mlp_branch, grad_mlp_input = plane_sum(mlp_part, grad_mlp_part)
    output = (residual + frame_scaled(mlp_branch, gate_two)).astype(BF)
    grad_gate_two = frame_sum(grad_rows * mlp_branch, frame_count)
    grad_from_mlp, grad_shift_two, grad_scale_two = back_mlp_input(grad_mlp_input)
    grad_rows = grad_rows + grad_from_mlp

    grad_low = gather(grad_rows.astype(BF), "sp")
    grad_cross_back = product_tn(cross_mixed, grad_low).astype(BF)
    grad_cross_mixed = product_nt(grad_low, cross_back).astype(BF)
    cross_saved = [*cross_kept[:2], cross_lse, *cross_kept[2:]]
    grad_cross_low, grad_text_low, gains_cross = attend_backward(
        all_keys, [cross_raw, text_raw], gain_own[2:], cosine, sine, False, 7, cross_saved, grad_cross_mixed
    )
    grad_cross_qproj = product_tn(cross_input, grad_cross_low).astype(BF)
    grad_cross_kvproj = product_tn(text_all, grad_text_low).astype(BF)
    kv_parts = grad_cross_kvproj.reshape(outer, 2, 2, in_rows, -1)
    q_parts = grad_cross_qproj.reshape(outer, 2, 2, in_rows, -1)
    kv_sent = lax.ppermute(lax.dynamic_index_in_dim(kv_parts, 1 - place_y, 1, False), "yb", exchange)
    q_sent = lax.ppermute(lax.dynamic_index_in_dim(q_parts, 1 - place_x, 2, False), "xc", exchange)
    grad_cross_input = pair_sum(product_nt(grad_cross_low, cross_qproj))
    grad_rows = grad_rows + back_cross_norm(grad_cross_input)[0]

    grad_gate_one = frame_sum(grad_rows * self_branch, frame_count)
    grad_self_low = gather(frame_scaled(grad_rows, gate_one).astype(BF), "sp")
    grad_self_back = product_tn(self_mixed, grad_self_low).astype(BF)
    grad_self_mixed = product_nt(grad_self_low, self_back).astype(BF)
    self_saved = [*self_kept[:2], self_lse, *self_kept[2:]]
    grad_joined_low, gains_self = attend_backward(
        live_keys, [joined], gain_own[:2], cosine, sine, True, 8, self_saved, grad_self_mixed
    )
    grad_self_proj = product_tn(attn_input, grad_joined_low).astype(BF)
    grad_attn_input = pair_sum(product_nt(grad_joined_low, self_proj))
    grad_from_attn, grad_shift_one, grad_scale_one = back_attn_input(grad_attn_input)
    grad_rows = grad_rows + grad_from_attn

    grad_modulation = jnp.concatenate(
        [grad_shift_one, grad_scale_one, grad_gate_one, grad_shift_two, grad_scale_two, grad_gate_two],
        axis=1,
    )
    grad_mod_half = swap(grad_modulation, 1, 0)
    grad_gains = jnp.concatenate([gains_self[:2], gains_cross[:2]])
    both = jnp.arange(2)[None, :, None] == core
    grad_gains = jnp.where(both, grad_gains[:, None, :], 0.0).reshape(4, shards, gain_len)
    grad_small = jnp.concatenate(
        [
            jnp.sum(grad_modulation, axis=0).reshape(shards, bias_len),
            grad_gains.transpose(1, 0, 2).reshape(shards, 4 * gain_len),
            jnp.zeros((shards, small_room - small_len), F32),
        ],
        axis=1,
    ).reshape(shards, small_rows, small_width)
    kv_near = lax.dynamic_index_in_dim(kv_parts, place_y, 1, False) + kv_sent
    q_near = lax.dynamic_index_in_dim(q_parts, place_x, 2, False) + q_sent
    owned, grad_mod_all, small_owned, mlp_in_grad, mlp_out_grad = reduce_weights(
        outer,
        ((1, OVER_Y), (2, OVER_X), (1, SPLIT), (1, SPLIT), (3, PLAIN)),
        [q_near, kv_near, grad_cross_back, grad_self_back, grad_self_proj],
        grad_mod_half.astype(BF),
        grad_small,
        up_owned.reshape(PLANE, -1, up_owned.shape[1]),
        down_owned,
    )
    cross_q_grad, cross_kv_grad, cross_out_grad, self_out_grad, self_in_grad = owned
    small_owned = small_owned.reshape(-1)[:small_len]
    sinus_all = sinus_features(steps_all).astype(BF)
    own_features = mod_weight.shape[1]
    sinus_own = lax.dynamic_slice_in_dim(sinus_all, chip * own_features, own_features, 1)
    mod_weight_grad = product_tn(sinus_own, grad_mod_all.reshape(-1, 6 * D))
    return (
        output,
        grad_rows,
        mod_weight_grad[None],
        small_owned[None, :bias_len],
        small_owned[bias_len:].reshape(1, 4, gain_len),
        self_in_grad[None],
        self_out_grad[None],
        cross_q_grad[None],
        cross_kv_grad[None],
        cross_out_grad[None],
        mlp_in_grad[None],
        mlp_out_grad[None],
    )


def solution(mesh):
    chips, cores = mesh.shape["fsdp"], mesh.shape["sp"]
    grid = mesh.devices.reshape(chips // PLANE, 2, PLANE // 2, cores)
    inner = Mesh(grid, ALL)
    rows, second = P(ALL, None), P(None, FS, None)
    in_specs = (
        rows,
        rows,
        P(FS),
        P(FS, None),
        second,
        P(None, FS),
        P(None, None, FS),
        *([second] * 7),
        rows,
    )
    out_specs = (rows, rows, second, P(None, FS), P(None, None, FS), *([second] * 7))

    return jax.shard_map(body, mesh=inner, in_specs=in_specs, out_specs=out_specs, check_vma=False)
```

```python
import functools
import math

import jax
import jax.numpy as jnp
import numpy as np
from jax import lax
from jax.experimental import pallas as pl
from jax.experimental.pallas import tpu as pltpu
from jax.sharding import Mesh
from jax.sharding import PartitionSpec as P


D = 1536
HD = 128
TXT = 512
FREQ = 256
WP = 8
FRAME_TOK = 64
PLANE = 4

EPSILON = 1e-06
NEGATIVE = -1e30

FS = ("za", "yb", "xc")
PL = ("yb", "xc")
ALL = ("za", "yb", "xc", "sp")
SCALE = 1.0 / math.sqrt(HD)
MESH = pl.DeviceIdType.MESH
BF = jnp.bfloat16
F32 = jnp.float32


def product(left, right):
    return jnp.dot(left, right, preferred_element_type=F32)


def product_tn(left, right):
    return lax.dot_general(left, right, (((0,), (0,)), ((), ())), preferred_element_type=F32)


def product_nt(left, right):
    return lax.dot_general(left, right, (((1,), (1,)), ((), ())), preferred_element_type=F32)


def layer_norm(values):
    centred = values - jnp.mean(values, axis=-1, keepdims=True)
    return centred * lax.rsqrt(jnp.mean(centred * centred, axis=-1, keepdims=True) + EPSILON)


def sinus_features(steps):
    half_dim = FREQ // 2
    rates = jnp.exp(jnp.arange(half_dim).astype(F32) * (-math.log(10000.0) / half_dim))
    angles = steps.astype(F32)[:, None] * rates[None, :]
    return jnp.concatenate([jnp.cos(angles), jnp.sin(angles)], axis=1)


def rotary_tables(frames):
    half_dim = HD // 2
    side_pairs = HD // 6
    lead_pairs = half_dim - 2 * side_pairs
    pair = np.arange(half_dim)
    lead = pair < lead_pairs
    side = (pair >= lead_pairs) & (pair < lead_pairs + side_pairs)
    last = pair >= lead_pairs + side_pairs

    def rates(part, start, count):
        rate = np.exp(np.float32(-math.log(10000.0)) * (pair - start).astype(np.float32) / np.float32(count))
        return np.where(part, rate, 0.0).astype(np.float32)

    spot = np.tile(np.arange(FRAME_TOK), frames)
    frame = np.repeat(np.arange(frames), FRAME_TOK).astype(np.float32)
    angles = (
        frame[:, None] * rates(lead, 0, lead_pairs)[None]
        + (spot // WP).astype(np.float32)[:, None] * rates(side, lead_pairs, side_pairs)[None]
        + (spot % WP).astype(np.float32)[:, None] * rates(last, lead_pairs + side_pairs, side_pairs)[None]
    ).astype(np.float32)
    cosine, sine = np.cos(angles), np.sin(angles)
    return np.concatenate([cosine, cosine], axis=1), np.concatenate([-sine, sine], axis=1)


def modulated(residual, shift, scale):
    frames = shift.shape[0]
    normed = layer_norm(residual).reshape(frames, -1, residual.shape[1])
    return (normed * (1.0 + scale[:, None, :]) + shift[:, None, :]).reshape(residual.shape)


def frame_scaled(rows, gate):
    frames = gate.shape[0]
    return (rows.reshape(frames, -1, rows.shape[1]) * gate[:, None, :]).reshape(rows.shape)


def frame_sum(values, frames):
    return jnp.sum(values.reshape(frames, -1, values.shape[1]), axis=1)


VM = pl.BlockSpec(memory_space=pltpu.VMEM)
SM = pl.BlockSpec(memory_space=pltpu.SMEM)
ANY = pl.BlockSpec(memory_space=pl.ANY)


def row_add(target, left, right, rows):
    step = 32 if rows % 32 == 0 else rows

    def chunk(index, carry):
        at = pl.ds(pl.multiple_of(index * step, step), step)
        target[at, :] = left[at, :] + right[at, :]
        return carry

    lax.fori_loop(0, rows // step, chunk, 0)


def row_sum(target, left, right, rows):
    step = 16 if rows % 16 == 0 else rows

    def chunk(index, carry):
        at = pl.ds(pl.multiple_of(index * step, step), step)
        target[at, :] = left[at, :].astype(F32) + right[at, :].astype(F32)
        return carry

    lax.fori_loop(0, rows // step, chunk, 0)


class Flights:
    def __init__(self):
        self.sent = []

    def send(self, source, target, send_sem, recv_sem, device, when=None):
        copy = pltpu.make_async_remote_copy(
            src_ref=source,
            dst_ref=target,
            send_sem=send_sem,
            recv_sem=recv_sem,
            device_id=device,
            device_id_type=MESH,
        )
        if when is None:
            copy.start()
        else:
            pl.when(when)(copy.start)
        self.sent.append((when, copy))

    def local(self, source, target, sem):
        copy = pltpu.make_async_copy(source, target, sem)
        copy.start()
        return copy

    def drain(self):
        for when, copy in self.sent:
            if when is None:
                copy.wait_send()
            else:
                pl.when(when)(copy.wait_send)


def landed(target, sem, device):
    pltpu.make_async_remote_copy(
        src_ref=target,
        dst_ref=target,
        send_sem=sem,
        recv_sem=sem,
        device_id=device,
        device_id_type=MESH,
    ).wait_recv()


def greet(devices, optional=()):
    barrier = pltpu.get_barrier_semaphore()
    for device in devices:
        pl.semaphore_signal(barrier, inc=1, device_id=device, device_id_type=MESH)
    for when, device in optional:

        @pl.when(when)
        def _(device=device):
            pl.semaphore_signal(barrier, inc=1, device_id=device, device_id_type=MESH)

    count = len(devices)
    for when, _ in optional:
        count = count + when.astype(jnp.int32)
    pl.semaphore_wait(barrier, count)


def raw_views(joint, refs):
    if joint:
        rows_ref, rest = refs[0], refs[1:]
        width = rows_ref.shape[1] // 3
        spans = ((rows_ref, 0), (rows_ref, width), (rows_ref, 2 * width))
    else:
        rows_ref, keys_ref, rest = refs[0], refs[1], refs[2:]
        width = rows_ref.shape[1]
        spans = ((rows_ref, 0), (keys_ref, 0), (keys_ref, width))

    def view(which, head):
        ref, base = spans[which]
        return ref[:, base + head * HD : base + (head + 1) * HD]

    return view, width, rest


def turned(values, cos_ref, sin_ref, sign):
    return values * cos_ref[...] + sign * (pltpu.roll(values, HD // 2, 1) * sin_ref[...])


def attend_forward_kernel(joint, rotary, live_ref, *refs):
    view, width, refs = raw_views(joint, refs)
    gain_ref, cos_ref, sin_ref, refs = *refs[:3], refs[3:]
    out_ref, lse_ref, query_ref, key_ref, inv_q_ref, inv_k_ref, refs = *refs[:6], refs[6:]
    q_sum, k_sum, q_peer, k_peer, send, recv = refs
    heads = width // HD
    core_peer = {"sp": 1 - lax.axis_index("sp")}
    fly = Flights()
    greet((core_peer,))
    for which, own, peer in ((0, q_sum, q_peer), (1, k_sum, k_peer)):
        total = view(which, 0) * view(which, 0)
        for head in range(1, heads):
            total = total + view(which, head) * view(which, head)
        own[...] = jnp.broadcast_to(jnp.sum(total, axis=1, keepdims=True), own.shape)
        fly.send(own, peer, send.at[which], recv.at[which], core_peer)
    for which, own, peer, kept in ((0, q_sum, q_peer, inv_q_ref), (1, k_sum, k_peer, inv_k_ref)):
        landed(peer, recv.at[which], core_peer)
        kept[...] = lax.rsqrt((own[...] + peer[...]) / D + EPSILON)
    rows, keys = query_ref.shape[0], key_ref.shape[0]
    spot = lax.broadcasted_iota(jnp.int32, (rows, keys), 1)
    allowed = spot < live_ref[0]
    for head in range(heads):
        part = slice(head * HD, (head + 1) * HD)
        query = view(0, head) * inv_q_ref[...] * gain_ref[0:1, part]
        key = view(1, head) * inv_k_ref[...] * gain_ref[1:2, part]
        if rotary:
            query, key = turned(query, cos_ref, sin_ref, 1.0), turned(key, cos_ref, sin_ref, 1.0)
        query, key, value = query.astype(BF), key.astype(BF), view(2, head).astype(BF)
        query_ref[:, part], key_ref[:, part] = query, key
        scores = jnp.where(allowed, product_nt(query, key) * SCALE, NEGATIVE)
        row_max = jnp.max(scores, axis=1, keepdims=True)
        log_total = row_max + jnp.log(jnp.sum(jnp.exp(scores - row_max), axis=1, keepdims=True))
        weights = jnp.exp(scores - log_total).astype(BF)
        out_ref[:, part] = product(weights, value).astype(BF)
        lse_ref[:, part] = jnp.broadcast_to(log_total, (rows, HD))
    fly.drain()


def attend_backward_kernel(joint, rotary, live_ref, *refs):
    view, width, refs = raw_views(joint, refs)
    gain_ref, cos_ref, sin_ref, refs = *refs[:3], refs[3:]
    query_ref, key_ref, lse_ref, inv_q_ref, inv_k_ref, do_ref, refs = *refs[:6], refs[6:]
    if joint:
        grad_refs, refs = ((refs[0], 0), (refs[0], width), (refs[0], 2 * width)), refs[1:]
    else:
        grad_refs, refs = ((refs[0], 0), (refs[1], 0), (refs[1], width)), refs[2:]
    gain_out, scaled_q, scaled_k, q_dot, k_dot, q_peer, k_peer, send, recv = refs
    heads = width // HD
    core_peer = {"sp": 1 - lax.axis_index("sp")}
    fly = Flights()
    greet((core_peer,))
    rows, keys = query_ref.shape[0], key_ref.shape[0]
    spot = lax.broadcasted_iota(jnp.int32, (rows, keys), 1)
    allowed = spot < live_ref[0]
    dots = [None, None]
    gain_out[...] = jnp.zeros_like(gain_out)
    for head in range(heads):
        part = slice(head * HD, (head + 1) * HD)
        query, key, grad = query_ref[:, part], key_ref[:, part], do_ref[:, part]
        value = view(2, head).astype(BF)
        scores = jnp.where(allowed, product_nt(query, key) * SCALE, NEGATIVE)
        weights = jnp.exp(scores - lse_ref[:, head * HD : head * HD + 1])
        grad_weights = product_nt(grad, value)
        delta = jnp.sum(weights * grad_weights, axis=1, keepdims=True)
        grad_scores = (weights * (grad_weights - delta)).astype(BF)
        grad_query = (product(grad_scores, key) * SCALE).astype(BF).astype(F32)
        grad_key = (product_tn(grad_scores, query) * SCALE).astype(BF).astype(F32)
        grad_value = product_tn(weights.astype(BF), grad).astype(BF)
        ref, base = grad_refs[2]
        ref[:, base + head * HD : base + (head + 1) * HD] = grad_value
        for which, grad_rows, inverse, held in ((0, grad_query, inv_q_ref, scaled_q), (1, grad_key, inv_k_ref, scaled_k)):
            if rotary:
                grad_rows = turned(grad_rows, cos_ref, sin_ref, -1.0)
            raw = view(which, head)
            gain_out[which : which + 1, part] = jnp.sum(grad_rows * raw * inverse[...], axis=0, keepdims=True)
            scaled = grad_rows * gain_ref[which : which + 1, part]
            held[:, part] = scaled
            dots[which] = scaled * raw if head == 0 else dots[which] + scaled * raw
    for which, own, peer in ((0, q_dot, q_peer), (1, k_dot, k_peer)):
        own[...] = jnp.broadcast_to(jnp.sum(dots[which], axis=1, keepdims=True), own.shape)
        fly.send(own, peer, send.at[which], recv.at[which], core_peer)
    for which, own, peer, inverse, held in (
        (0, q_dot, q_peer, inv_q_ref, scaled_q),
        (1, k_dot, k_peer, inv_k_ref, scaled_k),
    ):
        landed(peer, recv.at[which], core_peer)
        column = inverse[...]
        slope = column * column * column * ((own[...] + peer[...]) / D)
        ref, base = grad_refs[which]
        for head in range(heads):
            part = slice(head * HD, (head + 1) * HD)
            out = held[:, part] * column - view(which, head) * slope
            ref[:, base + head * HD : base + (head + 1) * HD] = out.astype(BF)
    fly.drain()


def attend_call(kernel, joint, rotary, number, live, raws, others, shapes, scratch, flops, exps):
    dma = pltpu.SemaphoreType.DMA
    arrays = [*raws, *others]
    moved = sum(v.size * v.dtype.itemsize for v in [*arrays, *shapes])
    return pl.pallas_call(
        functools.partial(kernel, joint, rotary),
        out_shape=shapes,
        in_specs=[SM] + [VM] * len(arrays),
        out_specs=[VM] * len(shapes),
        scratch_shapes=[*scratch, dma((2,)), dma((2,))],
        compiler_params=pltpu.CompilerParams(collective_id=number, has_side_effects=True),
        cost_estimate=pl.CostEstimate(flops=flops, bytes_accessed=moved, transcendentals=exps),
    )(live, *arrays)


def attend_sizes(raws):
    joint = len(raws) == 1
    rows, keys = raws[0].shape[0], raws[-1].shape[0]
    return joint, rows, keys, raws[0].shape[1] // 3 if joint else raws[0].shape[1]


def attend_forward(live, raws, gains, cosine, sine, rotary, number):
    joint, rows, keys, width = attend_sizes(raws)
    shape = jax.ShapeDtypeStruct
    shapes = [
        shape((rows, width), BF),
        shape((rows, width), F32),
        shape((rows, width), BF),
        shape((keys, width), BF),
        shape((rows, HD), F32),
        shape((keys, HD), F32),
    ]
    scratch = [pltpu.VMEM((n, HD), F32) for n in (rows, keys, rows, keys)]
    work = rows * keys * width
    return attend_call(
        attend_forward_kernel, joint, rotary, number, live, raws, [gains, cosine, sine],
        shapes, scratch, 4 * work, 2 * work // HD,
    )


def attend_backward(live, raws, gains, cosine, sine, rotary, number, saved, grad):
    joint, rows, keys, width = attend_sizes(raws)
    shape = jax.ShapeDtypeStruct
    shapes = [shape(raw.shape, BF) for raw in raws] + [shape((8, width), F32)]
    scratch = [pltpu.VMEM((rows, width), F32), pltpu.VMEM((keys, width), F32)]
    scratch += [pltpu.VMEM((n, HD), F32) for n in (rows, keys, rows, keys)]
    work = rows * keys * width
    return attend_call(
        attend_backward_kernel, joint, rotary, number, live, raws,
        [gains, cosine, sine, *saved, grad], shapes, scratch, 10 * work, work // HD,
    )


ALL_CHIPS, KEEP, HALF_X, HALF_Y = range(4)


def gather_kernel(outer, kinds, *refs):
    full = len(kinds)
    ins, refs = refs[:full], refs[full:]
    mlp_ref, text_ref, refs = refs[0], refs[1], refs[2:]
    outs, refs = list(refs[:full]), refs[full:]
    up_out, text_out, refs = refs[0], refs[1], refs[2:]
    own, refs = refs[:full], refs[full:]
    halves = [i for i, kind in enumerate(kinds) if kind[1] == KEEP]
    form = [kind[1] for kind in kinds]
    whole, refs = refs[: len(halves)], refs[len(halves) :]
    up_own, local_sem, zs, zr, s1, r1, s2, r2, a_s, a_r, f_s, f_r, f_l, t_s = refs
    z, y, x = (lax.axis_index(name) for name in FS)
    core = lax.axis_index("sp")
    here = 2 * y + x
    up = full
    fins = {}
    for j, i in enumerate(halves):
        fins[i] = outs[i]
        outs[i] = whole[j]
    fly = Flights()
    x_peer, y_peer = {"xc": 1 - x}, {"yb": 1 - y}
    diagonal = {"yb": 1 - y, "xc": 1 - x}
    around = ((x_peer, y, 1 - x), (y_peer, 1 - y, x), (diagonal, 1 - y, 1 - x))
    above, below = {"za": z + 1}, {"za": z - 1}
    core_peer = {"sp": 1 - core}
    has_above, has_below = z + 1 < outer, z >= 1
    greet((x_peer, y_peer, diagonal, core_peer), ((has_above, above), (has_below, below)))

    for i, (parts, _) in enumerate(kinds):
        if parts == 0:
            own[i][...] = ins[i][...]
        for part in range(parts):
            width = ins[i].shape[1] // (2 * parts)
            column = pl.multiple_of((2 * part + core) * width, width)
            own[i][:, part * width : (part + 1) * width] = ins[i][:, pl.ds(column, width)]

    def spot(i, slot, ty, tx):
        if form[i] == HALF_X:
            return outs[i].at[slot, tx]
        if form[i] == HALF_Y:
            return outs[i].at[slot, ty]
        return outs[i].at[slot, ty, tx]

    def shard(i, slot):
        return spot(i, slot, y, x) if i < full else up_out.at[slot]

    def z_send(i, way, hop, source=None):
        if hop > outer - 2:
            return
        slot = z - hop if way == 0 else z + hop
        when = jnp.logical_and(has_above, slot >= 0) if way == 0 else jnp.logical_and(has_below, slot < outer)
        fly.send(
            shard(i, slot) if source is None else source,
            shard(i, slot),
            zs.at[i, way, hop],
            zr.at[i, way, hop],
            above if way == 0 else below,
            when,
        )

    def z_slot(way, hop):
        slot = z - 1 - hop if way == 0 else z + 1 + hop
        return slot, (slot >= 0 if way == 0 else slot < outer)

    def z_wait(i, way, hop):
        slot, when = z_slot(way, hop)

        @pl.when(when)
        def _():
            landed(shard(i, slot), zr.at[i, way, hop], below if way == 0 else above)

    def turns(i, slot):
        turn = (slot + i) % 2
        first = ((y + turn) % 2, (x + 1 - turn) % 2)
        second = ((y + 1 - turn) % 2, (x + turn) % 2)
        return first, second

    def xy_own(i, slot, when=None, source=None):
        mine = spot(i, slot, y, x)
        source = mine if source is None else source
        if form[i] in (HALF_X, HALF_Y):
            peer = x_peer if form[i] == HALF_X else y_peer
            fly.send(source, mine, s1.at[i, slot], r1.at[i, slot], peer, when)
            return
        first, second = turns(i, slot)
        fly.send(source, mine, s1.at[i, slot], r1.at[i, slot], {"yb": first[0], "xc": first[1]}, when)
        fly.send(source, mine, s2.at[i, slot, 0], r2.at[i, slot, 0], {"yb": second[0], "xc": second[1]}, when)

    def xy_pass(i, slot, when=None):
        if form[i] in (HALF_X, HALF_Y):
            return
        first, second = turns(i, slot)
        theirs = outs[i].at[slot, first[0], first[1]]

        def wait():
            landed(theirs, r1.at[i, slot], {"yb": first[0], "xc": first[1]})

        if when is None:
            wait()
        else:
            pl.when(when)(wait)
        fly.send(theirs, theirs, s2.at[i, slot, 1], r2.at[i, slot, 1], {"yb": second[0], "xc": second[1]}, when)

    def xy_end(i, slot):
        if form[i] == HALF_X:
            landed(spot(i, slot, y, 1 - x), r1.at[i, slot], x_peer)
            return
        if form[i] == HALF_Y:
            landed(spot(i, slot, 1 - y, x), r1.at[i, slot], y_peer)
            return
        _, second = turns(i, slot)
        device = {"yb": second[0], "xc": second[1]}
        landed(outs[i].at[slot, second[0], second[1]], r2.at[i, slot, 0], device)
        landed(outs[i].at[slot, 1 - y, 1 - x], r2.at[i, slot, 1], device)

    for i in range(full):
        for way in range(2):
            z_send(i, way, 0, own[i])
        xy_own(i, z, None, own[i])
    locals_ = [fly.local(own[i], spot(i, z, y, x), local_sem.at[i]) for i in range(full)]

    fly.send(text_ref, text_out.at[core], t_s.at[0], t_s.at[1], core_peer)
    locals_.append(fly.local(text_ref, text_out.at[core], t_s.at[2]))
    hid = mlp_ref.shape[1] // (outer * PLANE * 2)
    for own_core in range(2):

        @pl.when(core == own_core)
        def _(own_core=own_core):
            for place in range(PLANE):
                for slot in range(outer):
                    column = ((slot * PLANE + place) * 2 + own_core) * hid
                    up_own[place, :, slot * hid : (slot + 1) * hid] = mlp_ref[:, column : column + hid]

    for hop in range(outer - 1):
        for i in range(full):
            for way in range(2):
                slot, when = z_slot(way, hop)
                z_wait(i, way, hop)
                z_send(i, way, hop + 1)
                xy_own(i, slot, when)
        if hop == 0:
            locals_.append(fly.local(up_own.at[here], up_out.at[z, here], local_sem.at[up]))
            for turn, (device, ty, tx) in enumerate(around):
                fly.send(up_own.at[2 * ty + tx], up_out.at[z, here], a_s.at[turn], a_r.at[turn], device)
    for copy in locals_:
        copy.wait()
    for turn, (device, ty, tx) in enumerate(around):
        landed(up_out.at[z, 2 * ty + tx], a_r.at[turn], device)
    for way in range(2):
        z_send(up, way, 0)
    for i in range(full):
        xy_pass(i, z)
    for hop in range(outer - 1):
        for i in range(full):
            for way in range(2):
                slot, when = z_slot(way, hop)
                xy_pass(i, slot, when)
        for way in range(2):
            z_wait(up, way, hop)
            z_send(up, way, hop + 1)
    for i in (*halves, *(i for i in range(full) if i not in halves)):
        for slot in range(outer):
            xy_end(i, slot)
        if i not in halves:
            continue
        j, part = halves.index(i), outer // 2
        width = own[i].shape[-1]
        columns = pl.ds(pl.multiple_of(core * width, width), width)
        theirs, ours = pl.ds((1 - core) * part, part), pl.ds(core * part, part)
        fly.send(outs[i].at[theirs], fins[i].at[:, :, :, :, columns], f_s.at[j], f_r.at[j], core_peer)
        fly.local(outs[i].at[ours], fins[i].at[:, :, :, :, columns], f_l.at[j])
    for j, i in enumerate(halves):
        width = own[i].shape[-1]
        columns = pl.ds(pl.multiple_of(core * width, width), width)
        others = pl.ds(pl.multiple_of((1 - core) * width, width), width)
        ours = pl.ds(core * (outer // 2), outer // 2)
        pltpu.make_async_copy(outs[i].at[ours], fins[i].at[:, :, :, :, columns], f_l.at[j]).wait()
        landed(fins[i].at[:, :, :, :, others], f_r.at[j], core_peer)
    landed(text_out.at[1 - core], t_s.at[1], core_peer)
    fly.drain()


def gather_weights(outer, kinds, arrays, mlp, text):
    shapes, own, whole = [], [], []
    for (parts, form), array in zip(kinds, arrays, strict=True):
        rows, width = array.shape
        half = width // 2 if parts else width
        own.append(pltpu.VMEM((rows, half), array.dtype))
        if form in (HALF_X, HALF_Y):
            shapes.append(jax.ShapeDtypeStruct((outer, 2, rows, half), array.dtype))
        elif form == KEEP:
            whole.append(pltpu.VMEM((outer, 2, 2, rows, half), array.dtype))
            shapes.append(jax.ShapeDtypeStruct((outer // 2, 2, 2, rows, width), array.dtype))
        else:
            shapes.append(jax.ShapeDtypeStruct((outer, 2, 2, rows, half), array.dtype))
    rows, units = mlp.shape
    mine = units // (2 * PLANE)
    shapes.append(jax.ShapeDtypeStruct((outer, PLANE, rows, mine), mlp.dtype))
    shapes.append(jax.ShapeDtypeStruct((2, *text.shape), text.dtype))
    dma = pltpu.SemaphoreType.DMA
    hops = outer - 1
    nf, nh = len(kinds), len(whole)
    results = pl.pallas_call(
        functools.partial(gather_kernel, outer, kinds),
        out_shape=shapes,
        in_specs=[VM] * (nf + 2),
        out_specs=[ANY] * len(shapes),
        scratch_shapes=[
            *own,
            *whole,
            pltpu.VMEM((PLANE, rows, mine), mlp.dtype),
            dma((nf + 1,)),
            dma((nf + 1, 2, hops)),
            dma((nf + 1, 2, hops)),
            dma((nf, outer)),
            dma((nf, outer)),
            dma((nf, outer, 2)),
            dma((nf, outer, 2)),
            dma((3,)),
            dma((3,)),
            dma((nh,)),
            dma((nh,)),
            dma((nh,)),
            dma((3,)),
        ],
        compiler_params=pltpu.CompilerParams(
            collective_id=0, has_side_effects=True, vmem_limit_bytes=40 * 1024 * 1024
        ),
        cost_estimate=pl.CostEstimate(flops=10**11, bytes_accessed=10**8, transcendentals=0),
        name="gather_weights",
    )(*arrays, mlp, text)
    return [value.reshape(-1, value.shape[-1]) if value.ndim != 4 or i >= nf else value for i, value in enumerate(results)]


def plane_gather_kernel(own_ref, out_ref, local_sem, send, recv):
    y, x, core = lax.axis_index("yb"), lax.axis_index("xc"), lax.axis_index("sp")
    x_peer, y_peer, core_peer = {"xc": 1 - x}, {"yb": 1 - y}, {"sp": 1 - core}
    fly = Flights()
    greet((x_peer, y_peer, core_peer))
    size = own_ref.shape[0] // 2
    top, low = pl.ds(0, size), pl.ds(size, size)
    fly.send(own_ref.at[top], out_ref.at[0, 1, 0, top], send.at[0], recv.at[0], x_peer)
    fly.send(own_ref.at[low], out_ref.at[1, 0, 0, low], send.at[1], recv.at[1], y_peer)
    fly.send(own_ref.at[low], out_ref.at[0, 1, 0, low], send.at[2], recv.at[2], x_peer)
    fly.send(own_ref.at[top], out_ref.at[1, 0, 0, top], send.at[3], recv.at[3], y_peer)
    fly.send(own_ref, out_ref.at[0, 0, 1], send.at[4], recv.at[4], core_peer)
    local = fly.local(own_ref, out_ref.at[0, 0, 0], local_sem.at[0])
    across = []

    def arrive(index, dy, dx, rows, device, onward=None):
        block = out_ref.at[dy, dx, 0, rows]
        landed(block, recv.at[index], device)
        if onward is not None:
            to, number = onward
            fly.send(block, out_ref.at[1, 1, 0, rows], send.at[number], recv.at[number], to)
        fly.send(block, out_ref.at[dy, dx, 1, rows], send.at[index + 7], recv.at[index + 7], core_peer)
        across.append((index + 7, dy, dx, rows))

    arrive(0, 0, 1, top, x_peer, (y_peer, 5))
    arrive(1, 1, 0, low, y_peer, (x_peer, 6))
    arrive(2, 0, 1, low, x_peer)
    arrive(3, 1, 0, top, y_peer)
    arrive(5, 1, 1, top, y_peer)
    arrive(6, 1, 1, low, x_peer)
    landed(out_ref.at[0, 0, 1], recv.at[4], core_peer)
    for index, dy, dx, rows in across:
        landed(out_ref.at[dy, dx, 1, rows], recv.at[index], core_peer)
    local.wait()
    fly.drain()


def plane_gather(own):
    rows, width = own.shape
    dma = pltpu.SemaphoreType.DMA
    out = pl.pallas_call(
        plane_gather_kernel,
        out_shape=jax.ShapeDtypeStruct((2, 2, 2, rows, width), own.dtype),
        in_specs=[VM],
        out_specs=VM,
        scratch_shapes=[dma((1,)), dma((14,)), dma((14,))],
        compiler_params=pltpu.CompilerParams(collective_id=1, has_side_effects=True),
        cost_estimate=pl.CostEstimate(flops=10**10, bytes_accessed=10**7, transcendentals=0),
        name="plane_gather",
    )(own)
    return out.reshape(8 * rows, width)


def plane_sum_kernel(part_a, part_b, out_a, out_b, core_in, first, second, keep, send, recv):
    y, x, core = lax.axis_index("yb"), lax.axis_index("xc"), lax.axis_index("sp")
    x_peer, y_peer, core_peer = {"xc": 1 - x}, {"yb": 1 - y}, {"sp": 1 - core}
    fly = Flights()
    greet((x_peer, y_peer, core_peer))
    rows = part_a.shape[3]
    chips = (((1, 1), (1, 0), (0, 1), (0, 0)), ((1, 1), (0, 1), (1, 0), (0, 0)))
    parts, outs, peers = (part_a, part_b), (out_a, out_b), ((y_peer, x_peer), (x_peer, y_peer))
    for index in range(4):
        for n in range(2):
            dy, dx = chips[n][index]
            fly.send(
                parts[n].at[dy, dx, 1], core_in.at[n, index], send.at[n, index], recv.at[n, index], core_peer
            )

    def core_sum(n, index):
        dy, dx = chips[n][index]
        landed(core_in.at[n, index], recv.at[n, index], core_peer)
        row_add(core_in.at[n, index], core_in.at[n, index], parts[n].at[dy, dx, 0], rows)

    for index in range(2):
        for n in range(2):
            core_sum(n, index)
            fly.send(
                core_in.at[n, index], first.at[n, index], send.at[n, index + 4], recv.at[n, index + 4], peers[n][0]
            )
    for index in (2, 3):
        for n in range(2):
            core_sum(n, index)
    for n in range(2):
        landed(first.at[n, 0], recv.at[n, 4], peers[n][0])
        row_add(second.at[n, 0], first.at[n, 0], core_in.at[n, 2], rows)
        fly.send(second.at[n, 0], second.at[n, 1], send.at[n, 6], recv.at[n, 6], peers[n][1])
    for n in range(2):
        landed(first.at[n, 1], recv.at[n, 5], peers[n][0])
        row_sum(keep.at[n], first.at[n, 1], core_in.at[n, 3], rows)
    for n in range(2):
        landed(second.at[n, 1], recv.at[n, 6], peers[n][1])
        row_sum(outs[n], keep.at[n], second.at[n, 1], rows)
    fly.drain()


def plane_sum(one, other):
    rows, width = one.shape[0] // 8, one.shape[1]
    dma = pltpu.SemaphoreType.DMA
    shape = jax.ShapeDtypeStruct((rows, width), F32)
    return pl.pallas_call(
        plane_sum_kernel,
        out_shape=(shape, shape),
        in_specs=[VM, VM],
        out_specs=(VM, VM),
        scratch_shapes=[
            pltpu.VMEM((2, 4, rows, width), BF),
            pltpu.VMEM((2, 2, rows, width), BF),
            pltpu.VMEM((2, 2, rows, width), BF),
            pltpu.VMEM((2, rows, width), F32),
            dma((2, 7)),
            dma((2, 7)),
        ],
        compiler_params=pltpu.CompilerParams(collective_id=2, has_side_effects=True),
        cost_estimate=pl.CostEstimate(flops=10**10, bytes_accessed=10**7, transcendentals=0),
        name="plane_sum",
    )(one.reshape(2, 2, 2, rows, width), other.reshape(2, 2, 2, rows, width))


def pair_sum_kernel(part_ref, out_ref, peer_in, send, recv):
    core = lax.axis_index("sp")
    core_peer = {"sp": 1 - core}
    fly = Flights()
    greet((core_peer,))
    size = part_ref.shape[1] // 2
    for index in range(2):
        rows = pl.ds(index * size, size)
        fly.send(part_ref.at[1 - core, rows], peer_in.at[rows], send.at[index], recv.at[index], core_peer)
    for index in range(2):
        rows = pl.ds(index * size, size)
        landed(peer_in.at[rows], recv.at[index], core_peer)
        row_sum(out_ref.at[rows], part_ref.at[core, rows], peer_in.at[rows], size)
    fly.drain()


def pair_sum(partial):
    rows, width = partial.shape[0] // 2, partial.shape[1]
    dma = pltpu.SemaphoreType.DMA
    return pl.pallas_call(
        pair_sum_kernel,
        out_shape=jax.ShapeDtypeStruct((rows, width), F32),
        in_specs=[VM],
        out_specs=VM,
        scratch_shapes=[pltpu.VMEM((rows, width), F32), dma((2,)), dma((2,))],
        compiler_params=pltpu.CompilerParams(collective_id=4, has_side_effects=True),
        cost_estimate=pl.CostEstimate(flops=10**9, bytes_accessed=10**7, transcendentals=0),
        name="pair_sum",
    )(partial.reshape(2, rows, width))


AHEAD, LAG_PLANE, LAG_CHAIN = 6, 2, 4
PLAIN, SPLIT, OVER_X, OVER_Y = range(4)


def reduce_kernel(outer, kinds, *refs):
    count = len(kinds)
    shards = outer * PLANE
    gs, refs = refs[:count], refs[count:]
    frames_ref, small_ref, up_ref, down_ref, refs = *refs[:4], refs[4:]
    outs, refs = refs[:count], refs[count:]
    frames_out, small_out, up_out, down_out, refs = *refs[:4], refs[4:]
    pieces = [(i, part) for i, (parts, _) in enumerate(kinds) for part in range(parts)]
    total = len(pieces)
    forms = [kinds[i][1] for i, _ in pieces]
    near_refs, near = list(refs), {}
    for p in range(total):
        if forms[p] in (PLAIN, SPLIT):
            near[p] = near_refs.pop(0)
    refs = near_refs
    plane, refs = refs[:total], refs[total:]
    chain, refs = refs[:total], refs[total:]
    split = [i for i, kind in enumerate(kinds) if kind[1] == SPLIT]
    whole, refs = refs[: len(split)], refs[len(split) :]
    small_in, small_own, small_peer, up_in, down_in, refs = *refs[:5], refs[5:]
    e_s, e_r, e_l, s1, r1, s2, r2, zs, zr, o_s, o_r, f_s, f_r, m_s, m_r, l_s, p_s, p_r = refs
    z, y, x = (lax.axis_index(name) for name in FS)
    core = lax.axis_index("sp")
    here = (z * 2 + y) * 2 + x
    core_peer = {"sp": 1 - core}
    above, below = {"za": z + 1}, {"za": z - 1}
    fly = Flights()

    def chip(index):
        return {"za": index // 4, "yb": (index // 2) % 2, "xc": index % 2}

    others = [(here + j) % shards for j in range(1, shards)]
    greet((core_peer, *[chip(index) for index in others]))

    part_slots = outer // 2
    ours, other_slots = pl.ds(core * part_slots, part_slots), pl.ds((1 - core) * part_slots, part_slots)
    for j, i in enumerate(split):
        width = whole[j].shape[-1]
        mine = pl.ds(pl.multiple_of(core * width, width), width)
        theirs = pl.ds(pl.multiple_of((1 - core) * width, width), width)
        fly.send(gs[i].at[:, :, :, :, theirs], whole[j].at[ours], e_s.at[j], e_r.at[j], core_peer)
        fly.local(gs[i].at[:, :, :, :, mine], whole[j].at[ours], e_l.at[j])

    def joined(i):
        j = split.index(i)
        width = whole[j].shape[-1]
        mine = pl.ds(pl.multiple_of(core * width, width), width)
        pltpu.make_async_copy(gs[i].at[:, :, :, :, mine], whole[j].at[ours], e_l.at[j]).wait()
        landed(whole[j].at[other_slots], e_r.at[j], core_peer)

    def width_of(p):
        return plane[p].shape[-1]

    def source(p, *place):
        i, part = pieces[p]
        held = whole[split.index(i)] if forms[p] == SPLIT else gs[i]
        width = width_of(p)
        return held.at[(*place, slice(None), pl.ds(part * width, width))]

    frame_copy = fly.local(frames_ref, frames_out.at[here, core], l_s.at[0])
    small_copy = fly.local(small_ref.at[here], small_in.at[here], l_s.at[1])
    for j, index in enumerate(others):
        fly.send(frames_ref, frames_out.at[here, core], f_s.at[j], f_r.at[here], chip(index))
        fly.send(small_ref.at[index], small_in.at[here], m_s.at[j], m_r.at[here], chip(index))

    near_by = ((y, 1 - x), (1 - y, x), (1 - y, 1 - x))
    up_copy = fly.local(up_ref.at[2 * y + x], up_in.at[core, 2 * y + x], p_s.at[0])
    for j, (ty, tx) in enumerate(near_by):
        fly.send(
            up_ref.at[2 * ty + tx],
            up_in.at[core, 2 * y + x],
            p_s.at[j + 1],
            p_r.at[j + 1],
            {"yb": ty, "xc": tx},
        )
    fly.send(down_ref, down_in, p_s.at[4], p_r.at[4], core_peer)

    def feed_forward_landed():
        up_copy.wait()
        for j, (ty, tx) in enumerate(near_by):
            landed(up_in.at[core, 2 * ty + tx], p_r.at[j + 1], {"yb": ty, "xc": tx})
        fly.send(up_in.at[core], up_in.at[core], p_s.at[5], p_r.at[5], core_peer)
        hid = down_ref.shape[0]
        landed(down_in, p_r.at[4], core_peer)
        for side in range(2):

            @pl.when(core == side)
            def _(side=side):
                down_out[side * hid : (side + 1) * hid, :] = down_ref[...].astype(F32)
                down_out[(1 - side) * hid : (2 - side) * hid, :] = down_in[...].astype(F32)

    def feed_forward_rows():
        hid = down_ref.shape[0]
        landed(up_in.at[1 - core], p_r.at[5], core_peer)
        for slot in range(outer):
            for place in range(PLANE):
                for side in range(2):
                    column = ((slot * PLANE + place) * 2 + side) * hid
                    up_out[:, column : column + hid] = up_in[side, place, :, slot * hid : (slot + 1) * hid].astype(F32)

    def slot_at(step):
        if step == outer - 1:
            return z
        falling = outer - 1 - step
        falling = jnp.where(falling > z, falling, falling - 1)
        rising = jnp.where(step < z, step, step + 1)
        return jnp.where(z < part_slots, falling, rising)

    units = [(slot_at(step), p) for step in range(outer) for p in range(total)]

    def turns(p, slot):
        turn = (slot + p) % 2
        first = ((y + 1 - turn) % 2, (x + turn) % 2)
        second = ((y + turn) % 2, (x + 1 - turn) % 2)
        return first, second

    def device(place):
        return {"yb": place[0], "xc": place[1]}

    def start(slot, p):
        first, _ = turns(p, slot)
        fly.send(
            source(p, slot, 1 - y, 1 - x), near[p].at[slot, 1], s1.at[p, slot, 1], r1.at[p, slot, 1], device(first)
        )
        fly.send(
            source(p, slot, first[0], first[1]), near[p].at[slot, 0], s1.at[p, slot, 0], r1.at[p, slot, 0], device(first)
        )

    def summed_over(p):
        return (x, {"xc": 1 - x}) if forms[p] == OVER_X else (y, {"yb": 1 - y})

    def pass_on(slot, p):
        rows = plane[p].shape[1]
        if p not in near:
            index, peer = summed_over(p)
            fly.send(source(p, slot, 1 - index), plane[p].at[slot], s2.at[p, slot], r2.at[p, slot], peer)
            return
        first, second = turns(p, slot)
        landed(near[p].at[slot, 1], r1.at[p, slot, 1], device(first))
        row_add(near[p].at[slot, 1], near[p].at[slot, 1], source(p, slot, second[0], second[1]), rows)
        fly.send(near[p].at[slot, 1], plane[p].at[slot], s2.at[p, slot], r2.at[p, slot], device(second))
        landed(near[p].at[slot, 0], r1.at[p, slot, 0], device(first))
        row_add(near[p].at[slot, 0], near[p].at[slot, 0], source(p, slot, y, x), rows)

    def plane_total(slot, p):
        rows = plane[p].shape[1]
        if p not in near:
            index, peer = summed_over(p)
            landed(plane[p].at[slot], r2.at[p, slot], peer)
            row_add(plane[p].at[slot], plane[p].at[slot], source(p, slot, index), rows)
            return
        _, second = turns(p, slot)
        landed(plane[p].at[slot], r2.at[p, slot], device(second))
        row_add(plane[p].at[slot], plane[p].at[slot], near[p].at[slot, 0], rows)

    def along(slot, p, last):
        rows, width = plane[p].shape[1:]
        if not last:
            for way, when, edge, ahead, behind in (
                (1, slot < z, z == outer - 1, below, above),
                (0, slot > z, z == 0, above, below),
            ):
                link = chain[p].at[slot + 1 - way]

                @pl.when(jnp.logical_and(when, jnp.logical_not(edge)))
                def _(way=way, link=link, behind=behind):
                    landed(link, zr.at[p, way, slot], behind)
                    row_add(plane[p].at[slot], plane[p].at[slot], link, rows)

                fly.send(plane[p].at[slot], link, zs.at[p, way, slot], zr.at[p, way, slot], ahead, when)
            return
        has_above, has_below = z < outer - 1, z > 0
        for way, when, behind in ((1, has_above, above), (0, has_below, below)):

            @pl.when(when)
            def _(way=way, behind=behind):
                landed(chain[p].at[slot + 1 - way], zr.at[p, way, slot], behind)

        step = 16 if rows % 16 == 0 else rows
        i, part = pieces[p]
        column = pl.multiple_of((2 * part + core) * width, width)

        def chunk(index, carry):
            at = pl.ds(pl.multiple_of(index * step, step), step)
            upper = jnp.where(has_above, chain[p][slot, at, :].astype(F32), 0.0)
            lower = jnp.where(has_below, chain[p][slot + 1, at, :].astype(F32), 0.0)
            outs[i][at, pl.ds(column, width)] = plane[p][slot, at, :].astype(F32) + upper + lower
            return carry

        lax.fori_loop(0, rows // step, chunk, 0)
        block = outs[i].at[:, pl.ds(column, width)]
        fly.send(block, block, o_s.at[p], o_r.at[p], core_peer)

    waiting = set(split)

    def begin(unit):
        slot, p = units[unit]
        if p not in near:
            return
        if pieces[p][0] in waiting:
            joined(pieces[p][0])
            waiting.discard(pieces[p][0])
        start(slot, p)

    for unit in range(min(AHEAD, len(units))):
        begin(unit)
    for tick in range(len(units) + LAG_CHAIN):
        if tick < len(units):
            pass_on(*units[tick])
            if tick + AHEAD < len(units):
                begin(tick + AHEAD)
        if 0 <= tick - LAG_PLANE < len(units):
            plane_total(*units[tick - LAG_PLANE])
        if tick == 4:
            feed_forward_landed()
        if tick == 10:
            feed_forward_rows()
        if 0 <= tick - LAG_CHAIN < len(units):
            unit = tick - LAG_CHAIN
            along(*units[unit], unit >= (outer - 1) * total)
        if tick == total:
            frame_copy.wait()
            for index in others:
                landed(frames_out.at[index, core], f_r.at[index], chip(index))
            fly.send(frames_out.at[:, core], frames_out.at[:, core], p_s.at[6], p_r.at[6], core_peer)
            small_copy.wait()
            for index in others:
                landed(small_in.at[index], m_r.at[index], chip(index))
            small_own[...] = jnp.sum(small_in[...], axis=0)
            fly.send(small_own, small_peer, l_s.at[2], l_s.at[3], core_peer)

    landed(frames_out.at[:, 1 - core], p_r.at[6], core_peer)
    landed(small_peer, l_s.at[3], core_peer)
    small_out[...] = small_own[...] + small_peer[...]
    for p, (i, part) in enumerate(pieces):
        width = width_of(p)
        column = pl.multiple_of((2 * part + 1 - core) * width, width)
        landed(outs[i].at[:, pl.ds(column, width)], o_r.at[p], core_peer)
    fly.drain()


def reduce_weights(outer, kinds, grads, frames, small, up, down):
    shards = outer * PLANE
    shaped, shapes, near, plane, chain, whole = [], [], [], [], [], []
    for (parts, form), grad in zip(kinds, grads, strict=True):
        full_width = grad.shape[-1] // 2 if form == SPLIT else grad.shape[-1]
        if form in (PLAIN, SPLIT):
            lead = outer // 2 if form == SPLIT else outer
            grad = grad.reshape(lead, 2, 2, -1, grad.shape[-1])
        rows, width = grad.shape[-2], full_width // parts
        shaped.append(grad)
        shapes.append(jax.ShapeDtypeStruct((rows, 2 * full_width), F32))
        for _ in range(parts):
            if form in (PLAIN, SPLIT):
                near.append(pltpu.VMEM((outer, 2, rows, width), BF))
            plane.append(pltpu.VMEM((outer, rows, width), BF))
            chain.append(pltpu.VMEM((outer + 1, rows, width), BF))
        if form == SPLIT:
            whole.append(pltpu.VMEM((outer, 2, 2, rows, full_width), BF))
    shapes.append(jax.ShapeDtypeStruct((shards, 2, *frames.shape), frames.dtype))
    shapes.append(jax.ShapeDtypeStruct(small.shape[1:], F32))
    shapes.append(jax.ShapeDtypeStruct((up.shape[1], 2 * PLANE * up.shape[2]), F32))
    shapes.append(jax.ShapeDtypeStruct((2 * down.shape[0], down.shape[1]), F32))
    dma = pltpu.SemaphoreType.DMA
    count, total, nsplit = len(kinds), len(plane), len(whole)
    results = pl.pallas_call(
        functools.partial(reduce_kernel, outer, kinds),
        out_shape=shapes,
        in_specs=[VM] * (count + 4),
        out_specs=[VM] * (count + 4),
        scratch_shapes=[
            *near,
            *plane,
            *chain,
            *whole,
            pltpu.VMEM(small.shape, F32),
            pltpu.VMEM(small.shape[1:], F32),
            pltpu.VMEM(small.shape[1:], F32),
            pltpu.VMEM((2, *up.shape), up.dtype),
            pltpu.VMEM(down.shape, down.dtype),
            dma((nsplit,)),
            dma((nsplit,)),
            dma((nsplit,)),
            dma((total, outer, 2)),
            dma((total, outer, 2)),
            dma((total, outer)),
            dma((total, outer)),
            dma((total, 2, outer)),
            dma((total, 2, outer)),
            dma((total,)),
            dma((total,)),
            dma((shards,)),
            dma((shards,)),
            dma((shards,)),
            dma((shards,)),
            dma((4,)),
            dma((7,)),
            dma((7,)),
        ],
        cost_estimate=pl.CostEstimate(flops=10**11, bytes_accessed=10**8, transcendentals=0),
        compiler_params=pltpu.CompilerParams(
            collective_id=3, has_side_effects=True, vmem_limit_bytes=67043328
        ),
        name="reduce_weights",
    )(*shaped, frames, small, up, down)
    return results[:count], *results[count:]


def modulation_kernel(sinus_ref, matrix_ref, bias_ref, out_ref, half, send, recv):
    core = lax.axis_index("sp")
    core_peer = {"sp": 1 - core}
    fly = Flights()
    greet((core_peer,))
    frames, width = out_ref.shape[0], matrix_ref.shape[1]
    half[...] = product(sinus_ref[...], matrix_ref[...]) + bias_ref[...]
    for side in range(2):

        @pl.when(core == side)
        def _(side=side):
            out_ref[:, side * width : (side + 1) * width] = half[side * frames : (side + 1) * frames, :]
            half[:frames, :] = half[(1 - side) * frames : (2 - side) * frames, :]

    columns = pl.ds(pl.multiple_of(core * width, width), width)
    others = pl.ds(pl.multiple_of((1 - core) * width, width), width)
    fly.send(half.at[pl.ds(0, frames)], out_ref.at[:, columns], send.at[0], recv.at[0], core_peer)
    landed(out_ref.at[:, others], recv.at[0], core_peer)
    fly.drain()


def modulate(sinus, matrix, bias):
    dma = pltpu.SemaphoreType.DMA
    frames, width = sinus.shape[0], matrix.shape[1]
    return pl.pallas_call(
        modulation_kernel,
        out_shape=jax.ShapeDtypeStruct((frames // 2, 2 * width), F32),
        in_specs=[VM, VM, VM],
        out_specs=VM,
        scratch_shapes=[pltpu.VMEM((frames, width), F32), dma((1,)), dma((1,))],
        compiler_params=pltpu.CompilerParams(collective_id=9, has_side_effects=True),
        cost_estimate=pl.CostEstimate(flops=10**9, bytes_accessed=10**7, transcendentals=0),
        name="modulation",
    )(sinus, matrix, bias)


def gather(value, axes, axis=0):
    return lax.all_gather(value, axes, axis=axis, tiled=True)


def scatter(value, axes, axis=0):
    return lax.psum_scatter(value, axes, scatter_dimension=axis, tiled=True)


def body(
    tokens,
    text,
    clip_frames,
    timestep,
    mod_weight,
    mod_bias,
    qk_gains,
    self_in,
    self_out,
    cross_q,
    cross_kv,
    cross_out,
    mlp_in,
    mlp_out,
    cotangent,
):
    half = D // 2
    row_count = tokens.shape[0]
    frame_count = row_count // FRAME_TOK
    group_frames = timestep.shape[1]
    shards = D // self_in.shape[1]
    outer = shards // PLANE
    core = lax.axis_index("sp")
    chip = lax.axis_index(FS)
    in_rows = self_in.shape[1]
    own_frame = core * frame_count

    bias_len, gain_len = mod_bias.shape[1], qk_gains.shape[2]
    small_len = bias_len + 4 * gain_len
    small_rows = 8
    small_width = -(-(small_len + group_frames) // (small_rows * 128)) * 128
    small_room = small_rows * small_width

    small = jnp.concatenate(
        [
            mod_bias[0].astype(F32),
            qk_gains[0].reshape(-1).astype(F32),
            timestep[0].astype(F32),
            jnp.zeros((small_room - small_len - group_frames,), F32),
        ]
    ).reshape(small_rows, small_width)
    gathered = gather_weights(
        outer,
        ((0, ALL_CHIPS), (1, ALL_CHIPS), (3, ALL_CHIPS), (1, KEEP), (1, ALL_CHIPS), (1, HALF_X), (1, HALF_Y), (1, KEEP)),
        [
            small,
            *(w[0] for w in (mod_weight, self_in, self_out, cross_q)),
            cross_kv[0, :, :D],
            cross_kv[0, :, D:],
            cross_out[0],
        ],
        mlp_in[0],
        text,
    )
    small_all, mod_matrix, self_proj, self_back, cross_qproj, k_half, v_half, cross_back = gathered[:8]
    up_matrix, text_all = gathered[8:]
    hid = mlp_out.shape[1] // 2
    down_part = lax.dynamic_slice_in_dim(mlp_out[0], core * hid, hid, 0)
    down_part, small_all = lax.optimization_barrier((down_part, small_all))
    down_matrix = gather(down_part, "za")
    small_all = small_all.reshape(shards, small_room)
    bias_all = small_all[:, :bias_len].reshape(-1)
    gain_all = (
        small_all[:, bias_len:small_len]
        .reshape(shards, 4, gain_len)
        .transpose(1, 0, 2)
        .reshape(4, 2, half)
    )
    gain_own = lax.dynamic_index_in_dim(gain_all, core, 1, keepdims=False)
    steps_all = small_all[:, small_len : small_len + group_frames].reshape(-1)

    live_keys = clip_frames * FRAME_TOK
    all_keys = jnp.full((1,), TXT, jnp.int32)
    own_steps = lax.dynamic_slice_in_dim(timestep[0], own_frame, frame_count)
    cosine, sine = (jnp.asarray(table) for table in rotary_tables(group_frames))
    sinus = sinus_features(timestep[0]).astype(BF)

    bias_half = lax.dynamic_slice_in_dim(bias_all, core * 3 * D, 3 * D)[None]
    modulation = modulate(sinus, mod_matrix, bias_half)
    shift_one, scale_one, gate_one, shift_two, scale_two, gate_two = jnp.split(
        modulation, 6, axis=1
    )

    grad_branch = frame_scaled(cotangent.astype(F32), gate_two).astype(BF)
    exchange = [(0, 1), (1, 0)]
    place_y, place_x = lax.axis_index("yb"), lax.axis_index("xc")
    k_other = lax.ppermute(k_half, "yb", exchange)
    v_other = lax.ppermute(v_half, "xc", exchange)
    residual = tokens.astype(F32)
    attn_float, back_attn_input = jax.vjp(modulated, residual, shift_one, scale_one)
    attn_input = gather(attn_float.astype(BF), "sp")
    joined = product(attn_input, self_proj)
    self_mixed, self_lse, *self_kept = attend_forward(
        live_keys, [joined], gain_own[:2], cosine, sine, True, 5
    )
    grad_branch, self_mixed = lax.optimization_barrier((grad_branch, self_mixed))
    beside = [
        grad_branch,
        lax.ppermute(grad_branch, "xc", exchange),
        lax.ppermute(grad_branch, "yb", exchange),
        lax.ppermute(grad_branch, PL, [(0, 3), (1, 2), (2, 1), (3, 0)]),
    ]
    self_branch = pair_sum(product(self_mixed, self_back))
    residual = residual + frame_scaled(self_branch, gate_one)

    def beside_own(own, other, place, axis):
        pair = jnp.where(place == 0, jnp.stack([own, other], axis), jnp.stack([other, own], axis))
        return pair.reshape(-1, own.shape[-1])

    cross_kvproj = jnp.concatenate(
        [beside_own(k_half, k_other, place_y, 1), beside_own(v_half, v_other, place_x, 2)], axis=1
    )
    text_raw = product(text_all, cross_kvproj)
    cross_float, back_cross_norm = jax.vjp(layer_norm, residual)
    cross_input = gather(cross_float.astype(BF), "sp")
    cross_raw = product(cross_input, cross_qproj)
    cross_mixed, cross_lse, *cross_kept = attend_forward(
        all_keys, [cross_raw, text_raw], gain_own[2:], cosine, sine, False, 6
    )
    cross_branch = pair_sum(product(cross_mixed, cross_back))
    residual = residual + cross_branch
    residual, *beside = lax.optimization_barrier((residual, *beside))
    beside = jnp.stack(beside)
    grad_branch_all = jnp.stack([beside, lax.ppermute(beside, "sp", exchange)], axis=1).reshape(-1, D)


    mlp_float, back_mlp_input = jax.vjp(modulated, residual, shift_two, scale_two)
    mlp_input = plane_gather(mlp_float.astype(BF))
    up_proj = product(mlp_input, up_matrix)
    activated_float, back_gelu = jax.vjp(
        lambda inner: jax.nn.gelu(inner, approximate=True), up_proj
    )
    activated = activated_float.astype(BF)

    mlp_part = product(activated, down_matrix).astype(BF)

    grad_rows = cotangent.astype(F32)
    grad_down = product_tn(activated, grad_branch_all).astype(BF)
    grad_up_low = back_gelu(product_nt(grad_branch_all, down_matrix))[0].astype(BF)
    grad_up = product_tn(mlp_input, grad_up_low).astype(BF)
    grad_mlp_part = product_nt(grad_up_low, up_matrix).astype(BF)
    grad_mlp_part, grad_up, grad_down = lax.optimization_barrier((grad_mlp_part, grad_up, grad_down))
    down_owned = scatter(grad_down, "za")
    up_owned = scatter(grad_up, "za")
    mlp_branch, grad_mlp_input = plane_sum(mlp_part, grad_mlp_part)
    output = (residual + frame_scaled(mlp_branch, gate_two)).astype(BF)
    grad_gate_two = frame_sum(grad_rows * mlp_branch, frame_count)
    grad_from_mlp, grad_shift_two, grad_scale_two = back_mlp_input(grad_mlp_input)
    grad_rows = grad_rows + grad_from_mlp

    grad_low = gather(grad_rows.astype(BF), "sp")
    grad_cross_back = product_tn(cross_mixed, grad_low).astype(BF)
    grad_cross_mixed = product_nt(grad_low, cross_back).astype(BF)
    cross_saved = [*cross_kept[:2], cross_lse, *cross_kept[2:]]
    grad_cross_low, grad_text_low, gains_cross = attend_backward(
        all_keys, [cross_raw, text_raw], gain_own[2:], cosine, sine, False, 7, cross_saved, grad_cross_mixed
    )
    grad_cross_qproj = product_tn(cross_input, grad_cross_low).astype(BF)
    grad_cross_kvproj = product_tn(text_all, grad_text_low).astype(BF)
    kv_parts = grad_cross_kvproj.reshape(outer, 2, 2, in_rows, -1)
    q_parts = grad_cross_qproj.reshape(outer, 2, 2, in_rows, -1)
    kv_sent = lax.ppermute(lax.dynamic_index_in_dim(kv_parts, 1 - place_y, 1, False), "yb", exchange)
    q_sent = lax.ppermute(lax.dynamic_index_in_dim(q_parts, 1 - place_x, 2, False), "xc", exchange)
    grad_cross_input = pair_sum(product_nt(grad_cross_low, cross_qproj))
    grad_rows = grad_rows + back_cross_norm(grad_cross_input)[0]

    grad_gate_one = frame_sum(grad_rows * self_branch, frame_count)
    grad_self_low = gather(frame_scaled(grad_rows, gate_one).astype(BF), "sp")
    grad_self_back = product_tn(self_mixed, grad_self_low).astype(BF)
    grad_self_mixed = product_nt(grad_self_low, self_back).astype(BF)
    self_saved = [*self_kept[:2], self_lse, *self_kept[2:]]
    grad_joined_low, gains_self = attend_backward(
        live_keys, [joined], gain_own[:2], cosine, sine, True, 8, self_saved, grad_self_mixed
    )
    grad_self_proj = product_tn(attn_input, grad_joined_low).astype(BF)
    grad_attn_input = pair_sum(product_nt(grad_joined_low, self_proj))
    grad_from_attn, grad_shift_one, grad_scale_one = back_attn_input(grad_attn_input)
    grad_rows = grad_rows + grad_from_attn

    grad_modulation = jnp.concatenate(
        [grad_shift_one, grad_scale_one, grad_gate_one, grad_shift_two, grad_scale_two, grad_gate_two],
        axis=1,
    )
    grad_gains = jnp.concatenate([gains_self[:2], gains_cross[:2]])
    both = jnp.arange(2)[None, :, None] == core
    grad_gains = jnp.where(both, grad_gains[:, None, :], 0.0).reshape(4, shards, gain_len)
    grad_small = jnp.concatenate(
        [
            jnp.sum(grad_modulation, axis=0).reshape(shards, bias_len),
            grad_gains.transpose(1, 0, 2).reshape(shards, 4 * gain_len),
            jnp.zeros((shards, small_room - small_len), F32),
        ],
        axis=1,
    ).reshape(shards, small_rows, small_width)
    kv_near = lax.dynamic_index_in_dim(kv_parts, place_y, 1, False) + kv_sent
    q_near = lax.dynamic_index_in_dim(q_parts, place_x, 2, False) + q_sent
    owned, grad_mod_all, small_owned, mlp_in_grad, mlp_out_grad = reduce_weights(
        outer,
        ((1, OVER_Y), (2, OVER_X), (1, SPLIT), (1, SPLIT), (3, PLAIN)),
        [q_near, kv_near, grad_cross_back, grad_self_back, grad_self_proj],
        grad_modulation.astype(BF),
        grad_small,
        up_owned.reshape(PLANE, -1, up_owned.shape[1]),
        down_owned,
    )
    cross_q_grad, cross_kv_grad, cross_out_grad, self_out_grad, self_in_grad = owned
    small_owned = small_owned.reshape(-1)[:small_len]
    sinus_all = sinus_features(steps_all).astype(BF)
    own_features = mod_weight.shape[1]
    sinus_own = lax.dynamic_slice_in_dim(sinus_all, chip * own_features, own_features, 1)
    mod_weight_grad = product_tn(sinus_own, grad_mod_all.reshape(-1, 6 * D))
    return (
        output,
        grad_rows,
        mod_weight_grad[None],
        small_owned[None, :bias_len],
        small_owned[bias_len:].reshape(1, 4, gain_len),
        self_in_grad[None],
        self_out_grad[None],
        cross_q_grad[None],
        cross_kv_grad[None],
        cross_out_grad[None],
        mlp_in_grad[None],
        mlp_out_grad[None],
    )


def solution(mesh):
    chips, cores = mesh.shape["fsdp"], mesh.shape["sp"]
    grid = mesh.devices.reshape(chips // PLANE, 2, PLANE // 2, cores)
    inner = Mesh(grid, ALL)
    rows, second = P(ALL, None), P(None, FS, None)
    in_specs = (
        rows,
        rows,
        P(FS),
        P(FS, None),
        second,
        P(None, FS),
        P(None, None, FS),
        *([second] * 7),
        rows,
    )
    out_specs = (rows, rows, second, P(None, FS), P(None, None, FS), *([second] * 7))

    return jax.shard_map(body, mesh=inner, in_specs=in_specs, out_specs=out_specs, check_vma=False)
```

```python
import functools
import math

import jax
import jax.numpy as jnp
import numpy as np
from jax import lax
from jax.experimental import pallas as pl
from jax.experimental.pallas import tpu as pltpu
from jax.sharding import Mesh
from jax.sharding import PartitionSpec as P


D = 1536
HD = 128
TXT = 512
FREQ = 256
WP = 8
FRAME_TOK = 64
PLANE = 4

EPSILON = 1e-06
NEGATIVE = -1e30

FS = ("za", "yb", "xc")
PL = ("yb", "xc")
ALL = ("za", "yb", "xc", "sp")
SCALE = 1.0 / math.sqrt(HD)
MESH = pl.DeviceIdType.MESH
BF = jnp.bfloat16
F32 = jnp.float32


def product(left, right):
    return jnp.dot(left, right, preferred_element_type=F32)


def product_tn(left, right):
    return lax.dot_general(left, right, (((0,), (0,)), ((), ())), preferred_element_type=F32)


def product_nt(left, right):
    return lax.dot_general(left, right, (((1,), (1,)), ((), ())), preferred_element_type=F32)


def layer_norm(values):
    centred = values - jnp.mean(values, axis=-1, keepdims=True)
    return centred * lax.rsqrt(jnp.mean(centred * centred, axis=-1, keepdims=True) + EPSILON)


def sinus_features(steps):
    half_dim = FREQ // 2
    rates = jnp.exp(jnp.arange(half_dim).astype(F32) * (-math.log(10000.0) / half_dim))
    angles = steps.astype(F32)[:, None] * rates[None, :]
    return jnp.concatenate([jnp.cos(angles), jnp.sin(angles)], axis=1)


def rotary_tables(frames):
    half_dim = HD // 2
    side_pairs = HD // 6
    lead_pairs = half_dim - 2 * side_pairs
    pair = np.arange(half_dim)
    lead = pair < lead_pairs
    side = (pair >= lead_pairs) & (pair < lead_pairs + side_pairs)
    last = pair >= lead_pairs + side_pairs

    def rates(part, start, count):
        rate = np.exp(np.float32(-math.log(10000.0)) * (pair - start).astype(np.float32) / np.float32(count))
        return np.where(part, rate, 0.0).astype(np.float32)

    spot = np.tile(np.arange(FRAME_TOK), frames)
    frame = np.repeat(np.arange(frames), FRAME_TOK).astype(np.float32)
    angles = (
        frame[:, None] * rates(lead, 0, lead_pairs)[None]
        + (spot // WP).astype(np.float32)[:, None] * rates(side, lead_pairs, side_pairs)[None]
        + (spot % WP).astype(np.float32)[:, None] * rates(last, lead_pairs + side_pairs, side_pairs)[None]
    ).astype(np.float32)
    cosine, sine = np.cos(angles), np.sin(angles)
    return np.concatenate([cosine, cosine], axis=1), np.concatenate([-sine, sine], axis=1)


def modulated(residual, shift, scale):
    frames = shift.shape[0]
    normed = layer_norm(residual).reshape(frames, -1, residual.shape[1])
    return (normed * (1.0 + scale[:, None, :]) + shift[:, None, :]).reshape(residual.shape)


def frame_scaled(rows, gate):
    frames = gate.shape[0]
    return (rows.reshape(frames, -1, rows.shape[1]) * gate[:, None, :]).reshape(rows.shape)


def frame_sum(values, frames):
    return jnp.sum(values.reshape(frames, -1, values.shape[1]), axis=1)


VM = pl.BlockSpec(memory_space=pltpu.VMEM)
SM = pl.BlockSpec(memory_space=pltpu.SMEM)
ANY = pl.BlockSpec(memory_space=pl.ANY)


def row_add(target, left, right, rows):
    step = 32 if rows % 32 == 0 else rows

    def chunk(index, carry):
        at = pl.ds(pl.multiple_of(index * step, step), step)
        target[at, :] = left[at, :] + right[at, :]
        return carry

    lax.fori_loop(0, rows // step, chunk, 0)


def row_sum(target, left, right, rows):
    step = 16 if rows % 16 == 0 else rows

    def chunk(index, carry):
        at = pl.ds(pl.multiple_of(index * step, step), step)
        target[at, :] = left[at, :].astype(F32) + right[at, :].astype(F32)
        return carry

    lax.fori_loop(0, rows // step, chunk, 0)


class Flights:
    def __init__(self):
        self.sent = []

    def send(self, source, target, send_sem, recv_sem, device, when=None):
        copy = pltpu.make_async_remote_copy(
            src_ref=source,
            dst_ref=target,
            send_sem=send_sem,
            recv_sem=recv_sem,
            device_id=device,
            device_id_type=MESH,
        )
        if when is None:
            copy.start()
        else:
            pl.when(when)(copy.start)
        self.sent.append((when, copy))

    def local(self, source, target, sem):
        copy = pltpu.make_async_copy(source, target, sem)
        copy.start()
        return copy

    def drain(self):
        for when, copy in self.sent:
            if when is None:
                copy.wait_send()
            else:
                pl.when(when)(copy.wait_send)


def landed(target, sem, device):
    pltpu.make_async_remote_copy(
        src_ref=target,
        dst_ref=target,
        send_sem=sem,
        recv_sem=sem,
        device_id=device,
        device_id_type=MESH,
    ).wait_recv()


def greet(devices, optional=()):
    barrier = pltpu.get_barrier_semaphore()
    for device in devices:
        pl.semaphore_signal(barrier, inc=1, device_id=device, device_id_type=MESH)
    for when, device in optional:

        @pl.when(when)
        def _(device=device):
            pl.semaphore_signal(barrier, inc=1, device_id=device, device_id_type=MESH)

    count = len(devices)
    for when, _ in optional:
        count = count + when.astype(jnp.int32)
    pl.semaphore_wait(barrier, count)


def raw_views(joint, refs):
    if joint:
        rows_ref, rest = refs[0], refs[1:]
        width = rows_ref.shape[1] // 3
        spans = ((rows_ref, 0), (rows_ref, width), (rows_ref, 2 * width))
    else:
        rows_ref, keys_ref, rest = refs[0], refs[1], refs[2:]
        width = rows_ref.shape[1]
        spans = ((rows_ref, 0), (keys_ref, 0), (keys_ref, width))

    def view(which, head):
        ref, base = spans[which]
        return ref[:, base + head * HD : base + (head + 1) * HD]

    return view, width, rest


def turned(values, cos_ref, sin_ref, sign):
    return values * cos_ref[...] + sign * (pltpu.roll(values, HD // 2, 1) * sin_ref[...])


def attend_forward_kernel(joint, rotary, gain_row, live_ref, *refs):
    view, width, refs = raw_views(joint, refs)
    gain_ref, cos_ref, sin_ref, refs = *refs[:3], refs[3:]
    out_ref, lse_ref, query_ref, key_ref, inv_q_ref, inv_k_ref, refs = *refs[:6], refs[6:]
    q_sum, k_sum, q_peer, k_peer, send, recv = refs
    heads = width // HD
    core_peer = {"sp": 1 - lax.axis_index("sp")}
    fly = Flights()
    greet((core_peer,))
    for which, own, peer in ((0, q_sum, q_peer), (1, k_sum, k_peer)):
        total = view(which, 0) * view(which, 0)
        for head in range(1, heads):
            total = total + view(which, head) * view(which, head)
        own[...] = jnp.broadcast_to(jnp.sum(total, axis=1, keepdims=True), own.shape)
        fly.send(own, peer, send.at[which], recv.at[which], core_peer)
    for which, own, peer, kept in ((0, q_sum, q_peer, inv_q_ref), (1, k_sum, k_peer, inv_k_ref)):
        landed(peer, recv.at[which], core_peer)
        kept[...] = lax.rsqrt((own[...] + peer[...]) / D + EPSILON)
    rows, keys = query_ref.shape[0], key_ref.shape[0]
    spot = lax.broadcasted_iota(jnp.int32, (rows, keys), 1)
    allowed = spot < live_ref[0]
    for head in range(heads):
        part = slice(head * HD, (head + 1) * HD)
        column = pl.ds(pl.multiple_of(lax.axis_index("sp") * width + head * HD, HD), HD)
        query = view(0, head) * inv_q_ref[...] * gain_ref[gain_row : gain_row + 1, column]
        key = view(1, head) * inv_k_ref[...] * gain_ref[gain_row + 1 : gain_row + 2, column]
        if rotary:
            query, key = turned(query, cos_ref, sin_ref, 1.0), turned(key, cos_ref, sin_ref, 1.0)
        query, key, value = query.astype(BF), key.astype(BF), view(2, head).astype(BF)
        query_ref[:, part], key_ref[:, part] = query, key
        scores = jnp.where(allowed, product_nt(query, key) * SCALE, NEGATIVE)
        row_max = jnp.max(scores, axis=1, keepdims=True)
        log_total = row_max + jnp.log(jnp.sum(jnp.exp(scores - row_max), axis=1, keepdims=True))
        weights = jnp.exp(scores - log_total).astype(BF)
        out_ref[:, part] = product(weights, value).astype(BF)
        lse_ref[:, part] = jnp.broadcast_to(log_total, (rows, HD))
    fly.drain()


def attend_backward_kernel(joint, rotary, gain_row, live_ref, *refs):
    view, width, refs = raw_views(joint, refs)
    gain_ref, cos_ref, sin_ref, refs = *refs[:3], refs[3:]
    query_ref, key_ref, lse_ref, inv_q_ref, inv_k_ref, do_ref, refs = *refs[:6], refs[6:]
    if joint:
        grad_refs, refs = ((refs[0], 0), (refs[0], width), (refs[0], 2 * width)), refs[1:]
    else:
        grad_refs, refs = ((refs[0], 0), (refs[1], 0), (refs[1], width)), refs[2:]
    gain_out, scaled_q, scaled_k, q_dot, k_dot, q_peer, k_peer, send, recv = refs
    heads = width // HD
    core_peer = {"sp": 1 - lax.axis_index("sp")}
    fly = Flights()
    greet((core_peer,))
    rows, keys = query_ref.shape[0], key_ref.shape[0]
    spot = lax.broadcasted_iota(jnp.int32, (rows, keys), 1)
    allowed = spot < live_ref[0]
    dots = [None, None]
    gain_out[...] = jnp.zeros_like(gain_out)
    for head in range(heads):
        part = slice(head * HD, (head + 1) * HD)
        query, key, grad = query_ref[:, part], key_ref[:, part], do_ref[:, part]
        value = view(2, head).astype(BF)
        scores = jnp.where(allowed, product_nt(query, key) * SCALE, NEGATIVE)
        weights = jnp.exp(scores - lse_ref[:, head * HD : head * HD + 1])
        grad_weights = product_nt(grad, value)
        delta = jnp.sum(weights * grad_weights, axis=1, keepdims=True)
        grad_scores = (weights * (grad_weights - delta)).astype(BF)
        grad_query = (product(grad_scores, key) * SCALE).astype(BF).astype(F32)
        grad_key = (product_tn(grad_scores, query) * SCALE).astype(BF).astype(F32)
        grad_value = product_tn(weights.astype(BF), grad).astype(BF)
        ref, base = grad_refs[2]
        ref[:, base + head * HD : base + (head + 1) * HD] = grad_value
        for which, grad_rows, inverse, held in ((0, grad_query, inv_q_ref, scaled_q), (1, grad_key, inv_k_ref, scaled_k)):
            if rotary:
                grad_rows = turned(grad_rows, cos_ref, sin_ref, -1.0)
            raw = view(which, head)
            gain_out[which : which + 1, part] = jnp.sum(grad_rows * raw * inverse[...], axis=0, keepdims=True)
            column = pl.ds(pl.multiple_of(lax.axis_index("sp") * width + head * HD, HD), HD)
            scaled = grad_rows * gain_ref[gain_row + which : gain_row + which + 1, column]
            held[:, part] = scaled
            dots[which] = scaled * raw if head == 0 else dots[which] + scaled * raw
    for which, own, peer in ((0, q_dot, q_peer), (1, k_dot, k_peer)):
        own[...] = jnp.broadcast_to(jnp.sum(dots[which], axis=1, keepdims=True), own.shape)
        fly.send(own, peer, send.at[which], recv.at[which], core_peer)
    for which, own, peer, inverse, held in (
        (0, q_dot, q_peer, inv_q_ref, scaled_q),
        (1, k_dot, k_peer, inv_k_ref, scaled_k),
    ):
        landed(peer, recv.at[which], core_peer)
        column = inverse[...]
        slope = column * column * column * ((own[...] + peer[...]) / D)
        ref, base = grad_refs[which]
        for head in range(heads):
            part = slice(head * HD, (head + 1) * HD)
            out = held[:, part] * column - view(which, head) * slope
            ref[:, base + head * HD : base + (head + 1) * HD] = out.astype(BF)
    fly.drain()


def attend_call(kernel, joint, rotary, number, live, raws, others, shapes, scratch, flops, exps):
    dma = pltpu.SemaphoreType.DMA
    arrays = [*raws, *others]
    moved = sum(v.size * v.dtype.itemsize for v in [*arrays, *shapes])
    return pl.pallas_call(
        functools.partial(kernel, joint, rotary, 0 if rotary else 2),
        out_shape=shapes,
        in_specs=[SM] + [VM] * len(arrays),
        out_specs=[VM] * len(shapes),
        scratch_shapes=[*scratch, dma((2,)), dma((2,))],
        compiler_params=pltpu.CompilerParams(collective_id=number, has_side_effects=True),
        cost_estimate=pl.CostEstimate(flops=flops, bytes_accessed=moved, transcendentals=exps),
    )(live, *arrays)


def attend_sizes(raws):
    joint = len(raws) == 1
    rows, keys = raws[0].shape[0], raws[-1].shape[0]
    return joint, rows, keys, raws[0].shape[1] // 3 if joint else raws[0].shape[1]


def attend_forward(live, raws, gains, cosine, sine, rotary, number):
    joint, rows, keys, width = attend_sizes(raws)
    shape = jax.ShapeDtypeStruct
    shapes = [
        shape((rows, width), BF),
        shape((rows, width), F32),
        shape((rows, width), BF),
        shape((keys, width), BF),
        shape((rows, HD), F32),
        shape((keys, HD), F32),
    ]
    scratch = [pltpu.VMEM((n, HD), F32) for n in (rows, keys, rows, keys)]
    work = rows * keys * width
    return attend_call(
        attend_forward_kernel, joint, rotary, number, live, raws, [gains, cosine, sine],
        shapes, scratch, 4 * work, 2 * work // HD,
    )


def attend_backward(live, raws, gains, cosine, sine, rotary, number, saved, grad):
    joint, rows, keys, width = attend_sizes(raws)
    shape = jax.ShapeDtypeStruct
    shapes = [shape(raw.shape, BF) for raw in raws] + [shape((8, width), F32)]
    scratch = [pltpu.VMEM((rows, width), F32), pltpu.VMEM((keys, width), F32)]
    scratch += [pltpu.VMEM((n, HD), F32) for n in (rows, keys, rows, keys)]
    work = rows * keys * width
    return attend_call(
        attend_backward_kernel, joint, rotary, number, live, raws,
        [gains, cosine, sine, *saved, grad], shapes, scratch, 10 * work, work // HD,
    )


ALL_CHIPS, KEEP, HALF_X, HALF_Y = range(4)


def gather_kernel(outer, kinds, *refs):
    full = len(kinds)
    ins, refs = refs[:full], refs[full:]
    mlp_in, text_ref, refs = refs[0], refs[1], refs[2:]
    outs, refs = list(refs[:full]), refs[full:]
    bias_out, gain_out, step_out, up_out, text_out, refs = *refs[:5], refs[5:]
    own, refs = refs[:full], refs[full:]
    halves = [i for i, kind in enumerate(kinds) if kind[1] == KEEP]
    form = [kind[1] for kind in kinds]
    whole, refs = refs[: len(halves)], refs[len(halves) :]
    small_all, mlp_ref, up_own, local_sem, zs, zr, s1, r1, s2, r2, a_s, a_r, f_s, f_r, f_l, t_s, i_s = refs
    outs[0] = small_all
    z, y, x = (lax.axis_index(name) for name in FS)
    core = lax.axis_index("sp")
    here = 2 * y + x
    up = full
    fins = {}
    for j, i in enumerate(halves):
        fins[i] = outs[i]
        outs[i] = whole[j]
    fly = Flights()
    x_peer, y_peer = {"xc": 1 - x}, {"yb": 1 - y}
    diagonal = {"yb": 1 - y, "xc": 1 - x}
    around = ((x_peer, y, 1 - x), (y_peer, 1 - y, x), (diagonal, 1 - y, 1 - x))
    above, below = {"za": z + 1}, {"za": z - 1}
    core_peer = {"sp": 1 - core}
    has_above, has_below = z + 1 < outer, z >= 1
    loads = []
    for i, (parts, _, base, of) in enumerate(kinds):
        width = ins[i].shape[1] // (2 * of)
        for part in range(parts):
            column = pl.multiple_of((2 * (base + part) + core) * width, width)
            span = slice(part * width, (part + 1) * width)
            loads.append((i, fly.local(ins[i].at[:, pl.ds(column, width)], own[i].at[:, span], i_s.at[i, part])))
        if parts == 0:
            loads.append((i, fly.local(ins[i], own[i], i_s.at[i, 0])))
    mlp_load = fly.local(mlp_in, mlp_ref, i_s.at[full, 0])
    greet((x_peer, y_peer, diagonal, core_peer), ((has_above, above), (has_below, below)))

    def spot(i, slot, ty, tx):
        if form[i] == HALF_X:
            return outs[i].at[slot, tx]
        if form[i] == HALF_Y:
            return outs[i].at[slot, ty]
        return outs[i].at[slot, ty, tx]

    def shard(i, slot):
        return spot(i, slot, y, x) if i < full else up_out.at[slot]

    def z_send(i, way, hop, source=None):
        if hop > outer - 2:
            return
        slot = z - hop if way == 0 else z + hop
        when = jnp.logical_and(has_above, slot >= 0) if way == 0 else jnp.logical_and(has_below, slot < outer)
        fly.send(
            shard(i, slot) if source is None else source,
            shard(i, slot),
            zs.at[i, way, hop],
            zr.at[i, way, hop],
            above if way == 0 else below,
            when,
        )

    def z_slot(way, hop):
        slot = z - 1 - hop if way == 0 else z + 1 + hop
        return slot, (slot >= 0 if way == 0 else slot < outer)

    def z_wait(i, way, hop):
        slot, when = z_slot(way, hop)

        @pl.when(when)
        def _():
            landed(shard(i, slot), zr.at[i, way, hop], below if way == 0 else above)

    def turns(i, slot):
        turn = (slot + i) % 2
        first = ((y + turn) % 2, (x + 1 - turn) % 2)
        second = ((y + 1 - turn) % 2, (x + turn) % 2)
        return first, second

    def xy_own(i, slot, when=None, source=None):
        mine = spot(i, slot, y, x)
        source = mine if source is None else source
        if form[i] in (HALF_X, HALF_Y):
            peer = x_peer if form[i] == HALF_X else y_peer
            fly.send(source, mine, s1.at[i, slot], r1.at[i, slot], peer, when)
            return
        first, second = turns(i, slot)
        fly.send(source, mine, s1.at[i, slot], r1.at[i, slot], {"yb": first[0], "xc": first[1]}, when)
        fly.send(source, mine, s2.at[i, slot, 0], r2.at[i, slot, 0], {"yb": second[0], "xc": second[1]}, when)

    def xy_pass(i, slot, when=None):
        if form[i] in (HALF_X, HALF_Y):
            return
        first, second = turns(i, slot)
        theirs = outs[i].at[slot, first[0], first[1]]

        def wait():
            landed(theirs, r1.at[i, slot], {"yb": first[0], "xc": first[1]})

        if when is None:
            wait()
        else:
            pl.when(when)(wait)
        fly.send(theirs, theirs, s2.at[i, slot, 1], r2.at[i, slot, 1], {"yb": second[0], "xc": second[1]}, when)

    def xy_end(i, slot):
        if form[i] == HALF_X:
            landed(spot(i, slot, y, 1 - x), r1.at[i, slot], x_peer)
            return
        if form[i] == HALF_Y:
            landed(spot(i, slot, 1 - y, x), r1.at[i, slot], y_peer)
            return
        _, second = turns(i, slot)
        device = {"yb": second[0], "xc": second[1]}
        landed(outs[i].at[slot, second[0], second[1]], r2.at[i, slot, 0], device)
        landed(outs[i].at[slot, 1 - y, 1 - x], r2.at[i, slot, 1], device)

    for i in range(full):
        for index, load in loads:
            if index == i:
                load.wait()
        for way in range(2):
            z_send(i, way, 0, own[i])
        xy_own(i, z, None, own[i])
    locals_ = [fly.local(own[i], spot(i, z, y, x), local_sem.at[i]) for i in range(full)]

    fly.send(text_ref, text_out.at[core], t_s.at[0], t_s.at[1], core_peer)
    locals_.append(fly.local(text_ref, text_out.at[core], t_s.at[2]))
    mlp_load.wait()
    hid = mlp_ref.shape[1] // (outer * PLANE * 2)
    for own_core in range(2):

        @pl.when(core == own_core)
        def _(own_core=own_core):
            for place in range(PLANE):
                for slot in range(outer):
                    column = ((slot * PLANE + place) * 2 + own_core) * hid
                    up_own[place, :, slot * hid : (slot + 1) * hid] = mlp_ref[:, column : column + hid]

    for hop in range(outer - 1):
        for i in range(full):
            for way in range(2):
                slot, when = z_slot(way, hop)
                z_wait(i, way, hop)
                z_send(i, way, hop + 1)
                xy_own(i, slot, when)
        if hop == 0:
            locals_.append(fly.local(up_own.at[here], up_out.at[z, here], local_sem.at[up]))
            for turn, (device, ty, tx) in enumerate(around):
                fly.send(up_own.at[2 * ty + tx], up_out.at[z, here], a_s.at[turn], a_r.at[turn], device)
    for copy in locals_:
        copy.wait()
    for turn, (device, ty, tx) in enumerate(around):
        landed(up_out.at[z, 2 * ty + tx], a_r.at[turn], device)
    for way in range(2):
        z_send(up, way, 0)
    for i in range(full):
        xy_pass(i, z)
    for hop in range(outer - 1):
        for i in range(full):
            for way in range(2):
                slot, when = z_slot(way, hop)
                xy_pass(i, slot, when)
        for way in range(2):
            z_wait(up, way, hop)
            z_send(up, way, hop + 1)
    for i in (*halves, *(i for i in range(full) if i not in halves)):
        for slot in range(outer):
            xy_end(i, slot)
        if i == 0:
            bias_len = bias_out.shape[1] // (outer * PLANE)
            gain_len = gain_out.shape[1] // (outer * PLANE)
            for chip in range(outer * PLANE):
                rows = small_all.at[chip // PLANE, (chip // 2) % 2, chip % 2]
                bias_out[:, chip * bias_len : (chip + 1) * bias_len] = rows[0:1, :bias_len]
                gain_out[:, chip * gain_len : (chip + 1) * gain_len] = rows[1:5, :gain_len]
                step_out[chip : chip + 1, :] = rows[5:6, : step_out.shape[1]]
        if i not in halves:
            continue
        j, part = halves.index(i), outer // 2
        width = own[i].shape[-1]
        columns = pl.ds(pl.multiple_of(core * width, width), width)
        theirs, ours = pl.ds((1 - core) * part, part), pl.ds(core * part, part)
        fly.send(outs[i].at[theirs], fins[i].at[:, :, :, :, columns], f_s.at[j], f_r.at[j], core_peer)
        fly.local(outs[i].at[ours], fins[i].at[:, :, :, :, columns], f_l.at[j])
    for j, i in enumerate(halves):
        width = own[i].shape[-1]
        columns = pl.ds(pl.multiple_of(core * width, width), width)
        others = pl.ds(pl.multiple_of((1 - core) * width, width), width)
        ours = pl.ds(core * (outer // 2), outer // 2)
        pltpu.make_async_copy(outs[i].at[ours], fins[i].at[:, :, :, :, columns], f_l.at[j]).wait()
        landed(fins[i].at[:, :, :, :, others], f_r.at[j], core_peer)
    landed(text_out.at[1 - core], t_s.at[1], core_peer)
    fly.drain()


def gather_weights(outer, kinds, arrays, mlp, text, small_lens):
    shapes, own, whole = [], [], []
    for (parts, form, _, of), array in zip(kinds, arrays, strict=True):
        rows, width = array.shape
        half = width * parts // (2 * of) if parts else width
        own.append(pltpu.VMEM((rows, half), array.dtype))
        if form in (HALF_X, HALF_Y):
            shapes.append(jax.ShapeDtypeStruct((outer, 2, rows, half), array.dtype))
        elif form == KEEP:
            whole.append(pltpu.VMEM((outer, 2, 2, rows, half), array.dtype))
            shapes.append(jax.ShapeDtypeStruct((outer // 2, 2, 2, rows, 2 * half), array.dtype))
        else:
            shapes.append(jax.ShapeDtypeStruct((outer, 2, 2, rows, half), array.dtype))
    bias_len, gain_len, _ = small_lens
    chips = outer * PLANE
    shapes[0] = jax.ShapeDtypeStruct((8, 128), F32)
    shapes.append(jax.ShapeDtypeStruct((1, chips * bias_len), F32))
    shapes.append(jax.ShapeDtypeStruct((4, chips * gain_len), F32))
    shapes.append(jax.ShapeDtypeStruct((chips, 128), F32))
    rows, units = mlp.shape
    mine = units // (2 * PLANE)
    shapes.append(jax.ShapeDtypeStruct((outer, PLANE, rows, mine), mlp.dtype))
    shapes.append(jax.ShapeDtypeStruct((2, *text.shape), text.dtype))
    dma = pltpu.SemaphoreType.DMA
    hops = outer - 1
    nf, nh = len(kinds), len(whole)
    results = pl.pallas_call(
        functools.partial(gather_kernel, outer, kinds),
        out_shape=shapes,
        in_specs=[ANY] * (nf + 2),
        out_specs=[*[ANY] * nf, VM, VM, VM, ANY, ANY],
        scratch_shapes=[
            *own,
            *whole,
            pltpu.VMEM((outer, 2, 2, *arrays[0].shape), F32),
            pltpu.VMEM(mlp.shape, mlp.dtype),
            pltpu.VMEM((PLANE, rows, mine), mlp.dtype),
            dma((nf + 1,)),
            dma((nf + 1, 2, hops)),
            dma((nf + 1, 2, hops)),
            dma((nf, outer)),
            dma((nf, outer)),
            dma((nf, outer, 2)),
            dma((nf, outer, 2)),
            dma((3,)),
            dma((3,)),
            dma((nh,)),
            dma((nh,)),
            dma((nh,)),
            dma((3,)),
            dma((nf + 1, 3)),
        ],
        compiler_params=pltpu.CompilerParams(
            collective_id=0, has_side_effects=True, vmem_limit_bytes=40 * 1024 * 1024
        ),
        cost_estimate=pl.CostEstimate(flops=10**11, bytes_accessed=10**8, transcendentals=0),
        name="gather_weights",
    )(*arrays, mlp, text)
    flat = [value.reshape(-1, value.shape[-1]) if value.ndim == 5 else value for value in results[1:nf]]
    bias, gains, steps, up, texts = results[nf:]
    return flat, bias, gains, steps, up.reshape(-1, up.shape[-1]), texts.reshape(-1, texts.shape[-1])


def plane_gather_kernel(own_ref, out_ref, local_sem, send, recv):
    y, x, core = lax.axis_index("yb"), lax.axis_index("xc"), lax.axis_index("sp")
    x_peer, y_peer, core_peer = {"xc": 1 - x}, {"yb": 1 - y}, {"sp": 1 - core}
    fly = Flights()
    greet((x_peer, y_peer, core_peer))
    size = own_ref.shape[0] // 2
    top, low = pl.ds(0, size), pl.ds(size, size)
    fly.send(own_ref.at[top], out_ref.at[0, 1, 0, top], send.at[0], recv.at[0], x_peer)
    fly.send(own_ref.at[low], out_ref.at[1, 0, 0, low], send.at[1], recv.at[1], y_peer)
    fly.send(own_ref.at[low], out_ref.at[0, 1, 0, low], send.at[2], recv.at[2], x_peer)
    fly.send(own_ref.at[top], out_ref.at[1, 0, 0, top], send.at[3], recv.at[3], y_peer)
    fly.send(own_ref, out_ref.at[0, 0, 1], send.at[4], recv.at[4], core_peer)
    local = fly.local(own_ref, out_ref.at[0, 0, 0], local_sem.at[0])
    across = []

    def arrive(index, dy, dx, rows, device, onward=None):
        block = out_ref.at[dy, dx, 0, rows]
        landed(block, recv.at[index], device)
        if onward is not None:
            to, number = onward
            fly.send(block, out_ref.at[1, 1, 0, rows], send.at[number], recv.at[number], to)
        fly.send(block, out_ref.at[dy, dx, 1, rows], send.at[index + 7], recv.at[index + 7], core_peer)
        across.append((index + 7, dy, dx, rows))

    arrive(0, 0, 1, top, x_peer, (y_peer, 5))
    arrive(1, 1, 0, low, y_peer, (x_peer, 6))
    arrive(2, 0, 1, low, x_peer)
    arrive(3, 1, 0, top, y_peer)
    arrive(5, 1, 1, top, y_peer)
    arrive(6, 1, 1, low, x_peer)
    landed(out_ref.at[0, 0, 1], recv.at[4], core_peer)
    for index, dy, dx, rows in across:
        landed(out_ref.at[dy, dx, 1, rows], recv.at[index], core_peer)
    local.wait()
    fly.drain()


def plane_gather(own):
    rows, width = own.shape
    dma = pltpu.SemaphoreType.DMA
    out = pl.pallas_call(
        plane_gather_kernel,
        out_shape=jax.ShapeDtypeStruct((2, 2, 2, rows, width), own.dtype),
        in_specs=[VM],
        out_specs=VM,
        scratch_shapes=[dma((1,)), dma((14,)), dma((14,))],
        compiler_params=pltpu.CompilerParams(collective_id=1, has_side_effects=True),
        cost_estimate=pl.CostEstimate(flops=10**10, bytes_accessed=10**7, transcendentals=0),
        name="plane_gather",
    )(own)
    return out.reshape(8 * rows, width)


def plane_sum_kernel(part_a, part_b, out_a, out_b, core_in, first, second, keep, send, recv):
    y, x, core = lax.axis_index("yb"), lax.axis_index("xc"), lax.axis_index("sp")
    x_peer, y_peer, core_peer = {"xc": 1 - x}, {"yb": 1 - y}, {"sp": 1 - core}
    fly = Flights()
    greet((x_peer, y_peer, core_peer))
    rows = part_a.shape[3]
    chips = (((1, 1), (1, 0), (0, 1), (0, 0)), ((1, 1), (0, 1), (1, 0), (0, 0)))
    parts, outs, peers = (part_a, part_b), (out_a, out_b), ((y_peer, x_peer), (x_peer, y_peer))
    for index in range(4):
        for n in range(2):
            dy, dx = chips[n][index]
            fly.send(
                parts[n].at[dy, dx, 1], core_in.at[n, index], send.at[n, index], recv.at[n, index], core_peer
            )

    def core_sum(n, index):
        dy, dx = chips[n][index]
        landed(core_in.at[n, index], recv.at[n, index], core_peer)
        row_add(core_in.at[n, index], core_in.at[n, index], parts[n].at[dy, dx, 0], rows)

    for index in range(2):
        for n in range(2):
            core_sum(n, index)
            fly.send(
                core_in.at[n, index], first.at[n, index], send.at[n, index + 4], recv.at[n, index + 4], peers[n][0]
            )
    for index in (2, 3):
        for n in range(2):
            core_sum(n, index)
    for n in range(2):
        landed(first.at[n, 0], recv.at[n, 4], peers[n][0])
        row_add(second.at[n, 0], first.at[n, 0], core_in.at[n, 2], rows)
        fly.send(second.at[n, 0], second.at[n, 1], send.at[n, 6], recv.at[n, 6], peers[n][1])
    for n in range(2):
        landed(first.at[n, 1], recv.at[n, 5], peers[n][0])
        row_sum(keep.at[n], first.at[n, 1], core_in.at[n, 3], rows)
    for n in range(2):
        landed(second.at[n, 1], recv.at[n, 6], peers[n][1])
        row_sum(outs[n], keep.at[n], second.at[n, 1], rows)
    fly.drain()


def plane_sum(one, other):
    rows, width = one.shape[0] // 8, one.shape[1]
    dma = pltpu.SemaphoreType.DMA
    shape = jax.ShapeDtypeStruct((rows, width), F32)
    return pl.pallas_call(
        plane_sum_kernel,
        out_shape=(shape, shape),
        in_specs=[VM, VM],
        out_specs=(VM, VM),
        scratch_shapes=[
            pltpu.VMEM((2, 4, rows, width), BF),
            pltpu.VMEM((2, 2, rows, width), BF),
            pltpu.VMEM((2, 2, rows, width), BF),
            pltpu.VMEM((2, rows, width), F32),
            dma((2, 7)),
            dma((2, 7)),
        ],
        compiler_params=pltpu.CompilerParams(collective_id=2, has_side_effects=True),
        cost_estimate=pl.CostEstimate(flops=10**10, bytes_accessed=10**7, transcendentals=0),
        name="plane_sum",
    )(one.reshape(2, 2, 2, rows, width), other.reshape(2, 2, 2, rows, width))


def pair_sum_kernel(part_ref, out_ref, peer_in, send, recv):
    core = lax.axis_index("sp")
    core_peer = {"sp": 1 - core}
    fly = Flights()
    greet((core_peer,))
    size = part_ref.shape[1] // 2
    for index in range(2):
        rows = pl.ds(index * size, size)
        fly.send(part_ref.at[1 - core, rows], peer_in.at[rows], send.at[index], recv.at[index], core_peer)
    for index in range(2):
        rows = pl.ds(index * size, size)
        landed(peer_in.at[rows], recv.at[index], core_peer)
        row_sum(out_ref.at[rows], part_ref.at[core, rows], peer_in.at[rows], size)
    fly.drain()


def pair_sum(partial):
    rows, width = partial.shape[0] // 2, partial.shape[1]
    dma = pltpu.SemaphoreType.DMA
    return pl.pallas_call(
        pair_sum_kernel,
        out_shape=jax.ShapeDtypeStruct((rows, width), F32),
        in_specs=[VM],
        out_specs=VM,
        scratch_shapes=[pltpu.VMEM((rows, width), F32), dma((2,)), dma((2,))],
        compiler_params=pltpu.CompilerParams(collective_id=4, has_side_effects=True),
        cost_estimate=pl.CostEstimate(flops=10**9, bytes_accessed=10**7, transcendentals=0),
        name="pair_sum",
    )(partial.reshape(2, rows, width))


AHEAD, LAG_PLANE, LAG_CHAIN = 6, 2, 4
PLAIN, SPLIT, OVER_X, OVER_Y = range(4)


def reduce_kernel(outer, kinds, *refs):
    count = len(kinds)
    shards = outer * PLANE
    gs, refs = refs[:count], refs[count:]
    frames_ref, small_ref, up_ref, down_ref, refs = *refs[:4], refs[4:]
    outs, refs = refs[:count], refs[count:]
    frames_out, small_out, up_out, down_out, refs = *refs[:4], refs[4:]
    pieces = [(i, part) for i, (parts, _) in enumerate(kinds) for part in range(parts)]
    total = len(pieces)
    forms = [kinds[i][1] for i, _ in pieces]
    near_refs, near = list(refs), {}
    for p in range(total):
        if forms[p] in (PLAIN, SPLIT):
            near[p] = near_refs.pop(0)
    refs = near_refs
    plane, refs = refs[:total], refs[total:]
    chain, refs = refs[:total], refs[total:]
    split = [i for i, kind in enumerate(kinds) if kind[1] == SPLIT]
    whole, refs = refs[: len(split)], refs[len(split) :]
    small_in, small_own, small_peer, up_in, down_in, refs = *refs[:5], refs[5:]
    e_s, e_r, e_l, s1, r1, s2, r2, zs, zr, o_s, o_r, f_s, f_r, m_s, m_r, l_s, p_s, p_r = refs
    z, y, x = (lax.axis_index(name) for name in FS)
    core = lax.axis_index("sp")
    here = (z * 2 + y) * 2 + x
    core_peer = {"sp": 1 - core}
    above, below = {"za": z + 1}, {"za": z - 1}
    fly = Flights()

    def chip(index):
        return {"za": index // 4, "yb": (index // 2) % 2, "xc": index % 2}

    others = [(here + j) % shards for j in range(1, shards)]
    greet((core_peer, *[chip(index) for index in others]))

    part_slots = outer // 2
    ours, other_slots = pl.ds(core * part_slots, part_slots), pl.ds((1 - core) * part_slots, part_slots)
    for j, i in enumerate(split):
        width = whole[j].shape[-1]
        mine = pl.ds(pl.multiple_of(core * width, width), width)
        theirs = pl.ds(pl.multiple_of((1 - core) * width, width), width)
        fly.send(gs[i].at[:, :, :, :, theirs], whole[j].at[ours], e_s.at[j], e_r.at[j], core_peer)
        fly.local(gs[i].at[:, :, :, :, mine], whole[j].at[ours], e_l.at[j])

    def joined(i):
        j = split.index(i)
        width = whole[j].shape[-1]
        mine = pl.ds(pl.multiple_of(core * width, width), width)
        pltpu.make_async_copy(gs[i].at[:, :, :, :, mine], whole[j].at[ours], e_l.at[j]).wait()
        landed(whole[j].at[other_slots], e_r.at[j], core_peer)

    def width_of(p):
        return plane[p].shape[-1]

    def source(p, *place):
        i, part = pieces[p]
        held = whole[split.index(i)] if forms[p] == SPLIT else gs[i]
        width = width_of(p)
        return held.at[(*place, slice(None), pl.ds(part * width, width))]

    frame_copy = fly.local(frames_ref, frames_out.at[here, core], l_s.at[0])
    small_copy = fly.local(small_ref.at[here], small_in.at[here], l_s.at[1])
    for j, index in enumerate(others):
        fly.send(frames_ref, frames_out.at[here, core], f_s.at[j], f_r.at[here], chip(index))
        fly.send(small_ref.at[index], small_in.at[here], m_s.at[j], m_r.at[here], chip(index))

    near_by = ((y, 1 - x), (1 - y, x), (1 - y, 1 - x))
    up_copy = fly.local(up_ref.at[2 * y + x], up_in.at[core, 2 * y + x], p_s.at[0])
    for j, (ty, tx) in enumerate(near_by):
        fly.send(
            up_ref.at[2 * ty + tx],
            up_in.at[core, 2 * y + x],
            p_s.at[j + 1],
            p_r.at[j + 1],
            {"yb": ty, "xc": tx},
        )
    fly.send(down_ref, down_in, p_s.at[4], p_r.at[4], core_peer)

    def feed_forward_landed():
        up_copy.wait()
        for j, (ty, tx) in enumerate(near_by):
            landed(up_in.at[core, 2 * ty + tx], p_r.at[j + 1], {"yb": ty, "xc": tx})
        fly.send(up_in.at[core], up_in.at[core], p_s.at[5], p_r.at[5], core_peer)
        hid = down_ref.shape[0]
        landed(down_in, p_r.at[4], core_peer)
        for side in range(2):

            @pl.when(core == side)
            def _(side=side):
                down_out[side * hid : (side + 1) * hid, :] = down_ref[...]
                down_out[(1 - side) * hid : (2 - side) * hid, :] = down_in[...]

    def feed_forward_rows():
        hid = down_ref.shape[0]
        landed(up_in.at[1 - core], p_r.at[5], core_peer)
        for slot in range(outer):
            for place in range(PLANE):
                for side in range(2):
                    column = ((slot * PLANE + place) * 2 + side) * hid
                    up_out[:, column : column + hid] = up_in[side, place, :, slot * hid : (slot + 1) * hid]

    def slot_at(step):
        if step == outer - 1:
            return z
        falling = outer - 1 - step
        falling = jnp.where(falling > z, falling, falling - 1)
        rising = jnp.where(step < z, step, step + 1)
        return jnp.where(z < part_slots, falling, rising)

    units = [(slot_at(step), p) for step in range(outer) for p in range(total)]

    def turns(p, slot):
        turn = (slot + p) % 2
        first = ((y + 1 - turn) % 2, (x + turn) % 2)
        second = ((y + turn) % 2, (x + 1 - turn) % 2)
        return first, second

    def device(place):
        return {"yb": place[0], "xc": place[1]}

    def start(slot, p):
        first, _ = turns(p, slot)
        fly.send(
            source(p, slot, 1 - y, 1 - x), near[p].at[slot, 1], s1.at[p, slot, 1], r1.at[p, slot, 1], device(first)
        )
        fly.send(
            source(p, slot, first[0], first[1]), near[p].at[slot, 0], s1.at[p, slot, 0], r1.at[p, slot, 0], device(first)
        )

    def summed_over(p):
        return (x, {"xc": 1 - x}) if forms[p] == OVER_X else (y, {"yb": 1 - y})

    def pass_on(slot, p):
        rows = plane[p].shape[1]
        if p not in near:
            index, peer = summed_over(p)
            fly.send(source(p, slot, 1 - index), plane[p].at[slot], s2.at[p, slot], r2.at[p, slot], peer)
            return
        first, second = turns(p, slot)
        landed(near[p].at[slot, 1], r1.at[p, slot, 1], device(first))
        row_add(near[p].at[slot, 1], near[p].at[slot, 1], source(p, slot, second[0], second[1]), rows)
        fly.send(near[p].at[slot, 1], plane[p].at[slot], s2.at[p, slot], r2.at[p, slot], device(second))
        landed(near[p].at[slot, 0], r1.at[p, slot, 0], device(first))
        row_add(near[p].at[slot, 0], near[p].at[slot, 0], source(p, slot, y, x), rows)

    def plane_total(slot, p):
        rows = plane[p].shape[1]
        if p not in near:
            index, peer = summed_over(p)
            landed(plane[p].at[slot], r2.at[p, slot], peer)
            row_add(plane[p].at[slot], plane[p].at[slot], source(p, slot, index), rows)
            return
        _, second = turns(p, slot)
        landed(plane[p].at[slot], r2.at[p, slot], device(second))
        row_add(plane[p].at[slot], plane[p].at[slot], near[p].at[slot, 0], rows)

    def along(slot, p, last):
        rows, width = plane[p].shape[1:]
        if not last:
            for way, when, edge, ahead, behind in (
                (1, slot < z, z == outer - 1, below, above),
                (0, slot > z, z == 0, above, below),
            ):
                link = chain[p].at[slot + 1 - way]

                @pl.when(jnp.logical_and(when, jnp.logical_not(edge)))
                def _(way=way, link=link, behind=behind):
                    landed(link, zr.at[p, way, slot], behind)
                    row_add(plane[p].at[slot], plane[p].at[slot], link, rows)

                fly.send(plane[p].at[slot], link, zs.at[p, way, slot], zr.at[p, way, slot], ahead, when)
            return
        has_above, has_below = z < outer - 1, z > 0
        for way, when, behind in ((1, has_above, above), (0, has_below, below)):

            @pl.when(when)
            def _(way=way, behind=behind):
                landed(chain[p].at[slot + 1 - way], zr.at[p, way, slot], behind)

        step = 16 if rows % 16 == 0 else rows
        i, part = pieces[p]
        column = pl.multiple_of((2 * part + core) * width, width)

        def chunk(index, carry):
            at = pl.ds(pl.multiple_of(index * step, step), step)
            upper = jnp.where(has_above, chain[p][slot, at, :].astype(F32), 0.0)
            lower = jnp.where(has_below, chain[p][slot + 1, at, :].astype(F32), 0.0)
            outs[i][at, pl.ds(column, width)] = (plane[p][slot, at, :].astype(F32) + upper + lower).astype(BF)
            return carry

        lax.fori_loop(0, rows // step, chunk, 0)
        block = outs[i].at[:, pl.ds(column, width)]
        fly.send(block, block, o_s.at[p], o_r.at[p], core_peer)

    waiting = set(split)

    def begin(unit):
        slot, p = units[unit]
        if p not in near:
            return
        if pieces[p][0] in waiting:
            joined(pieces[p][0])
            waiting.discard(pieces[p][0])
        start(slot, p)

    for unit in range(min(AHEAD, len(units))):
        begin(unit)
    for tick in range(len(units) + LAG_CHAIN):
        if tick < len(units):
            pass_on(*units[tick])
            if tick + AHEAD < len(units):
                begin(tick + AHEAD)
        if 0 <= tick - LAG_PLANE < len(units):
            plane_total(*units[tick - LAG_PLANE])
        if tick == 4:
            feed_forward_landed()
        if tick == 10:
            feed_forward_rows()
        if 0 <= tick - LAG_CHAIN < len(units):
            unit = tick - LAG_CHAIN
            along(*units[unit], unit >= (outer - 1) * total)
        if tick == total:
            frame_copy.wait()
            for index in others:
                landed(frames_out.at[index, core], f_r.at[index], chip(index))
            fly.send(frames_out.at[:, core], frames_out.at[:, core], p_s.at[6], p_r.at[6], core_peer)
            small_copy.wait()
            for index in others:
                landed(small_in.at[index], m_r.at[index], chip(index))
            small_own[...] = jnp.sum(small_in[...], axis=0)
            fly.send(small_own, small_peer, l_s.at[2], l_s.at[3], core_peer)

    landed(frames_out.at[:, 1 - core], p_r.at[6], core_peer)
    landed(small_peer, l_s.at[3], core_peer)
    small_out[...] = small_own[...] + small_peer[...]
    for p, (i, part) in enumerate(pieces):
        width = width_of(p)
        column = pl.multiple_of((2 * part + 1 - core) * width, width)
        landed(outs[i].at[:, pl.ds(column, width)], o_r.at[p], core_peer)
    fly.drain()


def reduce_weights(outer, kinds, grads, frames, small, up, down):
    shards = outer * PLANE
    shaped, shapes, near, plane, chain, whole = [], [], [], [], [], []
    for (parts, form), grad in zip(kinds, grads, strict=True):
        full_width = grad.shape[-1] // 2 if form == SPLIT else grad.shape[-1]
        if form in (PLAIN, SPLIT):
            lead = outer // 2 if form == SPLIT else outer
            grad = grad.reshape(lead, 2, 2, -1, grad.shape[-1])
        rows, width = grad.shape[-2], full_width // parts
        shaped.append(grad)
        shapes.append(jax.ShapeDtypeStruct((rows, 2 * full_width), BF))
        for _ in range(parts):
            if form in (PLAIN, SPLIT):
                near.append(pltpu.VMEM((outer, 2, rows, width), BF))
            plane.append(pltpu.VMEM((outer, rows, width), BF))
            chain.append(pltpu.VMEM((outer + 1, rows, width), BF))
        if form == SPLIT:
            whole.append(pltpu.VMEM((outer, 2, 2, rows, full_width), BF))
    shapes.append(jax.ShapeDtypeStruct((shards, 2, *frames.shape), frames.dtype))
    shapes.append(jax.ShapeDtypeStruct(small.shape[1:], F32))
    shapes.append(jax.ShapeDtypeStruct((up.shape[1], 2 * PLANE * up.shape[2]), BF))
    shapes.append(jax.ShapeDtypeStruct((2 * down.shape[0], down.shape[1]), BF))
    dma = pltpu.SemaphoreType.DMA
    count, total, nsplit = len(kinds), len(plane), len(whole)
    results = pl.pallas_call(
        functools.partial(reduce_kernel, outer, kinds),
        out_shape=shapes,
        in_specs=[VM] * (count + 4),
        out_specs=[VM] * (count + 4),
        scratch_shapes=[
            *near,
            *plane,
            *chain,
            *whole,
            pltpu.VMEM(small.shape, F32),
            pltpu.VMEM(small.shape[1:], F32),
            pltpu.VMEM(small.shape[1:], F32),
            pltpu.VMEM((2, *up.shape), up.dtype),
            pltpu.VMEM(down.shape, down.dtype),
            dma((nsplit,)),
            dma((nsplit,)),
            dma((nsplit,)),
            dma((total, outer, 2)),
            dma((total, outer, 2)),
            dma((total, outer)),
            dma((total, outer)),
            dma((total, 2, outer)),
            dma((total, 2, outer)),
            dma((total,)),
            dma((total,)),
            dma((shards,)),
            dma((shards,)),
            dma((shards,)),
            dma((shards,)),
            dma((4,)),
            dma((7,)),
            dma((7,)),
        ],
        cost_estimate=pl.CostEstimate(flops=10**11, bytes_accessed=10**8, transcendentals=0),
        compiler_params=pltpu.CompilerParams(
            collective_id=3, has_side_effects=True, vmem_limit_bytes=67043328
        ),
        name="reduce_weights",
    )(*shaped, frames, small, up, down)
    return results[:count], *results[count:]


def modulation_kernel(sinus_ref, matrix_ref, bias_ref, out_ref, half, send, recv):
    core = lax.axis_index("sp")
    core_peer = {"sp": 1 - core}
    fly = Flights()
    greet((core_peer,))
    frames, width = out_ref.shape[0], matrix_ref.shape[1]
    mine = pl.ds(pl.multiple_of(core * width, width), width)
    half[...] = product(sinus_ref[...], matrix_ref[...]) + bias_ref[:, mine]
    for side in range(2):

        @pl.when(core == side)
        def _(side=side):
            out_ref[:, side * width : (side + 1) * width] = half[side * frames : (side + 1) * frames, :]
            half[:frames, :] = half[(1 - side) * frames : (2 - side) * frames, :]

    columns = pl.ds(pl.multiple_of(core * width, width), width)
    others = pl.ds(pl.multiple_of((1 - core) * width, width), width)
    fly.send(half.at[pl.ds(0, frames)], out_ref.at[:, columns], send.at[0], recv.at[0], core_peer)
    landed(out_ref.at[:, others], recv.at[0], core_peer)
    fly.drain()


def modulate(sinus, matrix, bias):
    dma = pltpu.SemaphoreType.DMA
    frames, width = sinus.shape[0], matrix.shape[1]
    return pl.pallas_call(
        modulation_kernel,
        out_shape=jax.ShapeDtypeStruct((frames // 2, 2 * width), F32),
        in_specs=[VM, VM, VM],
        out_specs=VM,
        scratch_shapes=[pltpu.VMEM((frames, width), F32), dma((1,)), dma((1,))],
        compiler_params=pltpu.CompilerParams(collective_id=9, has_side_effects=True),
        cost_estimate=pl.CostEstimate(flops=10**9, bytes_accessed=10**7, transcendentals=0),
        name="modulation",
    )(sinus, matrix, bias)


def gather(value, axes, axis=0):
    return lax.all_gather(value, axes, axis=axis, tiled=True)


def scatter(value, axes, axis=0):
    return lax.psum_scatter(value, axes, scatter_dimension=axis, tiled=True)


def body(
    tokens,
    text,
    clip_frames,
    timestep,
    mod_weight,
    mod_bias,
    qk_gains,
    self_in,
    self_out,
    cross_q,
    cross_kv,
    cross_out,
    mlp_in,
    mlp_out,
    cotangent,
):
    row_count = tokens.shape[0]
    frame_count = row_count // FRAME_TOK
    group_frames = timestep.shape[1]
    shards = D // self_in.shape[1]
    outer = shards // PLANE
    core = lax.axis_index("sp")
    chip = lax.axis_index(FS)
    in_rows = self_in.shape[1]
    own_frame = core * frame_count

    bias_len, gain_len = mod_bias.shape[1], qk_gains.shape[2]
    small_len = bias_len + 4 * gain_len
    small_rows = 8
    small_width = -(-(small_len + group_frames) // (small_rows * 128)) * 128
    small_room = small_rows * small_width

    small_own = jnp.zeros((8, -(-max(bias_len, 128) // 128) * 128), F32)
    small_own = small_own.at[0, :bias_len].set(mod_bias[0].astype(F32))
    small_own = small_own.at[1:5, :gain_len].set(qk_gains[0].astype(F32))
    small_own = small_own.at[5, :group_frames].set(timestep[0].astype(F32))
    weights, bias_all, gain_all, steps_all, up_matrix, text_all = gather_weights(
        outer,
        (
            (0, ALL_CHIPS, 0, 1),
            (1, ALL_CHIPS, 0, 1),
            (3, ALL_CHIPS, 0, 3),
            (1, KEEP, 0, 1),
            (1, HALF_Y, 0, 1),
            (1, HALF_X, 0, 2),
            (1, HALF_Y, 1, 2),
            (1, KEEP, 0, 1),
        ),
        [
            small_own,
            *(w[0] for w in (mod_weight, self_in, self_out, cross_q, cross_kv, cross_kv, cross_out)),
        ],
        mlp_in[0],
        text,
        (bias_len, gain_len, group_frames),
    )
    mod_matrix, self_proj, self_back, q_half, k_half, v_half, cross_back = weights
    hid = mlp_out.shape[1] // 2
    down_part = lax.dynamic_slice_in_dim(mlp_out[0], core * hid, hid, 0)
    down_part, bias_all = lax.optimization_barrier((down_part, bias_all))
    down_matrix = gather(down_part, "za")
    steps_all = steps_all[:, :group_frames].reshape(-1)

    live_keys = clip_frames * FRAME_TOK
    all_keys = jnp.full((1,), TXT, jnp.int32)
    own_steps = lax.dynamic_slice_in_dim(timestep[0], own_frame, frame_count)
    cosine, sine = (jnp.asarray(table) for table in rotary_tables(group_frames))
    sinus = sinus_features(timestep[0]).astype(BF)

    modulation = modulate(sinus, mod_matrix, bias_all)
    shift_one, scale_one, gate_one, shift_two, scale_two, gate_two = jnp.split(
        modulation, 6, axis=1
    )

    grad_branch = frame_scaled(cotangent.astype(F32), gate_two).astype(BF)
    exchange = [(0, 1), (1, 0)]
    place_y, place_x = lax.axis_index("yb"), lax.axis_index("xc")
    k_other = lax.ppermute(k_half, "yb", exchange)
    v_other = lax.ppermute(v_half, "xc", exchange)
    q_other = lax.ppermute(q_half, "xc", exchange)
    residual = tokens.astype(F32)
    attn_float, back_attn_input = jax.vjp(modulated, residual, shift_one, scale_one)
    attn_input = gather(attn_float.astype(BF), "sp")
    joined = product(attn_input, self_proj)
    self_mixed, self_lse, *self_kept = attend_forward(
        live_keys, [joined], gain_all, cosine, sine, True, 5
    )
    grad_branch, self_mixed = lax.optimization_barrier((grad_branch, self_mixed))
    beside = [
        grad_branch,
        lax.ppermute(grad_branch, "xc", exchange),
        lax.ppermute(grad_branch, "yb", exchange),
        lax.ppermute(grad_branch, PL, [(0, 3), (1, 2), (2, 1), (3, 0)]),
    ]
    self_branch = pair_sum(product(self_mixed, self_back))
    residual = residual + frame_scaled(self_branch, gate_one)

    def beside_own(own, other, place, axis):
        pair = jnp.where(place == 0, jnp.stack([own, other], axis), jnp.stack([other, own], axis))
        return pair.reshape(-1, own.shape[-1])

    cross_kvproj = jnp.concatenate(
        [beside_own(k_half, k_other, place_y, 1), beside_own(v_half, v_other, place_x, 2)], axis=1
    )
    cross_qproj = beside_own(q_half, q_other, place_x, 2)
    text_raw = product(text_all, cross_kvproj)
    cross_float, back_cross_norm = jax.vjp(layer_norm, residual)
    cross_input = gather(cross_float.astype(BF), "sp")
    cross_raw = product(cross_input, cross_qproj)
    cross_mixed, cross_lse, *cross_kept = attend_forward(
        all_keys, [cross_raw, text_raw], gain_all, cosine, sine, False, 6
    )
    cross_branch = pair_sum(product(cross_mixed, cross_back))
    residual = residual + cross_branch
    residual, *beside = lax.optimization_barrier((residual, *beside))
    beside = jnp.stack(beside)
    grad_branch_all = jnp.stack([beside, lax.ppermute(beside, "sp", exchange)], axis=1).reshape(-1, D)


    mlp_float, back_mlp_input = jax.vjp(modulated, residual, shift_two, scale_two)
    mlp_input = plane_gather(mlp_float.astype(BF))
    up_proj = product(mlp_input, up_matrix)
    activated_float, back_gelu = jax.vjp(
        lambda inner: jax.nn.gelu(inner, approximate=True), up_proj
    )
    activated = activated_float.astype(BF)

    mlp_part = product(activated, down_matrix).astype(BF)

    grad_rows = cotangent.astype(F32)
    grad_down = product_tn(activated, grad_branch_all).astype(BF)
    grad_up_low = back_gelu(product_nt(grad_branch_all, down_matrix))[0].astype(BF)
    grad_up = product_tn(mlp_input, grad_up_low).astype(BF)
    grad_mlp_part = product_nt(grad_up_low, up_matrix).astype(BF)
    grad_mlp_part, grad_up, grad_down = lax.optimization_barrier((grad_mlp_part, grad_up, grad_down))
    down_owned = scatter(grad_down, "za")
    up_owned = scatter(grad_up, "za")
    mlp_branch, grad_mlp_input = plane_sum(mlp_part, grad_mlp_part)
    output = (residual + frame_scaled(mlp_branch, gate_two)).astype(BF)
    grad_gate_two = frame_sum(grad_rows * mlp_branch, frame_count)
    grad_from_mlp, grad_shift_two, grad_scale_two = back_mlp_input(grad_mlp_input)
    grad_rows = grad_rows + grad_from_mlp

    grad_low = gather(grad_rows.astype(BF), "sp")
    grad_cross_back = product_tn(cross_mixed, grad_low).astype(BF)
    grad_cross_mixed = product_nt(grad_low, cross_back).astype(BF)
    cross_saved = [*cross_kept[:2], cross_lse, *cross_kept[2:]]
    grad_cross_low, grad_text_low, gains_cross = attend_backward(
        all_keys, [cross_raw, text_raw], gain_all, cosine, sine, False, 7, cross_saved, grad_cross_mixed
    )
    grad_cross_qproj = product_tn(cross_input, grad_cross_low).astype(BF)
    grad_cross_kvproj = product_tn(text_all, grad_text_low).astype(BF)
    kv_parts = grad_cross_kvproj.reshape(outer, 2, 2, in_rows, -1)
    q_parts = grad_cross_qproj.reshape(outer, 2, 2, in_rows, -1)
    kv_sent = lax.ppermute(lax.dynamic_index_in_dim(kv_parts, 1 - place_y, 1, False), "yb", exchange)
    q_sent = lax.ppermute(lax.dynamic_index_in_dim(q_parts, 1 - place_x, 2, False), "xc", exchange)
    grad_cross_input = pair_sum(product_nt(grad_cross_low, cross_qproj))
    grad_rows = grad_rows + back_cross_norm(grad_cross_input)[0]

    grad_gate_one = frame_sum(grad_rows * self_branch, frame_count)
    grad_self_low = gather(frame_scaled(grad_rows, gate_one).astype(BF), "sp")
    grad_self_back = product_tn(self_mixed, grad_self_low).astype(BF)
    grad_self_mixed = product_nt(grad_self_low, self_back).astype(BF)
    self_saved = [*self_kept[:2], self_lse, *self_kept[2:]]
    grad_joined_low, gains_self = attend_backward(
        live_keys, [joined], gain_all, cosine, sine, True, 8, self_saved, grad_self_mixed
    )
    grad_self_proj = product_tn(attn_input, grad_joined_low).astype(BF)
    grad_attn_input = pair_sum(product_nt(grad_joined_low, self_proj))
    grad_from_attn, grad_shift_one, grad_scale_one = back_attn_input(grad_attn_input)
    grad_rows = grad_rows + grad_from_attn

    grad_modulation = jnp.concatenate(
        [grad_shift_one, grad_scale_one, grad_gate_one, grad_shift_two, grad_scale_two, grad_gate_two],
        axis=1,
    )
    grad_gains = jnp.concatenate([gains_self[:2], gains_cross[:2]])
    both = jnp.arange(2)[None, :, None] == core
    grad_gains = jnp.where(both, grad_gains[:, None, :], 0.0).reshape(4, shards, gain_len)
    grad_small = jnp.concatenate(
        [
            jnp.sum(grad_modulation, axis=0).reshape(shards, bias_len),
            grad_gains.transpose(1, 0, 2).reshape(shards, 4 * gain_len),
            jnp.zeros((shards, small_room - small_len), F32),
        ],
        axis=1,
    ).reshape(shards, small_rows, small_width)
    kv_near = lax.dynamic_index_in_dim(kv_parts, place_y, 1, False) + kv_sent
    q_near = lax.dynamic_index_in_dim(q_parts, place_x, 2, False) + q_sent
    owned, grad_mod_all, small_owned, mlp_in_grad, mlp_out_grad = reduce_weights(
        outer,
        ((1, OVER_Y), (2, OVER_X), (1, SPLIT), (1, SPLIT), (3, PLAIN)),
        [q_near, kv_near, grad_cross_back, grad_self_back, grad_self_proj],
        grad_modulation.astype(BF),
        grad_small,
        up_owned.reshape(PLANE, -1, up_owned.shape[1]),
        down_owned,
    )
    owned = [rows.astype(F32) for rows in (*owned, mlp_in_grad, mlp_out_grad)]
    cross_q_grad, cross_kv_grad, cross_out_grad, self_out_grad, self_in_grad, mlp_in_grad, mlp_out_grad = owned
    small_owned = small_owned.reshape(-1)[:small_len]
    sinus_all = sinus_features(steps_all).astype(BF)
    own_features = mod_weight.shape[1]
    sinus_own = lax.dynamic_slice_in_dim(sinus_all, chip * own_features, own_features, 1)
    mod_weight_grad = product_tn(sinus_own, grad_mod_all.reshape(-1, 6 * D))
    return (
        output,
        grad_rows,
        mod_weight_grad[None],
        small_owned[None, :bias_len],
        small_owned[bias_len:].reshape(1, 4, gain_len),
        self_in_grad[None],
        self_out_grad[None],
        cross_q_grad[None],
        cross_kv_grad[None],
        cross_out_grad[None],
        mlp_in_grad[None],
        mlp_out_grad[None],
    )


def solution(mesh):
    chips, cores = mesh.shape["fsdp"], mesh.shape["sp"]
    grid = mesh.devices.reshape(chips // PLANE, 2, PLANE // 2, cores)
    inner = Mesh(grid, ALL)
    rows, second = P(ALL, None), P(None, FS, None)
    in_specs = (
        rows,
        rows,
        P(FS),
        P(FS, None),
        second,
        P(None, FS),
        P(None, None, FS),
        *([second] * 7),
        rows,
    )
    out_specs = (rows, rows, second, P(None, FS), P(None, None, FS), *([second] * 7))

    return jax.shard_map(body, mesh=inner, in_specs=in_specs, out_specs=out_specs, check_vma=False)
```

```python
import functools
import math

import jax
import jax.numpy as jnp
import numpy as np
from jax import lax
from jax.experimental import pallas as pl
from jax.experimental.pallas import tpu as pltpu
from jax.experimental.layout import Layout, with_layout_constraint
from jax.sharding import Mesh
from jax.sharding import PartitionSpec as P


D = 1536
HD = 128
TXT = 512
FREQ = 256
WP = 8
FRAME_TOK = 64
PLANE = 4

EPSILON = 1e-06
NEGATIVE = -1e30

FS = ("za", "yb", "xc")
PL = ("yb", "xc")
ALL = ("za", "yb", "xc", "sp")
SCALE = 1.0 / math.sqrt(HD)
MESH = pl.DeviceIdType.MESH
BF = jnp.bfloat16
F32 = jnp.float32


def product(left, right):
    return jnp.dot(left, right, preferred_element_type=F32)


def product_tn(left, right):
    return lax.dot_general(left, right, (((0,), (0,)), ((), ())), preferred_element_type=F32)


def product_nt(left, right):
    return lax.dot_general(left, right, (((1,), (1,)), ((), ())), preferred_element_type=F32)


def layer_norm(values):
    centred = values - jnp.mean(values, axis=-1, keepdims=True)
    return centred * lax.rsqrt(jnp.mean(centred * centred, axis=-1, keepdims=True) + EPSILON)


def sinus_features(steps):
    half_dim = FREQ // 2
    rates = jnp.exp(jnp.arange(half_dim).astype(F32) * (-math.log(10000.0) / half_dim))
    angles = steps.astype(F32)[:, None] * rates[None, :]
    return jnp.concatenate([jnp.cos(angles), jnp.sin(angles)], axis=1)


def rotary_tables(frames):
    half_dim = HD // 2
    side_pairs = HD // 6
    lead_pairs = half_dim - 2 * side_pairs
    pair = np.arange(half_dim)
    lead = pair < lead_pairs
    side = (pair >= lead_pairs) & (pair < lead_pairs + side_pairs)
    last = pair >= lead_pairs + side_pairs

    def rates(part, start, count):
        rate = np.exp(np.float32(-math.log(10000.0)) * (pair - start).astype(np.float32) / np.float32(count))
        return np.where(part, rate, 0.0).astype(np.float32)

    spot = np.tile(np.arange(FRAME_TOK), frames)
    frame = np.repeat(np.arange(frames), FRAME_TOK).astype(np.float32)
    angles = (
        frame[:, None] * rates(lead, 0, lead_pairs)[None]
        + (spot // WP).astype(np.float32)[:, None] * rates(side, lead_pairs, side_pairs)[None]
        + (spot % WP).astype(np.float32)[:, None] * rates(last, lead_pairs + side_pairs, side_pairs)[None]
    ).astype(np.float32)
    cosine, sine = np.cos(angles), np.sin(angles)
    return np.concatenate([cosine, cosine], axis=1), np.concatenate([-sine, sine], axis=1)


def modulated(residual, shift, scale):
    frames = shift.shape[0]
    normed = layer_norm(residual).reshape(frames, -1, residual.shape[1])
    return (normed * (1.0 + scale[:, None, :]) + shift[:, None, :]).reshape(residual.shape)


def frame_scaled(rows, gate):
    frames = gate.shape[0]
    return (rows.reshape(frames, -1, rows.shape[1]) * gate[:, None, :]).reshape(rows.shape)


def frame_sum(values, frames):
    return jnp.sum(values.reshape(frames, -1, values.shape[1]), axis=1)


VM = pl.BlockSpec(memory_space=pltpu.VMEM)
SM = pl.BlockSpec(memory_space=pltpu.SMEM)
ANY = pl.BlockSpec(memory_space=pl.ANY)


def row_add(target, left, right, rows):
    step = 32 if rows % 32 == 0 else rows

    def chunk(index, carry):
        at = pl.ds(pl.multiple_of(index * step, step), step)
        target[at, :] = left[at, :] + right[at, :]
        return carry

    lax.fori_loop(0, rows // step, chunk, 0)


def row_sum(target, left, right, rows):
    step = 16 if rows % 16 == 0 else rows

    def chunk(index, carry):
        at = pl.ds(pl.multiple_of(index * step, step), step)
        target[at, :] = left[at, :].astype(F32) + right[at, :].astype(F32)
        return carry

    lax.fori_loop(0, rows // step, chunk, 0)


class Flights:
    def __init__(self):
        self.sent = []

    def send(self, source, target, send_sem, recv_sem, device, when=None):
        copy = pltpu.make_async_remote_copy(
            src_ref=source,
            dst_ref=target,
            send_sem=send_sem,
            recv_sem=recv_sem,
            device_id=device,
            device_id_type=MESH,
        )
        if when is None:
            copy.start()
        else:
            pl.when(when)(copy.start)
        self.sent.append((when, copy))

    def local(self, source, target, sem):
        copy = pltpu.make_async_copy(source, target, sem)
        copy.start()
        return copy

    def drain(self):
        for when, copy in self.sent:
            if when is None:
                copy.wait_send()
            else:
                pl.when(when)(copy.wait_send)


def landed(target, sem, device):
    pltpu.make_async_remote_copy(
        src_ref=target,
        dst_ref=target,
        send_sem=sem,
        recv_sem=sem,
        device_id=device,
        device_id_type=MESH,
    ).wait_recv()


def greet(devices, optional=()):
    barrier = pltpu.get_barrier_semaphore()
    for device in devices:
        pl.semaphore_signal(barrier, inc=1, device_id=device, device_id_type=MESH)
    for when, device in optional:

        @pl.when(when)
        def _(device=device):
            pl.semaphore_signal(barrier, inc=1, device_id=device, device_id_type=MESH)

    count = len(devices)
    for when, _ in optional:
        count = count + when.astype(jnp.int32)
    pl.semaphore_wait(barrier, count)


def raw_views(joint, refs):
    if joint:
        rows_ref, rest = refs[0], refs[1:]
        width = rows_ref.shape[1] // 3
        spans = ((rows_ref, 0), (rows_ref, width), (rows_ref, 2 * width))
    else:
        rows_ref, keys_ref, rest = refs[0], refs[1], refs[2:]
        width = rows_ref.shape[1]
        spans = ((rows_ref, 0), (keys_ref, 0), (keys_ref, width))

    def view(which, head):
        ref, base = spans[which]
        return ref[:, base + head * HD : base + (head + 1) * HD]

    return view, width, rest


def turned(values, cos_ref, sin_ref, sign):
    return values * cos_ref[...] + sign * (pltpu.roll(values, HD // 2, 1) * sin_ref[...])


def attend_forward_kernel(joint, rotary, gain_row, live_ref, *refs):
    view, width, refs = raw_views(joint, refs)
    gain_ref, cos_ref, sin_ref, refs = *refs[:3], refs[3:]
    out_ref, lse_ref, query_ref, key_ref, inv_q_ref, inv_k_ref, refs = *refs[:6], refs[6:]
    q_sum, k_sum, q_peer, k_peer, send, recv = refs
    heads = width // HD
    core_peer = {"sp": 1 - lax.axis_index("sp")}
    fly = Flights()
    greet((core_peer,))
    for which, own, peer in ((0, q_sum, q_peer), (1, k_sum, k_peer)):
        total = view(which, 0) * view(which, 0)
        for head in range(1, heads):
            total = total + view(which, head) * view(which, head)
        own[...] = jnp.broadcast_to(jnp.sum(total, axis=1, keepdims=True), own.shape)
        fly.send(own, peer, send.at[which], recv.at[which], core_peer)
    for which, own, peer, kept in ((0, q_sum, q_peer, inv_q_ref), (1, k_sum, k_peer, inv_k_ref)):
        landed(peer, recv.at[which], core_peer)
        kept[...] = lax.rsqrt((own[...] + peer[...]) / D + EPSILON)
    rows, keys = query_ref.shape[0], key_ref.shape[0]
    spot = lax.broadcasted_iota(jnp.int32, (rows, keys), 1)
    allowed = spot < live_ref[0]
    for head in range(heads):
        part = slice(head * HD, (head + 1) * HD)
        column = pl.ds(pl.multiple_of(lax.axis_index("sp") * width + head * HD, HD), HD)
        query = view(0, head) * inv_q_ref[...] * gain_ref[gain_row : gain_row + 1, column]
        key = view(1, head) * inv_k_ref[...] * gain_ref[gain_row + 1 : gain_row + 2, column]
        if rotary:
            query, key = turned(query, cos_ref, sin_ref, 1.0), turned(key, cos_ref, sin_ref, 1.0)
        query, key, value = query.astype(BF), key.astype(BF), view(2, head).astype(BF)
        query_ref[:, part], key_ref[:, part] = query, key
        scores = jnp.where(allowed, product_nt(query, key) * SCALE, NEGATIVE)
        row_max = jnp.max(scores, axis=1, keepdims=True)
        log_total = row_max + jnp.log(jnp.sum(jnp.exp(scores - row_max), axis=1, keepdims=True))
        weights = jnp.exp(scores - log_total).astype(BF)
        out_ref[:, part] = product(weights, value).astype(BF)
        lse_ref[:, part] = jnp.broadcast_to(log_total, (rows, HD))
    fly.drain()


def attend_backward_kernel(joint, rotary, gain_row, live_ref, *refs):
    view, width, refs = raw_views(joint, refs)
    gain_ref, cos_ref, sin_ref, refs = *refs[:3], refs[3:]
    query_ref, key_ref, lse_ref, inv_q_ref, inv_k_ref, do_ref, refs = *refs[:6], refs[6:]
    if joint:
        grad_refs, refs = ((refs[0], 0), (refs[0], width), (refs[0], 2 * width)), refs[1:]
    else:
        grad_refs, refs = ((refs[0], 0), (refs[1], 0), (refs[1], width)), refs[2:]
    gain_out, scaled_q, scaled_k, q_dot, k_dot, q_peer, k_peer, send, recv = refs
    heads = width // HD
    core_peer = {"sp": 1 - lax.axis_index("sp")}
    fly = Flights()
    greet((core_peer,))
    rows, keys = query_ref.shape[0], key_ref.shape[0]
    spot = lax.broadcasted_iota(jnp.int32, (rows, keys), 1)
    allowed = spot < live_ref[0]
    dots = [None, None]
    gain_out[...] = jnp.zeros_like(gain_out)
    for head in range(heads):
        part = slice(head * HD, (head + 1) * HD)
        query, key, grad = query_ref[:, part], key_ref[:, part], do_ref[:, part]
        value = view(2, head).astype(BF)
        scores = jnp.where(allowed, product_nt(query, key) * SCALE, NEGATIVE)
        weights = jnp.exp(scores - lse_ref[:, head * HD : head * HD + 1])
        grad_weights = product_nt(grad, value)
        delta = jnp.sum(weights * grad_weights, axis=1, keepdims=True)
        grad_scores = (weights * (grad_weights - delta)).astype(BF)
        grad_query = (product(grad_scores, key) * SCALE).astype(BF).astype(F32)
        grad_key = (product_tn(grad_scores, query) * SCALE).astype(BF).astype(F32)
        grad_value = product_tn(weights.astype(BF), grad).astype(BF)
        ref, base = grad_refs[2]
        ref[:, base + head * HD : base + (head + 1) * HD] = grad_value
        for which, grad_rows, inverse, held in ((0, grad_query, inv_q_ref, scaled_q), (1, grad_key, inv_k_ref, scaled_k)):
            if rotary:
                grad_rows = turned(grad_rows, cos_ref, sin_ref, -1.0)
            raw = view(which, head)
            gain_out[which : which + 1, part] = jnp.sum(grad_rows * raw * inverse[...], axis=0, keepdims=True)
            column = pl.ds(pl.multiple_of(lax.axis_index("sp") * width + head * HD, HD), HD)
            scaled = grad_rows * gain_ref[gain_row + which : gain_row + which + 1, column]
            held[:, part] = scaled
            dots[which] = scaled * raw if head == 0 else dots[which] + scaled * raw
    for which, own, peer in ((0, q_dot, q_peer), (1, k_dot, k_peer)):
        own[...] = jnp.broadcast_to(jnp.sum(dots[which], axis=1, keepdims=True), own.shape)
        fly.send(own, peer, send.at[which], recv.at[which], core_peer)
    for which, own, peer, inverse, held in (
        (0, q_dot, q_peer, inv_q_ref, scaled_q),
        (1, k_dot, k_peer, inv_k_ref, scaled_k),
    ):
        landed(peer, recv.at[which], core_peer)
        column = inverse[...]
        slope = column * column * column * ((own[...] + peer[...]) / D)
        ref, base = grad_refs[which]
        for head in range(heads):
            part = slice(head * HD, (head + 1) * HD)
            out = held[:, part] * column - view(which, head) * slope
            ref[:, base + head * HD : base + (head + 1) * HD] = out.astype(BF)
    fly.drain()


def attend_call(kernel, joint, rotary, number, live, raws, others, shapes, scratch, flops, exps):
    dma = pltpu.SemaphoreType.DMA
    arrays = [*raws, *others]
    moved = sum(v.size * v.dtype.itemsize for v in [*arrays, *shapes])
    return pl.pallas_call(
        functools.partial(kernel, joint, rotary, 0 if rotary else 2),
        out_shape=shapes,
        in_specs=[SM] + [VM] * len(arrays),
        out_specs=[VM] * len(shapes),
        scratch_shapes=[*scratch, dma((2,)), dma((2,))],
        compiler_params=pltpu.CompilerParams(collective_id=number, has_side_effects=True),
        cost_estimate=pl.CostEstimate(flops=flops, bytes_accessed=moved, transcendentals=exps),
    )(live, *arrays)


def attend_sizes(raws):
    joint = len(raws) == 1
    rows, keys = raws[0].shape[0], raws[-1].shape[0]
    return joint, rows, keys, raws[0].shape[1] // 3 if joint else raws[0].shape[1]


def attend_forward(live, raws, gains, cosine, sine, rotary, number):
    joint, rows, keys, width = attend_sizes(raws)
    shape = jax.ShapeDtypeStruct
    shapes = [
        shape((rows, width), BF),
        shape((rows, width), F32),
        shape((rows, width), BF),
        shape((keys, width), BF),
        shape((rows, HD), F32),
        shape((keys, HD), F32),
    ]
    scratch = [pltpu.VMEM((n, HD), F32) for n in (rows, keys, rows, keys)]
    work = rows * keys * width
    return attend_call(
        attend_forward_kernel, joint, rotary, number, live, raws, [gains, cosine, sine],
        shapes, scratch, 4 * work, 2 * work // HD,
    )


def attend_backward(live, raws, gains, cosine, sine, rotary, number, saved, grad):
    joint, rows, keys, width = attend_sizes(raws)
    shape = jax.ShapeDtypeStruct
    shapes = [shape(raw.shape, BF) for raw in raws] + [shape((8, width), F32)]
    scratch = [pltpu.VMEM((rows, width), F32), pltpu.VMEM((keys, width), F32)]
    scratch += [pltpu.VMEM((n, HD), F32) for n in (rows, keys, rows, keys)]
    work = rows * keys * width
    return attend_call(
        attend_backward_kernel, joint, rotary, number, live, raws,
        [gains, cosine, sine, *saved, grad], shapes, scratch, 10 * work, work // HD,
    )


ALL_CHIPS, KEEP, HALF_X, HALF_Y = range(4)


def gather_kernel(outer, kinds, *refs):
    full = len(kinds)
    ins, refs = refs[:full], refs[full:]
    mlp_in, text_ref, refs = refs[0], refs[1], refs[2:]
    outs, refs = list(refs[:full]), refs[full:]
    bias_out, gain_out, step_out, up_out, text_out, refs = *refs[:5], refs[5:]
    own, refs = refs[:full], refs[full:]
    halves = [i for i, kind in enumerate(kinds) if kind[1] == KEEP]
    form = [kind[1] for kind in kinds]
    whole, refs = refs[: len(halves)], refs[len(halves) :]
    small_all, mlp_ref, up_own, local_sem, zs, zr, s1, r1, s2, r2, a_s, a_r, f_s, f_r, f_l, t_s, i_s = refs
    outs[0] = small_all
    z, y, x = (lax.axis_index(name) for name in FS)
    core = lax.axis_index("sp")
    here = 2 * y + x
    up = full
    fins = {}
    for j, i in enumerate(halves):
        fins[i] = outs[i]
        outs[i] = whole[j]
    fly = Flights()
    x_peer, y_peer = {"xc": 1 - x}, {"yb": 1 - y}
    diagonal = {"yb": 1 - y, "xc": 1 - x}
    around = ((x_peer, y, 1 - x), (y_peer, 1 - y, x), (diagonal, 1 - y, 1 - x))
    above, below = {"za": z + 1}, {"za": z - 1}
    core_peer = {"sp": 1 - core}
    has_above, has_below = z + 1 < outer, z >= 1
    loads = []
    for i, (parts, _, base, of) in enumerate(kinds):
        width = ins[i].shape[1] // (2 * of)
        for part in range(parts):
            column = pl.multiple_of((2 * (base + part) + core) * width, width)
            span = slice(part * width, (part + 1) * width)
            loads.append((i, fly.local(ins[i].at[:, pl.ds(column, width)], own[i].at[:, span], i_s.at[i, part])))
        if parts == 0:
            loads.append((i, fly.local(ins[i], own[i], i_s.at[i, 0])))
    mlp_load = fly.local(mlp_in, mlp_ref, i_s.at[full, 0])
    greet((x_peer, y_peer, diagonal, core_peer), ((has_above, above), (has_below, below)))

    def spot(i, slot, ty, tx):
        if form[i] == HALF_X:
            return outs[i].at[slot, tx]
        if form[i] == HALF_Y:
            return outs[i].at[slot, ty]
        return outs[i].at[slot, ty, tx]

    def shard(i, slot):
        return spot(i, slot, y, x) if i < full else up_out.at[slot]

    def z_send(i, way, hop, source=None):
        if hop > outer - 2:
            return
        slot = z - hop if way == 0 else z + hop
        when = jnp.logical_and(has_above, slot >= 0) if way == 0 else jnp.logical_and(has_below, slot < outer)
        fly.send(
            shard(i, slot) if source is None else source,
            shard(i, slot),
            zs.at[i, way, hop],
            zr.at[i, way, hop],
            above if way == 0 else below,
            when,
        )

    def z_slot(way, hop):
        slot = z - 1 - hop if way == 0 else z + 1 + hop
        return slot, (slot >= 0 if way == 0 else slot < outer)

    def z_wait(i, way, hop):
        slot, when = z_slot(way, hop)

        @pl.when(when)
        def _():
            landed(shard(i, slot), zr.at[i, way, hop], below if way == 0 else above)

    def turns(i, slot):
        turn = (slot + i) % 2
        first = ((y + turn) % 2, (x + 1 - turn) % 2)
        second = ((y + 1 - turn) % 2, (x + turn) % 2)
        return first, second

    def xy_own(i, slot, when=None, source=None):
        mine = spot(i, slot, y, x)
        source = mine if source is None else source
        if form[i] in (HALF_X, HALF_Y):
            peer = x_peer if form[i] == HALF_X else y_peer
            fly.send(source, mine, s1.at[i, slot], r1.at[i, slot], peer, when)
            return
        first, second = turns(i, slot)
        fly.send(source, mine, s1.at[i, slot], r1.at[i, slot], {"yb": first[0], "xc": first[1]}, when)
        fly.send(source, mine, s2.at[i, slot, 0], r2.at[i, slot, 0], {"yb": second[0], "xc": second[1]}, when)

    def xy_pass(i, slot, when=None):
        if form[i] in (HALF_X, HALF_Y):
            return
        first, second = turns(i, slot)
        theirs = outs[i].at[slot, first[0], first[1]]

        def wait():
            landed(theirs, r1.at[i, slot], {"yb": first[0], "xc": first[1]})

        if when is None:
            wait()
        else:
            pl.when(when)(wait)
        fly.send(theirs, theirs, s2.at[i, slot, 1], r2.at[i, slot, 1], {"yb": second[0], "xc": second[1]}, when)

    def xy_end(i, slot):
        if form[i] == HALF_X:
            landed(spot(i, slot, y, 1 - x), r1.at[i, slot], x_peer)
            return
        if form[i] == HALF_Y:
            landed(spot(i, slot, 1 - y, x), r1.at[i, slot], y_peer)
            return
        _, second = turns(i, slot)
        device = {"yb": second[0], "xc": second[1]}
        landed(outs[i].at[slot, second[0], second[1]], r2.at[i, slot, 0], device)
        landed(outs[i].at[slot, 1 - y, 1 - x], r2.at[i, slot, 1], device)

    for i in range(full):
        for index, load in loads:
            if index == i:
                load.wait()
        for way in range(2):
            z_send(i, way, 0, own[i])
        xy_own(i, z, None, own[i])
    locals_ = [fly.local(own[i], spot(i, z, y, x), local_sem.at[i]) for i in range(full)]

    fly.send(text_ref, text_out.at[core], t_s.at[0], t_s.at[1], core_peer)
    locals_.append(fly.local(text_ref, text_out.at[core], t_s.at[2]))
    mlp_load.wait()
    hid = mlp_ref.shape[1] // (outer * PLANE * 2)
    for own_core in range(2):

        @pl.when(core == own_core)
        def _(own_core=own_core):
            for place in range(PLANE):
                for slot in range(outer):
                    column = ((slot * PLANE + place) * 2 + own_core) * hid
                    up_own[place, :, slot * hid : (slot + 1) * hid] = mlp_ref[:, column : column + hid]

    for hop in range(outer - 1):
        for i in range(full):
            for way in range(2):
                slot, when = z_slot(way, hop)
                z_wait(i, way, hop)
                z_send(i, way, hop + 1)
                xy_own(i, slot, when)
        if hop == 0:
            locals_.append(fly.local(up_own.at[here], up_out.at[z, here], local_sem.at[up]))
            for turn, (device, ty, tx) in enumerate(around):
                fly.send(up_own.at[2 * ty + tx], up_out.at[z, here], a_s.at[turn], a_r.at[turn], device)
    for copy in locals_:
        copy.wait()
    for turn, (device, ty, tx) in enumerate(around):
        landed(up_out.at[z, 2 * ty + tx], a_r.at[turn], device)
    for way in range(2):
        z_send(up, way, 0)
    for i in range(full):
        xy_pass(i, z)
    for hop in range(outer - 1):
        for i in range(full):
            for way in range(2):
                slot, when = z_slot(way, hop)
                xy_pass(i, slot, when)
        for way in range(2):
            z_wait(up, way, hop)
            z_send(up, way, hop + 1)
    for i in (*halves, *(i for i in range(full) if i not in halves)):
        for slot in range(outer):
            xy_end(i, slot)
        if i == 0:
            bias_len = bias_out.shape[1] // (outer * PLANE)
            gain_len = gain_out.shape[1] // (outer * PLANE)
            for chip in range(outer * PLANE):
                rows = small_all.at[chip // PLANE, (chip // 2) % 2, chip % 2]
                bias_out[:, chip * bias_len : (chip + 1) * bias_len] = rows[0:1, :bias_len]
                gain_out[:, chip * gain_len : (chip + 1) * gain_len] = rows[1:5, :gain_len]
                step_out[chip : chip + 1, :] = rows[5:6, : step_out.shape[1]]
        if i not in halves:
            continue
        j, part = halves.index(i), outer // 2
        width = own[i].shape[-1]
        columns = pl.ds(pl.multiple_of(core * width, width), width)
        theirs, ours = pl.ds((1 - core) * part, part), pl.ds(core * part, part)
        fly.send(outs[i].at[theirs], fins[i].at[:, :, :, :, columns], f_s.at[j], f_r.at[j], core_peer)
        fly.local(outs[i].at[ours], fins[i].at[:, :, :, :, columns], f_l.at[j])
    for j, i in enumerate(halves):
        width = own[i].shape[-1]
        columns = pl.ds(pl.multiple_of(core * width, width), width)
        others = pl.ds(pl.multiple_of((1 - core) * width, width), width)
        ours = pl.ds(core * (outer // 2), outer // 2)
        pltpu.make_async_copy(outs[i].at[ours], fins[i].at[:, :, :, :, columns], f_l.at[j]).wait()
        landed(fins[i].at[:, :, :, :, others], f_r.at[j], core_peer)
    landed(text_out.at[1 - core], t_s.at[1], core_peer)
    fly.drain()


def gather_weights(outer, kinds, arrays, mlp, text, small_lens):
    shapes, own, whole = [], [], []
    for (parts, form, _, of), array in zip(kinds, arrays, strict=True):
        rows, width = array.shape
        half = width * parts // (2 * of) if parts else width
        own.append(pltpu.VMEM((rows, half), array.dtype))
        if form in (HALF_X, HALF_Y):
            shapes.append(jax.ShapeDtypeStruct((outer, 2, rows, half), array.dtype))
        elif form == KEEP:
            whole.append(pltpu.VMEM((outer, 2, 2, rows, half), array.dtype))
            shapes.append(jax.ShapeDtypeStruct((outer // 2, 2, 2, rows, 2 * half), array.dtype))
        else:
            shapes.append(jax.ShapeDtypeStruct((outer, 2, 2, rows, half), array.dtype))
    bias_len, gain_len, _ = small_lens
    chips = outer * PLANE
    shapes[0] = jax.ShapeDtypeStruct((8, 128), F32)
    shapes.append(jax.ShapeDtypeStruct((1, chips * bias_len), F32))
    shapes.append(jax.ShapeDtypeStruct((4, chips * gain_len), F32))
    shapes.append(jax.ShapeDtypeStruct((chips, 128), F32))
    rows, units = mlp.shape
    mine = units // (2 * PLANE)
    shapes.append(jax.ShapeDtypeStruct((outer, PLANE, rows, mine), mlp.dtype))
    shapes.append(jax.ShapeDtypeStruct((2, *text.shape), text.dtype))
    dma = pltpu.SemaphoreType.DMA
    hops = outer - 1
    nf, nh = len(kinds), len(whole)
    results = pl.pallas_call(
        functools.partial(gather_kernel, outer, kinds),
        out_shape=shapes,
        in_specs=[ANY] * (nf + 2),
        out_specs=[*[ANY] * nf, VM, VM, VM, ANY, ANY],
        scratch_shapes=[
            *own,
            *whole,
            pltpu.VMEM((outer, 2, 2, *arrays[0].shape), F32),
            pltpu.VMEM(mlp.shape, mlp.dtype),
            pltpu.VMEM((PLANE, rows, mine), mlp.dtype),
            dma((nf + 1,)),
            dma((nf + 1, 2, hops)),
            dma((nf + 1, 2, hops)),
            dma((nf, outer)),
            dma((nf, outer)),
            dma((nf, outer, 2)),
            dma((nf, outer, 2)),
            dma((3,)),
            dma((3,)),
            dma((nh,)),
            dma((nh,)),
            dma((nh,)),
            dma((3,)),
            dma((nf + 1, 3)),
        ],
        compiler_params=pltpu.CompilerParams(
            collective_id=0, has_side_effects=True, vmem_limit_bytes=63 * 1024 * 1024
        ),
        cost_estimate=pl.CostEstimate(flops=10**11, bytes_accessed=10**8, transcendentals=0),
        name="gather_weights",
    )(*arrays, mlp, text)
    flat = [value.reshape(-1, value.shape[-1]) if value.ndim == 5 else value for value in results[1:nf]]
    bias, gains, steps, up, texts = results[nf:]
    return flat, bias, gains, steps, up.reshape(-1, up.shape[-1]), texts.reshape(-1, texts.shape[-1])


def plane_gather_kernel(own_ref, out_ref, local_sem, send, recv):
    y, x, core = lax.axis_index("yb"), lax.axis_index("xc"), lax.axis_index("sp")
    x_peer, y_peer, core_peer = {"xc": 1 - x}, {"yb": 1 - y}, {"sp": 1 - core}
    fly = Flights()
    greet((x_peer, y_peer, core_peer))
    size = own_ref.shape[0] // 2
    top, low = pl.ds(0, size), pl.ds(size, size)
    fly.send(own_ref.at[top], out_ref.at[0, 1, 0, top], send.at[0], recv.at[0], x_peer)
    fly.send(own_ref.at[low], out_ref.at[1, 0, 0, low], send.at[1], recv.at[1], y_peer)
    fly.send(own_ref.at[low], out_ref.at[0, 1, 0, low], send.at[2], recv.at[2], x_peer)
    fly.send(own_ref.at[top], out_ref.at[1, 0, 0, top], send.at[3], recv.at[3], y_peer)
    fly.send(own_ref, out_ref.at[0, 0, 1], send.at[4], recv.at[4], core_peer)
    local = fly.local(own_ref, out_ref.at[0, 0, 0], local_sem.at[0])
    across = []

    def arrive(index, dy, dx, rows, device, onward=None):
        block = out_ref.at[dy, dx, 0, rows]
        landed(block, recv.at[index], device)
        if onward is not None:
            to, number = onward
            fly.send(block, out_ref.at[1, 1, 0, rows], send.at[number], recv.at[number], to)
        fly.send(block, out_ref.at[dy, dx, 1, rows], send.at[index + 7], recv.at[index + 7], core_peer)
        across.append((index + 7, dy, dx, rows))

    arrive(0, 0, 1, top, x_peer, (y_peer, 5))
    arrive(1, 1, 0, low, y_peer, (x_peer, 6))
    arrive(2, 0, 1, low, x_peer)
    arrive(3, 1, 0, top, y_peer)
    arrive(5, 1, 1, top, y_peer)
    arrive(6, 1, 1, low, x_peer)
    landed(out_ref.at[0, 0, 1], recv.at[4], core_peer)
    for index, dy, dx, rows in across:
        landed(out_ref.at[dy, dx, 1, rows], recv.at[index], core_peer)
    local.wait()
    fly.drain()


def plane_gather(own):
    rows, width = own.shape
    dma = pltpu.SemaphoreType.DMA
    out = pl.pallas_call(
        plane_gather_kernel,
        out_shape=jax.ShapeDtypeStruct((2, 2, 2, rows, width), own.dtype),
        in_specs=[VM],
        out_specs=VM,
        scratch_shapes=[dma((1,)), dma((14,)), dma((14,))],
        compiler_params=pltpu.CompilerParams(collective_id=1, has_side_effects=True),
        cost_estimate=pl.CostEstimate(flops=10**10, bytes_accessed=10**7, transcendentals=0),
        name="plane_gather",
    )(own)
    return out.reshape(8 * rows, width)


def plane_sum_kernel(part_a, part_b, out_a, out_b, core_in, first, second, keep, send, recv):
    y, x, core = lax.axis_index("yb"), lax.axis_index("xc"), lax.axis_index("sp")
    x_peer, y_peer, core_peer = {"xc": 1 - x}, {"yb": 1 - y}, {"sp": 1 - core}
    fly = Flights()
    greet((x_peer, y_peer, core_peer))
    rows = part_a.shape[3]
    chips = (((1, 1), (1, 0), (0, 1), (0, 0)), ((1, 1), (0, 1), (1, 0), (0, 0)))
    parts, outs, peers = (part_a, part_b), (out_a, out_b), ((y_peer, x_peer), (x_peer, y_peer))
    for index in range(4):
        for n in range(2):
            dy, dx = chips[n][index]
            fly.send(
                parts[n].at[dy, dx, 1], core_in.at[n, index], send.at[n, index], recv.at[n, index], core_peer
            )

    def core_sum(n, index):
        dy, dx = chips[n][index]
        landed(core_in.at[n, index], recv.at[n, index], core_peer)
        row_add(core_in.at[n, index], core_in.at[n, index], parts[n].at[dy, dx, 0], rows)

    for index in range(2):
        for n in range(2):
            core_sum(n, index)
            fly.send(
                core_in.at[n, index], first.at[n, index], send.at[n, index + 4], recv.at[n, index + 4], peers[n][0]
            )
    for index in (2, 3):
        for n in range(2):
            core_sum(n, index)
    for n in range(2):
        landed(first.at[n, 0], recv.at[n, 4], peers[n][0])
        row_add(second.at[n, 0], first.at[n, 0], core_in.at[n, 2], rows)
        fly.send(second.at[n, 0], second.at[n, 1], send.at[n, 6], recv.at[n, 6], peers[n][1])
    for n in range(2):
        landed(first.at[n, 1], recv.at[n, 5], peers[n][0])
        row_sum(keep.at[n], first.at[n, 1], core_in.at[n, 3], rows)
    for n in range(2):
        landed(second.at[n, 1], recv.at[n, 6], peers[n][1])
        row_sum(outs[n], keep.at[n], second.at[n, 1], rows)
    fly.drain()


def plane_sum(one, other):
    rows, width = one.shape[0] // 8, one.shape[1]
    dma = pltpu.SemaphoreType.DMA
    shape = jax.ShapeDtypeStruct((rows, width), F32)
    return pl.pallas_call(
        plane_sum_kernel,
        out_shape=(shape, shape),
        in_specs=[VM, VM],
        out_specs=(VM, VM),
        scratch_shapes=[
            pltpu.VMEM((2, 4, rows, width), BF),
            pltpu.VMEM((2, 2, rows, width), BF),
            pltpu.VMEM((2, 2, rows, width), BF),
            pltpu.VMEM((2, rows, width), F32),
            dma((2, 7)),
            dma((2, 7)),
        ],
        compiler_params=pltpu.CompilerParams(collective_id=2, has_side_effects=True),
        cost_estimate=pl.CostEstimate(flops=10**10, bytes_accessed=10**7, transcendentals=0),
        name="plane_sum",
    )(one.reshape(2, 2, 2, rows, width), other.reshape(2, 2, 2, rows, width))


def pair_sum_kernel(part_ref, out_ref, peer_in, send, recv):
    core = lax.axis_index("sp")
    core_peer = {"sp": 1 - core}
    fly = Flights()
    greet((core_peer,))
    size = part_ref.shape[1] // 2
    for index in range(2):
        rows = pl.ds(index * size, size)
        fly.send(part_ref.at[1 - core, rows], peer_in.at[rows], send.at[index], recv.at[index], core_peer)
    for index in range(2):
        rows = pl.ds(index * size, size)
        landed(peer_in.at[rows], recv.at[index], core_peer)
        row_sum(out_ref.at[rows], part_ref.at[core, rows], peer_in.at[rows], size)
    fly.drain()


def pair_sum(partial):
    rows, width = partial.shape[0] // 2, partial.shape[1]
    dma = pltpu.SemaphoreType.DMA
    return pl.pallas_call(
        pair_sum_kernel,
        out_shape=jax.ShapeDtypeStruct((rows, width), F32),
        in_specs=[VM],
        out_specs=VM,
        scratch_shapes=[pltpu.VMEM((rows, width), F32), dma((2,)), dma((2,))],
        compiler_params=pltpu.CompilerParams(collective_id=4, has_side_effects=True),
        cost_estimate=pl.CostEstimate(flops=10**9, bytes_accessed=10**7, transcendentals=0),
        name="pair_sum",
    )(partial.reshape(2, rows, width))


AHEAD, LAG_PLANE, LAG_CHAIN = 14, 4, 6
PLAIN, SPLIT, OVER_X, OVER_Y = range(4)


def reduce_kernel(outer, kinds, *refs):
    count = len(kinds)
    shards = outer * PLANE
    gs, refs = refs[:count], refs[count:]
    frames_ref, small_ref, up_ref, down_ref, refs = *refs[:4], refs[4:]
    outs, refs = refs[:count], refs[count:]
    frames_out, small_out, up_out, down_out, refs = *refs[:4], refs[4:]
    pieces = [(i, part) for i, (parts, _) in enumerate(kinds) for part in range(parts)]
    total = len(pieces)
    forms = [kinds[i][1] for i, _ in pieces]
    near_refs, near = list(refs), {}
    for p in range(total):
        if forms[p] in (PLAIN, SPLIT):
            near[p] = near_refs.pop(0)
    refs = near_refs
    plane, refs = refs[:total], refs[total:]
    chain, refs = refs[:total], refs[total:]
    split = [i for i, kind in enumerate(kinds) if kind[1] == SPLIT]
    whole, refs = refs[: len(split)], refs[len(split) :]
    small_in, small_own, small_peer, up_in, down_in, refs = *refs[:5], refs[5:]
    e_s, e_r, e_l, s1, r1, s2, r2, zs, zr, o_s, o_r, f_s, f_r, m_s, m_r, l_s, p_s, p_r = refs
    z, y, x = (lax.axis_index(name) for name in FS)
    core = lax.axis_index("sp")
    here = (z * 2 + y) * 2 + x
    core_peer = {"sp": 1 - core}
    above, below = {"za": z + 1}, {"za": z - 1}
    fly = Flights()

    def chip(index):
        return {"za": index // 4, "yb": (index // 2) % 2, "xc": index % 2}

    others = [(here + j) % shards for j in range(1, shards)]
    greet((core_peer, *[chip(index) for index in others]))

    part_slots = outer // 2
    ours, other_slots = pl.ds(core * part_slots, part_slots), pl.ds((1 - core) * part_slots, part_slots)
    for j, i in enumerate(split):
        width = whole[j].shape[-1]
        mine = pl.ds(pl.multiple_of(core * width, width), width)
        theirs = pl.ds(pl.multiple_of((1 - core) * width, width), width)
        fly.send(gs[i].at[:, :, :, :, theirs], whole[j].at[ours], e_s.at[j], e_r.at[j], core_peer)
        fly.local(gs[i].at[:, :, :, :, mine], whole[j].at[ours], e_l.at[j])

    def joined(i):
        j = split.index(i)
        width = whole[j].shape[-1]
        mine = pl.ds(pl.multiple_of(core * width, width), width)
        pltpu.make_async_copy(gs[i].at[:, :, :, :, mine], whole[j].at[ours], e_l.at[j]).wait()
        landed(whole[j].at[other_slots], e_r.at[j], core_peer)

    def width_of(p):
        return plane[p].shape[-1]

    def source(p, *place):
        i, part = pieces[p]
        held = whole[split.index(i)] if forms[p] == SPLIT else gs[i]
        width = width_of(p)
        return held.at[(*place, slice(None), pl.ds(part * width, width))]

    frame_copy = fly.local(frames_ref, frames_out.at[here, core], l_s.at[0])
    small_copy = fly.local(small_ref.at[here], small_in.at[here], l_s.at[1])
    for j, index in enumerate(others):
        fly.send(frames_ref, frames_out.at[here, core], f_s.at[j], f_r.at[here], chip(index))
        fly.send(small_ref.at[index], small_in.at[here], m_s.at[j], m_r.at[here], chip(index))

    near_by = ((y, 1 - x), (1 - y, x), (1 - y, 1 - x))
    up_copy = fly.local(up_ref.at[2 * y + x], up_in.at[core, 2 * y + x], p_s.at[0])
    for j, (ty, tx) in enumerate(near_by):
        fly.send(
            up_ref.at[2 * ty + tx],
            up_in.at[core, 2 * y + x],
            p_s.at[j + 1],
            p_r.at[j + 1],
            {"yb": ty, "xc": tx},
        )
    fly.send(down_ref, down_in, p_s.at[4], p_r.at[4], core_peer)

    def feed_forward_landed():
        up_copy.wait()
        for j, (ty, tx) in enumerate(near_by):
            landed(up_in.at[core, 2 * ty + tx], p_r.at[j + 1], {"yb": ty, "xc": tx})
        fly.send(up_in.at[core], up_in.at[core], p_s.at[5], p_r.at[5], core_peer)
        hid = down_ref.shape[0]
        landed(down_in, p_r.at[4], core_peer)
        for side in range(2):

            @pl.when(core == side)
            def _(side=side):
                down_out[side * hid : (side + 1) * hid, :] = down_ref[...]
                down_out[(1 - side) * hid : (2 - side) * hid, :] = down_in[...]

    def feed_forward_rows():
        hid = down_ref.shape[0]
        landed(up_in.at[1 - core], p_r.at[5], core_peer)
        for slot in range(outer):
            for place in range(PLANE):
                for side in range(2):
                    column = ((slot * PLANE + place) * 2 + side) * hid
                    up_out[:, column : column + hid] = up_in[side, place, :, slot * hid : (slot + 1) * hid]

    def slot_at(step):
        if step == outer - 1:
            return z
        falling = outer - 1 - step
        falling = jnp.where(falling > z, falling, falling - 1)
        rising = jnp.where(step < z, step, step + 1)
        return jnp.where(z < part_slots, falling, rising)

    units = [(slot_at(step), p) for step in range(outer) for p in range(total)]

    def turns(p, slot):
        turn = (slot + p) % 2
        first = ((y + 1 - turn) % 2, (x + turn) % 2)
        second = ((y + turn) % 2, (x + 1 - turn) % 2)
        return first, second

    def device(place):
        return {"yb": place[0], "xc": place[1]}

    def start(slot, p):
        first, _ = turns(p, slot)
        fly.send(
            source(p, slot, 1 - y, 1 - x), near[p].at[slot, 1], s1.at[p, slot, 1], r1.at[p, slot, 1], device(first)
        )
        fly.send(
            source(p, slot, first[0], first[1]), near[p].at[slot, 0], s1.at[p, slot, 0], r1.at[p, slot, 0], device(first)
        )

    def summed_over(p):
        return (x, {"xc": 1 - x}) if forms[p] == OVER_X else (y, {"yb": 1 - y})

    def pass_on(slot, p):
        rows = plane[p].shape[1]
        if p not in near:
            index, peer = summed_over(p)
            fly.send(source(p, slot, 1 - index), plane[p].at[slot], s2.at[p, slot], r2.at[p, slot], peer)
            return
        first, second = turns(p, slot)
        landed(near[p].at[slot, 1], r1.at[p, slot, 1], device(first))
        row_add(near[p].at[slot, 1], near[p].at[slot, 1], source(p, slot, second[0], second[1]), rows)
        fly.send(near[p].at[slot, 1], plane[p].at[slot], s2.at[p, slot], r2.at[p, slot], device(second))
        landed(near[p].at[slot, 0], r1.at[p, slot, 0], device(first))
        row_add(near[p].at[slot, 0], near[p].at[slot, 0], source(p, slot, y, x), rows)

    def plane_total(slot, p):
        rows = plane[p].shape[1]
        if p not in near:
            index, peer = summed_over(p)
            landed(plane[p].at[slot], r2.at[p, slot], peer)
            row_add(plane[p].at[slot], plane[p].at[slot], source(p, slot, index), rows)
            return
        _, second = turns(p, slot)
        landed(plane[p].at[slot], r2.at[p, slot], device(second))
        row_add(plane[p].at[slot], plane[p].at[slot], near[p].at[slot, 0], rows)

    def along(slot, p, last):
        rows, width = plane[p].shape[1:]
        if not last:
            for way, when, edge, ahead, behind in (
                (1, slot < z, z == outer - 1, below, above),
                (0, slot > z, z == 0, above, below),
            ):
                link = chain[p].at[slot + 1 - way]

                @pl.when(jnp.logical_and(when, jnp.logical_not(edge)))
                def _(way=way, link=link, behind=behind):
                    landed(link, zr.at[p, way, slot], behind)
                    row_add(plane[p].at[slot], plane[p].at[slot], link, rows)

                fly.send(plane[p].at[slot], link, zs.at[p, way, slot], zr.at[p, way, slot], ahead, when)
            return
        has_above, has_below = z < outer - 1, z > 0
        for way, when, behind in ((1, has_above, above), (0, has_below, below)):

            @pl.when(when)
            def _(way=way, behind=behind):
                landed(chain[p].at[slot + 1 - way], zr.at[p, way, slot], behind)

        step = 16 if rows % 16 == 0 else rows
        i, part = pieces[p]
        column = pl.multiple_of((2 * part + core) * width, width)

        def chunk(index, carry):
            at = pl.ds(pl.multiple_of(index * step, step), step)
            upper = jnp.where(has_above, chain[p][slot, at, :].astype(F32), 0.0)
            lower = jnp.where(has_below, chain[p][slot + 1, at, :].astype(F32), 0.0)
            outs[i][at, pl.ds(column, width)] = (plane[p][slot, at, :].astype(F32) + upper + lower).astype(BF)
            return carry

        lax.fori_loop(0, rows // step, chunk, 0)
        block = outs[i].at[:, pl.ds(column, width)]
        fly.send(block, block, o_s.at[p], o_r.at[p], core_peer)

    waiting = set(split)

    def begin(unit):
        slot, p = units[unit]
        if p not in near:
            return
        if pieces[p][0] in waiting:
            joined(pieces[p][0])
            waiting.discard(pieces[p][0])
        start(slot, p)

    for unit in range(min(AHEAD, len(units))):
        begin(unit)
    for tick in range(len(units) + LAG_CHAIN):
        if tick < len(units):
            pass_on(*units[tick])
            if tick + AHEAD < len(units):
                begin(tick + AHEAD)
        if 0 <= tick - LAG_PLANE < len(units):
            plane_total(*units[tick - LAG_PLANE])
        if tick == 4:
            feed_forward_landed()
        if tick == 10:
            feed_forward_rows()
        if 0 <= tick - LAG_CHAIN < len(units):
            unit = tick - LAG_CHAIN
            along(*units[unit], unit >= (outer - 1) * total)
        if tick == total:
            frame_copy.wait()
            for index in others:
                landed(frames_out.at[index, core], f_r.at[index], chip(index))
            fly.send(frames_out.at[:, core], frames_out.at[:, core], p_s.at[6], p_r.at[6], core_peer)
            small_copy.wait()
            for index in others:
                landed(small_in.at[index], m_r.at[index], chip(index))
            small_own[...] = jnp.sum(small_in[...], axis=0)
            fly.send(small_own, small_peer, l_s.at[2], l_s.at[3], core_peer)

    landed(frames_out.at[:, 1 - core], p_r.at[6], core_peer)
    landed(small_peer, l_s.at[3], core_peer)
    small_out[...] = small_own[...] + small_peer[...]
    for p, (i, part) in enumerate(pieces):
        width = width_of(p)
        column = pl.multiple_of((2 * part + 1 - core) * width, width)
        landed(outs[i].at[:, pl.ds(column, width)], o_r.at[p], core_peer)
    fly.drain()


def reduce_weights(outer, kinds, grads, frames, small, up, down):
    shards = outer * PLANE
    shaped, shapes, near, plane, chain, whole = [], [], [], [], [], []
    for (parts, form), grad in zip(kinds, grads, strict=True):
        full_width = grad.shape[-1] // 2 if form == SPLIT else grad.shape[-1]
        if form in (PLAIN, SPLIT):
            lead = outer // 2 if form == SPLIT else outer
            grad = grad.reshape(lead, 2, 2, -1, grad.shape[-1])
        rows, width = grad.shape[-2], full_width // parts
        shaped.append(grad)
        shapes.append(jax.ShapeDtypeStruct((rows, 2 * full_width), BF))
        for _ in range(parts):
            if form in (PLAIN, SPLIT):
                near.append(pltpu.VMEM((outer, 2, rows, width), BF))
            plane.append(pltpu.VMEM((outer, rows, width), BF))
            chain.append(pltpu.VMEM((outer + 1, rows, width), BF))
        if form == SPLIT:
            whole.append(pltpu.VMEM((outer, 2, 2, rows, full_width), BF))
    shapes.append(jax.ShapeDtypeStruct((shards, 2, *frames.shape), frames.dtype))
    shapes.append(jax.ShapeDtypeStruct(small.shape[1:], F32))
    shapes.append(jax.ShapeDtypeStruct((up.shape[1], 2 * PLANE * up.shape[2]), BF))
    shapes.append(jax.ShapeDtypeStruct((2 * down.shape[0], down.shape[1]), BF))
    dma = pltpu.SemaphoreType.DMA
    count, total, nsplit = len(kinds), len(plane), len(whole)
    results = pl.pallas_call(
        functools.partial(reduce_kernel, outer, kinds),
        out_shape=shapes,
        in_specs=[VM] * (count + 4),
        out_specs=[VM] * (count + 4),
        scratch_shapes=[
            *near,
            *plane,
            *chain,
            *whole,
            pltpu.VMEM(small.shape, F32),
            pltpu.VMEM(small.shape[1:], F32),
            pltpu.VMEM(small.shape[1:], F32),
            pltpu.VMEM((2, *up.shape), up.dtype),
            pltpu.VMEM(down.shape, down.dtype),
            dma((nsplit,)),
            dma((nsplit,)),
            dma((nsplit,)),
            dma((total, outer, 2)),
            dma((total, outer, 2)),
            dma((total, outer)),
            dma((total, outer)),
            dma((total, 2, outer)),
            dma((total, 2, outer)),
            dma((total,)),
            dma((total,)),
            dma((shards,)),
            dma((shards,)),
            dma((shards,)),
            dma((shards,)),
            dma((4,)),
            dma((7,)),
            dma((7,)),
        ],
        cost_estimate=pl.CostEstimate(flops=10**11, bytes_accessed=10**8, transcendentals=0),
        compiler_params=pltpu.CompilerParams(
            collective_id=3, has_side_effects=True, vmem_limit_bytes=67043328
        ),
        name="reduce_weights",
    )(*shaped, frames, small, up, down)
    return results[:count], *results[count:]


def modulation_kernel(sinus_ref, matrix_ref, bias_ref, out_ref, half, send, recv):
    core = lax.axis_index("sp")
    core_peer = {"sp": 1 - core}
    fly = Flights()
    greet((core_peer,))
    frames, width = out_ref.shape[0], matrix_ref.shape[1]
    mine = pl.ds(pl.multiple_of(core * width, width), width)
    half[...] = product(sinus_ref[...], matrix_ref[...]) + bias_ref[:, mine]
    for side in range(2):

        @pl.when(core == side)
        def _(side=side):
            out_ref[:, side * width : (side + 1) * width] = half[side * frames : (side + 1) * frames, :]
            half[:frames, :] = half[(1 - side) * frames : (2 - side) * frames, :]

    columns = pl.ds(pl.multiple_of(core * width, width), width)
    others = pl.ds(pl.multiple_of((1 - core) * width, width), width)
    fly.send(half.at[pl.ds(0, frames)], out_ref.at[:, columns], send.at[0], recv.at[0], core_peer)
    landed(out_ref.at[:, others], recv.at[0], core_peer)
    fly.drain()


def modulate(sinus, matrix, bias):
    dma = pltpu.SemaphoreType.DMA
    frames, width = sinus.shape[0], matrix.shape[1]
    return pl.pallas_call(
        modulation_kernel,
        out_shape=jax.ShapeDtypeStruct((frames // 2, 2 * width), F32),
        in_specs=[VM, VM, VM],
        out_specs=VM,
        scratch_shapes=[pltpu.VMEM((frames, width), F32), dma((1,)), dma((1,))],
        compiler_params=pltpu.CompilerParams(collective_id=9, has_side_effects=True),
        cost_estimate=pl.CostEstimate(flops=10**9, bytes_accessed=10**7, transcendentals=0),
        name="modulation",
    )(sinus, matrix, bias)


def gather(value, axes, axis=0):
    return lax.all_gather(value, axes, axis=axis, tiled=True)


def scatter(value, axes, axis=0):
    return lax.psum_scatter(value, axes, scatter_dimension=axis, tiled=True)


def body(
    tokens,
    text,
    clip_frames,
    timestep,
    mod_weight,
    mod_bias,
    qk_gains,
    self_in,
    self_out,
    cross_q,
    cross_kv,
    cross_out,
    mlp_in,
    mlp_out,
    cotangent,
):
    row_count = tokens.shape[0]
    frame_count = row_count // FRAME_TOK
    group_frames = timestep.shape[1]
    shards = D // self_in.shape[1]
    outer = shards // PLANE
    core = lax.axis_index("sp")
    chip = lax.axis_index(FS)
    in_rows = self_in.shape[1]
    own_frame = core * frame_count

    bias_len, gain_len = mod_bias.shape[1], qk_gains.shape[2]
    small_len = bias_len + 4 * gain_len
    small_rows = 8
    small_width = -(-(small_len + group_frames) // (small_rows * 128)) * 128
    small_room = small_rows * small_width

    small_own = jnp.zeros((8, -(-max(bias_len, 128) // 128) * 128), F32)
    small_own = small_own.at[0, :bias_len].set(mod_bias[0].astype(F32))
    small_own = small_own.at[1:5, :gain_len].set(qk_gains[0].astype(F32))
    small_own = small_own.at[5, :group_frames].set(timestep[0].astype(F32))
    weights, bias_all, gain_all, steps_all, up_matrix, text_all = gather_weights(
        outer,
        (
            (0, ALL_CHIPS, 0, 1),
            (1, ALL_CHIPS, 0, 1),
            (3, ALL_CHIPS, 0, 3),
            (1, KEEP, 0, 1),
            (1, HALF_Y, 0, 1),
            (1, HALF_X, 0, 2),
            (1, HALF_Y, 1, 2),
            (1, KEEP, 0, 1),
        ),
        [
            small_own,
            *(w[0] for w in (mod_weight, self_in, self_out, cross_q, cross_kv, cross_kv, cross_out)),
        ],
        mlp_in[0],
        text,
        (bias_len, gain_len, group_frames),
    )
    mod_matrix, self_proj, self_back, q_half, k_half, v_half, cross_back = weights
    hid = mlp_out.shape[1] // 2
    down_part = lax.dynamic_slice_in_dim(mlp_out[0], core * hid, hid, 0)
    down_part, bias_all = lax.optimization_barrier((down_part, bias_all))
    down_matrix = gather(down_part, "za")
    steps_all = steps_all[:, :group_frames].reshape(-1)

    live_keys = clip_frames * FRAME_TOK
    all_keys = jnp.full((1,), TXT, jnp.int32)
    own_steps = lax.dynamic_slice_in_dim(timestep[0], own_frame, frame_count)
    cosine, sine = (jnp.asarray(table) for table in rotary_tables(group_frames))
    sinus = sinus_features(timestep[0]).astype(BF)

    modulation = modulate(sinus, mod_matrix, bias_all)
    shift_one, scale_one, gate_one, shift_two, scale_two, gate_two = jnp.split(
        modulation, 6, axis=1
    )

    grad_branch = frame_scaled(cotangent.astype(F32), gate_two).astype(BF)
    exchange = [(0, 1), (1, 0)]
    place_y, place_x = lax.axis_index("yb"), lax.axis_index("xc")
    k_other = lax.ppermute(k_half, "yb", exchange)
    v_other = lax.ppermute(v_half, "xc", exchange)
    q_other = lax.ppermute(q_half, "xc", exchange)
    residual = tokens.astype(F32)
    attn_float, back_attn_input = jax.vjp(modulated, residual, shift_one, scale_one)
    attn_input = gather(attn_float.astype(BF), "sp")
    joined = product(attn_input, self_proj)
    self_mixed, self_lse, *self_kept = attend_forward(
        live_keys, [joined], gain_all, cosine, sine, True, 5
    )
    grad_branch, self_mixed = lax.optimization_barrier((grad_branch, self_mixed))
    beside = [
        grad_branch,
        lax.ppermute(grad_branch, "xc", exchange),
        lax.ppermute(grad_branch, "yb", exchange),
        lax.ppermute(grad_branch, PL, [(0, 3), (1, 2), (2, 1), (3, 0)]),
    ]
    self_branch = pair_sum(product(self_mixed, self_back))
    residual = residual + frame_scaled(self_branch, gate_one)

    def beside_own(own, other, place, axis):
        pair = jnp.where(place == 0, jnp.stack([own, other], axis), jnp.stack([other, own], axis))
        return pair.reshape(-1, own.shape[-1])

    cross_kvproj = jnp.concatenate(
        [beside_own(k_half, k_other, place_y, 1), beside_own(v_half, v_other, place_x, 2)], axis=1
    )
    cross_qproj = beside_own(q_half, q_other, place_x, 2)
    text_raw = product(text_all, cross_kvproj)
    cross_float, back_cross_norm = jax.vjp(layer_norm, residual)
    cross_input = gather(cross_float.astype(BF), "sp")
    cross_raw = product(cross_input, cross_qproj)
    cross_mixed, cross_lse, *cross_kept = attend_forward(
        all_keys, [cross_raw, text_raw], gain_all, cosine, sine, False, 6
    )
    cross_branch = pair_sum(product(cross_mixed, cross_back))
    residual = residual + cross_branch
    residual, *beside = lax.optimization_barrier((residual, *beside))
    beside = jnp.stack(beside)
    grad_branch_all = jnp.stack([beside, lax.ppermute(beside, "sp", exchange)], axis=1).reshape(-1, D)


    mlp_float, back_mlp_input = jax.vjp(modulated, residual, shift_two, scale_two)
    mlp_input = plane_gather(mlp_float.astype(BF))
    up_proj = product(mlp_input, up_matrix)
    activated_float, back_gelu = jax.vjp(
        lambda inner: jax.nn.gelu(inner, approximate=True), up_proj
    )
    activated = activated_float.astype(BF)

    mlp_part = product(activated, down_matrix).astype(BF)

    grad_rows = cotangent.astype(F32)
    grad_down = product_tn(activated, grad_branch_all).astype(BF)
    grad_up_low = back_gelu(product_nt(grad_branch_all, down_matrix))[0].astype(BF)
    grad_up = with_layout_constraint(product_tn(mlp_input, grad_up_low).astype(BF), Layout(major_to_minor=(0, 1)))
    grad_mlp_part = product_nt(grad_up_low, up_matrix).astype(BF)
    grad_mlp_part, grad_up, grad_down = lax.optimization_barrier((grad_mlp_part, grad_up, grad_down))
    down_owned = scatter(grad_down, "za")
    up_owned = scatter(grad_up, "za")
    mlp_branch, grad_mlp_input = plane_sum(mlp_part, grad_mlp_part)
    output = (residual + frame_scaled(mlp_branch, gate_two)).astype(BF)
    grad_gate_two = frame_sum(grad_rows * mlp_branch, frame_count)
    grad_from_mlp, grad_shift_two, grad_scale_two = back_mlp_input(grad_mlp_input)
    grad_rows = grad_rows + grad_from_mlp

    grad_low = gather(grad_rows.astype(BF), "sp")
    grad_cross_back = product_tn(cross_mixed, grad_low).astype(BF)
    grad_cross_mixed = product_nt(grad_low, cross_back).astype(BF)
    cross_saved = [*cross_kept[:2], cross_lse, *cross_kept[2:]]
    grad_cross_low, grad_text_low, gains_cross = attend_backward(
        all_keys, [cross_raw, text_raw], gain_all, cosine, sine, False, 7, cross_saved, grad_cross_mixed
    )
    grad_cross_qproj = product_tn(cross_input, grad_cross_low).astype(BF)
    grad_cross_kvproj = product_tn(text_all, grad_text_low).astype(BF)
    kv_parts = grad_cross_kvproj.reshape(outer, 2, 2, in_rows, -1)
    q_parts = grad_cross_qproj.reshape(outer, 2, 2, in_rows, -1)
    kv_sent = lax.ppermute(lax.dynamic_index_in_dim(kv_parts, 1 - place_y, 1, False), "yb", exchange)
    q_sent = lax.ppermute(lax.dynamic_index_in_dim(q_parts, 1 - place_x, 2, False), "xc", exchange)
    grad_cross_input = pair_sum(product_nt(grad_cross_low, cross_qproj))
    grad_rows = grad_rows + back_cross_norm(grad_cross_input)[0]

    grad_gate_one = frame_sum(grad_rows * self_branch, frame_count)
    grad_self_low = gather(frame_scaled(grad_rows, gate_one).astype(BF), "sp")
    grad_self_back = product_tn(self_mixed, grad_self_low).astype(BF)
    grad_self_mixed = product_nt(grad_self_low, self_back).astype(BF)
    self_saved = [*self_kept[:2], self_lse, *self_kept[2:]]
    grad_joined_low, gains_self = attend_backward(
        live_keys, [joined], gain_all, cosine, sine, True, 8, self_saved, grad_self_mixed
    )
    grad_self_proj = product_tn(attn_input, grad_joined_low).astype(BF)
    grad_attn_input = pair_sum(product_nt(grad_joined_low, self_proj))
    grad_from_attn, grad_shift_one, grad_scale_one = back_attn_input(grad_attn_input)
    grad_rows = grad_rows + grad_from_attn

    grad_modulation = jnp.concatenate(
        [grad_shift_one, grad_scale_one, grad_gate_one, grad_shift_two, grad_scale_two, grad_gate_two],
        axis=1,
    )
    grad_gains = jnp.concatenate([gains_self[:2], gains_cross[:2]])
    both = jnp.arange(2)[None, :, None] == core
    grad_gains = jnp.where(both, grad_gains[:, None, :], 0.0).reshape(4, shards, gain_len)
    grad_small = jnp.concatenate(
        [
            jnp.sum(grad_modulation, axis=0).reshape(shards, bias_len),
            grad_gains.transpose(1, 0, 2).reshape(shards, 4 * gain_len),
            jnp.zeros((shards, small_room - small_len), F32),
        ],
        axis=1,
    ).reshape(shards, small_rows, small_width)
    kv_near = lax.dynamic_index_in_dim(kv_parts, place_y, 1, False) + kv_sent
    q_near = lax.dynamic_index_in_dim(q_parts, place_x, 2, False) + q_sent
    owned, grad_mod_all, small_owned, mlp_in_grad, mlp_out_grad = reduce_weights(
        outer,
        ((1, OVER_Y), (2, OVER_X), (1, SPLIT), (1, SPLIT), (3, PLAIN)),
        [q_near, kv_near, grad_cross_back, grad_self_back, grad_self_proj],
        grad_modulation.astype(BF),
        grad_small,
        up_owned.reshape(PLANE, -1, up_owned.shape[1]),
        down_owned,
    )
    owned = [rows.astype(F32) for rows in (*owned, mlp_in_grad, mlp_out_grad)]
    cross_q_grad, cross_kv_grad, cross_out_grad, self_out_grad, self_in_grad, mlp_in_grad, mlp_out_grad = owned
    small_owned = small_owned.reshape(-1)[:small_len]
    sinus_all = sinus_features(steps_all).astype(BF)
    own_features = mod_weight.shape[1]
    sinus_own = lax.dynamic_slice_in_dim(sinus_all, chip * own_features, own_features, 1)
    mod_weight_grad = product_tn(sinus_own, grad_mod_all.reshape(-1, 6 * D))
    return (
        output,
        grad_rows,
        mod_weight_grad[None],
        small_owned[None, :bias_len],
        small_owned[bias_len:].reshape(1, 4, gain_len),
        self_in_grad[None],
        self_out_grad[None],
        cross_q_grad[None],
        cross_kv_grad[None],
        cross_out_grad[None],
        mlp_in_grad[None],
        mlp_out_grad[None],
    )


def solution(mesh):
    chips, cores = mesh.shape["fsdp"], mesh.shape["sp"]
    grid = mesh.devices.reshape(chips // PLANE, 2, PLANE // 2, cores)
    inner = Mesh(grid, ALL)
    rows, second = P(ALL, None), P(None, FS, None)
    in_specs = (
        rows,
        rows,
        P(FS),
        P(FS, None),
        second,
        P(None, FS),
        P(None, None, FS),
        *([second] * 7),
        rows,
    )
    out_specs = (rows, rows, second, P(None, FS), P(None, None, FS), *([second] * 7))

    return jax.shard_map(body, mesh=inner, in_specs=in_specs, out_specs=out_specs, check_vma=False)
```
